256 devices in a mesh: gx: 8 (over y, core), gy: 32 (over x, z).
Axes of the slice: x: 4, y: 4, z: 8, core: 2. Of those that a mesh axis runs over, the one named last changes fastest.
Arguments:
- source: float32 [64, 32, 4096], P(None, 'gx', 'gy'), may hold values from -6 to 6
- initial: float32 [64, 32, 4096], P(None, 'gx', 'gy'), may hold values from -6 to 6
- reaction: float32 [64, 32, 4096], P(None, 'gx', 'gy'), may hold values from 1 to 3
- stiffness: float32 [32, 4096], P('gx', 'gy'), may hold values from 0.5 to 2
- line_op: float32 [8, 8], replicated, may hold values from -1.6 to 5.6
- face_deriv: float32 [8], replicated, may hold values from -2 to 2
- wall_flags: int32 [4, 32, 4096], P(None, 'gx', 'gy'), may hold values 0 or 1
Outputs:
- hessenberg: float32 [6, 5], replicated
- krylov_basis: float32 [6, 64, 32, 4096], P(None, None, 'gx', 'gy')
The draws below stay inside these ranges and needn't reach their ends.
All inputs are finite; a program needn't handle non-finite values. No bound on the sum of `wall_flags` on one device may be relied on, other than what follows from the above.
Results may differ from the reference program's by a relative error of at most 0.0003.
Values sent between devices are 32-bit elements; how exact they have to be, the bound alone decides.
No kernel may reach another device: no remote copies, remote signals or barrier semaphores. Data moves between devices by JAX's collectives and lax.ppermute only.
A program may use at most 64 MiB of HBM per device.

```python
import math
import jax
import jax.numpy as jnp
from jax import lax

P_SIZE = 8
ITERS = 5
NEX = 32
NEY = 4096


def draw_line_op(key, part):
    first_key, second_key = jax.random.split(jax.random.fold_in(key, 11))
    offdiag = jnp.clip(jax.random.normal(first_key, (P_SIZE, P_SIZE), jnp.float32) * 0.4, -1.6, 1.6)
    diagonal = jax.random.uniform(second_key, (P_SIZE,), jnp.float32, 2.0, 4.0)
    return offdiag * (1.0 - jnp.eye(P_SIZE, dtype=jnp.float32)) + jnp.diag(diagonal)


def place_ends(values, rng, least, largest):
    longest = values.shape.index(max(values.shape))
    spots = []
    for shift in (0, 1):
        where = [jax.random.randint(jax.random.fold_in(rng, axis), (), 0, length) for axis, length in enumerate(values.shape)]
        where[longest] = (where[longest] + shift) % values.shape[longest]
        spots.append(tuple(where))
    return values.at[spots[0]].set(least).at[spots[1]].set(largest)


def block_scale(rng, extent, cuts, low, largest):
    def one(position, shards_of):
        draws = jax.random.uniform(jax.random.fold_in(jax.random.fold_in(rng, 6), position), (shards_of,), jnp.float32, low / len(cuts), largest / len(cuts))
        return jnp.repeat(jnp.exp(draws), extent[position] // shards_of).reshape((-1,) + (1,) * (len(extent) - position - 1))

    factor_of = one(*cuts[0])
    for cut in cuts[1:]:
        factor_of = factor_of * one(*cut)
    return factor_of


def gaussian(rng, extent, deviation, most, cuts=(), held_as=jnp.bfloat16):
    values = deviation * jax.random.normal(rng, extent, jnp.float32)
    if cuts:
        values = values * block_scale(rng, extent, cuts, -0.22, 0.18)
    return jnp.clip(values, -most, most).astype(held_as)


def setup_inputs(seed: int = 0) -> dict:
    streams_of = jax.random.split(jax.random.key(seed), 8)
    source = gaussian(streams_of[0], (P_SIZE * P_SIZE, NEX, NEY), 1.0, 6.0, ((1, 8), (2, 32)), jnp.float32)
    initial = gaussian(streams_of[1], (P_SIZE * P_SIZE, NEX, NEY), 1.0, 6.0, ((1, 8), (2, 32)), jnp.float32)
    reaction = jnp.clip(1.0 + 2.0 * jax.random.uniform(streams_of[2], (P_SIZE * P_SIZE, NEX, NEY), jnp.float32) ** block_scale(streams_of[2], (P_SIZE * P_SIZE, NEX, NEY), ((1, 8), (2, 32)), -0.2, 0.2), 1.0, 3.0)
    stiffness = jnp.clip(jnp.exp(math.log(2.0) - 1.3862944 * jax.random.uniform(streams_of[3], (NEX, NEY), jnp.float32) ** block_scale(streams_of[3], (NEX, NEY), ((0, 8), (1, 32)), -0.2, 0.2)), 0.5, 2.0)
    line_op = draw_line_op(jax.random.fold_in(streams_of[7], 71), 0)
    face_deriv = gaussian(streams_of[5], (P_SIZE,), 0.5, 2.0, (), jnp.float32)
    wall_flags = place_ends((jax.random.randint(streams_of[6], (4, NEX, NEY), 0, 4) < 1).astype(jnp.int32), jax.random.fold_in(streams_of[6], 1), 0, 1)
    return {"source": source, "initial": initial, "reaction": reaction, "stiffness": stiffness, "line_op": line_op, "face_deriv": face_deriv, "wall_flags": wall_flags}


TAU = 2.0
FLOOR = 0.1

def block_sum(values):
    flat = values.reshape(-1)
    width = 1024
    extra = -flat.shape[0] % width
    flat = jnp.concatenate([flat, jnp.zeros((extra,), flat.dtype)])
    return jnp.sum(lax.optimization_barrier(jnp.sum(flat.reshape(-1, width), axis=1)))

def apply_op(field, reaction, stiffness, line_op, face_deriv, wall_flags):
    highest = lax.Precision.HIGHEST
    nodes = field.reshape(P_SIZE, P_SIZE, field.shape[1], field.shape[2])
    interior = stiffness * (jnp.einsum('ac,cbxy->abxy', line_op, nodes, precision=highest) + jnp.einsum('bc,acxy->abxy', line_op, nodes, precision=highest))
    reversed_w = face_deriv[::-1]
    west_val = nodes[0]
    east_val = nodes[P_SIZE - 1]
    south_val = nodes[:, 0]
    north_val = nodes[:, P_SIZE - 1]
    west_der = jnp.einsum('c,cbxy->bxy', face_deriv, nodes, precision=highest)
    east_der = jnp.einsum('c,cbxy->bxy', reversed_w, nodes, precision=highest)
    south_der = jnp.einsum('c,acxy->axy', face_deriv, nodes, precision=highest)
    north_der = jnp.einsum('c,acxy->axy', reversed_w, nodes, precision=highest)
    opened = 1.0 - wall_flags.astype(field.dtype)
    add_east = TAU * (east_val - opened[1] * jnp.roll(west_val, -1, 1)) + 0.5 * (east_der - opened[1] * jnp.roll(west_der, -1, 1))
    add_west = TAU * (west_val - opened[0] * jnp.roll(east_val, 1, 1)) + 0.5 * (west_der - opened[0] * jnp.roll(east_der, 1, 1))
    add_north = TAU * (north_val - opened[3] * jnp.roll(south_val, -1, 2)) + 0.5 * (north_der - opened[3] * jnp.roll(south_der, -1, 2))
    add_south = TAU * (south_val - opened[2] * jnp.roll(north_val, 1, 2)) + 0.5 * (south_der - opened[2] * jnp.roll(north_der, 1, 2))
    result = reaction.reshape(nodes.shape) * nodes + interior
    result = result.at[0].add(add_west).at[P_SIZE - 1].add(add_east)
    result = result.at[:, 0].add(add_south).at[:, P_SIZE - 1].add(add_north)
    return result.reshape(field.shape)

def reference(source, initial, reaction, stiffness, line_op, face_deriv, wall_flags):
    total = float(P_SIZE * P_SIZE * NEX * NEY)

    def operate(field):
        return apply_op(field, reaction, stiffness, line_op, face_deriv, wall_flags)
    first = source - operate(initial)
    beta_first = jnp.sqrt(block_sum(first * first) / total + FLOOR)
    vectors = [first / beta_first]
    hessen = jnp.zeros((ITERS + 1, ITERS), source.dtype)
    for step in range(ITERS):
        image = operate(vectors[step])
        coeffs = [block_sum(vector * image) / total for vector in vectors]
        for index in range(len(vectors)):
            image = image - coeffs[index] * vectors[index]
            hessen = hessen.at[index, step].set(coeffs[index])
        beta = jnp.sqrt(block_sum(image * image) / total + FLOOR)
        hessen = hessen.at[step + 1, step].set(beta)
        vectors.append(image / beta)
    return (hessen, jnp.stack(vectors))
```

```python
import functools

import jax
import jax.numpy as jnp
from jax import lax
from jax.experimental import pallas as pl
from jax.experimental.pallas import tpu as pltpu
from jax.sharding import Mesh
from jax.sharding import PartitionSpec as P

P_SIZE = 8
ITERS = 5
GX = ("gx_0", "gx_1")
GY = ("gy_0", "gy_1")


TAU = 2.0
FLOOR = 0.1


def extended(array, sides, width):
    for axis, dim in sides:
        devices, length = (lax.axis_size(axis), array.shape[dim])
        up = [(i, (i + 1) % devices) for i in range(devices)]
        down = [(j, i) for i, j in up]
        last = lax.slice_in_dim(array, length - width, length, axis=dim)
        leading = lax.slice_in_dim(array, 0, width, axis=dim)
        before = lax.ppermute(last, axis, up)
        after = lax.ppermute(leading, axis, down)
        array = jnp.concatenate([before, array, after], axis=dim)
    return array


def sent_to_all(array, axis):
    copies = jnp.broadcast_to(array, (lax.axis_size(axis), *array.shape))
    return lax.all_to_all(copies, axis, split_axis=0, concat_axis=0, tiled=True)


def over_copies(array, axis):
    everything = sent_to_all(array, axis)
    return jnp.sum(everything, axis=0)


def by_axis(array, axes):
    far, near = axes
    nearer = over_copies(array, near)
    return over_copies(nearer, far)


def together(arrays, axis):
    vector, at, gathered = (jnp.concatenate([a.reshape(-1) for a in arrays]), 0, [])
    subtotal = by_axis(vector, axis)
    for a in arrays:
        gathered.append(subtotal[at : at + a.size].reshape(a.shape))
        at += a.size
    return tuple(gathered)


def local_total(values):
    return jnp.sum(jnp.sum(values, axis=0))


def x_traces(nodes, face_deriv):
    highest = lax.Precision.HIGHEST
    lower = jnp.einsum("c,cbxy->bxy", face_deriv, nodes, precision=highest)
    upper = jnp.einsum("c,cbxy->bxy", face_deriv[::-1], nodes, precision=highest)
    return jnp.stack([nodes[0], lower, nodes[-1], upper])


def y_traces(nodes, face_deriv):
    highest = lax.Precision.HIGHEST
    lower = jnp.einsum("c,acxy->axy", face_deriv, nodes, precision=highest)
    upper = jnp.einsum("c,acxy->axy", face_deriv[::-1], nodes, precision=highest)
    return jnp.stack([nodes[:, 0], lower, nodes[:, -1], upper])


def apply_op(field, reaction, stiffness, line_op, face_deriv, opened):
    highest = lax.Precision.HIGHEST
    nodes = field.reshape(P_SIZE, P_SIZE, field.shape[1], field.shape[2])
    interior = stiffness * (
        jnp.einsum("ac,cbxy->abxy", line_op, nodes, precision=highest)
        + jnp.einsum("bc,acxy->abxy", line_op, nodes, precision=highest)
    )
    xside = extended(x_traces(nodes, face_deriv), ((GX, 2),), 1)
    yside = extended(y_traces(nodes, face_deriv), ((GY, 3),), 1)
    x_own = xside[:, :, 1:-1]
    y_own = yside[:, :, :, 1:-1]
    east_nb = xside[0:2, :, 2:]
    west_nb = xside[2:4, :, :-2]
    north_nb = yside[0:2, :, :, 2:]
    south_nb = yside[2:4, :, :, :-2]
    add_east = TAU * (x_own[2] - opened[1] * east_nb[0]) + 0.5 * (x_own[3] - opened[1] * east_nb[1])
    add_west = TAU * (x_own[0] - opened[0] * west_nb[0]) + 0.5 * (x_own[1] - opened[0] * west_nb[1])
    add_north = TAU * (y_own[2] - opened[3] * north_nb[0]) + 0.5 * (
        y_own[3] - opened[3] * north_nb[1]
    )
    add_south = TAU * (y_own[0] - opened[2] * south_nb[0]) + 0.5 * (
        y_own[1] - opened[2] * south_nb[1]
    )
    result = reaction.reshape(nodes.shape) * nodes + interior
    result = result.at[0].add(add_west).at[P_SIZE - 1].add(add_east)
    result = result.at[:, 0].add(add_south).at[:, P_SIZE - 1].add(add_north)
    return result.reshape(field.shape)


def norm_scale(vector, total):
    squares = by_axis(local_total(vector * vector), (("gx_0", "gx_1"), ("gy_0", "gy_1")))
    return jnp.sqrt(squares / total + FLOOR)


def stepwise(source, initial, reaction, stiffness, line_op, face_deriv, wall_flags):
    highest = lax.Precision.HIGHEST
    total = float(
        P_SIZE * P_SIZE * source.shape[1] * lax.axis_size(GX) * source.shape[2] * lax.axis_size(GY)
    )
    opened = 1.0 - wall_flags.astype(jnp.float32)

    def operate(field):
        return apply_op(field, reaction, stiffness, line_op, face_deriv, opened)

    def products(basis, image):
        per_cell = jnp.einsum("kqxy,qxy->kxy", basis, image, precision=highest)
        return jnp.sum(per_cell, axis=(1, 2))

    first = source - operate(initial)
    basis = jnp.zeros((ITERS + 1,) + source.shape, jnp.float32)
    hessen = jnp.zeros((ITERS + 1, ITERS), jnp.float32)
    rows = lax.broadcasted_iota(jnp.int32, (ITERS + 1, ITERS), 0)
    cols = lax.broadcasted_iota(jnp.int32, (ITERS + 1, ITERS), 1)
    slots = lax.broadcasted_iota(jnp.int32, (ITERS + 1,), 0)

    def advance(step, carry):
        basis, hessen, pending = carry
        image = operate(pending)
        local = products(basis, image)
        projected, crossed, squares = together(
            (local, local_total(pending * image), local_total(pending * pending)),
            (("gx_0", "gx_1"), ("gy_0", "gy_1")),
        )
        beta = jnp.sqrt(squares / total + FLOOR)
        basis = lax.dynamic_update_index_in_dim(basis, pending / beta, step, 0)
        coeffs = projected / (total * beta) + jnp.where(
            slots == step, crossed / (total * beta * beta), 0.0
        )
        pending = image / beta - jnp.einsum("k,kqxy->qxy", coeffs, basis, precision=highest)
        hessen = hessen + jnp.where(cols == step, coeffs[:, None], 0.0)
        hessen = hessen + jnp.where((rows == step) & (cols == step - 1), beta, 0.0)
        return (basis, hessen, pending)

    basis, hessen, pending = lax.fori_loop(0, ITERS, advance, (basis, hessen, first))
    beta = norm_scale(pending, total)
    basis = basis.at[ITERS].set(pending / beta)
    hessen = hessen + jnp.where((rows == ITERS) & (cols == ITERS - 1), beta, 0.0)
    return (hessen, basis)


NODES = P_SIZE * P_SIZE
ROWS = 16
DEPTH = 6
LANES = 128
SCALE = 0.125
AMP_LIMIT = 100.0
GRAM = [(k, l) for k in range(ITERS + 1) for l in range(k + 1)]
HIGHEST = lax.Precision.HIGHEST


def centre(line_ref, deriv_ref):
    trace = line_ref[0, 0]
    for a in range(1, P_SIZE):
        trace = trace + line_ref[a, a]
    return 2.0 + 0.3125 * trace + 0.5 * (TAU + 0.5 * deriv_ref[0])


def lane_ids(rows):
    return lax.broadcasted_iota(jnp.int32, (rows, LANES), 1)


def turned(value, shift):
    shift = shift % LANES
    return value if shift == 0 else pltpu.roll(value, shift, 1)


def strided(ref, start, count):
    return ref[pl.ds(start, count, stride=4), :]


def pack_kernel(source, initial, reaction, stiffness, walls, near, low2, high2, to_up, to_down):
    opened = 1.0 - walls[...].astype(jnp.float32)
    near[0:256, :] = initial[...]
    near[256:512, :] = source[...]
    near[512:768, :] = reaction[...]
    near[768:772, :] = stiffness[...]
    near[772:788, :] = opened
    near[788:792, :] = jnp.zeros((4, LANES), jnp.float32)
    for out, far, close in ((high2, 2, 3), (low2, 1, 0)):
        out[0:64, :] = strided(initial, far, NODES)
        out[64:128, :] = strided(initial, close, NODES)
        out[128:192, :] = strided(source, close, NODES)
        out[192:256, :] = strided(reaction, close, NODES)
        out[256:257, :] = stiffness[close : close + 1, :]
        for f in range(4):
            out[257 + f : 258 + f, :] = opened[4 * f + close : 4 * f + close + 1, :]
        out[261:264, :] = jnp.zeros((3, LANES), jnp.float32)
    lanes = lane_ids(NODES)
    lanes8 = lane_ids(8)
    for out, first in ((to_up, 120), (to_down, 0)):
        total = jnp.zeros((NODES, LANES), jnp.float32)
        extra = jnp.zeros((8, LANES), jnp.float32)
        for x in range(4):
            for field, ref in enumerate((initial, source, reaction)):
                at = 32 * field + 8 * x
                moved = turned(strided(ref, x, NODES), at - first)
                total = jnp.where((lanes >= at) & (lanes < at + 8), moved, total)
            at = 96 + 8 * x
            rows = [stiffness[x : x + 1, :]] + [opened[4 * f + x : 4 * f + x + 1, :] for f in range(4)]
            rows = jnp.concatenate(rows + [jnp.zeros((3, LANES), jnp.float32)], axis=0)
            extra = jnp.where((lanes8 >= at) & (lanes8 < at + 8), turned(rows, at - first), extra)
        out[...] = total
        out[0:8, :] = total[0:8] + extra


def weights_in(line_ref, deriv_ref):
    def grid(rows, columns):
        return (
            lax.broadcasted_iota(jnp.int32, (rows, columns), 0),
            lax.broadcasted_iota(jnp.int32, (rows, columns), 1),
        )

    r, s = grid(NODES, NODES)
    ra, rb, sa, sb = r // 8, r % 8, s // 8, s % 8
    full = jnp.zeros((NODES, NODES), jnp.float32)
    for a in range(P_SIZE):
        for c in range(P_SIZE):
            value = line_ref[a, c]
            full = full + jnp.where((ra == a) & (sa == c) & (rb == sb), value, 0.0)
            full = full + jnp.where((rb == a) & (sb == c) & (ra == sa), value, 0.0)
    r, s = grid(8, NODES)
    sa, sb = s // 8, s % 8
    parts = [full]
    for along, across in ((sa, sb), (sb, sa)):
        for flip in (False, True):
            part = jnp.zeros((8, NODES), jnp.float32)
            for c in range(P_SIZE):
                value = 0.5 * deriv_ref[c] + (TAU if c == 0 else 0.0)
                place = P_SIZE - 1 - c if flip else c
                part = part + jnp.where((across == r) & (along == place), value, 0.0)
            parts.append(part * SCALE)
    return jnp.concatenate(parts, axis=0)


def powers_kernel(
    line_ref, deriv_ref, source, initial, reaction, stiffness, walls,
    below1, above1, below2, above2, own_strip, strip_b1, strip_a1, strip_b2, strip_a2,
    basis_out, gram_out, field_a, field_b, weight, image, react, stiff, opened,
):
    shift = centre(line_ref, deriv_ref)
    weight[...] = weights_in(line_ref, deriv_ref)

    def put(row, value_initial, value_reaction, value_stiffness, value_open):
        cols = slice(row * LANES, (row + 1) * LANES)
        field_a[:, cols] = value_initial
        react[:, cols] = (value_reaction - shift) * SCALE
        stiff[:, cols] = jnp.broadcast_to(value_stiffness * SCALE, (8, LANES))
        for f in range(4):
            opened[8 * f : 8 * f + 8, cols] = jnp.broadcast_to(value_open[f], (8, LANES))

    own_open = 1.0 - walls[...].astype(jnp.float32)
    for x in range(4):
        put(
            6 + x, strided(initial, x, NODES), strided(reaction, x, NODES), stiffness[x : x + 1, :],
            [own_open[4 * f + x : 4 * f + x + 1, :] for f in range(4)],
        )
        for ref, row in ((below1, 2 + x), (above1, 10 + x)):
            put(
                row, strided(ref, x, NODES), strided(ref, 512 + x, NODES), ref[768 + x : 769 + x, :],
                [ref[772 + 4 * f + x : 773 + 4 * f + x, :] for f in range(4)],
            )
    for ref, far, close in ((below2, 0, 1), (above2, 15, 14)):
        put(
            close, ref[64:128, :], ref[192:256, :], ref[256:257, :],
            [ref[257 + f : 258 + f, :] for f in range(4)],
        )
        field_a[:, far * LANES : (far + 1) * LANES] = ref[0:64, :]

    lanes64 = lane_ids(NODES)
    lanes = lane_ids(8)
    pieces = ((strip_b2, 0, 16, -16), (strip_b1, 16, 48, 16), (own_strip, 48, 80, 48),
              (strip_a1, 80, 112, 80), (strip_a2, 112, 128, 112))
    strip_source = []
    for side in range(2):
        rows = slice(NODES * side, NODES * side + NODES)
        made = []
        for field in range(4):
            count = NODES if field < 3 else 8
            ids = lanes64 if field < 3 else lanes
            value = jnp.zeros((count, LANES), jnp.float32)
            for ref, start, stop, zero in pieces:
                part = ref[NODES * side : NODES * side + count, :]
                value = jnp.where((ids >= start) & (ids < stop), turned(part, zero - 32 * field), value)
            made.append(value)
        put(ROWS + side, made[0], made[2], made[3][0:1], [made[3][1 + f : 2 + f] for f in range(4)])
        strip_source.append(made[1])

    def columns(row):
        return slice(row * LANES, (row + 1) * LANES)

    low, high = ROWS, ROWS + 1
    sub = lax.broadcasted_iota(jnp.int32, (8, LANES), 0)
    TW, TE, TS, TN = (slice(64 + 8 * f, 72 + 8 * f) for f in range(4))

    def source_of(row):
        if row >= ROWS:
            return strip_source[row - ROWS]
        if 6 <= row < 10:
            return strided(source, row - 6, NODES)
        if 2 <= row < 6:
            return strided(below1, 256 + row - 2, NODES)
        if 10 <= row < 14:
            return strided(above1, 256 + row - 10, NODES)
        return (below2 if row < 2 else above2)[128:192, :]

    def apply(old, new, step, first):
        start, stop = step, ROWS - step
        image[:, start * LANES : stop * LANES] = jnp.dot(
            weight[...], old[:, start * LANES : stop * LANES],
            precision=HIGHEST, preferred_element_type=jnp.float32,
        )
        image[:, ROWS * LANES : (ROWS + 2) * LANES] = jnp.dot(
            weight[...], old[:, ROWS * LANES : (ROWS + 2) * LANES],
            precision=HIGHEST, preferred_element_type=jnp.float32,
        )

        def finish(row, from_west, from_east, from_south, from_north):
            cols = columns(row)
            west = image[TW, cols] - opened[0:8, cols] * from_west
            east = image[TE, cols] - opened[8:16, cols] * from_east
            south = image[TS, cols] - opened[16:24, cols] * from_south
            north = image[TN, cols] - opened[24:32, cols] * from_north
            for a in range(P_SIZE):
                rows = slice(8 * a, 8 * a + 8)
                value = react[rows, cols] * old[rows, cols] + stiff[:, cols] * image[rows, cols]
                if a == 0:
                    value = value + west
                if a == P_SIZE - 1:
                    value = value + east
                edge = jnp.where(sub == 0, south[a : a + 1, :], 0.0)
                edge = jnp.where(sub == P_SIZE - 1, north[a : a + 1, :], edge)
                value = value + edge
                if first:
                    value = -8.0 * value - shift * old[rows, cols]
                new[rows, cols] = value
            if first:
                new[:, cols] = new[:, cols] + source_of(row)

        north_low = image[TN, columns(low)]
        south_high = image[TS, columns(high)]
        for row in range(start + 1, stop - 1):
            cols = columns(row)
            from_south = jnp.where(
                lanes == 0, turned(north_low, -(8 * row + 7)), turned(image[TN, cols], 1)
            )
            from_north = jnp.where(
                lanes == LANES - 1, turned(south_high, 127 - 8 * row), turned(image[TS, cols], -1)
            )
            finish(row, image[TE, columns(row - 1)], image[TW, columns(row + 1)], from_south, from_north)
        if step == DEPTH - 1:
            return
        to_low = turned(image[TS, columns(low)], -1)
        to_high = turned(image[TN, columns(high)], 1)
        for row in range(start, stop):
            cols = columns(row)
            to_low = jnp.where(lanes == 8 * row + 7, turned(image[TS, cols], 8 * row + 7), to_low)
            to_high = jnp.where(lanes == 8 * row, turned(image[TN, cols], 8 * row + 1), to_high)
        cols = columns(low)
        finish(low, turned(image[TE, cols], 8), turned(image[TW, cols], -8), turned(image[TN, cols], 1), to_low)
        cols = columns(high)
        finish(high, turned(image[TE, cols], 8), turned(image[TW, cols], -8), to_high, turned(image[TS, cols], -1))

    old, new = field_a, field_b
    for step in range(DEPTH):
        apply(old, new, step, step == 0)
        basis_out[step, :, :] = new[:, 6 * LANES : 10 * LANES]
        old, new = new, old

    sums = [jnp.zeros((8, LANES), jnp.float32) for _ in GRAM]
    for x in range(4):
        for a in range(P_SIZE):
            values = [basis_out[k, 8 * a : 8 * a + 8, x * LANES : (x + 1) * LANES] for k in range(ITERS + 1)]
            sums = [total + values[k] * values[l] for total, (k, l) in zip(sums, GRAM)]
    rows = [jnp.sum(total, axis=0, keepdims=True) for total in sums]
    rows = jnp.concatenate(rows + [jnp.zeros((24 - len(GRAM), LANES), jnp.float32)], axis=0)
    totals = jnp.sum(rows, axis=1, keepdims=True)
    place = lax.broadcasted_iota(jnp.int32, (24, LANES), 0) == lax.broadcasted_iota(jnp.int32, (24, LANES), 1)
    gram_out[...] = jnp.sum(jnp.where(place, totals, 0.0), axis=0, keepdims=True)


def combine_kernel(nodes, line_ref, deriv_ref, powers, gathered, basis_out, hess_out, amp_out):
    shift = centre(line_ref, deriv_ref)
    row = jnp.sum(gathered[...], axis=0, keepdims=True) * (1.0 / nodes)
    spread = jnp.broadcast_to(row, (8, LANES))
    gram = {}
    for at, (k, l) in enumerate(GRAM):
        gram[k, l] = gram[l, k] = jnp.broadcast_to(spread[:, at : at + 1], (8, LANES))
    sizes = [jnp.sqrt(gram[k, k]) for k in range(ITERS + 1)]
    sub = lax.broadcasted_iota(jnp.int32, (8, LANES), 0)
    lanes = lane_ids(8)
    hess = jnp.zeros((8, LANES), jnp.float32)
    beta = jnp.sqrt(gram[0, 0] + FLOOR)
    coeffs = [[1.0 / beta]]
    amp = sizes[0] * coeffs[0][0]

    def put(hess, i, j, value):
        return jnp.where((sub == i) & (lanes == j), value, hess)

    for j in range(ITERS):
        last = coeffs[j]
        image = [shift * c for c in last] + [None]
        for k in range(j + 1):
            moved = last[k] * 8.0
            image[k + 1] = moved if image[k + 1] is None else image[k + 1] + moved
        weighted = [
            sum(gram[k, l] * image[l] for l in range(1, j + 2)) + gram[k, 0] * image[0] for k in range(j + 2)
        ]
        pending = list(image)
        for i in range(j + 1):
            h = sum(c * weighted[k] for k, c in enumerate(coeffs[i]))
            hess = put(hess, i, j, h)
            for k, c in enumerate(coeffs[i]):
                pending[k] = pending[k] - h * c
        square = sum(
            pending[k] * sum(gram[k, l] * pending[l] for l in range(j + 2)) for k in range(j + 2)
        )
        beta = jnp.sqrt(jnp.maximum(square, 0.0) + FLOOR)
        hess = put(hess, j + 1, j, beta)
        scale = 1.0 / beta
        coeffs.append([p * scale for p in pending])
        amp = jnp.maximum(amp, sum(jnp.abs(c) * s for c, s in zip(coeffs[-1], sizes)))
    hess_out[...] = hess[0 : ITERS + 1, 0:ITERS]
    amp_out[...] = amp[0:1, :]
    for x in range(4):
        for a in range(P_SIZE):
            values = [powers[k, 8 * a : 8 * a + 8, x * LANES : (x + 1) * LANES] for k in range(ITERS + 1)]
            for j in range(ITERS + 1):
                total = coeffs[j][0] * values[0]
                for k in range(1, j + 1):
                    total = total + coeffs[j][k] * values[k]
                basis_out[j, pl.ds(32 * a + x, 8, stride=4), :] = total


def fast(source, initial, reaction, stiffness, line_op, face_deriv, wall_flags):
    vmem = pl.BlockSpec(memory_space=pltpu.VMEM)
    smem = pl.BlockSpec(memory_space=pltpu.SMEM)
    f32 = jnp.float32
    flat = [v.reshape(4 * NODES, LANES) for v in (source, initial, reaction)]
    walls = wall_flags.reshape(16, LANES)
    nx, ny = lax.axis_size(GX), lax.axis_size(GY)

    def moved(value, axis, size, by):
        return lax.ppermute(value, axis, [(i, (i + by) % size) for i in range(size)])

    near, low2, high2, to_up, to_down = pl.pallas_call(
        pack_kernel,
        out_shape=[jax.ShapeDtypeStruct((n, LANES), f32) for n in (792, 264, 264, NODES, NODES)],
        in_specs=[vmem] * 5,
        out_specs=[vmem] * 5,
    )(*flat, stiffness, walls)
    below1 = moved(near, GX, nx, 1)
    above1 = moved(near, GX, nx, -1)
    below2 = moved(high2, GX, nx, 2)
    above2 = moved(low2, GX, nx, -2)
    left = moved(to_up, GY, ny, 1)
    right = moved(to_down, GY, ny, -1)
    own_strip = jnp.concatenate([left, right], axis=0)
    strips = [moved(own_strip, GX, nx, by) for by in (1, -1, 2, -2)]

    powers, gram = pl.pallas_call(
        powers_kernel,
        out_shape=[
            jax.ShapeDtypeStruct((ITERS + 1, NODES, 4 * LANES), f32),
            jax.ShapeDtypeStruct((1, LANES), f32),
        ],
        in_specs=[smem, smem] + [vmem] * 14,
        out_specs=[vmem] * 2,
        scratch_shapes=[
            pltpu.VMEM((NODES, (ROWS + 2) * LANES), f32),
            pltpu.VMEM((NODES, (ROWS + 2) * LANES), f32),
            pltpu.VMEM((NODES + 32, NODES), f32),
            pltpu.VMEM((NODES + 32, (ROWS + 2) * LANES), f32),
            pltpu.VMEM((NODES, (ROWS + 2) * LANES), f32),
            pltpu.VMEM((8, (ROWS + 2) * LANES), f32),
            pltpu.VMEM((32, (ROWS + 2) * LANES), f32),
        ],
    )(line_op, face_deriv, *flat, stiffness, walls, below1, above1, below2, above2, own_strip, *strips)
    every = GX + GY
    copies = jnp.broadcast_to(gram, (nx * ny, LANES))
    gathered = lax.all_to_all(copies, every, split_axis=0, concat_axis=0, tiled=True)
    basis, hess, amp = pl.pallas_call(
        functools.partial(combine_kernel, float(NODES * 4 * nx * LANES * ny)),
        out_shape=[
            jax.ShapeDtypeStruct((ITERS + 1, 4 * NODES, LANES), f32),
            jax.ShapeDtypeStruct((ITERS + 1, ITERS), f32),
            jax.ShapeDtypeStruct((1, LANES), f32),
        ],
        in_specs=[smem, smem] + [vmem] * 2,
        out_specs=[vmem] * 3,
    )(line_op, face_deriv, powers, gathered)
    return hess, basis.reshape(ITERS + 1, NODES, 4, LANES), amp[0, 0]


def body(*args):
    hess, basis, amp = fast(*args)

    def again(carry):
        return (jnp.bool_(True),) + stepwise(*args)

    done = amp <= AMP_LIMIT
    _, hess, basis = lax.while_loop(lambda carry: jnp.logical_not(carry[0]), again, (done, hess, basis))
    return (hess, basis)


def solution(mesh):
    finer = Mesh(mesh.devices.reshape(4, 2, 4, 8), ("gx_0", "gx_1", "gy_0", "gy_1"))
    placed = (
        P(None, GX, GY),
        P(None, GX, GY),
        P(None, GX, GY),
        P(GX, GY),
        P(),
        P(),
        P(None, GX, GY),
    )
    return jax.shard_map(
        body, mesh=finer, in_specs=placed, out_specs=(P(), P(None, None, GX, GY)), check_vma=False
    )
```

```python
import functools

import jax
import jax.numpy as jnp
from jax import lax
from jax.experimental import pallas as pl
from jax.experimental.pallas import tpu as pltpu
from jax.sharding import Mesh
from jax.sharding import PartitionSpec as P

P_SIZE = 8
ITERS = 5
GX = ("gx_0", "gx_1")
GY = ("gy_0", "gy_1")


TAU = 2.0
FLOOR = 0.1


def extended(array, sides, width):
    for axis, dim in sides:
        devices, length = (lax.axis_size(axis), array.shape[dim])
        up = [(i, (i + 1) % devices) for i in range(devices)]
        down = [(j, i) for i, j in up]
        last = lax.slice_in_dim(array, length - width, length, axis=dim)
        leading = lax.slice_in_dim(array, 0, width, axis=dim)
        before = lax.ppermute(last, axis, up)
        after = lax.ppermute(leading, axis, down)
        array = jnp.concatenate([before, array, after], axis=dim)
    return array


def sent_to_all(array, axis):
    copies = jnp.broadcast_to(array, (lax.axis_size(axis), *array.shape))
    return lax.all_to_all(copies, axis, split_axis=0, concat_axis=0, tiled=True)


def over_copies(array, axis):
    everything = sent_to_all(array, axis)
    return jnp.sum(everything, axis=0)


def by_axis(array, axes):
    far, near = axes
    nearer = over_copies(array, near)
    return over_copies(nearer, far)


def together(arrays, axis):
    vector, at, gathered = (jnp.concatenate([a.reshape(-1) for a in arrays]), 0, [])
    subtotal = by_axis(vector, axis)
    for a in arrays:
        gathered.append(subtotal[at : at + a.size].reshape(a.shape))
        at += a.size
    return tuple(gathered)


def local_total(values):
    return jnp.sum(jnp.sum(values, axis=0))


def x_traces(nodes, face_deriv):
    highest = lax.Precision.HIGHEST
    lower = jnp.einsum("c,cbxy->bxy", face_deriv, nodes, precision=highest)
    upper = jnp.einsum("c,cbxy->bxy", face_deriv[::-1], nodes, precision=highest)
    return jnp.stack([nodes[0], lower, nodes[-1], upper])


def y_traces(nodes, face_deriv):
    highest = lax.Precision.HIGHEST
    lower = jnp.einsum("c,acxy->axy", face_deriv, nodes, precision=highest)
    upper = jnp.einsum("c,acxy->axy", face_deriv[::-1], nodes, precision=highest)
    return jnp.stack([nodes[:, 0], lower, nodes[:, -1], upper])


def apply_op(field, reaction, stiffness, line_op, face_deriv, opened):
    highest = lax.Precision.HIGHEST
    nodes = field.reshape(P_SIZE, P_SIZE, field.shape[1], field.shape[2])
    interior = stiffness * (
        jnp.einsum("ac,cbxy->abxy", line_op, nodes, precision=highest)
        + jnp.einsum("bc,acxy->abxy", line_op, nodes, precision=highest)
    )
    xside = extended(x_traces(nodes, face_deriv), ((GX, 2),), 1)
    yside = extended(y_traces(nodes, face_deriv), ((GY, 3),), 1)
    x_own = xside[:, :, 1:-1]
    y_own = yside[:, :, :, 1:-1]
    east_nb = xside[0:2, :, 2:]
    west_nb = xside[2:4, :, :-2]
    north_nb = yside[0:2, :, :, 2:]
    south_nb = yside[2:4, :, :, :-2]
    add_east = TAU * (x_own[2] - opened[1] * east_nb[0]) + 0.5 * (x_own[3] - opened[1] * east_nb[1])
    add_west = TAU * (x_own[0] - opened[0] * west_nb[0]) + 0.5 * (x_own[1] - opened[0] * west_nb[1])
    add_north = TAU * (y_own[2] - opened[3] * north_nb[0]) + 0.5 * (
        y_own[3] - opened[3] * north_nb[1]
    )
    add_south = TAU * (y_own[0] - opened[2] * south_nb[0]) + 0.5 * (
        y_own[1] - opened[2] * south_nb[1]
    )
    result = reaction.reshape(nodes.shape) * nodes + interior
    result = result.at[0].add(add_west).at[P_SIZE - 1].add(add_east)
    result = result.at[:, 0].add(add_south).at[:, P_SIZE - 1].add(add_north)
    return result.reshape(field.shape)


def norm_scale(vector, total):
    squares = by_axis(local_total(vector * vector), (("gx_0", "gx_1"), ("gy_0", "gy_1")))
    return jnp.sqrt(squares / total + FLOOR)


def stepwise(source, initial, reaction, stiffness, line_op, face_deriv, wall_flags):
    highest = lax.Precision.HIGHEST
    total = float(
        P_SIZE * P_SIZE * source.shape[1] * lax.axis_size(GX) * source.shape[2] * lax.axis_size(GY)
    )
    opened = 1.0 - wall_flags.astype(jnp.float32)

    def operate(field):
        return apply_op(field, reaction, stiffness, line_op, face_deriv, opened)

    def products(basis, image):
        per_cell = jnp.einsum("kqxy,qxy->kxy", basis, image, precision=highest)
        return jnp.sum(per_cell, axis=(1, 2))

    first = source - operate(initial)
    basis = jnp.zeros((ITERS + 1,) + source.shape, jnp.float32)
    hessen = jnp.zeros((ITERS + 1, ITERS), jnp.float32)
    rows = lax.broadcasted_iota(jnp.int32, (ITERS + 1, ITERS), 0)
    cols = lax.broadcasted_iota(jnp.int32, (ITERS + 1, ITERS), 1)
    slots = lax.broadcasted_iota(jnp.int32, (ITERS + 1,), 0)

    def advance(step, carry):
        basis, hessen, pending = carry
        image = operate(pending)
        local = products(basis, image)
        projected, crossed, squares = together(
            (local, local_total(pending * image), local_total(pending * pending)),
            (("gx_0", "gx_1"), ("gy_0", "gy_1")),
        )
        beta = jnp.sqrt(squares / total + FLOOR)
        basis = lax.dynamic_update_index_in_dim(basis, pending / beta, step, 0)
        coeffs = projected / (total * beta) + jnp.where(
            slots == step, crossed / (total * beta * beta), 0.0
        )
        pending = image / beta - jnp.einsum("k,kqxy->qxy", coeffs, basis, precision=highest)
        hessen = hessen + jnp.where(cols == step, coeffs[:, None], 0.0)
        hessen = hessen + jnp.where((rows == step) & (cols == step - 1), beta, 0.0)
        return (basis, hessen, pending)

    basis, hessen, pending = lax.fori_loop(0, ITERS, advance, (basis, hessen, first))
    beta = norm_scale(pending, total)
    basis = basis.at[ITERS].set(pending / beta)
    hessen = hessen + jnp.where((rows == ITERS) & (cols == ITERS - 1), beta, 0.0)
    return (hessen, basis)


NODES = P_SIZE * P_SIZE
ROWS = 16
DEPTH = 6
LANES = 128
SCALE = 0.125
AMP_LIMIT = 100.0
GRAM = [(k, l) for k in range(ITERS + 1) for l in range(k + 1)]
HIGHEST = lax.Precision.HIGHEST


def centre(line_ref, deriv_ref):
    trace = line_ref[0, 0]
    for a in range(1, P_SIZE):
        trace = trace + line_ref[a, a]
    return 2.0 + 0.3125 * trace + 0.5 * (TAU + 0.5 * deriv_ref[0])


def lane_ids(rows):
    return lax.broadcasted_iota(jnp.int32, (rows, LANES), 1)


def turned(value, shift):
    shift = shift % LANES
    return value if shift == 0 else pltpu.roll(value, shift, 1)


def strided(ref, start, count):
    return ref[pl.ds(start, count, stride=4), :]


def pack_kernel(source, initial, reaction, stiffness, walls, near, low2, high2, to_up, to_down):
    opened = 1.0 - walls[...].astype(jnp.float32)
    near[0:256, :] = initial[...]
    near[256:512, :] = source[...]
    near[512:768, :] = reaction[...]
    near[768:772, :] = stiffness[...]
    near[772:788, :] = opened
    near[788:792, :] = jnp.zeros((4, LANES), jnp.float32)
    for out, far, close in ((high2, 2, 3), (low2, 1, 0)):
        out[0:64, :] = strided(initial, far, NODES)
        out[64:128, :] = strided(initial, close, NODES)
        out[128:192, :] = strided(source, close, NODES)
        out[192:256, :] = strided(reaction, close, NODES)
        out[256:257, :] = stiffness[close : close + 1, :]
        for f in range(4):
            out[257 + f : 258 + f, :] = opened[4 * f + close : 4 * f + close + 1, :]
        out[261:264, :] = jnp.zeros((3, LANES), jnp.float32)
    lanes = lane_ids(NODES)
    lanes8 = lane_ids(8)
    for out, first in ((to_up, 120), (to_down, 0)):
        total = jnp.zeros((NODES, LANES), jnp.float32)
        extra = jnp.zeros((8, LANES), jnp.float32)
        for x in range(4):
            for field, ref in enumerate((initial, source, reaction)):
                at = 32 * field + 8 * x
                moved = turned(strided(ref, x, NODES), at - first)
                total = jnp.where((lanes >= at) & (lanes < at + 8), moved, total)
            at = 96 + 8 * x
            rows = [stiffness[x : x + 1, :]] + [opened[4 * f + x : 4 * f + x + 1, :] for f in range(4)]
            rows = jnp.concatenate(rows + [jnp.zeros((3, LANES), jnp.float32)], axis=0)
            extra = jnp.where((lanes8 >= at) & (lanes8 < at + 8), turned(rows, at - first), extra)
        out[...] = total
        out[0:8, :] = total[0:8] + extra


def weights_in(line_ref, deriv_ref):
    def grid(rows, columns):
        return (
            lax.broadcasted_iota(jnp.int32, (rows, columns), 0),
            lax.broadcasted_iota(jnp.int32, (rows, columns), 1),
        )

    r, s = grid(NODES, NODES)
    ra, rb, sa, sb = r // 8, r % 8, s // 8, s % 8
    full = jnp.zeros((NODES, NODES), jnp.float32)
    for a in range(P_SIZE):
        for c in range(P_SIZE):
            value = line_ref[a, c]
            full = full + jnp.where((ra == a) & (sa == c) & (rb == sb), value, 0.0)
            full = full + jnp.where((rb == a) & (sb == c) & (ra == sa), value, 0.0)
    r, s = grid(8, NODES)
    sa, sb = s // 8, s % 8
    parts = [full]
    for along, across in ((sa, sb), (sb, sa)):
        for flip in (False, True):
            part = jnp.zeros((8, NODES), jnp.float32)
            for c in range(P_SIZE):
                value = 0.5 * deriv_ref[c] + (TAU if c == 0 else 0.0)
                place = P_SIZE - 1 - c if flip else c
                part = part + jnp.where((across == r) & (along == place), value, 0.0)
            parts.append(part * SCALE)
    return jnp.concatenate(parts, axis=0)


def powers_kernel(
    line_ref, deriv_ref, source, initial, reaction, stiffness, walls,
    below1, above1, below2, above2, own_strip, strip_b1, strip_a1, strip_b2, strip_a2,
    basis_out, gram_out, field_a, field_b, weight, image, react, stiff, opened,
):
    shift = centre(line_ref, deriv_ref)
    weight[...] = weights_in(line_ref, deriv_ref)

    def put(row, value_initial, value_reaction, value_stiffness, value_open):
        cols = slice(row * LANES, (row + 1) * LANES)
        field_a[:, cols] = value_initial
        react[:, cols] = (value_reaction - shift) * SCALE
        stiff[:, cols] = jnp.broadcast_to(value_stiffness * SCALE, (8, LANES))
        for f in range(4):
            opened[8 * f : 8 * f + 8, cols] = jnp.broadcast_to(value_open[f], (8, LANES))

    own_open = 1.0 - walls[...].astype(jnp.float32)
    for x in range(4):
        put(
            6 + x, strided(initial, x, NODES), strided(reaction, x, NODES), stiffness[x : x + 1, :],
            [own_open[4 * f + x : 4 * f + x + 1, :] for f in range(4)],
        )
        for ref, row in ((below1, 2 + x), (above1, 10 + x)):
            put(
                row, strided(ref, x, NODES), strided(ref, 512 + x, NODES), ref[768 + x : 769 + x, :],
                [ref[772 + 4 * f + x : 773 + 4 * f + x, :] for f in range(4)],
            )
    for ref, far, close in ((below2, 0, 1), (above2, 15, 14)):
        put(
            close, ref[64:128, :], ref[192:256, :], ref[256:257, :],
            [ref[257 + f : 258 + f, :] for f in range(4)],
        )
        field_a[:, far * LANES : (far + 1) * LANES] = ref[0:64, :]

    lanes64 = lane_ids(NODES)
    lanes = lane_ids(8)
    pieces = ((strip_b2, 0, 16, -16), (strip_b1, 16, 48, 16), (own_strip, 48, 80, 48),
              (strip_a1, 80, 112, 80), (strip_a2, 112, 128, 112))
    strip_source = []
    for side in range(2):
        rows = slice(NODES * side, NODES * side + NODES)
        made = []
        for field in range(4):
            count = NODES if field < 3 else 8
            ids = lanes64 if field < 3 else lanes
            value = jnp.zeros((count, LANES), jnp.float32)
            for ref, start, stop, zero in pieces:
                part = ref[NODES * side : NODES * side + count, :]
                value = jnp.where((ids >= start) & (ids < stop), turned(part, zero - 32 * field), value)
            made.append(value)
        put(ROWS + side, made[0], made[2], made[3][0:1], [made[3][1 + f : 2 + f] for f in range(4)])
        strip_source.append(made[1])

    def columns(row):
        return slice(row * LANES, (row + 1) * LANES)

    low, high = ROWS, ROWS + 1
    sub = lax.broadcasted_iota(jnp.int32, (8, LANES), 0)
    TW, TE, TS, TN = (slice(64 + 8 * f, 72 + 8 * f) for f in range(4))

    def source_of(row):
        if row >= ROWS:
            return strip_source[row - ROWS]
        if 6 <= row < 10:
            return strided(source, row - 6, NODES)
        if 2 <= row < 6:
            return strided(below1, 256 + row - 2, NODES)
        if 10 <= row < 14:
            return strided(above1, 256 + row - 10, NODES)
        return (below2 if row < 2 else above2)[128:192, :]

    def apply(old, new, step, first):
        start, stop = step, ROWS - step
        image[:, start * LANES : stop * LANES] = jnp.dot(
            weight[...], old[:, start * LANES : stop * LANES],
            precision=HIGHEST, preferred_element_type=jnp.float32,
        )
        image[:, ROWS * LANES : (ROWS + 2) * LANES] = jnp.dot(
            weight[...], old[:, ROWS * LANES : (ROWS + 2) * LANES],
            precision=HIGHEST, preferred_element_type=jnp.float32,
        )

        def finish(row, from_west, from_east, from_south, from_north):
            cols = columns(row)
            west = image[TW, cols] - opened[0:8, cols] * from_west
            east = image[TE, cols] - opened[8:16, cols] * from_east
            south = image[TS, cols] - opened[16:24, cols] * from_south
            north = image[TN, cols] - opened[24:32, cols] * from_north
            for a in range(P_SIZE):
                rows = slice(8 * a, 8 * a + 8)
                value = react[rows, cols] * old[rows, cols] + stiff[:, cols] * image[rows, cols]
                if a == 0:
                    value = value + west
                if a == P_SIZE - 1:
                    value = value + east
                edge = jnp.where(sub == 0, south[a : a + 1, :], 0.0)
                edge = jnp.where(sub == P_SIZE - 1, north[a : a + 1, :], edge)
                value = value + edge
                if first:
                    value = -8.0 * value - shift * old[rows, cols]
                new[rows, cols] = value
            if first:
                new[:, cols] = new[:, cols] + source_of(row)

        north_low = image[TN, columns(low)]
        south_high = image[TS, columns(high)]
        for row in range(start + 1, stop - 1):
            cols = columns(row)
            from_south = jnp.where(
                lanes == 0, turned(north_low, -(8 * row + 7)), turned(image[TN, cols], 1)
            )
            from_north = jnp.where(
                lanes == LANES - 1, turned(south_high, 127 - 8 * row), turned(image[TS, cols], -1)
            )
            finish(row, image[TE, columns(row - 1)], image[TW, columns(row + 1)], from_south, from_north)
        if step == DEPTH - 1:
            return
        to_low = turned(image[TS, columns(low)], -1)
        to_high = turned(image[TN, columns(high)], 1)
        for row in range(start, stop):
            cols = columns(row)
            to_low = jnp.where(lanes == 8 * row + 7, turned(image[TS, cols], 8 * row + 7), to_low)
            to_high = jnp.where(lanes == 8 * row, turned(image[TN, cols], 8 * row + 1), to_high)
        cols = columns(low)
        finish(low, turned(image[TE, cols], 8), turned(image[TW, cols], -8), turned(image[TN, cols], 1), to_low)
        cols = columns(high)
        finish(high, turned(image[TE, cols], 8), turned(image[TW, cols], -8), to_high, turned(image[TS, cols], -1))

    old, new = field_a, field_b
    for step in range(DEPTH):
        apply(old, new, step, step == 0)
        basis_out[step, :, :] = new[:, 6 * LANES : 10 * LANES]
        old, new = new, old

    sums = [jnp.zeros((8, LANES), jnp.float32) for _ in GRAM]
    for x in range(4):
        for a in range(P_SIZE):
            values = [basis_out[k, 8 * a : 8 * a + 8, x * LANES : (x + 1) * LANES] for k in range(ITERS + 1)]
            sums = [total + values[k] * values[l] for total, (k, l) in zip(sums, GRAM)]
    rows = [jnp.sum(total, axis=0, keepdims=True) for total in sums]
    rows = jnp.concatenate(rows + [jnp.zeros((24 - len(GRAM), LANES), jnp.float32)], axis=0)
    totals = jnp.sum(rows, axis=1, keepdims=True)
    place = lax.broadcasted_iota(jnp.int32, (24, LANES), 0) == lax.broadcasted_iota(jnp.int32, (24, LANES), 1)
    totals = jnp.sum(jnp.where(place, totals, 0.0), axis=0, keepdims=True)
    gram_out[...] = jnp.broadcast_to(totals, gram_out.shape)


def combine_kernel(nodes, line_ref, deriv_ref, powers, gathered, basis_out, hess_out, amp_out):
    shift = centre(line_ref, deriv_ref)
    row = jnp.sum(gathered[...], axis=0, keepdims=True) * (1.0 / nodes)
    spread = jnp.broadcast_to(row, (8, LANES))
    gram = {}
    for at, (k, l) in enumerate(GRAM):
        gram[k, l] = gram[l, k] = jnp.broadcast_to(spread[:, at : at + 1], (8, LANES))
    sizes = [jnp.sqrt(gram[k, k]) for k in range(ITERS + 1)]
    sub = lax.broadcasted_iota(jnp.int32, (8, LANES), 0)
    lanes = lane_ids(8)
    hess = jnp.zeros((8, LANES), jnp.float32)
    beta = jnp.sqrt(gram[0, 0] + FLOOR)
    coeffs = [[1.0 / beta]]
    amp = sizes[0] * coeffs[0][0]

    def put(hess, i, j, value):
        return jnp.where((sub == i) & (lanes == j), value, hess)

    for j in range(ITERS):
        last = coeffs[j]
        image = [shift * c for c in last] + [None]
        for k in range(j + 1):
            moved = last[k] * 8.0
            image[k + 1] = moved if image[k + 1] is None else image[k + 1] + moved
        weighted = [
            sum(gram[k, l] * image[l] for l in range(1, j + 2)) + gram[k, 0] * image[0] for k in range(j + 2)
        ]
        pending = list(image)
        for i in range(j + 1):
            h = sum(c * weighted[k] for k, c in enumerate(coeffs[i]))
            hess = put(hess, i, j, h)
            for k, c in enumerate(coeffs[i]):
                pending[k] = pending[k] - h * c
        square = sum(
            pending[k] * sum(gram[k, l] * pending[l] for l in range(j + 2)) for k in range(j + 2)
        )
        beta = jnp.sqrt(jnp.maximum(square, 0.0) + FLOOR)
        hess = put(hess, j + 1, j, beta)
        scale = 1.0 / beta
        coeffs.append([p * scale for p in pending])
        amp = jnp.maximum(amp, sum(jnp.abs(c) * s for c, s in zip(coeffs[-1], sizes)))
    hess_out[...] = hess[0 : ITERS + 1, 0:ITERS]
    amp_out[...] = amp[0:1, :]
    for x in range(4):
        for a in range(P_SIZE):
            values = [powers[k, 8 * a : 8 * a + 8, x * LANES : (x + 1) * LANES] for k in range(ITERS + 1)]
            for j in range(ITERS + 1):
                total = coeffs[j][0] * values[0]
                for k in range(1, j + 1):
                    total = total + coeffs[j][k] * values[k]
                basis_out[j, pl.ds(32 * a + x, 8, stride=4), :] = total


def fast(source, initial, reaction, stiffness, line_op, face_deriv, wall_flags):
    vmem = pl.BlockSpec(memory_space=pltpu.VMEM)
    smem = pl.BlockSpec(memory_space=pltpu.SMEM)
    grant = pltpu.CompilerParams(vmem_limit_bytes=16 * 2**20)
    f32 = jnp.float32
    flat = [v.reshape(4 * NODES, LANES) for v in (source, initial, reaction)]
    walls = wall_flags.reshape(16, LANES)
    nx, ny = lax.axis_size(GX), lax.axis_size(GY)

    def moved(value, axis, size, by):
        return lax.ppermute(value, axis, [(i, (i + by) % size) for i in range(size)])

    near, low2, high2, to_up, to_down = pl.pallas_call(
        pack_kernel,
        out_shape=[jax.ShapeDtypeStruct((n, LANES), f32) for n in (792, 264, 264, NODES, NODES)],
        in_specs=[vmem] * 5,
        out_specs=[vmem] * 5,
        compiler_params=grant,
    )(*flat, stiffness, walls)
    below1 = moved(near, GX, nx, 1)
    above1 = moved(near, GX, nx, -1)
    below2 = moved(high2, GX, nx, 2)
    above2 = moved(low2, GX, nx, -2)
    left = moved(to_up, GY, ny, 1)
    right = moved(to_down, GY, ny, -1)
    own_strip = jnp.concatenate([left, right], axis=0)
    strips = [moved(own_strip, GX, nx, by) for by in (1, -1, 2, -2)]

    powers, gram = pl.pallas_call(
        powers_kernel,
        out_shape=[
            jax.ShapeDtypeStruct((ITERS + 1, NODES, 4 * LANES), f32),
            jax.ShapeDtypeStruct((nx * ny, LANES), f32),
        ],
        in_specs=[smem, smem] + [vmem] * 14,
        out_specs=[vmem] * 2,
        scratch_shapes=[
            pltpu.VMEM((NODES, (ROWS + 2) * LANES), f32),
            pltpu.VMEM((NODES, (ROWS + 2) * LANES), f32),
            pltpu.VMEM((NODES + 32, NODES), f32),
            pltpu.VMEM((NODES + 32, (ROWS + 2) * LANES), f32),
            pltpu.VMEM((NODES, (ROWS + 2) * LANES), f32),
            pltpu.VMEM((8, (ROWS + 2) * LANES), f32),
            pltpu.VMEM((32, (ROWS + 2) * LANES), f32),
        ],
        compiler_params=grant,
    )(line_op, face_deriv, *flat, stiffness, walls, below1, above1, below2, above2, own_strip, *strips)
    every = GX + GY
    gathered = lax.all_to_all(gram, every, split_axis=0, concat_axis=0, tiled=True)
    basis, hess, amp = pl.pallas_call(
        functools.partial(combine_kernel, float(NODES * 4 * nx * LANES * ny)),
        out_shape=[
            jax.ShapeDtypeStruct((ITERS + 1, 4 * NODES, LANES), f32),
            jax.ShapeDtypeStruct((ITERS + 1, ITERS), f32),
            jax.ShapeDtypeStruct((1, LANES), f32),
        ],
        in_specs=[smem, smem] + [vmem] * 2,
        out_specs=[vmem] * 3,
        compiler_params=grant,
    )(line_op, face_deriv, powers, gathered)
    return hess, basis, amp[0, 0]


def body(*args):
    hess, basis, amp = fast(*args)

    def again(carry):
        hess, basis = stepwise(*args)
        return jnp.bool_(True), hess, basis.reshape(ITERS + 1, 4 * NODES, LANES)

    done = amp <= AMP_LIMIT
    _, hess, basis = lax.while_loop(lambda carry: jnp.logical_not(carry[0]), again, (done, hess, basis))
    return (hess, basis.reshape(ITERS + 1, NODES, 4, LANES))


def solution(mesh):
    finer = Mesh(mesh.devices.reshape(4, 2, 4, 8), ("gx_0", "gx_1", "gy_0", "gy_1"))
    placed = (
        P(None, GX, GY),
        P(None, GX, GY),
        P(None, GX, GY),
        P(GX, GY),
        P(),
        P(),
        P(None, GX, GY),
    )
    return jax.shard_map(
        body, mesh=finer, in_specs=placed, out_specs=(P(), P(None, None, GX, GY)), check_vma=False
    )
```

```python
import functools

import jax
import jax.numpy as jnp
from jax import lax
from jax.experimental import pallas as pl
from jax.experimental.pallas import tpu as pltpu
from jax.sharding import Mesh
from jax.sharding import PartitionSpec as P

P_SIZE = 8
ITERS = 5
GX = ("gx_0", "gx_1")
GY = ("gy_0", "gy_1")


TAU = 2.0
FLOOR = 0.1


def extended(array, sides, width):
    for axis, dim in sides:
        devices, length = (lax.axis_size(axis), array.shape[dim])
        up = [(i, (i + 1) % devices) for i in range(devices)]
        down = [(j, i) for i, j in up]
        last = lax.slice_in_dim(array, length - width, length, axis=dim)
        leading = lax.slice_in_dim(array, 0, width, axis=dim)
        before = lax.ppermute(last, axis, up)
        after = lax.ppermute(leading, axis, down)
        array = jnp.concatenate([before, array, after], axis=dim)
    return array


def sent_to_all(array, axis):
    copies = jnp.broadcast_to(array, (lax.axis_size(axis), *array.shape))
    return lax.all_to_all(copies, axis, split_axis=0, concat_axis=0, tiled=True)


def over_copies(array, axis):
    everything = sent_to_all(array, axis)
    return jnp.sum(everything, axis=0)


def by_axis(array, axes):
    far, near = axes
    nearer = over_copies(array, near)
    return over_copies(nearer, far)


def together(arrays, axis):
    vector, at, gathered = (jnp.concatenate([a.reshape(-1) for a in arrays]), 0, [])
    subtotal = by_axis(vector, axis)
    for a in arrays:
        gathered.append(subtotal[at : at + a.size].reshape(a.shape))
        at += a.size
    return tuple(gathered)


def local_total(values):
    return jnp.sum(jnp.sum(values, axis=0))


def x_traces(nodes, face_deriv):
    highest = lax.Precision.HIGHEST
    lower = jnp.einsum("c,cbxy->bxy", face_deriv, nodes, precision=highest)
    upper = jnp.einsum("c,cbxy->bxy", face_deriv[::-1], nodes, precision=highest)
    return jnp.stack([nodes[0], lower, nodes[-1], upper])


def y_traces(nodes, face_deriv):
    highest = lax.Precision.HIGHEST
    lower = jnp.einsum("c,acxy->axy", face_deriv, nodes, precision=highest)
    upper = jnp.einsum("c,acxy->axy", face_deriv[::-1], nodes, precision=highest)
    return jnp.stack([nodes[:, 0], lower, nodes[:, -1], upper])


def apply_op(field, reaction, stiffness, line_op, face_deriv, opened):
    highest = lax.Precision.HIGHEST
    nodes = field.reshape(P_SIZE, P_SIZE, field.shape[1], field.shape[2])
    interior = stiffness * (
        jnp.einsum("ac,cbxy->abxy", line_op, nodes, precision=highest)
        + jnp.einsum("bc,acxy->abxy", line_op, nodes, precision=highest)
    )
    xside = extended(x_traces(nodes, face_deriv), ((GX, 2),), 1)
    yside = extended(y_traces(nodes, face_deriv), ((GY, 3),), 1)
    x_own = xside[:, :, 1:-1]
    y_own = yside[:, :, :, 1:-1]
    east_nb = xside[0:2, :, 2:]
    west_nb = xside[2:4, :, :-2]
    north_nb = yside[0:2, :, :, 2:]
    south_nb = yside[2:4, :, :, :-2]
    add_east = TAU * (x_own[2] - opened[1] * east_nb[0]) + 0.5 * (x_own[3] - opened[1] * east_nb[1])
    add_west = TAU * (x_own[0] - opened[0] * west_nb[0]) + 0.5 * (x_own[1] - opened[0] * west_nb[1])
    add_north = TAU * (y_own[2] - opened[3] * north_nb[0]) + 0.5 * (
        y_own[3] - opened[3] * north_nb[1]
    )
    add_south = TAU * (y_own[0] - opened[2] * south_nb[0]) + 0.5 * (
        y_own[1] - opened[2] * south_nb[1]
    )
    result = reaction.reshape(nodes.shape) * nodes + interior
    result = result.at[0].add(add_west).at[P_SIZE - 1].add(add_east)
    result = result.at[:, 0].add(add_south).at[:, P_SIZE - 1].add(add_north)
    return result.reshape(field.shape)


def norm_scale(vector, total):
    squares = by_axis(local_total(vector * vector), (("gx_0", "gx_1"), ("gy_0", "gy_1")))
    return jnp.sqrt(squares / total + FLOOR)


def stepwise(source, initial, reaction, stiffness, line_op, face_deriv, wall_flags):
    highest = lax.Precision.HIGHEST
    total = float(
        P_SIZE * P_SIZE * source.shape[1] * lax.axis_size(GX) * source.shape[2] * lax.axis_size(GY)
    )
    opened = 1.0 - wall_flags.astype(jnp.float32)

    def operate(field):
        return apply_op(field, reaction, stiffness, line_op, face_deriv, opened)

    def products(basis, image):
        per_cell = jnp.einsum("kqxy,qxy->kxy", basis, image, precision=highest)
        return jnp.sum(per_cell, axis=(1, 2))

    first = source - operate(initial)
    basis = jnp.zeros((ITERS + 1,) + source.shape, jnp.float32)
    hessen = jnp.zeros((ITERS + 1, ITERS), jnp.float32)
    rows = lax.broadcasted_iota(jnp.int32, (ITERS + 1, ITERS), 0)
    cols = lax.broadcasted_iota(jnp.int32, (ITERS + 1, ITERS), 1)
    slots = lax.broadcasted_iota(jnp.int32, (ITERS + 1,), 0)

    def advance(step, carry):
        basis, hessen, pending = carry
        image = operate(pending)
        local = products(basis, image)
        projected, crossed, squares = together(
            (local, local_total(pending * image), local_total(pending * pending)),
            (("gx_0", "gx_1"), ("gy_0", "gy_1")),
        )
        beta = jnp.sqrt(squares / total + FLOOR)
        basis = lax.dynamic_update_index_in_dim(basis, pending / beta, step, 0)
        coeffs = projected / (total * beta) + jnp.where(
            slots == step, crossed / (total * beta * beta), 0.0
        )
        pending = image / beta - jnp.einsum("k,kqxy->qxy", coeffs, basis, precision=highest)
        hessen = hessen + jnp.where(cols == step, coeffs[:, None], 0.0)
        hessen = hessen + jnp.where((rows == step) & (cols == step - 1), beta, 0.0)
        return (basis, hessen, pending)

    basis, hessen, pending = lax.fori_loop(0, ITERS, advance, (basis, hessen, first))
    beta = norm_scale(pending, total)
    basis = basis.at[ITERS].set(pending / beta)
    hessen = hessen + jnp.where((rows == ITERS) & (cols == ITERS - 1), beta, 0.0)
    return (hessen, basis)


NODES = P_SIZE * P_SIZE
ROWS = 16
DEPTH = 6
LANES = 128
SCALE = 0.125
AMP_LIMIT = 100.0
GRAM = [(k, l) for k in range(ITERS + 1) for l in range(k + 1)]
HIGHEST = lax.Precision.HIGHEST


def centre(line_ref, deriv_ref):
    trace = line_ref[0, 0]
    for a in range(1, P_SIZE):
        trace = trace + line_ref[a, a]
    return 2.0 + 0.3125 * trace + 0.5 * (TAU + 0.5 * deriv_ref[0])


def lane_ids(rows):
    return lax.broadcasted_iota(jnp.int32, (rows, LANES), 1)


def turned(value, shift):
    shift = shift % LANES
    return value if shift == 0 else pltpu.roll(value, shift, 1)


def strided(ref, start, count):
    return ref[pl.ds(start, count, stride=4), :]


def pack_kernel(source, initial, reaction, stiffness, walls, near, low2, high2, to_up, to_down, flags, sems):
    moves = []
    for at, ref in ((0, initial), (256, source), (512, reaction)):
        for half in (0, 128):
            moves.append((ref.at[pl.ds(half, 128), :], near.at[pl.ds(at + half, 128), :]))
    moves.append((stiffness, near.at[pl.ds(768, 4), :]))
    moves.append((walls, flags))
    copies = [pltpu.make_async_copy(a, b, sems.at[n]) for n, (a, b) in enumerate(moves)]
    for copy in copies:
        copy.start()
    for copy in copies:
        copy.wait()
    opened = 1.0 - flags[...].astype(jnp.float32)
    near[772:788, :] = opened
    near[788:792, :] = jnp.zeros((4, LANES), jnp.float32)
    thick = near[768:772, :]
    for out, far, close in ((high2, 2, 3), (low2, 1, 0)):
        out[0:64, :] = strided(near, far, NODES)
        out[64:128, :] = strided(near, close, NODES)
        out[128:192, :] = strided(near, 256 + close, NODES)
        out[192:256, :] = strided(near, 512 + close, NODES)
        out[256:257, :] = thick[close : close + 1, :]
        for f in range(4):
            out[257 + f : 258 + f, :] = opened[4 * f + close : 4 * f + close + 1, :]
        out[261:264, :] = jnp.zeros((3, LANES), jnp.float32)
    lanes = lane_ids(NODES)
    lanes8 = lane_ids(8)
    for out, first in ((to_up, 120), (to_down, 0)):
        total = jnp.zeros((NODES, LANES), jnp.float32)
        extra = jnp.zeros((8, LANES), jnp.float32)
        for x in range(4):
            for field in range(3):
                at = 32 * field + 8 * x
                moved = turned(strided(near, 256 * field + x, NODES), at - first)
                total = jnp.where((lanes >= at) & (lanes < at + 8), moved, total)
            at = 96 + 8 * x
            rows = [thick[x : x + 1, :]] + [opened[4 * f + x : 4 * f + x + 1, :] for f in range(4)]
            rows = jnp.concatenate(rows + [jnp.zeros((3, LANES), jnp.float32)], axis=0)
            extra = jnp.where((lanes8 >= at) & (lanes8 < at + 8), turned(rows, at - first), extra)
        out[...] = total
        out[0:8, :] = total[0:8] + extra


def weights_in(line_ref, deriv_ref):
    def grid(rows, columns):
        return (
            lax.broadcasted_iota(jnp.int32, (rows, columns), 0),
            lax.broadcasted_iota(jnp.int32, (rows, columns), 1),
        )

    r, s = grid(NODES, NODES)
    ra, rb, sa, sb = r // 8, r % 8, s // 8, s % 8
    full = jnp.zeros((NODES, NODES), jnp.float32)
    for a in range(P_SIZE):
        for c in range(P_SIZE):
            value = line_ref[a, c]
            full = full + jnp.where((ra == a) & (sa == c) & (rb == sb), value, 0.0)
            full = full + jnp.where((rb == a) & (sb == c) & (ra == sa), value, 0.0)
    r, s = grid(8, NODES)
    sa, sb = s // 8, s % 8
    parts = [full]
    for along, across in ((sa, sb), (sb, sa)):
        for flip in (False, True):
            part = jnp.zeros((8, NODES), jnp.float32)
            for c in range(P_SIZE):
                value = 0.5 * deriv_ref[c] + (TAU if c == 0 else 0.0)
                place = P_SIZE - 1 - c if flip else c
                part = part + jnp.where((across == r) & (along == place), value, 0.0)
            parts.append(part * SCALE)
    return jnp.concatenate(parts, axis=0)


def split(value):
    high = value.astype(jnp.bfloat16)
    rest = value - high.astype(jnp.float32)
    middle = rest.astype(jnp.bfloat16)
    low = (rest - middle.astype(jnp.float32)).astype(jnp.bfloat16)
    return high, middle, low


def weights_kernel(line_ref, deriv_ref, after, out):
    high, middle, low = split(weights_in(line_ref, deriv_ref))
    out[...] = jnp.concatenate([high, high, high, middle, middle, low], axis=1)


def product(weight, value):
    high, middle, low = split(value)
    stacked = jnp.concatenate([high, middle, low, high, middle, high], axis=0)
    return jnp.dot(weight[...], stacked, preferred_element_type=jnp.float32)


def powers_kernel(
    line_ref, deriv_ref, weight, near,
    below1, above1, below2, above2, own_strip, strip_b1, strip_a1, strip_b2, strip_a2,
    basis_out, gram_out, field_a, field_b, image, react, stiff, opened,
):
    shift = centre(line_ref, deriv_ref)

    def put(row, value_initial, value_reaction, value_stiffness, value_open):
        cols = slice(row * LANES, (row + 1) * LANES)
        field_a[:, cols] = value_initial
        react[:, cols] = (value_reaction - shift) * SCALE
        stiff[:, cols] = jnp.broadcast_to(value_stiffness * SCALE, (8, LANES))
        for f in range(4):
            opened[8 * f : 8 * f + 8, cols] = jnp.broadcast_to(value_open[f], (8, LANES))

    for x in range(4):
        for ref, row in ((near, 6 + x), (below1, 2 + x), (above1, 10 + x)):
            put(
                row, strided(ref, x, NODES), strided(ref, 512 + x, NODES), ref[768 + x : 769 + x, :],
                [ref[772 + 4 * f + x : 773 + 4 * f + x, :] for f in range(4)],
            )
    for ref, far, close in ((below2, 0, 1), (above2, 15, 14)):
        put(
            close, ref[64:128, :], ref[192:256, :], ref[256:257, :],
            [ref[257 + f : 258 + f, :] for f in range(4)],
        )
        field_a[:, far * LANES : (far + 1) * LANES] = ref[0:64, :]

    lanes64 = lane_ids(NODES)
    lanes = lane_ids(8)
    pieces = ((strip_b2, 0, 16, -16), (strip_b1, 16, 48, 16), (own_strip, 48, 80, 48),
              (strip_a1, 80, 112, 80), (strip_a2, 112, 128, 112))
    strip_source = []
    for side in range(2):
        rows = slice(NODES * side, NODES * side + NODES)
        made = []
        for field in range(4):
            count = NODES if field < 3 else 8
            ids = lanes64 if field < 3 else lanes
            value = jnp.zeros((count, LANES), jnp.float32)
            for ref, start, stop, zero in pieces:
                part = ref[NODES * side : NODES * side + count, :]
                value = jnp.where((ids >= start) & (ids < stop), turned(part, zero - 32 * field), value)
            made.append(value)
        put(ROWS + side, made[0], made[2], made[3][0:1], [made[3][1 + f : 2 + f] for f in range(4)])
        strip_source.append(made[1])

    def columns(row):
        return slice(row * LANES, (row + 1) * LANES)

    low, high = ROWS, ROWS + 1
    sub = lax.broadcasted_iota(jnp.int32, (8, LANES), 0)
    TW, TE, TS, TN = (slice(64 + 8 * f, 72 + 8 * f) for f in range(4))

    def source_of(row):
        if row >= ROWS:
            return strip_source[row - ROWS]
        if 6 <= row < 10:
            return strided(near, 256 + row - 6, NODES)
        if 2 <= row < 6:
            return strided(below1, 256 + row - 2, NODES)
        if 10 <= row < 14:
            return strided(above1, 256 + row - 10, NODES)
        return (below2 if row < 2 else above2)[128:192, :]

    def apply(old, new, step, first):
        start, stop = step, ROWS - step
        for first_row, last_row in ((start, stop), (ROWS, ROWS + 2)):
            for row in range(first_row, last_row, 2):
                cols = slice(row * LANES, (row + 2) * LANES)
                image[:, cols] = product(weight, old[:, cols])

        def finish(row, from_west, from_east, from_south, from_north):
            cols = columns(row)
            west = image[TW, cols] - opened[0:8, cols] * from_west
            east = image[TE, cols] - opened[8:16, cols] * from_east
            south = image[TS, cols] - opened[16:24, cols] * from_south
            north = image[TN, cols] - opened[24:32, cols] * from_north
            for a in range(P_SIZE):
                rows = slice(8 * a, 8 * a + 8)
                value = react[rows, cols] * old[rows, cols] + stiff[:, cols] * image[rows, cols]
                if a == 0:
                    value = value + west
                if a == P_SIZE - 1:
                    value = value + east
                edge = jnp.where(sub == 0, south[a : a + 1, :], 0.0)
                edge = jnp.where(sub == P_SIZE - 1, north[a : a + 1, :], edge)
                value = value + edge
                if first:
                    value = -8.0 * value - shift * old[rows, cols]
                new[rows, cols] = value
            if first:
                new[:, cols] = new[:, cols] + source_of(row)

        north_low = image[TN, columns(low)]
        south_high = image[TS, columns(high)]
        for row in range(start + 1, stop - 1):
            cols = columns(row)
            from_south = jnp.where(
                lanes == 0, turned(north_low, -(8 * row + 7)), turned(image[TN, cols], 1)
            )
            from_north = jnp.where(
                lanes == LANES - 1, turned(south_high, 127 - 8 * row), turned(image[TS, cols], -1)
            )
            finish(row, image[TE, columns(row - 1)], image[TW, columns(row + 1)], from_south, from_north)
        if step == DEPTH - 1:
            return
        to_low = turned(image[TS, columns(low)], -1)
        to_high = turned(image[TN, columns(high)], 1)
        for row in range(start, stop):
            cols = columns(row)
            to_low = jnp.where(lanes == 8 * row + 7, turned(image[TS, cols], 8 * row + 7), to_low)
            to_high = jnp.where(lanes == 8 * row, turned(image[TN, cols], 8 * row + 1), to_high)
        cols = columns(low)
        finish(low, turned(image[TE, cols], 8), turned(image[TW, cols], -8), turned(image[TN, cols], 1), to_low)
        cols = columns(high)
        finish(high, turned(image[TE, cols], 8), turned(image[TW, cols], -8), to_high, turned(image[TS, cols], -1))

    old, new = field_a, field_b
    for step in range(DEPTH):
        apply(old, new, step, step == 0)
        basis_out[step, :, :] = new[:, 6 * LANES : 10 * LANES]
        old, new = new, old

    sums = [jnp.zeros((8, LANES), jnp.float32) for _ in GRAM]
    for x in range(4):
        for a in range(P_SIZE):
            values = [basis_out[k, 8 * a : 8 * a + 8, x * LANES : (x + 1) * LANES] for k in range(ITERS + 1)]
            sums = [total + values[k] * values[l] for total, (k, l) in zip(sums, GRAM)]
    rows = [jnp.sum(total, axis=0, keepdims=True) for total in sums]
    rows = jnp.concatenate(rows + [jnp.zeros((24 - len(GRAM), LANES), jnp.float32)], axis=0)
    totals = jnp.sum(rows, axis=1, keepdims=True)
    place = lax.broadcasted_iota(jnp.int32, (24, LANES), 0) == lax.broadcasted_iota(jnp.int32, (24, LANES), 1)
    totals = jnp.sum(jnp.where(place, totals, 0.0), axis=0, keepdims=True)
    gram_out[...] = jnp.broadcast_to(totals, gram_out.shape)


def combine_kernel(nodes, line_ref, deriv_ref, powers, gathered, basis_out, hess_out, amp_out, made, sems):
    shift = centre(line_ref, deriv_ref)
    row = jnp.sum(gathered[...], axis=0, keepdims=True) * (1.0 / nodes)
    spread = jnp.broadcast_to(row, (8, LANES))
    gram = {}
    for at, (k, l) in enumerate(GRAM):
        gram[k, l] = gram[l, k] = jnp.broadcast_to(spread[:, at : at + 1], (8, LANES))
    sizes = [jnp.sqrt(gram[k, k]) for k in range(ITERS + 1)]
    sub = lax.broadcasted_iota(jnp.int32, (8, LANES), 0)
    lanes = lane_ids(8)
    hess = jnp.zeros((8, LANES), jnp.float32)
    beta = jnp.sqrt(gram[0, 0] + FLOOR)
    coeffs = [[1.0 / beta]]
    amp = sizes[0] * coeffs[0][0]

    def put(hess, i, j, value):
        return jnp.where((sub == i) & (lanes == j), value, hess)

    for j in range(ITERS):
        last = coeffs[j]
        image = [shift * c for c in last] + [None]
        for k in range(j + 1):
            moved = last[k] * 8.0
            image[k + 1] = moved if image[k + 1] is None else image[k + 1] + moved
        weighted = [
            sum(gram[k, l] * image[l] for l in range(1, j + 2)) + gram[k, 0] * image[0] for k in range(j + 2)
        ]
        pending = list(image)
        for i in range(j + 1):
            h = sum(c * weighted[k] for k, c in enumerate(coeffs[i]))
            hess = put(hess, i, j, h)
            for k, c in enumerate(coeffs[i]):
                pending[k] = pending[k] - h * c
        square = sum(
            pending[k] * sum(gram[k, l] * pending[l] for l in range(j + 2)) for k in range(j + 2)
        )
        beta = jnp.sqrt(jnp.maximum(square, 0.0) + FLOOR)
        hess = put(hess, j + 1, j, beta)
        scale = 1.0 / beta
        coeffs.append([p * scale for p in pending])
        amp = jnp.maximum(amp, sum(jnp.abs(c) * s for c, s in zip(coeffs[-1], sizes)))
    hess_out[...] = hess[0 : ITERS + 1, 0:ITERS]
    amp_out[...] = amp[0:1, :]
    copies = []
    for j in range(ITERS + 1):
        for half in range(2):
            for a in range(4 * half, 4 * half + 4):
                for x in range(4):
                    rows, cols = slice(8 * a, 8 * a + 8), slice(x * LANES, (x + 1) * LANES)
                    total = coeffs[j][0] * powers[0, rows, cols]
                    for k in range(1, j + 1):
                        total = total + coeffs[j][k] * powers[k, rows, cols]
                    made[j, pl.ds(32 * a + x, 8, stride=4), :] = total
            part = pl.ds(128 * half, 128)
            copies.append(
                pltpu.make_async_copy(made.at[j, part, :], basis_out.at[j, part, :], sems.at[2 * j + half])
            )
            copies[-1].start()
    for copy in copies:
        copy.wait()


def fast(source, initial, reaction, stiffness, line_op, face_deriv, wall_flags):
    vmem = pl.BlockSpec(memory_space=pltpu.VMEM)
    smem = pl.BlockSpec(memory_space=pltpu.SMEM)
    hbm = pl.BlockSpec(memory_space=pltpu.HBM)
    grant = pltpu.CompilerParams(vmem_limit_bytes=16 * 2**20)
    f32 = jnp.float32
    nx, ny = lax.axis_size(GX), lax.axis_size(GY)
    wide = (ROWS + 2) * LANES

    def moved(value, axis, size, by):
        return lax.ppermute(value, axis, [(i, (i + by) % size) for i in range(size)])

    near, low2, high2, to_up, to_down = pl.pallas_call(
        pack_kernel,
        out_shape=[jax.ShapeDtypeStruct((n, LANES), f32) for n in (792, 264, 264, NODES, NODES)],
        in_specs=[hbm] * 5,
        out_specs=[vmem] * 5,
        scratch_shapes=[pltpu.VMEM((16, LANES), jnp.int32), pltpu.SemaphoreType.DMA((8,))],
        compiler_params=grant,
    )(source, initial, reaction, stiffness, wall_flags)
    left = moved(to_up, GY, ny, 1)
    right = moved(to_down, GY, ny, -1)
    below1 = moved(near, GX, nx, 1)
    above1 = moved(near, GX, nx, -1)
    below2 = moved(high2, GX, nx, 2)
    above2 = moved(low2, GX, nx, -2)
    own_strip = jnp.concatenate([left, right], axis=0)
    strips = [moved(own_strip, GX, nx, by) for by in (1, -1, 2, -2)]
    weight = pl.pallas_call(
        weights_kernel,
        out_shape=jax.ShapeDtypeStruct((NODES + 32, 6 * NODES), jnp.bfloat16),
        in_specs=[smem, smem, vmem],
        out_specs=vmem,
        compiler_params=grant,
        cost_estimate=pl.CostEstimate(flops=4000000, bytes_accessed=100000, transcendentals=0),
    )(line_op, face_deriv, own_strip)

    powers, gram = pl.pallas_call(
        powers_kernel,
        out_shape=[
            jax.ShapeDtypeStruct((ITERS + 1, NODES, 4 * LANES), f32),
            jax.ShapeDtypeStruct((1, LANES), f32),
        ],
        in_specs=[smem, smem] + [vmem] * 11,
        out_specs=[vmem] * 2,
        scratch_shapes=[pltpu.VMEM((n, wide), f32) for n in (NODES, NODES, NODES + 32, NODES, 8, 32)],
        compiler_params=grant,
    )(line_op, face_deriv, weight, near, below1, above1, below2, above2, own_strip, *strips)
    every = GX + GY
    copies = jnp.broadcast_to(gram, (nx * ny, LANES))
    gathered = lax.all_to_all(copies, every, split_axis=0, concat_axis=0, tiled=True)
    basis, hess, amp = pl.pallas_call(
        functools.partial(combine_kernel, float(NODES * 4 * nx * LANES * ny)),
        out_shape=[
            jax.ShapeDtypeStruct((ITERS + 1, 4 * NODES, LANES), f32),
            jax.ShapeDtypeStruct((ITERS + 1, ITERS), f32),
            jax.ShapeDtypeStruct((1, LANES), f32),
        ],
        in_specs=[smem, smem] + [vmem] * 2,
        out_specs=[hbm, vmem, vmem],
        scratch_shapes=[
            pltpu.VMEM((ITERS + 1, 4 * NODES, LANES), f32),
            pltpu.SemaphoreType.DMA((2 * ITERS + 2,)),
        ],
        compiler_params=grant,
    )(line_op, face_deriv, powers, gathered)
    return hess, basis, amp[0, 0]


def body(source, initial, reaction, stiffness, line_op, face_deriv, wall_flags):
    flat = [v.reshape(4 * NODES, LANES) for v in (source, initial, reaction)]
    rest = (stiffness, line_op, face_deriv)
    walls = wall_flags.reshape(16, LANES)
    hess, basis, amp = fast(*flat, *rest, walls)

    def again(carry):
        full = [v.reshape(NODES, 4, LANES) for v in flat]
        hess, basis = stepwise(*full, *rest, walls.reshape(4, 4, LANES))
        return jnp.bool_(True), hess, basis.reshape(ITERS + 1, 4 * NODES, LANES)

    done = amp <= AMP_LIMIT
    _, hess, basis = lax.while_loop(lambda carry: jnp.logical_not(carry[0]), again, (done, hess, basis))
    return (hess, basis.reshape(ITERS + 1, NODES, 4, LANES))


def solution(mesh):
    finer = Mesh(mesh.devices.reshape(4, 2, 4, 8), ("gx_0", "gx_1", "gy_0", "gy_1"))
    placed = (
        P(None, GX, GY),
        P(None, GX, GY),
        P(None, GX, GY),
        P(GX, GY),
        P(),
        P(),
        P(None, GX, GY),
    )
    return jax.shard_map(
        body, mesh=finer, in_specs=placed, out_specs=(P(), P(None, None, GX, GY)), check_vma=False
    )
```

```python
import functools

import jax
import jax.numpy as jnp
from jax import lax
from jax.experimental import pallas as pl
from jax.experimental.pallas import tpu as pltpu
from jax.sharding import Mesh
from jax.sharding import PartitionSpec as P

P_SIZE = 8
ITERS = 5
GX = ("gx_0", "gx_1")
GY = ("gy_0", "gy_1")


TAU = 2.0
FLOOR = 0.1


def extended(array, sides, width):
    for axis, dim in sides:
        devices, length = (lax.axis_size(axis), array.shape[dim])
        up = [(i, (i + 1) % devices) for i in range(devices)]
        down = [(j, i) for i, j in up]
        last = lax.slice_in_dim(array, length - width, length, axis=dim)
        leading = lax.slice_in_dim(array, 0, width, axis=dim)
        before = lax.ppermute(last, axis, up)
        after = lax.ppermute(leading, axis, down)
        array = jnp.concatenate([before, array, after], axis=dim)
    return array


def sent_to_all(array, axis):
    copies = jnp.broadcast_to(array, (lax.axis_size(axis), *array.shape))
    return lax.all_to_all(copies, axis, split_axis=0, concat_axis=0, tiled=True)


def over_copies(array, axis):
    everything = sent_to_all(array, axis)
    return jnp.sum(everything, axis=0)


def by_axis(array, axes):
    far, near = axes
    nearer = over_copies(array, near)
    return over_copies(nearer, far)


def together(arrays, axis):
    vector, at, gathered = (jnp.concatenate([a.reshape(-1) for a in arrays]), 0, [])
    subtotal = by_axis(vector, axis)
    for a in arrays:
        gathered.append(subtotal[at : at + a.size].reshape(a.shape))
        at += a.size
    return tuple(gathered)


def local_total(values):
    return jnp.sum(jnp.sum(values, axis=0))


def x_traces(nodes, face_deriv):
    highest = lax.Precision.HIGHEST
    lower = jnp.einsum("c,cbxy->bxy", face_deriv, nodes, precision=highest)
    upper = jnp.einsum("c,cbxy->bxy", face_deriv[::-1], nodes, precision=highest)
    return jnp.stack([nodes[0], lower, nodes[-1], upper])


def y_traces(nodes, face_deriv):
    highest = lax.Precision.HIGHEST
    lower = jnp.einsum("c,acxy->axy", face_deriv, nodes, precision=highest)
    upper = jnp.einsum("c,acxy->axy", face_deriv[::-1], nodes, precision=highest)
    return jnp.stack([nodes[:, 0], lower, nodes[:, -1], upper])


def apply_op(field, reaction, stiffness, line_op, face_deriv, opened):
    highest = lax.Precision.HIGHEST
    nodes = field.reshape(P_SIZE, P_SIZE, field.shape[1], field.shape[2])
    interior = stiffness * (
        jnp.einsum("ac,cbxy->abxy", line_op, nodes, precision=highest)
        + jnp.einsum("bc,acxy->abxy", line_op, nodes, precision=highest)
    )
    xside = extended(x_traces(nodes, face_deriv), ((GX, 2),), 1)
    yside = extended(y_traces(nodes, face_deriv), ((GY, 3),), 1)
    x_own = xside[:, :, 1:-1]
    y_own = yside[:, :, :, 1:-1]
    east_nb = xside[0:2, :, 2:]
    west_nb = xside[2:4, :, :-2]
    north_nb = yside[0:2, :, :, 2:]
    south_nb = yside[2:4, :, :, :-2]
    add_east = TAU * (x_own[2] - opened[1] * east_nb[0]) + 0.5 * (x_own[3] - opened[1] * east_nb[1])
    add_west = TAU * (x_own[0] - opened[0] * west_nb[0]) + 0.5 * (x_own[1] - opened[0] * west_nb[1])
    add_north = TAU * (y_own[2] - opened[3] * north_nb[0]) + 0.5 * (
        y_own[3] - opened[3] * north_nb[1]
    )
    add_south = TAU * (y_own[0] - opened[2] * south_nb[0]) + 0.5 * (
        y_own[1] - opened[2] * south_nb[1]
    )
    result = reaction.reshape(nodes.shape) * nodes + interior
    result = result.at[0].add(add_west).at[P_SIZE - 1].add(add_east)
    result = result.at[:, 0].add(add_south).at[:, P_SIZE - 1].add(add_north)
    return result.reshape(field.shape)


def norm_scale(vector, total):
    squares = by_axis(local_total(vector * vector), (("gx_0", "gx_1"), ("gy_0", "gy_1")))
    return jnp.sqrt(squares / total + FLOOR)


def stepwise(source, initial, reaction, stiffness, line_op, face_deriv, opened):
    highest = lax.Precision.HIGHEST
    total = float(
        P_SIZE * P_SIZE * source.shape[1] * lax.axis_size(GX) * source.shape[2] * lax.axis_size(GY)
    )

    def operate(field):
        return apply_op(field, reaction, stiffness, line_op, face_deriv, opened)

    def products(basis, image):
        per_cell = jnp.einsum("kqxy,qxy->kxy", basis, image, precision=highest)
        return jnp.sum(per_cell, axis=(1, 2))

    first = source - operate(initial)
    basis = jnp.zeros((ITERS + 1,) + source.shape, jnp.float32)
    hessen = jnp.zeros((ITERS + 1, ITERS), jnp.float32)
    rows = lax.broadcasted_iota(jnp.int32, (ITERS + 1, ITERS), 0)
    cols = lax.broadcasted_iota(jnp.int32, (ITERS + 1, ITERS), 1)
    slots = lax.broadcasted_iota(jnp.int32, (ITERS + 1,), 0)

    def advance(step, carry):
        basis, hessen, pending = carry
        image = operate(pending)
        local = products(basis, image)
        projected, crossed, squares = together(
            (local, local_total(pending * image), local_total(pending * pending)),
            (("gx_0", "gx_1"), ("gy_0", "gy_1")),
        )
        beta = jnp.sqrt(squares / total + FLOOR)
        basis = lax.dynamic_update_index_in_dim(basis, pending / beta, step, 0)
        coeffs = projected / (total * beta) + jnp.where(
            slots == step, crossed / (total * beta * beta), 0.0
        )
        pending = image / beta - jnp.einsum("k,kqxy->qxy", coeffs, basis, precision=highest)
        hessen = hessen + jnp.where(cols == step, coeffs[:, None], 0.0)
        hessen = hessen + jnp.where((rows == step) & (cols == step - 1), beta, 0.0)
        return (basis, hessen, pending)

    basis, hessen, pending = lax.fori_loop(0, ITERS, advance, (basis, hessen, first))
    beta = norm_scale(pending, total)
    basis = basis.at[ITERS].set(pending / beta)
    hessen = hessen + jnp.where((rows == ITERS) & (cols == ITERS - 1), beta, 0.0)
    return (hessen, basis)


NODES = P_SIZE * P_SIZE
ROWS = 16
DEPTH = 6
LANES = 128
SCALE = 0.125
AMP_LIMIT = 100.0
GRAM = [(k, l) for k in range(ITERS + 1) for l in range(k + 1)]
HIGHEST = lax.Precision.HIGHEST


def centre(line_ref, deriv_ref):
    trace = line_ref[0, 0]
    for a in range(1, P_SIZE):
        trace = trace + line_ref[a, a]
    return 2.0 + 0.3125 * trace + 0.5 * (TAU + 0.5 * deriv_ref[0])


def lane_ids(rows):
    return lax.broadcasted_iota(jnp.int32, (rows, LANES), 1)


def turned(value, shift):
    shift = shift % LANES
    return value if shift == 0 else pltpu.roll(value, shift, 1)


def strided(ref, start, count):
    return ref[pl.ds(start, count, stride=4), :]


def pack_kernel(source, initial, reaction, stiffness, walls, near, low2, high2, to_up, to_down, flags, sems):
    moves = []
    for at, ref in ((0, initial), (256, source), (512, reaction)):
        for half in (0, 128):
            moves.append((ref.at[pl.ds(half, 128), :], near.at[pl.ds(at + half, 128), :]))
    moves.append((stiffness, near.at[pl.ds(768, 4), :]))
    moves.append((walls, flags))
    copies = [pltpu.make_async_copy(a, b, sems.at[n]) for n, (a, b) in enumerate(moves)]
    for copy in copies:
        copy.start()
    for copy in copies:
        copy.wait()
    opened = 1.0 - flags[...].astype(jnp.float32)
    near[772:788, :] = opened
    near[788:792, :] = jnp.zeros((4, LANES), jnp.float32)
    thick = near[768:772, :]
    for out, far, close in ((high2, 2, 3), (low2, 1, 0)):
        out[0:64, :] = strided(near, far, NODES)
        out[64:128, :] = strided(near, close, NODES)
        out[128:192, :] = strided(near, 256 + close, NODES)
        out[192:256, :] = strided(near, 512 + close, NODES)
        out[256:257, :] = thick[close : close + 1, :]
        for f in range(4):
            out[257 + f : 258 + f, :] = opened[4 * f + close : 4 * f + close + 1, :]
        out[261:264, :] = jnp.zeros((3, LANES), jnp.float32)
    lanes = lane_ids(NODES)
    lanes8 = lane_ids(8)
    for out, first in ((to_up, 120), (to_down, 0)):
        total = jnp.zeros((NODES, LANES), jnp.float32)
        extra = jnp.zeros((8, LANES), jnp.float32)
        for x in range(4):
            for field in range(3):
                at = 32 * field + 8 * x
                moved = turned(strided(near, 256 * field + x, NODES), at - first)
                total = jnp.where((lanes >= at) & (lanes < at + 8), moved, total)
            at = 96 + 8 * x
            rows = [thick[x : x + 1, :]] + [opened[4 * f + x : 4 * f + x + 1, :] for f in range(4)]
            rows = jnp.concatenate(rows + [jnp.zeros((3, LANES), jnp.float32)], axis=0)
            extra = jnp.where((lanes8 >= at) & (lanes8 < at + 8), turned(rows, at - first), extra)
        out[...] = total
        out[0:8, :] = total[0:8] + extra


def weights_in(line_ref, deriv_ref):
    def grid(rows, columns):
        return (
            lax.broadcasted_iota(jnp.int32, (rows, columns), 0),
            lax.broadcasted_iota(jnp.int32, (rows, columns), 1),
        )

    r, s = grid(NODES, NODES)
    ra, rb, sa, sb = r // 8, r % 8, s // 8, s % 8
    full = jnp.zeros((NODES, NODES), jnp.float32)
    for a in range(P_SIZE):
        for c in range(P_SIZE):
            value = line_ref[a, c]
            full = full + jnp.where((ra == a) & (sa == c) & (rb == sb), value, 0.0)
            full = full + jnp.where((rb == a) & (sb == c) & (ra == sa), value, 0.0)
    r, s = grid(8, NODES)
    sa, sb = s // 8, s % 8
    parts = [full]
    for along, across in ((sa, sb), (sb, sa)):
        for flip in (False, True):
            part = jnp.zeros((8, NODES), jnp.float32)
            for c in range(P_SIZE):
                value = 0.5 * deriv_ref[c] + (TAU if c == 0 else 0.0)
                place = P_SIZE - 1 - c if flip else c
                part = part + jnp.where((across == r) & (along == place), value, 0.0)
            parts.append(part * SCALE)
    return jnp.concatenate(parts, axis=0)


def split(value):
    high = value.astype(jnp.bfloat16)
    rest = value - high.astype(jnp.float32)
    middle = rest.astype(jnp.bfloat16)
    low = (rest - middle.astype(jnp.float32)).astype(jnp.bfloat16)
    return high, middle, low


def weights_kernel(line_ref, deriv_ref, after, out):
    high, middle, low = split(weights_in(line_ref, deriv_ref))
    out[...] = jnp.concatenate([high, high, high, middle, middle, low], axis=1)


def product(weight, value):
    high, middle, low = split(value)
    stacked = jnp.concatenate([high, middle, low, high, middle, high], axis=0)
    return jnp.dot(weight[...], stacked, preferred_element_type=jnp.float32)


def powers_kernel(
    line_ref, deriv_ref, weight, near,
    below1, above1, below2, above2, own_strip, strip_b1, strip_a1, strip_b2, strip_a2,
    basis_out, gram_out, field_a, field_b, image, react, stiff, opened,
):
    shift = centre(line_ref, deriv_ref)

    def put(row, value_initial, value_reaction, value_stiffness, value_open):
        cols = slice(row * LANES, (row + 1) * LANES)
        field_a[:, cols] = value_initial
        react[:, cols] = (value_reaction - shift) * SCALE
        stiff[:, cols] = jnp.broadcast_to(value_stiffness * SCALE, (8, LANES))
        for f in range(4):
            opened[8 * f : 8 * f + 8, cols] = jnp.broadcast_to(value_open[f], (8, LANES))

    for x in range(4):
        for ref, row in ((near, 6 + x), (below1, 2 + x), (above1, 10 + x)):
            put(
                row, strided(ref, x, NODES), strided(ref, 512 + x, NODES), ref[768 + x : 769 + x, :],
                [ref[772 + 4 * f + x : 773 + 4 * f + x, :] for f in range(4)],
            )
    for ref, far, close in ((below2, 0, 1), (above2, 15, 14)):
        put(
            close, ref[64:128, :], ref[192:256, :], ref[256:257, :],
            [ref[257 + f : 258 + f, :] for f in range(4)],
        )
        field_a[:, far * LANES : (far + 1) * LANES] = ref[0:64, :]

    lanes64 = lane_ids(NODES)
    lanes = lane_ids(8)
    pieces = ((strip_b2, 0, 16, -16), (strip_b1, 16, 48, 16), (own_strip, 48, 80, 48),
              (strip_a1, 80, 112, 80), (strip_a2, 112, 128, 112))
    strip_source = []
    for side in range(2):
        rows = slice(NODES * side, NODES * side + NODES)
        made = []
        for field in range(4):
            count = NODES if field < 3 else 8
            ids = lanes64 if field < 3 else lanes
            value = jnp.zeros((count, LANES), jnp.float32)
            for ref, start, stop, zero in pieces:
                part = ref[NODES * side : NODES * side + count, :]
                value = jnp.where((ids >= start) & (ids < stop), turned(part, zero - 32 * field), value)
            made.append(value)
        put(ROWS + side, made[0], made[2], made[3][0:1], [made[3][1 + f : 2 + f] for f in range(4)])
        strip_source.append(made[1])

    def columns(row):
        return slice(row * LANES, (row + 1) * LANES)

    low, high = ROWS, ROWS + 1
    sub = lax.broadcasted_iota(jnp.int32, (8, LANES), 0)
    TW, TE, TS, TN = (slice(64 + 8 * f, 72 + 8 * f) for f in range(4))

    def source_of(row):
        if row >= ROWS:
            return strip_source[row - ROWS]
        if 6 <= row < 10:
            return strided(near, 256 + row - 6, NODES)
        if 2 <= row < 6:
            return strided(below1, 256 + row - 2, NODES)
        if 10 <= row < 14:
            return strided(above1, 256 + row - 10, NODES)
        return (below2 if row < 2 else above2)[128:192, :]

    def apply(old, new, step, first):
        start, stop = step, ROWS - step
        for first_row, last_row in ((start, stop), (ROWS, ROWS + 2)):
            for row in range(first_row, last_row, 2):
                cols = slice(row * LANES, (row + 2) * LANES)
                image[:, cols] = product(weight, old[:, cols])

        def finish(row, from_west, from_east, from_south, from_north):
            cols = columns(row)
            west = image[TW, cols] - opened[0:8, cols] * from_west
            east = image[TE, cols] - opened[8:16, cols] * from_east
            south = image[TS, cols] - opened[16:24, cols] * from_south
            north = image[TN, cols] - opened[24:32, cols] * from_north
            for a in range(P_SIZE):
                rows = slice(8 * a, 8 * a + 8)
                value = react[rows, cols] * old[rows, cols] + stiff[:, cols] * image[rows, cols]
                if a == 0:
                    value = value + west
                if a == P_SIZE - 1:
                    value = value + east
                edge = jnp.where(sub == 0, south[a : a + 1, :], 0.0)
                edge = jnp.where(sub == P_SIZE - 1, north[a : a + 1, :], edge)
                value = value + edge
                if first:
                    value = -8.0 * value - shift * old[rows, cols]
                new[rows, cols] = value
            if first:
                new[:, cols] = new[:, cols] + source_of(row)

        north_low = image[TN, columns(low)]
        south_high = image[TS, columns(high)]
        for row in range(start + 1, stop - 1):
            cols = columns(row)
            from_south = jnp.where(
                lanes == 0, turned(north_low, -(8 * row + 7)), turned(image[TN, cols], 1)
            )
            from_north = jnp.where(
                lanes == LANES - 1, turned(south_high, 127 - 8 * row), turned(image[TS, cols], -1)
            )
            finish(row, image[TE, columns(row - 1)], image[TW, columns(row + 1)], from_south, from_north)
        if step == DEPTH - 1:
            return
        to_low = turned(image[TS, columns(low)], -1)
        to_high = turned(image[TN, columns(high)], 1)
        for row in range(start, stop):
            cols = columns(row)
            to_low = jnp.where(lanes == 8 * row + 7, turned(image[TS, cols], 8 * row + 7), to_low)
            to_high = jnp.where(lanes == 8 * row, turned(image[TN, cols], 8 * row + 1), to_high)
        cols = columns(low)
        finish(low, turned(image[TE, cols], 8), turned(image[TW, cols], -8), turned(image[TN, cols], 1), to_low)
        cols = columns(high)
        finish(high, turned(image[TE, cols], 8), turned(image[TW, cols], -8), to_high, turned(image[TS, cols], -1))

    old, new = field_a, field_b
    for step in range(DEPTH):
        apply(old, new, step, step == 0)
        basis_out[step, :, :] = new[:, 6 * LANES : 10 * LANES]
        old, new = new, old

    sums = [jnp.zeros((8, LANES), jnp.float32) for _ in GRAM]
    for x in range(4):
        for a in range(P_SIZE):
            values = [basis_out[k, 8 * a : 8 * a + 8, x * LANES : (x + 1) * LANES] for k in range(ITERS + 1)]
            sums = [total + values[k] * values[l] for total, (k, l) in zip(sums, GRAM)]
    rows = [jnp.sum(total, axis=0, keepdims=True) for total in sums]
    rows = jnp.concatenate(rows + [jnp.zeros((24 - len(GRAM), LANES), jnp.float32)], axis=0)
    totals = jnp.sum(rows, axis=1, keepdims=True)
    place = lax.broadcasted_iota(jnp.int32, (24, LANES), 0) == lax.broadcasted_iota(jnp.int32, (24, LANES), 1)
    totals = jnp.sum(jnp.where(place, totals, 0.0), axis=0, keepdims=True)
    gram_out[...] = jnp.broadcast_to(totals, gram_out.shape)


def combine_kernel(nodes, line_ref, deriv_ref, powers, gathered, basis_out, hess_out, amp_out):
    shift = centre(line_ref, deriv_ref)
    row = jnp.sum(gathered[...], axis=0, keepdims=True) * (1.0 / nodes)
    spread = jnp.broadcast_to(row, (8, LANES))
    gram = {}
    for at, (k, l) in enumerate(GRAM):
        gram[k, l] = gram[l, k] = jnp.broadcast_to(spread[:, at : at + 1], (8, LANES))
    sizes = [jnp.sqrt(gram[k, k]) for k in range(ITERS + 1)]
    sub = lax.broadcasted_iota(jnp.int32, (8, LANES), 0)
    lanes = lane_ids(8)
    hess = jnp.zeros((8, LANES), jnp.float32)
    beta = jnp.sqrt(gram[0, 0] + FLOOR)
    coeffs = [[1.0 / beta]]
    amp = sizes[0] * coeffs[0][0]

    def put(hess, i, j, value):
        return jnp.where((sub == i) & (lanes == j), value, hess)

    for j in range(ITERS):
        last = coeffs[j]
        image = [shift * c for c in last] + [None]
        for k in range(j + 1):
            moved = last[k] * 8.0
            image[k + 1] = moved if image[k + 1] is None else image[k + 1] + moved
        weighted = [
            sum(gram[k, l] * image[l] for l in range(1, j + 2)) + gram[k, 0] * image[0] for k in range(j + 2)
        ]
        pending = list(image)
        for i in range(j + 1):
            h = sum(c * weighted[k] for k, c in enumerate(coeffs[i]))
            hess = put(hess, i, j, h)
            for k, c in enumerate(coeffs[i]):
                pending[k] = pending[k] - h * c
        square = sum(
            pending[k] * sum(gram[k, l] * pending[l] for l in range(j + 2)) for k in range(j + 2)
        )
        beta = jnp.sqrt(jnp.maximum(square, 0.0) + FLOOR)
        hess = put(hess, j + 1, j, beta)
        scale = 1.0 / beta
        coeffs.append([p * scale for p in pending])
        amp = jnp.maximum(amp, sum(jnp.abs(c) * s for c, s in zip(coeffs[-1], sizes)))
    hess_out[...] = hess[0 : ITERS + 1, 0:ITERS]
    amp_out[...] = amp[0:1, :]
    for x in range(4):
        for a in range(P_SIZE):
            values = [powers[k, 8 * a : 8 * a + 8, x * LANES : (x + 1) * LANES] for k in range(ITERS + 1)]
            for j in range(ITERS + 1):
                total = coeffs[j][0] * values[0]
                for k in range(1, j + 1):
                    total = total + coeffs[j][k] * values[k]
                basis_out[j, pl.ds(32 * a + x, 8, stride=4), :] = total


def fast(source, initial, reaction, stiffness, line_op, face_deriv, walls):
    vmem = pl.BlockSpec(memory_space=pltpu.VMEM)
    smem = pl.BlockSpec(memory_space=pltpu.SMEM)
    hbm = pl.BlockSpec(memory_space=pltpu.HBM)
    grant = pltpu.CompilerParams(vmem_limit_bytes=16 * 2**20)
    f32 = jnp.float32
    nx, ny = lax.axis_size(GX), lax.axis_size(GY)
    wide = (ROWS + 2) * LANES

    def moved(value, axis, size, by):
        return lax.ppermute(value, axis, [(i, (i + by) % size) for i in range(size)])

    near, low2, high2, to_up, to_down = pl.pallas_call(
        pack_kernel,
        out_shape=[jax.ShapeDtypeStruct((n, LANES), f32) for n in (792, 264, 264, NODES, NODES)],
        in_specs=[hbm] * 5,
        out_specs=[vmem] * 5,
        scratch_shapes=[pltpu.VMEM((16, LANES), jnp.int32), pltpu.SemaphoreType.DMA((8,))],
        compiler_params=grant,
    )(*[pltpu.with_memory_space_constraint(v, pltpu.HBM) for v in (source, initial, reaction, stiffness, walls)])
    left = moved(to_up, GY, ny, 1)
    right = moved(to_down, GY, ny, -1)
    below1 = moved(near, GX, nx, 1)
    above1 = moved(near, GX, nx, -1)
    below2 = moved(high2, GX, nx, 2)
    above2 = moved(low2, GX, nx, -2)
    own_strip = jnp.concatenate([left, right], axis=0)
    strips = [moved(own_strip, GX, nx, by) for by in (1, -1, 2, -2)]
    weight = pl.pallas_call(
        weights_kernel,
        out_shape=jax.ShapeDtypeStruct((NODES + 32, 6 * NODES), jnp.bfloat16),
        in_specs=[smem, smem, vmem],
        out_specs=vmem,
        compiler_params=grant,
        cost_estimate=pl.CostEstimate(flops=4000000, bytes_accessed=100000, transcendentals=0),
    )(line_op, face_deriv, own_strip)

    powers, gram = pl.pallas_call(
        powers_kernel,
        out_shape=[
            jax.ShapeDtypeStruct((ITERS + 1, NODES, 4 * LANES), f32),
            jax.ShapeDtypeStruct((1, LANES), f32),
        ],
        in_specs=[smem, smem] + [vmem] * 11,
        out_specs=[vmem] * 2,
        scratch_shapes=[pltpu.VMEM((n, wide), f32) for n in (NODES, NODES, NODES + 32, NODES, 8, 32)],
        compiler_params=grant,
    )(line_op, face_deriv, weight, near, below1, above1, below2, above2, own_strip, *strips)
    every = GX + GY
    copies = jnp.broadcast_to(gram, (nx * ny, LANES))
    gathered = lax.all_to_all(copies, every, split_axis=0, concat_axis=0, tiled=True)
    basis, hess, amp = pl.pallas_call(
        functools.partial(combine_kernel, float(NODES * 4 * nx * LANES * ny)),
        out_shape=[
            jax.ShapeDtypeStruct((ITERS + 1, 4 * NODES, LANES), f32),
            jax.ShapeDtypeStruct((ITERS + 1, ITERS), f32),
            jax.ShapeDtypeStruct((1, LANES), f32),
        ],
        in_specs=[smem, smem] + [vmem] * 2,
        out_specs=[vmem] * 3,
        compiler_params=grant,
    )(line_op, face_deriv, powers, gathered)
    return hess, basis, amp[0, 0], near


def body(source, initial, reaction, stiffness, line_op, face_deriv, wall_flags):
    flat = [v.reshape(4 * NODES, LANES) for v in (source, initial, reaction)]
    hess, basis, amp, near = fast(*flat, stiffness, line_op, face_deriv, wall_flags.reshape(16, LANES))

    def again(carry):
        near = lax.optimization_barrier(carry[3])
        initial, source, reaction = near[0:768].reshape(3, NODES, 4, LANES)
        opened = near[772:788].reshape(4, 4, LANES)
        hess, basis = stepwise(source, initial, reaction, near[768:772], line_op, face_deriv, opened)
        return jnp.bool_(True), hess, basis.reshape(ITERS + 1, 4 * NODES, LANES), near

    done = amp <= AMP_LIMIT
    carry = lax.while_loop(lambda carry: jnp.logical_not(carry[0]), again, (done, hess, basis, near))
    return (carry[1], carry[2].reshape(ITERS + 1, NODES, 4, LANES))


def solution(mesh):
    finer = Mesh(mesh.devices.reshape(4, 2, 4, 8), ("gx_0", "gx_1", "gy_0", "gy_1"))
    placed = (
        P(None, GX, GY),
        P(None, GX, GY),
        P(None, GX, GY),
        P(GX, GY),
        P(),
        P(),
        P(None, GX, GY),
    )
    return jax.shard_map(
        body, mesh=finer, in_specs=placed, out_specs=(P(), P(None, None, GX, GY)), check_vma=False
    )
```

```python
import functools

import jax
import jax.numpy as jnp
from jax import lax
from jax.experimental import pallas as pl
from jax.experimental.pallas import tpu as pltpu
from jax.sharding import Mesh
from jax.sharding import PartitionSpec as P

P_SIZE = 8
ITERS = 5
GX = ("gx_0", "gx_1")
GY = ("gy_0", "gy_1")


TAU = 2.0
FLOOR = 0.1


def extended(array, sides, width):
    for axis, dim in sides:
        devices, length = (lax.axis_size(axis), array.shape[dim])
        up = [(i, (i + 1) % devices) for i in range(devices)]
        down = [(j, i) for i, j in up]
        last = lax.slice_in_dim(array, length - width, length, axis=dim)
        leading = lax.slice_in_dim(array, 0, width, axis=dim)
        before = lax.ppermute(last, axis, up)
        after = lax.ppermute(leading, axis, down)
        array = jnp.concatenate([before, array, after], axis=dim)
    return array


def sent_to_all(array, axis):
    copies = jnp.broadcast_to(array, (lax.axis_size(axis), *array.shape))
    return lax.all_to_all(copies, axis, split_axis=0, concat_axis=0, tiled=True)


def over_copies(array, axis):
    everything = sent_to_all(array, axis)
    return jnp.sum(everything, axis=0)


def by_axis(array, axes):
    far, near = axes
    nearer = over_copies(array, near)
    return over_copies(nearer, far)


def together(arrays, axis):
    vector, at, gathered = (jnp.concatenate([a.reshape(-1) for a in arrays]), 0, [])
    subtotal = by_axis(vector, axis)
    for a in arrays:
        gathered.append(subtotal[at : at + a.size].reshape(a.shape))
        at += a.size
    return tuple(gathered)


def local_total(values):
    return jnp.sum(jnp.sum(values, axis=0))


def x_traces(nodes, face_deriv):
    highest = lax.Precision.HIGHEST
    lower = jnp.einsum("c,cbxy->bxy", face_deriv, nodes, precision=highest)
    upper = jnp.einsum("c,cbxy->bxy", face_deriv[::-1], nodes, precision=highest)
    return jnp.stack([nodes[0], lower, nodes[-1], upper])


def y_traces(nodes, face_deriv):
    highest = lax.Precision.HIGHEST
    lower = jnp.einsum("c,acxy->axy", face_deriv, nodes, precision=highest)
    upper = jnp.einsum("c,acxy->axy", face_deriv[::-1], nodes, precision=highest)
    return jnp.stack([nodes[:, 0], lower, nodes[:, -1], upper])


def apply_op(field, reaction, stiffness, line_op, face_deriv, opened):
    highest = lax.Precision.HIGHEST
    nodes = field.reshape(P_SIZE, P_SIZE, field.shape[1], field.shape[2])
    interior = stiffness * (
        jnp.einsum("ac,cbxy->abxy", line_op, nodes, precision=highest)
        + jnp.einsum("bc,acxy->abxy", line_op, nodes, precision=highest)
    )
    xside = extended(x_traces(nodes, face_deriv), ((GX, 2),), 1)
    yside = extended(y_traces(nodes, face_deriv), ((GY, 3),), 1)
    x_own = xside[:, :, 1:-1]
    y_own = yside[:, :, :, 1:-1]
    east_nb = xside[0:2, :, 2:]
    west_nb = xside[2:4, :, :-2]
    north_nb = yside[0:2, :, :, 2:]
    south_nb = yside[2:4, :, :, :-2]
    add_east = TAU * (x_own[2] - opened[1] * east_nb[0]) + 0.5 * (x_own[3] - opened[1] * east_nb[1])
    add_west = TAU * (x_own[0] - opened[0] * west_nb[0]) + 0.5 * (x_own[1] - opened[0] * west_nb[1])
    add_north = TAU * (y_own[2] - opened[3] * north_nb[0]) + 0.5 * (
        y_own[3] - opened[3] * north_nb[1]
    )
    add_south = TAU * (y_own[0] - opened[2] * south_nb[0]) + 0.5 * (
        y_own[1] - opened[2] * south_nb[1]
    )
    result = reaction.reshape(nodes.shape) * nodes + interior
    result = result.at[0].add(add_west).at[P_SIZE - 1].add(add_east)
    result = result.at[:, 0].add(add_south).at[:, P_SIZE - 1].add(add_north)
    return result.reshape(field.shape)


def norm_scale(vector, total):
    squares = by_axis(local_total(vector * vector), (("gx_0", "gx_1"), ("gy_0", "gy_1")))
    return jnp.sqrt(squares / total + FLOOR)


def stepwise(source, initial, reaction, stiffness, line_op, face_deriv, opened):
    highest = lax.Precision.HIGHEST
    total = float(
        P_SIZE * P_SIZE * source.shape[1] * lax.axis_size(GX) * source.shape[2] * lax.axis_size(GY)
    )

    def operate(field):
        return apply_op(field, reaction, stiffness, line_op, face_deriv, opened)

    def products(basis, image):
        per_cell = jnp.einsum("kqxy,qxy->kxy", basis, image, precision=highest)
        return jnp.sum(per_cell, axis=(1, 2))

    first = source - operate(initial)
    basis = jnp.zeros((ITERS + 1,) + source.shape, jnp.float32)
    hessen = jnp.zeros((ITERS + 1, ITERS), jnp.float32)
    rows = lax.broadcasted_iota(jnp.int32, (ITERS + 1, ITERS), 0)
    cols = lax.broadcasted_iota(jnp.int32, (ITERS + 1, ITERS), 1)
    slots = lax.broadcasted_iota(jnp.int32, (ITERS + 1,), 0)

    def advance(step, carry):
        basis, hessen, pending = carry
        image = operate(pending)
        local = products(basis, image)
        projected, crossed, squares = together(
            (local, local_total(pending * image), local_total(pending * pending)),
            (("gx_0", "gx_1"), ("gy_0", "gy_1")),
        )
        beta = jnp.sqrt(squares / total + FLOOR)
        basis = lax.dynamic_update_index_in_dim(basis, pending / beta, step, 0)
        coeffs = projected / (total * beta) + jnp.where(
            slots == step, crossed / (total * beta * beta), 0.0
        )
        pending = image / beta - jnp.einsum("k,kqxy->qxy", coeffs, basis, precision=highest)
        hessen = hessen + jnp.where(cols == step, coeffs[:, None], 0.0)
        hessen = hessen + jnp.where((rows == step) & (cols == step - 1), beta, 0.0)
        return (basis, hessen, pending)

    basis, hessen, pending = lax.fori_loop(0, ITERS, advance, (basis, hessen, first))
    beta = norm_scale(pending, total)
    basis = basis.at[ITERS].set(pending / beta)
    hessen = hessen + jnp.where((rows == ITERS) & (cols == ITERS - 1), beta, 0.0)
    return (hessen, basis)


NODES = P_SIZE * P_SIZE
ROWS = 16
DEPTH = 6
LANES = 128
SCALE = 0.125
AMP_LIMIT = 100.0
GRAM = [(k, l) for k in range(ITERS + 1) for l in range(k + 1)]


def centre(line_ref, deriv_ref):
    trace = line_ref[0, 0]
    for a in range(1, P_SIZE):
        trace = trace + line_ref[a, a]
    return 2.0 + 0.3125 * trace + 0.5 * (TAU + 0.5 * deriv_ref[0])


def lane_ids(rows):
    return lax.broadcasted_iota(jnp.int32, (rows, LANES), 1)


def turned(value, shift):
    shift = shift % LANES
    return value if shift == 0 else pltpu.roll(value, shift, 1)


def strided(ref, start, count):
    return ref[pl.ds(start, count, stride=4), :]


def pack_kernel(source, initial, reaction, stiffness, walls, near, to_up, to_down, flags, sems):
    moves = []
    for at, ref in ((0, initial), (256, source), (512, reaction)):
        for half in (0, 128):
            moves.append((ref.at[pl.ds(half, 128), :], near.at[pl.ds(at + half, 128), :]))
    moves.append((stiffness, near.at[pl.ds(768, 4), :]))
    moves.append((walls, flags))
    copies = [pltpu.make_async_copy(a, b, sems.at[n]) for n, (a, b) in enumerate(moves)]
    for copy in copies:
        copy.start()
    for copy in copies:
        copy.wait()
    opened = 1.0 - flags[...].astype(jnp.float32)
    near[772:788, :] = opened
    near[788:792, :] = jnp.zeros((4, LANES), jnp.float32)
    thick = near[768:772, :]
    lanes = lane_ids(NODES)
    lanes8 = lane_ids(8)
    for out, first in ((to_up, 120), (to_down, 0)):
        total = jnp.zeros((NODES, LANES), jnp.float32)
        extra = jnp.zeros((8, LANES), jnp.float32)
        for x in range(4):
            for field in range(3):
                at = 32 * field + 8 * x
                moved = turned(strided(near, 256 * field + x, NODES), at - first)
                total = jnp.where((lanes >= at) & (lanes < at + 8), moved, total)
            at = 96 + 8 * x
            rows = [thick[x : x + 1, :]] + [opened[4 * f + x : 4 * f + x + 1, :] for f in range(4)]
            rows = jnp.concatenate(rows + [jnp.zeros((3, LANES), jnp.float32)], axis=0)
            extra = jnp.where((lanes8 >= at) & (lanes8 < at + 8), turned(rows, at - first), extra)
        out[...] = total
        out[0:8, :] = total[0:8] + extra


def far_kernel(near, left, right, strip, high2, low2):
    strip[0:64, :] = left[...]
    strip[64:128, :] = right[...]
    lanes = lane_ids(NODES)
    corner = jnp.where(lanes < 32, left[...], turned(right[...], 32))
    for out, far, close in ((high2, 2, 3), (low2, 1, 0)):
        out[0:64, :] = strided(near, far, NODES)
        out[64:128, :] = strided(near, close, NODES)
        out[128:192, :] = strided(near, 256 + close, NODES)
        out[192:256, :] = strided(near, 512 + close, NODES)
        out[256:320, :] = corner
        out[320:321, :] = near[768 + close : 769 + close, :]
        for f in range(4):
            out[321 + f : 322 + f, :] = near[772 + 4 * f + close : 773 + 4 * f + close, :]
        out[325:328, :] = jnp.zeros((3, LANES), jnp.float32)


def split(value):
    high = value.astype(jnp.bfloat16)
    rest = value - high.astype(jnp.float32)
    middle = rest.astype(jnp.bfloat16)
    low = (rest - middle.astype(jnp.float32)).astype(jnp.bfloat16)
    return high, middle, low


def weights_in(line, deriv_ref):
    sub = lax.broadcasted_iota(jnp.int32, (8, NODES), 0)
    lane = lax.broadcasted_iota(jnp.int32, (8, NODES), 1)
    along, across = lane // 8, lane % 8
    outer = jnp.zeros((8, NODES), jnp.float32)
    inner = jnp.zeros((8, NODES), jnp.float32)
    for c in range(P_SIZE):
        column = jnp.broadcast_to(line[:, c : c + 1], (8, NODES))
        outer = jnp.where(along == c, column, outer)
        inner = jnp.where(across == c, column, inner)
    parts = []
    for a in range(P_SIZE):
        row = jnp.broadcast_to(outer[a : a + 1, :], (8, NODES))
        parts.append(jnp.where(across == sub, row, 0.0) + jnp.where(along == a, inner, 0.0))
    for first, second in ((along, across), (across, along)):
        for flip in (False, True):
            part = jnp.zeros((8, NODES), jnp.float32)
            for c in range(P_SIZE):
                value = SCALE * (0.5 * deriv_ref[c] + (TAU if c == 0 else 0.0))
                part = jnp.where(first == (P_SIZE - 1 - c if flip else c), value, part)
            parts.append(jnp.where(second == sub, part, 0.0))
    high, middle, low = split(jnp.concatenate(parts, axis=0))
    return jnp.concatenate([high, high, high, middle, middle, low], axis=1)


def product(weight, value):
    high, middle, low = split(value)
    stacked = jnp.concatenate([high, middle, low, high, middle, high], axis=0)
    return jnp.dot(weight[...], stacked, preferred_element_type=jnp.float32)


def powers_kernel(
    line_ref, deriv_ref, line, near, below1, above1, below2, above2, own_strip, strip_b1, strip_a1,
    basis_out, gram_out, field_a, field_b, image, react, stiff, opened, weight,
):
    shift = centre(line_ref, deriv_ref)
    weight[...] = weights_in(line, deriv_ref)

    def put(row, value_initial, value_reaction, value_stiffness, value_open):
        cols = slice(row * LANES, (row + 1) * LANES)
        field_a[:, cols] = value_initial
        react[:, cols] = (value_reaction - shift) * SCALE
        stiff[:, cols] = jnp.broadcast_to(value_stiffness * SCALE, (8, LANES))
        for f in range(4):
            opened[8 * f : 8 * f + 8, cols] = jnp.broadcast_to(value_open[f], (8, LANES))

    for x in range(4):
        for ref, row in ((near, 6 + x), (below1, 2 + x), (above1, 10 + x)):
            put(
                row, strided(ref, x, NODES), strided(ref, 512 + x, NODES), ref[768 + x : 769 + x, :],
                [ref[772 + 4 * f + x : 773 + 4 * f + x, :] for f in range(4)],
            )
    for ref, far, close in ((below2, 0, 1), (above2, 15, 14)):
        put(
            close, ref[64:128, :], ref[192:256, :], ref[320:321, :],
            [ref[321 + f : 322 + f, :] for f in range(4)],
        )
        field_a[:, far * LANES : (far + 1) * LANES] = ref[0:64, :]

    lanes64 = lane_ids(NODES)
    lanes = lane_ids(8)
    pieces = ((strip_b1, 16, 48, 16), (own_strip, 48, 80, 48), (strip_a1, 80, 112, 80))
    strip_source = []
    for side in range(2):
        made = []
        for field in range(4):
            count = NODES if field < 3 else 8
            ids = lanes64 if field < 3 else lanes
            value = jnp.zeros((count, LANES), jnp.float32)
            for ref, start, stop, zero in pieces:
                part = ref[NODES * side : NODES * side + count, :]
                value = jnp.where((ids >= start) & (ids < stop), turned(part, zero - 32 * field), value)
            if field == 0:
                value = jnp.where(ids < 16, turned(below2[256:320, :], -16 - 32 * side), value)
                value = jnp.where(ids >= 112, turned(above2[256:320, :], 112 - 32 * side), value)
            made.append(value)
        put(ROWS + side, made[0], made[2], made[3][0:1], [made[3][1 + f : 2 + f] for f in range(4)])
        strip_source.append(made[1])

    def columns(row):
        return slice(row * LANES, (row + 1) * LANES)

    low, high = ROWS, ROWS + 1
    sub = lax.broadcasted_iota(jnp.int32, (8, LANES), 0)
    TW, TE, TS, TN = (slice(64 + 8 * f, 72 + 8 * f) for f in range(4))

    def source_of(row):
        if row >= ROWS:
            return strip_source[row - ROWS]
        if 6 <= row < 10:
            return strided(near, 256 + row - 6, NODES)
        if 2 <= row < 6:
            return strided(below1, 256 + row - 2, NODES)
        if 10 <= row < 14:
            return strided(above1, 256 + row - 10, NODES)
        return (below2 if row < 2 else above2)[128:192, :]

    def apply(old, new, step, first):
        start, stop = step, ROWS - step
        for first_row, last_row in ((start, stop), (ROWS, ROWS + 2)):
            for row in range(first_row, last_row, 2):
                cols = slice(row * LANES, (row + 2) * LANES)
                image[:, cols] = product(weight, old[:, cols])

        def finish(row, from_west, from_east, from_south, from_north):
            cols = columns(row)
            west = image[TW, cols] - opened[0:8, cols] * from_west
            east = image[TE, cols] - opened[8:16, cols] * from_east
            south = image[TS, cols] - opened[16:24, cols] * from_south
            north = image[TN, cols] - opened[24:32, cols] * from_north
            for a in range(P_SIZE):
                rows = slice(8 * a, 8 * a + 8)
                value = react[rows, cols] * old[rows, cols] + stiff[:, cols] * image[rows, cols]
                if a == 0:
                    value = value + west
                if a == P_SIZE - 1:
                    value = value + east
                edge = jnp.where(sub == 0, south[a : a + 1, :], 0.0)
                edge = jnp.where(sub == P_SIZE - 1, north[a : a + 1, :], edge)
                value = value + edge
                if first:
                    value = -8.0 * value - shift * old[rows, cols]
                new[rows, cols] = value
            if first:
                new[:, cols] = new[:, cols] + source_of(row)

        north_low = image[TN, columns(low)]
        south_high = image[TS, columns(high)]
        for row in range(start + 1, stop - 1):
            cols = columns(row)
            from_south = jnp.where(
                lanes == 0, turned(north_low, -(8 * row + 7)), turned(image[TN, cols], 1)
            )
            from_north = jnp.where(
                lanes == LANES - 1, turned(south_high, 127 - 8 * row), turned(image[TS, cols], -1)
            )
            finish(row, image[TE, columns(row - 1)], image[TW, columns(row + 1)], from_south, from_north)
        if step == DEPTH - 1:
            return
        to_low = turned(image[TS, columns(low)], -1)
        to_high = turned(image[TN, columns(high)], 1)
        for row in range(start, stop):
            cols = columns(row)
            to_low = jnp.where(lanes == 8 * row + 7, turned(image[TS, cols], 8 * row + 7), to_low)
            to_high = jnp.where(lanes == 8 * row, turned(image[TN, cols], 8 * row + 1), to_high)
        cols = columns(low)
        finish(low, turned(image[TE, cols], 8), turned(image[TW, cols], -8), turned(image[TN, cols], 1), to_low)
        cols = columns(high)
        finish(high, turned(image[TE, cols], 8), turned(image[TW, cols], -8), to_high, turned(image[TS, cols], -1))

    old, new = field_a, field_b
    for step in range(DEPTH):
        apply(old, new, step, step == 0)
        basis_out[step, :, :] = new[:, 6 * LANES : 10 * LANES]
        old, new = new, old

    sums = [jnp.zeros((8, LANES), jnp.float32) for _ in GRAM]
    for x in range(4):
        for a in range(P_SIZE):
            values = [basis_out[k, 8 * a : 8 * a + 8, x * LANES : (x + 1) * LANES] for k in range(ITERS + 1)]
            sums = [total + values[k] * values[l] for total, (k, l) in zip(sums, GRAM)]
    rows = [jnp.sum(total, axis=0, keepdims=True) for total in sums]
    rows = jnp.concatenate(rows + [jnp.zeros((24 - len(GRAM), LANES), jnp.float32)], axis=0)
    totals = jnp.sum(rows, axis=1, keepdims=True)
    place = lax.broadcasted_iota(jnp.int32, (24, LANES), 0) == lax.broadcasted_iota(jnp.int32, (24, LANES), 1)
    totals = jnp.sum(jnp.where(place, totals, 0.0), axis=0, keepdims=True)
    gram_out[...] = jnp.broadcast_to(totals, gram_out.shape)


def combine_kernel(nodes, line_ref, deriv_ref, powers, gathered, basis_out, hess_out, amp_out):
    shift = centre(line_ref, deriv_ref)
    row = jnp.sum(gathered[...], axis=0, keepdims=True) * (1.0 / nodes)
    spread = jnp.broadcast_to(row, (8, LANES))
    gram = {}
    for at, (k, l) in enumerate(GRAM):
        gram[k, l] = gram[l, k] = jnp.broadcast_to(spread[:, at : at + 1], (8, LANES))
    sizes = [jnp.sqrt(gram[k, k]) for k in range(ITERS + 1)]
    sub = lax.broadcasted_iota(jnp.int32, (8, LANES), 0)
    lanes = lane_ids(8)
    hess = jnp.zeros((8, LANES), jnp.float32)
    beta = jnp.sqrt(gram[0, 0] + FLOOR)
    coeffs = [[1.0 / beta]]
    amp = sizes[0] * coeffs[0][0]

    def put(hess, i, j, value):
        return jnp.where((sub == i) & (lanes == j), value, hess)

    for j in range(ITERS):
        last = coeffs[j]
        image = [shift * c for c in last] + [None]
        for k in range(j + 1):
            moved = last[k] * 8.0
            image[k + 1] = moved if image[k + 1] is None else image[k + 1] + moved
        weighted = [
            sum(gram[k, l] * image[l] for l in range(1, j + 2)) + gram[k, 0] * image[0] for k in range(j + 2)
        ]
        pending = list(image)
        for i in range(j + 1):
            h = sum(c * weighted[k] for k, c in enumerate(coeffs[i]))
            hess = put(hess, i, j, h)
            for k, c in enumerate(coeffs[i]):
                pending[k] = pending[k] - h * c
        square = sum(
            pending[k] * sum(gram[k, l] * pending[l] for l in range(j + 2)) for k in range(j + 2)
        )
        beta = jnp.sqrt(jnp.maximum(square, 0.0) + FLOOR)
        hess = put(hess, j + 1, j, beta)
        scale = 1.0 / beta
        coeffs.append([p * scale for p in pending])
        amp = jnp.maximum(amp, sum(jnp.abs(c) * s for c, s in zip(coeffs[-1], sizes)))
    hess_out[...] = hess[0 : ITERS + 1, 0:ITERS]
    amp_out[...] = amp[0:1, :]
    for x in range(4):
        for a in range(P_SIZE):
            values = [powers[k, 8 * a : 8 * a + 8, x * LANES : (x + 1) * LANES] for k in range(ITERS + 1)]
            for j in range(ITERS + 1):
                total = coeffs[j][0] * values[0]
                for k in range(1, j + 1):
                    total = total + coeffs[j][k] * values[k]
                basis_out[j, pl.ds(32 * a + x, 8, stride=4), :] = total


def fast(source, initial, reaction, stiffness, line_op, face_deriv, walls):
    vmem = pl.BlockSpec(memory_space=pltpu.VMEM)
    smem = pl.BlockSpec(memory_space=pltpu.SMEM)
    hbm = pl.BlockSpec(memory_space=pltpu.HBM)
    grant = pltpu.CompilerParams(vmem_limit_bytes=16 * 2**20)
    f32 = jnp.float32
    nx, ny = lax.axis_size(GX), lax.axis_size(GY)
    wide = (ROWS + 2) * LANES

    def moved(value, axis, size, by):
        return lax.ppermute(value, axis, [(i, (i + by) % size) for i in range(size)])

    near, to_up, to_down = pl.pallas_call(
        pack_kernel,
        out_shape=[jax.ShapeDtypeStruct((n, LANES), f32) for n in (792, NODES, NODES)],
        in_specs=[hbm] * 5,
        out_specs=[vmem] * 3,
        scratch_shapes=[pltpu.VMEM((16, LANES), jnp.int32), pltpu.SemaphoreType.DMA((8,))],
        compiler_params=grant,
    )(*[pltpu.with_memory_space_constraint(v, pltpu.HBM) for v in (source, initial, reaction, stiffness, walls)])
    left = moved(to_up, GY, ny, 1)
    right = moved(to_down, GY, ny, -1)
    below1 = moved(near, GX, nx, 1)
    above1 = moved(near, GX, nx, -1)
    strip, high2, low2 = pl.pallas_call(
        far_kernel,
        out_shape=[jax.ShapeDtypeStruct((n, LANES), f32) for n in (2 * NODES, 328, 328)],
        in_specs=[vmem] * 3,
        out_specs=[vmem] * 3,
        compiler_params=grant,
    )(near, left, right)
    below2 = moved(high2, GX, nx, 2)
    above2 = moved(low2, GX, nx, -2)
    strips = [moved(strip, GX, nx, by) for by in (1, -1)]

    powers, gram = pl.pallas_call(
        powers_kernel,
        out_shape=[
            jax.ShapeDtypeStruct((ITERS + 1, NODES, 4 * LANES), f32),
            jax.ShapeDtypeStruct((1, LANES), f32),
        ],
        in_specs=[smem, smem] + [vmem] * 9,
        out_specs=[vmem] * 2,
        scratch_shapes=[pltpu.VMEM((n, wide), f32) for n in (NODES, NODES, NODES + 32, NODES, 8, 32)]
        + [pltpu.VMEM((NODES + 32, 6 * NODES), jnp.bfloat16)],
        compiler_params=grant,
    )(line_op, face_deriv, line_op, near, below1, above1, below2, above2, strip, *strips)
    every = GX + GY
    copies = jnp.broadcast_to(gram, (nx * ny, LANES))
    gathered = lax.all_to_all(copies, every, split_axis=0, concat_axis=0, tiled=True)
    basis, hess, amp = pl.pallas_call(
        functools.partial(combine_kernel, float(NODES * 4 * nx * LANES * ny)),
        out_shape=[
            jax.ShapeDtypeStruct((ITERS + 1, 4 * NODES, LANES), f32),
            jax.ShapeDtypeStruct((ITERS + 1, ITERS), f32),
            jax.ShapeDtypeStruct((1, LANES), f32),
        ],
        in_specs=[smem, smem] + [vmem] * 2,
        out_specs=[vmem] * 3,
        compiler_params=grant,
    )(line_op, face_deriv, powers, gathered)
    return hess, basis, amp[0, 0], near


def body(source, initial, reaction, stiffness, line_op, face_deriv, wall_flags):
    flat = [v.reshape(4 * NODES, LANES) for v in (source, initial, reaction)]
    hess, basis, amp, near = fast(*flat, stiffness, line_op, face_deriv, wall_flags.reshape(16, LANES))

    def again(carry):
        near = lax.optimization_barrier(carry[3])
        initial, source, reaction = near[0:768].reshape(3, NODES, 4, LANES)
        opened = near[772:788].reshape(4, 4, LANES)
        hess, basis = stepwise(source, initial, reaction, near[768:772], line_op, face_deriv, opened)
        return jnp.bool_(True), hess, basis.reshape(ITERS + 1, 4 * NODES, LANES), near

    done = amp <= AMP_LIMIT
    carry = lax.while_loop(lambda carry: jnp.logical_not(carry[0]), again, (done, hess, basis, near))
    return (carry[1], carry[2].reshape(ITERS + 1, NODES, 4, LANES))


def solution(mesh):
    finer = Mesh(mesh.devices.reshape(4, 2, 4, 8), ("gx_0", "gx_1", "gy_0", "gy_1"))
    placed = (
        P(None, GX, GY),
        P(None, GX, GY),
        P(None, GX, GY),
        P(GX, GY),
        P(),
        P(),
        P(None, GX, GY),
    )
    return jax.shard_map(
        body, mesh=finer, in_specs=placed, out_specs=(P(), P(None, None, GX, GY)), check_vma=False
    )
```

```python
import functools

import jax
import jax.numpy as jnp
from jax import lax
from jax.experimental import pallas as pl
from jax.experimental.pallas import tpu as pltpu
from jax.sharding import Mesh
from jax.sharding import PartitionSpec as P

P_SIZE = 8
ITERS = 5
GX = ("gx_0", "gx_1")
GY = ("gy_0", "gy_1")


TAU = 2.0
FLOOR = 0.1


def extended(array, sides, width):
    for axis, dim in sides:
        devices, length = (lax.axis_size(axis), array.shape[dim])
        up = [(i, (i + 1) % devices) for i in range(devices)]
        down = [(j, i) for i, j in up]
        last = lax.slice_in_dim(array, length - width, length, axis=dim)
        leading = lax.slice_in_dim(array, 0, width, axis=dim)
        before = lax.ppermute(last, axis, up)
        after = lax.ppermute(leading, axis, down)
        array = jnp.concatenate([before, array, after], axis=dim)
    return array


def sent_to_all(array, axis):
    copies = jnp.broadcast_to(array, (lax.axis_size(axis), *array.shape))
    return lax.all_to_all(copies, axis, split_axis=0, concat_axis=0, tiled=True)


def over_copies(array, axis):
    everything = sent_to_all(array, axis)
    return jnp.sum(everything, axis=0)


def by_axis(array, axes):
    far, near = axes
    nearer = over_copies(array, near)
    return over_copies(nearer, far)


def together(arrays, axis):
    vector, at, gathered = (jnp.concatenate([a.reshape(-1) for a in arrays]), 0, [])
    subtotal = by_axis(vector, axis)
    for a in arrays:
        gathered.append(subtotal[at : at + a.size].reshape(a.shape))
        at += a.size
    return tuple(gathered)


def local_total(values):
    return jnp.sum(jnp.sum(values, axis=0))


def x_traces(nodes, face_deriv):
    highest = lax.Precision.HIGHEST
    lower = jnp.einsum("c,cbxy->bxy", face_deriv, nodes, precision=highest)
    upper = jnp.einsum("c,cbxy->bxy", face_deriv[::-1], nodes, precision=highest)
    return jnp.stack([nodes[0], lower, nodes[-1], upper])


def y_traces(nodes, face_deriv):
    highest = lax.Precision.HIGHEST
    lower = jnp.einsum("c,acxy->axy", face_deriv, nodes, precision=highest)
    upper = jnp.einsum("c,acxy->axy", face_deriv[::-1], nodes, precision=highest)
    return jnp.stack([nodes[:, 0], lower, nodes[:, -1], upper])


def apply_op(field, reaction, stiffness, line_op, face_deriv, opened):
    highest = lax.Precision.HIGHEST
    nodes = field.reshape(P_SIZE, P_SIZE, field.shape[1], field.shape[2])
    interior = stiffness * (
        jnp.einsum("ac,cbxy->abxy", line_op, nodes, precision=highest)
        + jnp.einsum("bc,acxy->abxy", line_op, nodes, precision=highest)
    )
    xside = extended(x_traces(nodes, face_deriv), ((GX, 2),), 1)
    yside = extended(y_traces(nodes, face_deriv), ((GY, 3),), 1)
    x_own = xside[:, :, 1:-1]
    y_own = yside[:, :, :, 1:-1]
    east_nb = xside[0:2, :, 2:]
    west_nb = xside[2:4, :, :-2]
    north_nb = yside[0:2, :, :, 2:]
    south_nb = yside[2:4, :, :, :-2]
    add_east = TAU * (x_own[2] - opened[1] * east_nb[0]) + 0.5 * (x_own[3] - opened[1] * east_nb[1])
    add_west = TAU * (x_own[0] - opened[0] * west_nb[0]) + 0.5 * (x_own[1] - opened[0] * west_nb[1])
    add_north = TAU * (y_own[2] - opened[3] * north_nb[0]) + 0.5 * (
        y_own[3] - opened[3] * north_nb[1]
    )
    add_south = TAU * (y_own[0] - opened[2] * south_nb[0]) + 0.5 * (
        y_own[1] - opened[2] * south_nb[1]
    )
    result = reaction.reshape(nodes.shape) * nodes + interior
    result = result.at[0].add(add_west).at[P_SIZE - 1].add(add_east)
    result = result.at[:, 0].add(add_south).at[:, P_SIZE - 1].add(add_north)
    return result.reshape(field.shape)


def norm_scale(vector, total):
    squares = by_axis(local_total(vector * vector), (("gx_0", "gx_1"), ("gy_0", "gy_1")))
    return jnp.sqrt(squares / total + FLOOR)


def stepwise(source, initial, reaction, stiffness, line_op, face_deriv, opened):
    highest = lax.Precision.HIGHEST
    total = float(
        P_SIZE * P_SIZE * source.shape[1] * lax.axis_size(GX) * source.shape[2] * lax.axis_size(GY)
    )

    def operate(field):
        return apply_op(field, reaction, stiffness, line_op, face_deriv, opened)

    def products(basis, image):
        per_cell = jnp.einsum("kqxy,qxy->kxy", basis, image, precision=highest)
        return jnp.sum(per_cell, axis=(1, 2))

    first = source - operate(initial)
    basis = jnp.zeros((ITERS + 1,) + source.shape, jnp.float32)
    hessen = jnp.zeros((ITERS + 1, ITERS), jnp.float32)
    rows = lax.broadcasted_iota(jnp.int32, (ITERS + 1, ITERS), 0)
    cols = lax.broadcasted_iota(jnp.int32, (ITERS + 1, ITERS), 1)
    slots = lax.broadcasted_iota(jnp.int32, (ITERS + 1,), 0)

    def advance(step, carry):
        basis, hessen, pending = carry
        image = operate(pending)
        local = products(basis, image)
        projected, crossed, squares = together(
            (local, local_total(pending * image), local_total(pending * pending)),
            (("gx_0", "gx_1"), ("gy_0", "gy_1")),
        )
        beta = jnp.sqrt(squares / total + FLOOR)
        basis = lax.dynamic_update_index_in_dim(basis, pending / beta, step, 0)
        coeffs = projected / (total * beta) + jnp.where(
            slots == step, crossed / (total * beta * beta), 0.0
        )
        pending = image / beta - jnp.einsum("k,kqxy->qxy", coeffs, basis, precision=highest)
        hessen = hessen + jnp.where(cols == step, coeffs[:, None], 0.0)
        hessen = hessen + jnp.where((rows == step) & (cols == step - 1), beta, 0.0)
        return (basis, hessen, pending)

    basis, hessen, pending = lax.fori_loop(0, ITERS, advance, (basis, hessen, first))
    beta = norm_scale(pending, total)
    basis = basis.at[ITERS].set(pending / beta)
    hessen = hessen + jnp.where((rows == ITERS) & (cols == ITERS - 1), beta, 0.0)
    return (hessen, basis)


NODES = P_SIZE * P_SIZE
ROWS = 16
DEPTH = 6
LANES = 128
SCALE = 0.125
AMP_LIMIT = 100.0
GRAM = [(k, l) for k in range(ITERS + 1) for l in range(k + 1)]


def lane_ids(rows):
    return lax.broadcasted_iota(jnp.int32, (rows, LANES), 1)


def turned(value, shift):
    shift = shift % LANES
    return value if shift == 0 else pltpu.roll(value, shift, 1)


def strided(ref, start, count):
    return ref[pl.ds(start, count, stride=4), :]


BLOCK = 168
Q, REACT, FACES, THICK, OPEN = 0, 64, 128, 160, 161


def split(value):
    high = value.astype(jnp.bfloat16)
    rest = value - high.astype(jnp.float32)
    middle = rest.astype(jnp.bfloat16)
    low = (rest - middle.astype(jnp.float32)).astype(jnp.bfloat16)
    return high, middle, low


def weights_in(line, deriv):
    sub = lax.broadcasted_iota(jnp.int32, (8, NODES), 0)
    lane = lax.broadcasted_iota(jnp.int32, (8, NODES), 1)
    along, across = lane // 8, lane % 8
    outer = jnp.zeros((8, NODES), jnp.float32)
    inner = jnp.zeros((8, NODES), jnp.float32)
    for c in range(P_SIZE):
        column = jnp.broadcast_to(line[:, c : c + 1], (8, NODES))
        outer = jnp.where(along == c, column, outer)
        inner = jnp.where(across == c, column, inner)
    parts = []
    for a in range(P_SIZE):
        row = jnp.broadcast_to(outer[a : a + 1, :], (8, NODES))
        parts.append(jnp.where(across == sub, row, 0.0) + jnp.where(along == a, inner, 0.0))
    for first, second in ((along, across), (across, along)):
        for flip in (False, True):
            part = jnp.zeros((8, NODES), jnp.float32)
            for c in range(P_SIZE):
                value = SCALE * (0.5 * deriv[0:1, c : c + 1] + (TAU if c == 0 else 0.0))
                part = jnp.where(first == (P_SIZE - 1 - c if flip else c), value, part)
            parts.append(jnp.where(second == sub, part, 0.0))
    high, middle, low = split(jnp.concatenate(parts, axis=0))
    return jnp.concatenate([high, high, high, middle, middle, low], axis=1)


def product(weight, value):
    high, middle, low = split(value)
    stacked = jnp.concatenate([high, middle, low, high, middle, high], axis=0)
    return jnp.dot(weight[...], stacked, preferred_element_type=jnp.float32)


def centre(line, deriv):
    diagonal = lax.broadcasted_iota(jnp.int32, (8, 8), 0) == lax.broadcasted_iota(jnp.int32, (8, 8), 1)
    trace = jnp.sum(jnp.where(diagonal, line, 0.0), axis=1, keepdims=True)
    trace = jnp.sum(trace, axis=0, keepdims=True)
    return 2.0 + 0.3125 * trace + 0.5 * (TAU + 0.5 * deriv[0:1, 0:1])


def edges(a, west, east, south, north, sub):
    value = jnp.where(sub == 0, south[a : a + 1, :], 0.0)
    value = jnp.where(sub == P_SIZE - 1, north[a : a + 1, :], value)
    if a == 0:
        value = value + west
    if a == P_SIZE - 1:
        value = value + east
    return value


def pack_kernel(
    line_in, deriv_in, source, initial, reaction, stiffness, walls,
    raw, near, to_up, to_down, weight, shift_out, line, deriv, flags, sems,
):
    moves = [(line_in, line), (deriv_in, deriv)]
    for at, ref in ((0, initial), (256, source), (512, reaction)):
        for half in (0, 128):
            moves.append((ref.at[pl.ds(half, 128), :], raw.at[pl.ds(at + half, 128), :]))
    moves.append((stiffness, raw.at[pl.ds(768, 4), :]))
    moves.append((walls, flags))
    copies = [pltpu.make_async_copy(a, b, sems.at[n]) for n, (a, b) in enumerate(moves)]
    for copy in copies:
        copy.start()
    for copy in copies[:2]:
        copy.wait()
    line, deriv = line[...], deriv[...]
    weight[...] = weights_in(line, deriv)
    shift_out[...] = jnp.broadcast_to(centre(line, deriv), (8, LANES))
    for copy in copies[2:]:
        copy.wait()
    opened = 1.0 - flags[...].astype(jnp.float32)
    raw[772:788, :] = opened
    raw[788:796, 0:P_SIZE] = line
    raw[796:797, 0:P_SIZE] = deriv
    thick = raw[768:772, :]
    sub = lax.broadcasted_iota(jnp.int32, (8, LANES), 0)
    for x in range(0, 4, 2):
        pair = jnp.concatenate([strided(raw, x, NODES), strided(raw, x + 1, NODES)], axis=1)
        image = product(weight, pair)
        for k in range(2):
            at = BLOCK * (x + k)
            cols = slice(k * LANES, (k + 1) * LANES)
            traces = image[NODES:, cols]
            near[at + FACES : at + THICK, :] = traces
            faces = [8.0 * traces[8 * f : 8 * f + 8] for f in range(4)]
            width = jnp.broadcast_to(thick[x + k : x + k + 1, :], (8, LANES))
            for a in range(P_SIZE):
                rows = slice(8 * a, 8 * a + 8)
                value = strided(raw, 512 + 32 * a + x + k, 8) * pair[rows, cols] + width * image[rows, cols]
                value = value + edges(a, *faces, sub)
                near[at + 8 * a : at + 8 * a + 8, :] = strided(raw, 256 + 32 * a + x + k, 8) - value
            near[at + REACT : at + FACES, :] = strided(raw, 512 + x + k, NODES)
            rows = [thick[x + k : x + k + 1, :]]
            rows += [opened[4 * f + x + k : 4 * f + x + k + 1, :] for f in range(4)]
            near[at + THICK : at + BLOCK, :] = jnp.concatenate(
                rows + [jnp.zeros((3, LANES), jnp.float32)], axis=0
            )
    lanes = lane_ids(NODES)
    for out, first in ((to_up, 120), (to_down, 0)):
        totals = [jnp.zeros((n, LANES), jnp.float32) for n in (NODES, 32, 8)]
        for x in range(4):
            for field, (part, start, count) in enumerate(((0, Q, 64), (0, REACT, 64), (1, FACES, 32), (2, THICK, 8))):
                at = 32 * field + 8 * x
                value = turned(near[BLOCK * x + start : BLOCK * x + start + count, :], at - first)
                ids = lanes[0:count]
                totals[part] = jnp.where((ids >= at) & (ids < at + 8), value, totals[part])
        out[0:8, :] = totals[0][0:8] + totals[1][0:8] + totals[2]
        out[8:32, :] = totals[0][8:32] + totals[1][8:32]
        out[32:64, :] = totals[0][32:64]


def far_kernel(near, left, right, strip, high2, low2):
    strip[0:64, :] = left[...]
    strip[64:128, :] = right[...]
    corner = jnp.where(lane_ids(32) < 32, turned(left[0:32, :], -64), turned(right[0:32, :], -32))
    for out, far, close, face in ((high2, 2, 3, 8), (low2, 1, 0, 0)):
        out[0:BLOCK, :] = near[BLOCK * close : BLOCK * close + BLOCK, :]
        at = BLOCK * far + FACES + face
        out[BLOCK : BLOCK + 8, :] = near[at : at + 8, :]
        out[BLOCK + 8 : BLOCK + 40, :] = corner


def powers_kernel(
    shift_in, weight, near, below1, above1, below2, above2, own_strip, strip_b1, strip_a1,
    basis_out, gram_out, field_a, field_b, image, react, stiff, opened,
):
    shift = shift_in[0:1, :]

    def put(row, value_reaction, value_stiffness, value_open, value_faces):
        cols = slice(row * LANES, (row + 1) * LANES)
        react[:, cols] = (value_reaction - shift) * SCALE
        stiff[:, cols] = jnp.broadcast_to(value_stiffness * SCALE, (8, LANES))
        for f in range(4):
            opened[8 * f : 8 * f + 8, cols] = jnp.broadcast_to(value_open[f], (8, LANES))
        image[NODES:, cols] = value_faces

    local = {}

    def put_block(row, ref, at):
        put(
            row, ref[at + REACT : at + FACES, :], ref[at + THICK : at + OPEN, :],
            [ref[at + OPEN + f : at + OPEN + f + 1, :] for f in range(4)], ref[at + FACES : at + THICK, :],
        )
        local[row] = lambda a: ref[at + 8 * a : at + 8 * a + 8, :]

    for x in range(4):
        for ref, row in ((below1, 2 + x), (near, 6 + x), (above1, 10 + x)):
            put_block(row, ref, BLOCK * x)
    put_block(1, below2, 0)
    put_block(ROWS - 2, above2, 0)
    image[72:80, 0:LANES] = below2[BLOCK : BLOCK + 8, :]
    image[64:72, (ROWS - 1) * LANES : ROWS * LANES] = above2[BLOCK : BLOCK + 8, :]

    lanes64 = lane_ids(NODES)
    lanes = lane_ids(8)
    pieces = ((strip_b1, 16, 48, 16), (own_strip, 48, 80, 48), (strip_a1, 80, 112, 80))
    for side in range(2):
        made = []
        for field, count in enumerate((64, 64, 32, 8)):
            ids = lanes64[0:count]
            value = jnp.zeros((count, LANES), jnp.float32)
            for ref, start, stop, zero in pieces:
                part = ref[NODES * side : NODES * side + count, :]
                value = jnp.where((ids >= start) & (ids < stop), turned(part, zero - 32 * field), value)
            if field == 2:
                corner = slice(BLOCK + 8, BLOCK + 40)
                value = jnp.where(ids < 16, turned(below2[corner, :], -16 - 32 * side), value)
                value = jnp.where(ids >= 112, turned(above2[corner, :], 112 - 32 * side), value)
            made.append(value)
        put(ROWS + side, made[1], made[3][0:1], [made[3][1 + f : 2 + f] for f in range(4)], made[2])
        local[ROWS + side] = functools.partial(lambda value, a: value[8 * a : 8 * a + 8], made[0])

    def columns(row):
        return slice(row * LANES, (row + 1) * LANES)

    low, high = ROWS, ROWS + 1
    sub = lax.broadcasted_iota(jnp.int32, (8, LANES), 0)
    TW, TE, TS, TN = (slice(64 + 8 * f, 72 + 8 * f) for f in range(4))

    def apply(old, new, step):
        start, stop = step, ROWS - step
        if step:
            for first_row, last_row in ((start, stop), (ROWS, ROWS + 2)):
                for row in range(first_row, last_row, 2):
                    cols = slice(row * LANES, (row + 2) * LANES)
                    image[:, cols] = product(weight, old[:, cols])

        def finish(row, from_west, from_east, from_south, from_north):
            cols = columns(row)
            faces = [
                opened[8 * f : 8 * f + 8, cols] * value
                for f, value in enumerate((from_west, from_east, from_south, from_north))
            ]
            if step:
                faces = [image[own, cols] - value for own, value in zip((TW, TE, TS, TN), faces)]
            else:
                faces = [8.0 * value for value in faces]
            for a in range(P_SIZE):
                rows = slice(8 * a, 8 * a + 8)
                if step:
                    value = react[rows, cols] * old[rows, cols] + stiff[:, cols] * image[rows, cols]
                else:
                    value = local[row](a)
                new[rows, cols] = value + edges(a, *faces, sub)

        north_low = image[TN, columns(low)]
        south_high = image[TS, columns(high)]
        for row in range(start + 1, stop - 1):
            cols = columns(row)
            from_south = jnp.where(
                lanes == 0, turned(north_low, -(8 * row + 7)), turned(image[TN, cols], 1)
            )
            from_north = jnp.where(
                lanes == LANES - 1, turned(south_high, 127 - 8 * row), turned(image[TS, cols], -1)
            )
            finish(row, image[TE, columns(row - 1)], image[TW, columns(row + 1)], from_south, from_north)
        if step == DEPTH - 1:
            return
        to_low = turned(image[TS, columns(low)], -1)
        to_high = turned(image[TN, columns(high)], 1)
        inner = 0 if step else 1
        for row in range(start + inner, stop - inner):
            cols = columns(row)
            to_low = jnp.where(lanes == 8 * row + 7, turned(image[TS, cols], 8 * row + 7), to_low)
            to_high = jnp.where(lanes == 8 * row, turned(image[TN, cols], 8 * row + 1), to_high)
        cols = columns(low)
        finish(low, turned(image[TE, cols], 8), turned(image[TW, cols], -8), turned(image[TN, cols], 1), to_low)
        cols = columns(high)
        finish(high, turned(image[TE, cols], 8), turned(image[TW, cols], -8), to_high, turned(image[TS, cols], -1))

    old, new = field_a, field_b
    for step in range(DEPTH):
        apply(old, new, step)
        basis_out[step, :, :] = new[:, 6 * LANES : 10 * LANES]
        old, new = new, old

    sums = [jnp.zeros((8, LANES), jnp.float32) for _ in GRAM]
    for x in range(4):
        for a in range(P_SIZE):
            values = [basis_out[k, 8 * a : 8 * a + 8, x * LANES : (x + 1) * LANES] for k in range(ITERS + 1)]
            sums = [total + values[k] * values[l] for total, (k, l) in zip(sums, GRAM)]
    rows = [jnp.sum(total, axis=0, keepdims=True) for total in sums]
    rows = jnp.concatenate(rows + [jnp.zeros((24 - len(GRAM), LANES), jnp.float32)], axis=0)
    totals = jnp.sum(rows, axis=1, keepdims=True)
    place = lax.broadcasted_iota(jnp.int32, (24, LANES), 0) == lax.broadcasted_iota(jnp.int32, (24, LANES), 1)
    totals = jnp.sum(jnp.where(place, totals, 0.0), axis=0, keepdims=True)
    gram_out[...] = jnp.broadcast_to(totals, gram_out.shape)


def combine_kernel(nodes, shift_in, powers, gathered, basis_out, hess_out, amp_out):
    shift = shift_in[...]
    row = jnp.sum(gathered[...], axis=0, keepdims=True) * (1.0 / nodes)
    spread = jnp.broadcast_to(row, (8, LANES))
    gram = {}
    for at, (k, l) in enumerate(GRAM):
        gram[k, l] = gram[l, k] = jnp.broadcast_to(spread[:, at : at + 1], (8, LANES))
    sizes = [jnp.sqrt(gram[k, k]) for k in range(ITERS + 1)]
    sub = lax.broadcasted_iota(jnp.int32, (8, LANES), 0)
    lanes = lane_ids(8)
    hess = jnp.zeros((8, LANES), jnp.float32)
    beta = jnp.sqrt(gram[0, 0] + FLOOR)
    coeffs = [[1.0 / beta]]
    amp = sizes[0] * coeffs[0][0]

    def put(hess, i, j, value):
        return jnp.where((sub == i) & (lanes == j), value, hess)

    for j in range(ITERS):
        last = coeffs[j]
        image = [shift * c for c in last] + [None]
        for k in range(j + 1):
            moved = last[k] * 8.0
            image[k + 1] = moved if image[k + 1] is None else image[k + 1] + moved
        weighted = [
            sum(gram[k, l] * image[l] for l in range(1, j + 2)) + gram[k, 0] * image[0] for k in range(j + 2)
        ]
        pending = list(image)
        for i in range(j + 1):
            h = sum(c * weighted[k] for k, c in enumerate(coeffs[i]))
            hess = put(hess, i, j, h)
            for k, c in enumerate(coeffs[i]):
                pending[k] = pending[k] - h * c
        square = sum(
            pending[k] * sum(gram[k, l] * pending[l] for l in range(j + 2)) for k in range(j + 2)
        )
        beta = jnp.sqrt(jnp.maximum(square, 0.0) + FLOOR)
        hess = put(hess, j + 1, j, beta)
        scale = 1.0 / beta
        coeffs.append([p * scale for p in pending])
        amp = jnp.maximum(amp, sum(jnp.abs(c) * s for c, s in zip(coeffs[-1], sizes)))
    hess_out[...] = hess[0 : ITERS + 1, 0:ITERS]
    amp_out[...] = amp[0:1, :]
    for x in range(4):
        for a in range(P_SIZE):
            values = [powers[k, 8 * a : 8 * a + 8, x * LANES : (x + 1) * LANES] for k in range(ITERS + 1)]
            for j in range(ITERS + 1):
                total = coeffs[j][0] * values[0]
                for k in range(1, j + 1):
                    total = total + coeffs[j][k] * values[k]
                basis_out[j, pl.ds(32 * a + x, 8, stride=4), :] = total


def fast(source, initial, reaction, stiffness, line_op, face_deriv, walls):
    vmem = pl.BlockSpec(memory_space=pltpu.VMEM)
    hbm = pl.BlockSpec(memory_space=pltpu.HBM)
    grant = pltpu.CompilerParams(vmem_limit_bytes=16 * 2**20)
    f32 = jnp.float32
    nx, ny = lax.axis_size(GX), lax.axis_size(GY)
    wide = (ROWS + 2) * LANES

    def moved(value, axis, size, by):
        return lax.ppermute(value, axis, [(i, (i + by) % size) for i in range(size)])

    held = (line_op, face_deriv.reshape(1, P_SIZE), source, initial, reaction, stiffness, walls)
    raw, near, to_up, to_down, weight, shift = pl.pallas_call(
        pack_kernel,
        out_shape=[jax.ShapeDtypeStruct((n, LANES), f32) for n in (800, 4 * BLOCK, NODES, NODES)]
        + [jax.ShapeDtypeStruct((NODES + 32, 6 * NODES), jnp.bfloat16), jax.ShapeDtypeStruct((8, LANES), f32)],
        in_specs=[hbm] * 7,
        out_specs=[vmem] * 6,
        scratch_shapes=[
            pltpu.VMEM((P_SIZE, P_SIZE), f32),
            pltpu.VMEM((1, P_SIZE), f32),
            pltpu.VMEM((16, LANES), jnp.int32),
            pltpu.SemaphoreType.DMA((10,)),
        ],
        compiler_params=grant,
    )(*[pltpu.with_memory_space_constraint(v, pltpu.HBM) for v in held])
    left = moved(to_up, GY, ny, 1)
    right = moved(to_down, GY, ny, -1)
    below1 = moved(near, GX, nx, 1)
    above1 = moved(near, GX, nx, -1)
    strip, high2, low2 = pl.pallas_call(
        far_kernel,
        out_shape=[jax.ShapeDtypeStruct((n, LANES), f32) for n in (2 * NODES, BLOCK + 40, BLOCK + 40)],
        in_specs=[vmem] * 3,
        out_specs=[vmem] * 3,
        compiler_params=grant,
    )(near, left, right)
    below2 = moved(high2, GX, nx, 2)
    above2 = moved(low2, GX, nx, -2)
    strips = [moved(strip, GX, nx, by) for by in (1, -1)]

    powers, gram = pl.pallas_call(
        powers_kernel,
        out_shape=[
            jax.ShapeDtypeStruct((ITERS + 1, NODES, 4 * LANES), f32),
            jax.ShapeDtypeStruct((1, LANES), f32),
        ],
        in_specs=[vmem] * 10,
        out_specs=[vmem] * 2,
        scratch_shapes=[pltpu.VMEM((n, wide), f32) for n in (NODES, NODES, NODES + 32, NODES, 8, 32)],
        compiler_params=grant,
    )(shift, weight, near, below1, above1, below2, above2, strip, *strips)
    every = GX + GY
    copies = jnp.broadcast_to(gram, (nx * ny, LANES))
    gathered = lax.all_to_all(copies, every, split_axis=0, concat_axis=0, tiled=True)
    basis, hess, amp = pl.pallas_call(
        functools.partial(combine_kernel, float(NODES * 4 * nx * LANES * ny)),
        out_shape=[
            jax.ShapeDtypeStruct((ITERS + 1, 4 * NODES, LANES), f32),
            jax.ShapeDtypeStruct((ITERS + 1, ITERS), f32),
            jax.ShapeDtypeStruct((1, LANES), f32),
        ],
        in_specs=[vmem] * 3,
        out_specs=[vmem] * 3,
        compiler_params=grant,
    )(shift, powers, gathered)
    return hess, basis, amp[0, 0], raw


def body(source, initial, reaction, stiffness, line_op, face_deriv, wall_flags):
    flat = [v.reshape(4 * NODES, LANES) for v in (source, initial, reaction)]
    hess, basis, amp, raw = fast(*flat, stiffness, line_op, face_deriv, wall_flags.reshape(16, LANES))

    def again(carry):
        raw = lax.optimization_barrier(carry[3])
        initial, source, reaction = raw[0:768].reshape(3, NODES, 4, LANES)
        opened = raw[772:788].reshape(4, 4, LANES)
        line_op, face_deriv = raw[788:796, 0:P_SIZE], raw[796, 0:P_SIZE]
        hess, basis = stepwise(source, initial, reaction, raw[768:772], line_op, face_deriv, opened)
        return jnp.bool_(True), hess, basis.reshape(ITERS + 1, 4 * NODES, LANES), raw

    done = amp <= AMP_LIMIT
    carry = lax.while_loop(lambda carry: jnp.logical_not(carry[0]), again, (done, hess, basis, raw))
    return (carry[1], carry[2].reshape(ITERS + 1, NODES, 4, LANES))


def solution(mesh):
    finer = Mesh(mesh.devices.reshape(4, 2, 4, 8), ("gx_0", "gx_1", "gy_0", "gy_1"))
    placed = (
        P(None, GX, GY),
        P(None, GX, GY),
        P(None, GX, GY),
        P(GX, GY),
        P(),
        P(),
        P(None, GX, GY),
    )
    return jax.shard_map(
        body, mesh=finer, in_specs=placed, out_specs=(P(), P(None, None, GX, GY)), check_vma=False
    )
```

```python
import functools

import jax
import jax.numpy as jnp
from jax import lax
from jax.experimental import pallas as pl
from jax.experimental.pallas import tpu as pltpu
from jax.sharding import Mesh
from jax.sharding import PartitionSpec as P

P_SIZE = 8
ITERS = 5
GX = ("gx_0", "gx_1")
GY = ("gy_0", "gy_1")


TAU = 2.0
FLOOR = 0.1


def extended(array, sides, width):
    for axis, dim in sides:
        devices, length = (lax.axis_size(axis), array.shape[dim])
        up = [(i, (i + 1) % devices) for i in range(devices)]
        down = [(j, i) for i, j in up]
        last = lax.slice_in_dim(array, length - width, length, axis=dim)
        leading = lax.slice_in_dim(array, 0, width, axis=dim)
        before = lax.ppermute(last, axis, up)
        after = lax.ppermute(leading, axis, down)
        array = jnp.concatenate([before, array, after], axis=dim)
    return array


def sent_to_all(array, axis):
    copies = jnp.broadcast_to(array, (lax.axis_size(axis), *array.shape))
    return lax.all_to_all(copies, axis, split_axis=0, concat_axis=0, tiled=True)


def over_copies(array, axis):
    everything = sent_to_all(array, axis)
    return jnp.sum(everything, axis=0)


def by_axis(array, axes):
    far, near = axes
    nearer = over_copies(array, near)
    return over_copies(nearer, far)


def together(arrays, axis):
    vector, at, gathered = (jnp.concatenate([a.reshape(-1) for a in arrays]), 0, [])
    subtotal = by_axis(vector, axis)
    for a in arrays:
        gathered.append(subtotal[at : at + a.size].reshape(a.shape))
        at += a.size
    return tuple(gathered)


def local_total(values):
    return jnp.sum(jnp.sum(values, axis=0))


def x_traces(nodes, face_deriv):
    highest = lax.Precision.HIGHEST
    lower = jnp.einsum("c,cbxy->bxy", face_deriv, nodes, precision=highest)
    upper = jnp.einsum("c,cbxy->bxy", face_deriv[::-1], nodes, precision=highest)
    return jnp.stack([nodes[0], lower, nodes[-1], upper])


def y_traces(nodes, face_deriv):
    highest = lax.Precision.HIGHEST
    lower = jnp.einsum("c,acxy->axy", face_deriv, nodes, precision=highest)
    upper = jnp.einsum("c,acxy->axy", face_deriv[::-1], nodes, precision=highest)
    return jnp.stack([nodes[:, 0], lower, nodes[:, -1], upper])


def apply_op(field, reaction, stiffness, line_op, face_deriv, opened):
    highest = lax.Precision.HIGHEST
    nodes = field.reshape(P_SIZE, P_SIZE, field.shape[1], field.shape[2])
    interior = stiffness * (
        jnp.einsum("ac,cbxy->abxy", line_op, nodes, precision=highest)
        + jnp.einsum("bc,acxy->abxy", line_op, nodes, precision=highest)
    )
    xside = extended(x_traces(nodes, face_deriv), ((GX, 2),), 1)
    yside = extended(y_traces(nodes, face_deriv), ((GY, 3),), 1)
    x_own = xside[:, :, 1:-1]
    y_own = yside[:, :, :, 1:-1]
    east_nb = xside[0:2, :, 2:]
    west_nb = xside[2:4, :, :-2]
    north_nb = yside[0:2, :, :, 2:]
    south_nb = yside[2:4, :, :, :-2]
    add_east = TAU * (x_own[2] - opened[1] * east_nb[0]) + 0.5 * (x_own[3] - opened[1] * east_nb[1])
    add_west = TAU * (x_own[0] - opened[0] * west_nb[0]) + 0.5 * (x_own[1] - opened[0] * west_nb[1])
    add_north = TAU * (y_own[2] - opened[3] * north_nb[0]) + 0.5 * (
        y_own[3] - opened[3] * north_nb[1]
    )
    add_south = TAU * (y_own[0] - opened[2] * south_nb[0]) + 0.5 * (
        y_own[1] - opened[2] * south_nb[1]
    )
    result = reaction.reshape(nodes.shape) * nodes + interior
    result = result.at[0].add(add_west).at[P_SIZE - 1].add(add_east)
    result = result.at[:, 0].add(add_south).at[:, P_SIZE - 1].add(add_north)
    return result.reshape(field.shape)


def norm_scale(vector, total):
    squares = by_axis(local_total(vector * vector), (("gx_0", "gx_1"), ("gy_0", "gy_1")))
    return jnp.sqrt(squares / total + FLOOR)


def stepwise(source, initial, reaction, stiffness, line_op, face_deriv, opened):
    highest = lax.Precision.HIGHEST
    total = float(
        P_SIZE * P_SIZE * source.shape[1] * lax.axis_size(GX) * source.shape[2] * lax.axis_size(GY)
    )

    def operate(field):
        return apply_op(field, reaction, stiffness, line_op, face_deriv, opened)

    def products(basis, image):
        per_cell = jnp.einsum("kqxy,qxy->kxy", basis, image, precision=highest)
        return jnp.sum(per_cell, axis=(1, 2))

    first = source - operate(initial)
    basis = jnp.zeros((ITERS + 1,) + source.shape, jnp.float32)
    hessen = jnp.zeros((ITERS + 1, ITERS), jnp.float32)
    rows = lax.broadcasted_iota(jnp.int32, (ITERS + 1, ITERS), 0)
    cols = lax.broadcasted_iota(jnp.int32, (ITERS + 1, ITERS), 1)
    slots = lax.broadcasted_iota(jnp.int32, (ITERS + 1,), 0)

    def advance(step, carry):
        basis, hessen, pending = carry
        image = operate(pending)
        local = products(basis, image)
        projected, crossed, squares = together(
            (local, local_total(pending * image), local_total(pending * pending)),
            (("gx_0", "gx_1"), ("gy_0", "gy_1")),
        )
        beta = jnp.sqrt(squares / total + FLOOR)
        basis = lax.dynamic_update_index_in_dim(basis, pending / beta, step, 0)
        coeffs = projected / (total * beta) + jnp.where(
            slots == step, crossed / (total * beta * beta), 0.0
        )
        pending = image / beta - jnp.einsum("k,kqxy->qxy", coeffs, basis, precision=highest)
        hessen = hessen + jnp.where(cols == step, coeffs[:, None], 0.0)
        hessen = hessen + jnp.where((rows == step) & (cols == step - 1), beta, 0.0)
        return (basis, hessen, pending)

    basis, hessen, pending = lax.fori_loop(0, ITERS, advance, (basis, hessen, first))
    beta = norm_scale(pending, total)
    basis = basis.at[ITERS].set(pending / beta)
    hessen = hessen + jnp.where((rows == ITERS) & (cols == ITERS - 1), beta, 0.0)
    return (hessen, basis)


NODES = P_SIZE * P_SIZE
ROWS = 16
DEPTH = 6
LANES = 128
SCALE = 0.125
AMP_LIMIT = 100.0
GRAM = [(k, l) for k in range(ITERS + 1) for l in range(k + 1)]


def lane_ids(rows):
    return lax.broadcasted_iota(jnp.int32, (rows, LANES), 1)


def turned(value, shift):
    shift = shift % LANES
    return value if shift == 0 else pltpu.roll(value, shift, 1)


def strided(ref, start, count):
    return ref[pl.ds(start, count, stride=4), :]


BLOCK = 168
Q, REACT, FACES, THICK, OPEN = 0, 64, 128, 160, 161


def split(value):
    high = value.astype(jnp.bfloat16)
    rest = value - high.astype(jnp.float32)
    middle = rest.astype(jnp.bfloat16)
    low = (rest - middle.astype(jnp.float32)).astype(jnp.bfloat16)
    return high, middle, low


def weights_in(line, deriv):
    sub = lax.broadcasted_iota(jnp.int32, (8, NODES), 0)
    lane = lax.broadcasted_iota(jnp.int32, (8, NODES), 1)
    along, across = lane // 8, lane % 8
    outer = jnp.zeros((8, NODES), jnp.float32)
    inner = jnp.zeros((8, NODES), jnp.float32)
    for c in range(P_SIZE):
        column = jnp.broadcast_to(line[:, c : c + 1], (8, NODES))
        outer = jnp.where(along == c, column, outer)
        inner = jnp.where(across == c, column, inner)
    parts = []
    for a in range(P_SIZE):
        row = jnp.broadcast_to(outer[a : a + 1, :], (8, NODES))
        parts.append(jnp.where(across == sub, row, 0.0) + jnp.where(along == a, inner, 0.0))
    for first, second in ((along, across), (across, along)):
        for flip in (False, True):
            part = jnp.zeros((8, NODES), jnp.float32)
            for c in range(P_SIZE):
                value = SCALE * (0.5 * deriv[0:1, c : c + 1] + (TAU if c == 0 else 0.0))
                part = jnp.where(first == (P_SIZE - 1 - c if flip else c), value, part)
            parts.append(jnp.where(second == sub, part, 0.0))
    high, middle, low = split(jnp.concatenate(parts, axis=0))
    return jnp.concatenate([high, high, high, middle, middle, low], axis=1)


def product(weight, value):
    high, middle, low = split(value)
    stacked = jnp.concatenate([high, middle, low, high, middle, high], axis=0)
    return jnp.dot(weight[...], stacked, preferred_element_type=jnp.float32)


def centre(line, deriv):
    diagonal = lax.broadcasted_iota(jnp.int32, (8, 8), 0) == lax.broadcasted_iota(jnp.int32, (8, 8), 1)
    trace = jnp.sum(jnp.where(diagonal, line, 0.0), axis=1, keepdims=True)
    trace = jnp.sum(trace, axis=0, keepdims=True)
    return 2.0 + 0.3125 * trace + 0.5 * (TAU + 0.5 * deriv[0:1, 0:1])


def edges(a, west, east, south, north, sub):
    value = jnp.where(sub == 0, south[a : a + 1, :], 0.0)
    value = jnp.where(sub == P_SIZE - 1, north[a : a + 1, :], value)
    if a == 0:
        value = value + west
    if a == P_SIZE - 1:
        value = value + east
    return value


def pack_kernel(
    line_in, deriv_in, source, initial, reaction, stiffness, walls,
    raw, near, to_up, to_down, weight, shift_out, line, deriv, flags, sems,
):
    moves = [(line_in, line), (deriv_in, deriv)]
    for at, ref in ((0, initial), (256, source), (512, reaction)):
        for half in (0, 128):
            moves.append((ref.at[pl.ds(half, 128), :], raw.at[pl.ds(at + half, 128), :]))
    moves.append((stiffness, raw.at[pl.ds(768, 4), :]))
    moves.append((walls, flags))
    copies = [pltpu.make_async_copy(a, b, sems.at[n]) for n, (a, b) in enumerate(moves)]
    for copy in copies:
        copy.start()
    for copy in copies[:2]:
        copy.wait()
    line, deriv = line[...], deriv[...]
    weight[...] = weights_in(line, deriv)
    shift_out[...] = jnp.broadcast_to(centre(line, deriv), (8, LANES))
    for copy in copies[2:]:
        copy.wait()
    opened = 1.0 - flags[...].astype(jnp.float32)
    raw[772:788, :] = opened
    raw[788:796, 0:P_SIZE] = line
    raw[796:797, 0:P_SIZE] = deriv
    thick = raw[768:772, :]
    sub = lax.broadcasted_iota(jnp.int32, (8, LANES), 0)
    for x in range(0, 4, 2):
        pair = jnp.concatenate([strided(raw, x, NODES), strided(raw, x + 1, NODES)], axis=1)
        image = product(weight, pair)
        for k in range(2):
            at = BLOCK * (x + k)
            cols = slice(k * LANES, (k + 1) * LANES)
            traces = image[NODES:, cols]
            near[at + FACES : at + THICK, :] = traces
            faces = [8.0 * traces[8 * f : 8 * f + 8] for f in range(4)]
            width = jnp.broadcast_to(thick[x + k : x + k + 1, :], (8, LANES))
            for a in range(P_SIZE):
                rows = slice(8 * a, 8 * a + 8)
                value = strided(raw, 512 + 32 * a + x + k, 8) * pair[rows, cols] + width * image[rows, cols]
                value = value + edges(a, *faces, sub)
                near[at + 8 * a : at + 8 * a + 8, :] = strided(raw, 256 + 32 * a + x + k, 8) - value
            near[at + REACT : at + FACES, :] = strided(raw, 512 + x + k, NODES)
            rows = [thick[x + k : x + k + 1, :]]
            rows += [opened[4 * f + x + k : 4 * f + x + k + 1, :] for f in range(4)]
            near[at + THICK : at + BLOCK, :] = jnp.concatenate(
                rows + [jnp.zeros((3, LANES), jnp.float32)], axis=0
            )
    lanes = lane_ids(NODES)
    for out, first in ((to_up, 120), (to_down, 0)):
        totals = [jnp.zeros((n, LANES), jnp.float32) for n in (NODES, 32, 8)]
        for x in range(4):
            for field, (part, start, count) in enumerate(((0, Q, 64), (0, REACT, 64), (1, FACES, 32), (2, THICK, 8))):
                at = 32 * field + 8 * x
                value = turned(near[BLOCK * x + start : BLOCK * x + start + count, :], at - first)
                ids = lanes[0:count]
                totals[part] = jnp.where((ids >= at) & (ids < at + 8), value, totals[part])
        out[0:8, :] = totals[0][0:8] + totals[1][0:8] + totals[2]
        out[8:32, :] = totals[0][8:32] + totals[1][8:32]
        out[32:64, :] = totals[0][32:64]


def far_kernel(near, left, right, strip, high2, low2):
    strip[0:64, :] = left[...]
    strip[64:128, :] = right[...]
    corner = jnp.where(lane_ids(32) < 32, turned(left[0:32, :], -64), turned(right[0:32, :], -32))
    for out, far, close, face in ((high2, 2, 3, 8), (low2, 1, 0, 0)):
        out[0:64, :] = near[BLOCK * close : BLOCK * close + 64, :]
        out[64:104, :] = near[BLOCK * close + FACES : BLOCK * close + BLOCK, :]
        at = BLOCK * far + FACES + face
        out[104:112, :] = near[at : at + 8, :]
        out[112:144, :] = corner


def powers_kernel(
    shift_in, weight, near, below1, above1, below2, above2, own_strip, strip_b1, strip_a1,
    basis_out, gram_out, field_a, field_b, image, react, stiff, opened,
):
    shift = shift_in[0:1, :]

    def put(row, value_reaction, value_stiffness, value_open, value_faces):
        cols = slice(row * LANES, (row + 1) * LANES)
        react[:, cols] = (value_reaction - shift) * SCALE
        stiff[:, cols] = jnp.broadcast_to(value_stiffness * SCALE, (8, LANES))
        for f in range(4):
            opened[8 * f : 8 * f + 8, cols] = jnp.broadcast_to(value_open[f], (8, LANES))
        image[NODES:, cols] = value_faces

    local = {}

    def put_block(row, ref, at):
        put(
            row, ref[at + REACT : at + FACES, :], ref[at + THICK : at + OPEN, :],
            [ref[at + OPEN + f : at + OPEN + f + 1, :] for f in range(4)], ref[at + FACES : at + THICK, :],
        )
        local[row] = lambda a: ref[at + 8 * a : at + 8 * a + 8, :]

    for x in range(4):
        for ref, row in ((below1, 2 + x), (near, 6 + x), (above1, 10 + x)):
            put_block(row, ref, BLOCK * x)
    for row, ref in ((1, below2), (ROWS - 2, above2)):
        cols = slice(row * LANES, (row + 1) * LANES)
        for f in range(4):
            opened[8 * f : 8 * f + 8, cols] = jnp.broadcast_to(ref[97 + f : 98 + f, :], (8, LANES))
        image[NODES:, cols] = ref[64:96, :]
        local[row] = functools.partial(lambda ref, a: ref[8 * a : 8 * a + 8, :], ref)
    image[72:80, 0:LANES] = below2[104:112, :]
    image[64:72, (ROWS - 1) * LANES : ROWS * LANES] = above2[104:112, :]

    lanes64 = lane_ids(NODES)
    lanes = lane_ids(8)
    pieces = ((strip_b1, 16, 48, 16), (own_strip, 48, 80, 48), (strip_a1, 80, 112, 80))
    for side in range(2):
        made = []
        for field, count in enumerate((64, 64, 32, 8)):
            ids = lanes64[0:count]
            value = jnp.zeros((count, LANES), jnp.float32)
            for ref, start, stop, zero in pieces:
                part = ref[NODES * side : NODES * side + count, :]
                value = jnp.where((ids >= start) & (ids < stop), turned(part, zero - 32 * field), value)
            if field == 2:
                corner = slice(112, 144)
                value = jnp.where(ids < 16, turned(below2[corner, :], -16 - 32 * side), value)
                value = jnp.where(ids >= 112, turned(above2[corner, :], 112 - 32 * side), value)
            made.append(value)
        put(ROWS + side, made[1], made[3][0:1], [made[3][1 + f : 2 + f] for f in range(4)], made[2])
        local[ROWS + side] = functools.partial(lambda value, a: value[8 * a : 8 * a + 8], made[0])

    def columns(row):
        return slice(row * LANES, (row + 1) * LANES)

    low, high = ROWS, ROWS + 1
    sub = lax.broadcasted_iota(jnp.int32, (8, LANES), 0)
    TW, TE, TS, TN = (slice(64 + 8 * f, 72 + 8 * f) for f in range(4))

    def apply(old, new, step):
        start, stop = step, ROWS - step
        if step:
            for first_row, last_row in ((start, stop), (ROWS, ROWS + 2)):
                for row in range(first_row, last_row, 2):
                    cols = slice(row * LANES, (row + 2) * LANES)
                    image[:, cols] = product(weight, old[:, cols])

        def finish(row, from_west, from_east, from_south, from_north):
            cols = columns(row)
            faces = [
                opened[8 * f : 8 * f + 8, cols] * value
                for f, value in enumerate((from_west, from_east, from_south, from_north))
            ]
            if step:
                faces = [image[own, cols] - value for own, value in zip((TW, TE, TS, TN), faces)]
            else:
                faces = [8.0 * value for value in faces]
            for a in range(P_SIZE):
                rows = slice(8 * a, 8 * a + 8)
                if step:
                    value = react[rows, cols] * old[rows, cols] + stiff[:, cols] * image[rows, cols]
                else:
                    value = local[row](a)
                new[rows, cols] = value + edges(a, *faces, sub)

        north_low = image[TN, columns(low)]
        south_high = image[TS, columns(high)]
        for row in range(start + 1, stop - 1):
            cols = columns(row)
            from_south = jnp.where(
                lanes == 0, turned(north_low, -(8 * row + 7)), turned(image[TN, cols], 1)
            )
            from_north = jnp.where(
                lanes == LANES - 1, turned(south_high, 127 - 8 * row), turned(image[TS, cols], -1)
            )
            finish(row, image[TE, columns(row - 1)], image[TW, columns(row + 1)], from_south, from_north)
        if step == DEPTH - 1:
            return
        to_low = turned(image[TS, columns(low)], -1)
        to_high = turned(image[TN, columns(high)], 1)
        inner = 0 if step else 1
        for row in range(start + inner, stop - inner):
            cols = columns(row)
            to_low = jnp.where(lanes == 8 * row + 7, turned(image[TS, cols], 8 * row + 7), to_low)
            to_high = jnp.where(lanes == 8 * row, turned(image[TN, cols], 8 * row + 1), to_high)
        cols = columns(low)
        finish(low, turned(image[TE, cols], 8), turned(image[TW, cols], -8), turned(image[TN, cols], 1), to_low)
        cols = columns(high)
        finish(high, turned(image[TE, cols], 8), turned(image[TW, cols], -8), to_high, turned(image[TS, cols], -1))

    old, new = field_a, field_b
    for step in range(DEPTH):
        apply(old, new, step)
        basis_out[step, :, :] = new[:, 6 * LANES : 10 * LANES]
        old, new = new, old

    sums = [jnp.zeros((8, LANES), jnp.float32) for _ in GRAM]
    for x in range(4):
        for a in range(P_SIZE):
            values = [basis_out[k, 8 * a : 8 * a + 8, x * LANES : (x + 1) * LANES] for k in range(ITERS + 1)]
            sums = [total + values[k] * values[l] for total, (k, l) in zip(sums, GRAM)]
    rows = [jnp.sum(total, axis=0, keepdims=True) for total in sums]
    rows = jnp.concatenate(rows + [jnp.zeros((24 - len(GRAM), LANES), jnp.float32)], axis=0)
    totals = jnp.sum(rows, axis=1, keepdims=True)
    place = lax.broadcasted_iota(jnp.int32, (24, LANES), 0) == lax.broadcasted_iota(jnp.int32, (24, LANES), 1)
    totals = jnp.sum(jnp.where(place, totals, 0.0), axis=0, keepdims=True)
    gram_out[...] = jnp.broadcast_to(totals, gram_out.shape)


def combine_kernel(nodes, shift_in, powers, gathered, basis_out, hess_out, amp_out):
    shift = shift_in[...]
    row = jnp.sum(gathered[...], axis=0, keepdims=True) * (1.0 / nodes)
    spread = jnp.broadcast_to(row, (8, LANES))
    gram = {}
    for at, (k, l) in enumerate(GRAM):
        gram[k, l] = gram[l, k] = jnp.broadcast_to(spread[:, at : at + 1], (8, LANES))
    sizes = [jnp.sqrt(gram[k, k]) for k in range(ITERS + 1)]
    sub = lax.broadcasted_iota(jnp.int32, (8, LANES), 0)
    lanes = lane_ids(8)
    hess = jnp.zeros((8, LANES), jnp.float32)
    beta = jnp.sqrt(gram[0, 0] + FLOOR)
    coeffs = [[1.0 / beta]]
    amp = sizes[0] * coeffs[0][0]

    def put(hess, i, j, value):
        return jnp.where((sub == i) & (lanes == j), value, hess)

    for j in range(ITERS):
        last = coeffs[j]
        image = [shift * c for c in last] + [None]
        for k in range(j + 1):
            moved = last[k] * 8.0
            image[k + 1] = moved if image[k + 1] is None else image[k + 1] + moved
        weighted = [
            sum(gram[k, l] * image[l] for l in range(1, j + 2)) + gram[k, 0] * image[0] for k in range(j + 2)
        ]
        pending = list(image)
        for i in range(j + 1):
            h = sum(c * weighted[k] for k, c in enumerate(coeffs[i]))
            hess = put(hess, i, j, h)
            for k, c in enumerate(coeffs[i]):
                pending[k] = pending[k] - h * c
        square = sum(
            pending[k] * sum(gram[k, l] * pending[l] for l in range(j + 2)) for k in range(j + 2)
        )
        beta = jnp.sqrt(jnp.maximum(square, 0.0) + FLOOR)
        hess = put(hess, j + 1, j, beta)
        scale = 1.0 / beta
        coeffs.append([p * scale for p in pending])
        amp = jnp.maximum(amp, sum(jnp.abs(c) * s for c, s in zip(coeffs[-1], sizes)))
    hess_out[...] = hess[0 : ITERS + 1, 0:ITERS]
    amp_out[...] = amp[0:1, :]
    for x in range(4):
        for a in range(P_SIZE):
            values = [powers[k, 8 * a : 8 * a + 8, x * LANES : (x + 1) * LANES] for k in range(ITERS + 1)]
            for j in range(ITERS + 1):
                total = coeffs[j][0] * values[0]
                for k in range(1, j + 1):
                    total = total + coeffs[j][k] * values[k]
                basis_out[j, pl.ds(32 * a + x, 8, stride=4), :] = total


def fast(source, initial, reaction, stiffness, line_op, face_deriv, walls):
    vmem = pl.BlockSpec(memory_space=pltpu.VMEM)
    hbm = pl.BlockSpec(memory_space=pltpu.HBM)
    grant = pltpu.CompilerParams(vmem_limit_bytes=16 * 2**20)
    f32 = jnp.float32
    nx, ny = lax.axis_size(GX), lax.axis_size(GY)
    wide = (ROWS + 2) * LANES

    def moved(value, axis, size, by):
        return lax.ppermute(value, axis, [(i, (i + by) % size) for i in range(size)])

    held = (line_op, face_deriv.reshape(1, P_SIZE), source, initial, reaction, stiffness, walls)
    raw, near, to_up, to_down, weight, shift = pl.pallas_call(
        pack_kernel,
        out_shape=[jax.ShapeDtypeStruct((n, LANES), f32) for n in (800, 4 * BLOCK, NODES, NODES)]
        + [jax.ShapeDtypeStruct((NODES + 32, 6 * NODES), jnp.bfloat16), jax.ShapeDtypeStruct((8, LANES), f32)],
        in_specs=[hbm] * 7,
        out_specs=[vmem] * 6,
        scratch_shapes=[
            pltpu.VMEM((P_SIZE, P_SIZE), f32),
            pltpu.VMEM((1, P_SIZE), f32),
            pltpu.VMEM((16, LANES), jnp.int32),
            pltpu.SemaphoreType.DMA((10,)),
        ],
        compiler_params=grant,
    )(*[pltpu.with_memory_space_constraint(v, pltpu.HBM) for v in held])
    left = moved(to_up, GY, ny, 1)
    right = moved(to_down, GY, ny, -1)
    below1 = moved(near, GX, nx, 1)
    above1 = moved(near, GX, nx, -1)
    strip, high2, low2 = pl.pallas_call(
        far_kernel,
        out_shape=[jax.ShapeDtypeStruct((n, LANES), f32) for n in (2 * NODES, 144, 144)],
        in_specs=[vmem] * 3,
        out_specs=[vmem] * 3,
        compiler_params=grant,
    )(near, left, right)
    below2 = moved(high2, GX, nx, 2)
    above2 = moved(low2, GX, nx, -2)
    strips = [moved(strip, GX, nx, by) for by in (1, -1)]

    powers, gram = pl.pallas_call(
        powers_kernel,
        out_shape=[
            jax.ShapeDtypeStruct((ITERS + 1, NODES, 4 * LANES), f32),
            jax.ShapeDtypeStruct((1, LANES), f32),
        ],
        in_specs=[vmem] * 10,
        out_specs=[vmem] * 2,
        scratch_shapes=[pltpu.VMEM((n, wide), f32) for n in (NODES, NODES, NODES + 32, NODES, 8, 32)],
        compiler_params=grant,
    )(shift, weight, near, below1, above1, below2, above2, strip, *strips)
    every = GX + GY
    copies = jnp.broadcast_to(gram, (nx * ny, LANES))
    gathered = lax.all_to_all(copies, every, split_axis=0, concat_axis=0, tiled=True)
    basis, hess, amp = pl.pallas_call(
        functools.partial(combine_kernel, float(NODES * 4 * nx * LANES * ny)),
        out_shape=[
            jax.ShapeDtypeStruct((ITERS + 1, 4 * NODES, LANES), f32),
            jax.ShapeDtypeStruct((ITERS + 1, ITERS), f32),
            jax.ShapeDtypeStruct((1, LANES), f32),
        ],
        in_specs=[vmem] * 3,
        out_specs=[vmem] * 3,
        compiler_params=grant,
    )(shift, powers, gathered)
    return hess, basis, amp[0, 0], raw


def body(source, initial, reaction, stiffness, line_op, face_deriv, wall_flags):
    flat = [v.reshape(4 * NODES, LANES) for v in (source, initial, reaction)]
    hess, basis, amp, raw = fast(*flat, stiffness, line_op, face_deriv, wall_flags.reshape(16, LANES))

    def again(carry):
        raw = lax.optimization_barrier(carry[3])
        initial, source, reaction = raw[0:768].reshape(3, NODES, 4, LANES)
        opened = raw[772:788].reshape(4, 4, LANES)
        line_op, face_deriv = raw[788:796, 0:P_SIZE], raw[796, 0:P_SIZE]
        hess, basis = stepwise(source, initial, reaction, raw[768:772], line_op, face_deriv, opened)
        return jnp.bool_(True), hess, basis.reshape(ITERS + 1, 4 * NODES, LANES), raw

    done = amp <= AMP_LIMIT
    carry = lax.while_loop(lambda carry: jnp.logical_not(carry[0]), again, (done, hess, basis, raw))
    return (carry[1], carry[2].reshape(ITERS + 1, NODES, 4, LANES))


def solution(mesh):
    finer = Mesh(mesh.devices.reshape(4, 2, 4, 8), ("gx_0", "gx_1", "gy_0", "gy_1"))
    placed = (
        P(None, GX, GY),
        P(None, GX, GY),
        P(None, GX, GY),
        P(GX, GY),
        P(),
        P(),
        P(None, GX, GY),
    )
    return jax.shard_map(
        body, mesh=finer, in_specs=placed, out_specs=(P(), P(None, None, GX, GY)), check_vma=False
    )
```

```python
import functools

import jax
import jax.numpy as jnp
from jax import lax
from jax.experimental import pallas as pl
from jax.experimental.pallas import tpu as pltpu
from jax.sharding import Mesh
from jax.sharding import PartitionSpec as P

P_SIZE = 8
ITERS = 5
GX = ("gx_0", "gx_1")
GY = ("gy_0", "gy_1")


TAU = 2.0
FLOOR = 0.1


def extended(array, sides, width):
    for axis, dim in sides:
        devices, length = (lax.axis_size(axis), array.shape[dim])
        up = [(i, (i + 1) % devices) for i in range(devices)]
        down = [(j, i) for i, j in up]
        last = lax.slice_in_dim(array, length - width, length, axis=dim)
        leading = lax.slice_in_dim(array, 0, width, axis=dim)
        before = lax.ppermute(last, axis, up)
        after = lax.ppermute(leading, axis, down)
        array = jnp.concatenate([before, array, after], axis=dim)
    return array


def sent_to_all(array, axis):
    copies = jnp.broadcast_to(array, (lax.axis_size(axis), *array.shape))
    return lax.all_to_all(copies, axis, split_axis=0, concat_axis=0, tiled=True)


def over_copies(array, axis):
    everything = sent_to_all(array, axis)
    return jnp.sum(everything, axis=0)


def by_axis(array, axes):
    far, near = axes
    nearer = over_copies(array, near)
    return over_copies(nearer, far)


def together(arrays, axis):
    vector, at, gathered = (jnp.concatenate([a.reshape(-1) for a in arrays]), 0, [])
    subtotal = by_axis(vector, axis)
    for a in arrays:
        gathered.append(subtotal[at : at + a.size].reshape(a.shape))
        at += a.size
    return tuple(gathered)


def local_total(values):
    return jnp.sum(jnp.sum(values, axis=0))


def x_traces(nodes, face_deriv):
    highest = lax.Precision.HIGHEST
    lower = jnp.einsum("c,cbxy->bxy", face_deriv, nodes, precision=highest)
    upper = jnp.einsum("c,cbxy->bxy", face_deriv[::-1], nodes, precision=highest)
    return jnp.stack([nodes[0], lower, nodes[-1], upper])


def y_traces(nodes, face_deriv):
    highest = lax.Precision.HIGHEST
    lower = jnp.einsum("c,acxy->axy", face_deriv, nodes, precision=highest)
    upper = jnp.einsum("c,acxy->axy", face_deriv[::-1], nodes, precision=highest)
    return jnp.stack([nodes[:, 0], lower, nodes[:, -1], upper])


def apply_op(field, reaction, stiffness, line_op, face_deriv, opened):
    highest = lax.Precision.HIGHEST
    nodes = field.reshape(P_SIZE, P_SIZE, field.shape[1], field.shape[2])
    interior = stiffness * (
        jnp.einsum("ac,cbxy->abxy", line_op, nodes, precision=highest)
        + jnp.einsum("bc,acxy->abxy", line_op, nodes, precision=highest)
    )
    xside = extended(x_traces(nodes, face_deriv), ((GX, 2),), 1)
    yside = extended(y_traces(nodes, face_deriv), ((GY, 3),), 1)
    x_own = xside[:, :, 1:-1]
    y_own = yside[:, :, :, 1:-1]
    east_nb = xside[0:2, :, 2:]
    west_nb = xside[2:4, :, :-2]
    north_nb = yside[0:2, :, :, 2:]
    south_nb = yside[2:4, :, :, :-2]
    add_east = TAU * (x_own[2] - opened[1] * east_nb[0]) + 0.5 * (x_own[3] - opened[1] * east_nb[1])
    add_west = TAU * (x_own[0] - opened[0] * west_nb[0]) + 0.5 * (x_own[1] - opened[0] * west_nb[1])
    add_north = TAU * (y_own[2] - opened[3] * north_nb[0]) + 0.5 * (
        y_own[3] - opened[3] * north_nb[1]
    )
    add_south = TAU * (y_own[0] - opened[2] * south_nb[0]) + 0.5 * (
        y_own[1] - opened[2] * south_nb[1]
    )
    result = reaction.reshape(nodes.shape) * nodes + interior
    result = result.at[0].add(add_west).at[P_SIZE - 1].add(add_east)
    result = result.at[:, 0].add(add_south).at[:, P_SIZE - 1].add(add_north)
    return result.reshape(field.shape)


def norm_scale(vector, total):
    squares = by_axis(local_total(vector * vector), (("gx_0", "gx_1"), ("gy_0", "gy_1")))
    return jnp.sqrt(squares / total + FLOOR)


def stepwise(source, initial, reaction, stiffness, line_op, face_deriv, opened):
    highest = lax.Precision.HIGHEST
    total = float(
        P_SIZE * P_SIZE * source.shape[1] * lax.axis_size(GX) * source.shape[2] * lax.axis_size(GY)
    )

    def operate(field):
        return apply_op(field, reaction, stiffness, line_op, face_deriv, opened)

    def products(basis, image):
        per_cell = jnp.einsum("kqxy,qxy->kxy", basis, image, precision=highest)
        return jnp.sum(per_cell, axis=(1, 2))

    first = source - operate(initial)
    basis = jnp.zeros((ITERS + 1,) + source.shape, jnp.float32)
    hessen = jnp.zeros((ITERS + 1, ITERS), jnp.float32)
    rows = lax.broadcasted_iota(jnp.int32, (ITERS + 1, ITERS), 0)
    cols = lax.broadcasted_iota(jnp.int32, (ITERS + 1, ITERS), 1)
    slots = lax.broadcasted_iota(jnp.int32, (ITERS + 1,), 0)

    def advance(step, carry):
        basis, hessen, pending = carry
        image = operate(pending)
        local = products(basis, image)
        projected, crossed, squares = together(
            (local, local_total(pending * image), local_total(pending * pending)),
            (("gx_0", "gx_1"), ("gy_0", "gy_1")),
        )
        beta = jnp.sqrt(squares / total + FLOOR)
        basis = lax.dynamic_update_index_in_dim(basis, pending / beta, step, 0)
        coeffs = projected / (total * beta) + jnp.where(
            slots == step, crossed / (total * beta * beta), 0.0
        )
        pending = image / beta - jnp.einsum("k,kqxy->qxy", coeffs, basis, precision=highest)
        hessen = hessen + jnp.where(cols == step, coeffs[:, None], 0.0)
        hessen = hessen + jnp.where((rows == step) & (cols == step - 1), beta, 0.0)
        return (basis, hessen, pending)

    basis, hessen, pending = lax.fori_loop(0, ITERS, advance, (basis, hessen, first))
    beta = norm_scale(pending, total)
    basis = basis.at[ITERS].set(pending / beta)
    hessen = hessen + jnp.where((rows == ITERS) & (cols == ITERS - 1), beta, 0.0)
    return (hessen, basis)


NODES = P_SIZE * P_SIZE
ROWS = 16
DEPTH = 6
LANES = 128
SCALE = 0.125
AMP_LIMIT = 100.0
GRAM = [(k, l) for k in range(ITERS + 1) for l in range(k + 1)]


def lane_ids(rows):
    return lax.broadcasted_iota(jnp.int32, (rows, LANES), 1)


def turned(value, shift):
    shift = shift % LANES
    return value if shift == 0 else pltpu.roll(value, shift, 1)


def strided(ref, start, count):
    return ref[pl.ds(start, count, stride=4), :]


BLOCK = 136
REACT, THICK, OPEN = 64, 128, 129
FIRST_WEST, LAST_EAST, ENDS, STRIP = 544, 552, 560, 568


def split(value):
    high = value.astype(jnp.bfloat16)
    rest = value - high.astype(jnp.float32)
    middle = rest.astype(jnp.bfloat16)
    low = (rest - middle.astype(jnp.float32)).astype(jnp.bfloat16)
    return high, middle, low


def weights_in(line, deriv):
    sub = lax.broadcasted_iota(jnp.int32, (8, NODES), 0)
    lane = lax.broadcasted_iota(jnp.int32, (8, NODES), 1)
    along, across = lane // 8, lane % 8
    outer = jnp.zeros((8, NODES), jnp.float32)
    inner = jnp.zeros((8, NODES), jnp.float32)
    for c in range(P_SIZE):
        column = jnp.broadcast_to(line[:, c : c + 1], (8, NODES))
        outer = jnp.where(along == c, column, outer)
        inner = jnp.where(across == c, column, inner)
    parts = []
    for a in range(P_SIZE):
        row = jnp.broadcast_to(outer[a : a + 1, :], (8, NODES))
        parts.append(jnp.where(across == sub, row, 0.0) + jnp.where(along == a, inner, 0.0))
    for first, second in ((along, across), (across, along)):
        for flip in (False, True):
            part = jnp.zeros((8, NODES), jnp.float32)
            for c in range(P_SIZE):
                value = SCALE * (0.5 * deriv[0:1, c : c + 1] + (TAU if c == 0 else 0.0))
                part = jnp.where(first == (P_SIZE - 1 - c if flip else c), value, part)
            parts.append(jnp.where(second == sub, part, 0.0))
    high, middle, low = split(jnp.concatenate(parts, axis=0))
    return jnp.concatenate([high, high, high, middle, middle, low], axis=1)


def product(weight, value):
    high, middle, low = split(value)
    stacked = jnp.concatenate([high, middle, low, high, middle, high], axis=0)
    return jnp.dot(weight[...], stacked, preferred_element_type=jnp.float32)


def centre(line, deriv):
    diagonal = lax.broadcasted_iota(jnp.int32, (8, 8), 0) == lax.broadcasted_iota(jnp.int32, (8, 8), 1)
    trace = jnp.sum(jnp.where(diagonal, line, 0.0), axis=1, keepdims=True)
    trace = jnp.sum(trace, axis=0, keepdims=True)
    return 2.0 + 0.3125 * trace + 0.5 * (TAU + 0.5 * deriv[0:1, 0:1])


def edges(a, west, east, south, north, sub):
    value = jnp.where(sub == 0, south[a : a + 1, :], 0.0)
    value = jnp.where(sub == P_SIZE - 1, north[a : a + 1, :], value)
    if a == 0 and west is not None:
        value = value + west
    if a == P_SIZE - 1 and east is not None:
        value = value + east
    return value


def pack_kernel(
    line_in, deriv_in, source, initial, reaction, stiffness, walls,
    raw, near, to_up, to_down, weight, shift_out, line, deriv, flags, sems,
):
    moves = [(line_in, line), (deriv_in, deriv)]
    for at, ref in ((0, initial), (256, source), (512, reaction)):
        for half in (0, 128):
            moves.append((ref.at[pl.ds(half, 128), :], raw.at[pl.ds(at + half, 128), :]))
    moves.append((stiffness, raw.at[pl.ds(768, 4), :]))
    moves.append((walls, flags))
    copies = [pltpu.make_async_copy(a, b, sems.at[n]) for n, (a, b) in enumerate(moves)]
    for copy in copies:
        copy.start()
    for copy in copies[:2]:
        copy.wait()
    line, deriv = line[...], deriv[...]
    weight[...] = weights_in(line, deriv)
    shift_out[...] = jnp.broadcast_to(centre(line, deriv), (8, LANES))
    for copy in copies[2:]:
        copy.wait()
    opened = 1.0 - flags[...].astype(jnp.float32)
    raw[772:788, :] = opened
    raw[788:796, 0:P_SIZE] = line
    raw[796:797, 0:P_SIZE] = deriv
    thick = raw[768:772, :]
    sub = lax.broadcasted_iota(jnp.int32, (8, LANES), 0)
    lanes8 = lane_ids(8)
    fields, images = [], []
    for x in range(0, 4, 2):
        pair = jnp.concatenate([strided(raw, x, NODES), strided(raw, x + 1, NODES)], axis=1)
        image = product(weight, pair)
        for k in range(2):
            fields.append(pair[:, k * LANES : (k + 1) * LANES])
            images.append(image[:, k * LANES : (k + 1) * LANES])
    traces = [[image[64 + 8 * f : 72 + 8 * f] for f in range(4)] for image in images]
    ends = jnp.zeros((8, LANES), jnp.float32)
    for x in range(4):
        at = BLOCK * x
        allowed = [jnp.broadcast_to(opened[4 * f + x : 4 * f + x + 1, :], (8, LANES)) for f in range(4)]
        faces = list(traces[x])
        if x > 0:
            faces[0] = faces[0] - allowed[0] * traces[x - 1][1]
        if x < 3:
            faces[1] = faces[1] - allowed[1] * traces[x + 1][0]
        faces[2] = faces[2] - allowed[2] * jnp.where(lanes8 == 0, 0.0, turned(traces[x][3], 1))
        faces[3] = faces[3] - allowed[3] * jnp.where(lanes8 == LANES - 1, 0.0, turned(traces[x][2], -1))
        faces = [8.0 * face for face in faces]
        ends = jnp.where(lanes8 == 8 * x + 7, turned(traces[x][2], 8 * x + 7), ends)
        ends = jnp.where(lanes8 == 8 * x, turned(traces[x][3], 8 * x + 1), ends)
        width = jnp.broadcast_to(thick[x : x + 1, :], (8, LANES))
        for a in range(P_SIZE):
            rows = slice(8 * a, 8 * a + 8)
            value = strided(raw, 512 + 32 * a + x, 8) * fields[x][rows] + width * images[x][rows]
            value = value + edges(a, *faces, sub)
            near[at + 8 * a : at + 8 * a + 8, :] = strided(raw, 256 + 32 * a + x, 8) - value
        near[at + REACT : at + THICK, :] = strided(raw, 512 + x, NODES)
        rows = [thick[x : x + 1, :]] + [opened[4 * f + x : 4 * f + x + 1, :] for f in range(4)]
        near[at + THICK : at + BLOCK, :] = jnp.concatenate(rows + [jnp.zeros((3, LANES), jnp.float32)], axis=0)
    near[FIRST_WEST:LAST_EAST, :] = traces[0][0]
    near[LAST_EAST:ENDS, :] = traces[3][1]
    near[ENDS : ENDS + 8, :] = ends
    lanes = lane_ids(NODES)
    for out, first in ((to_up, 120), (to_down, 0)):
        totals = [jnp.zeros((n, LANES), jnp.float32) for n in (NODES, 32, 8)]
        for x in range(4):
            block = BLOCK * x
            parts = (
                (0, near[block : block + 64, :]),
                (0, near[block + REACT : block + THICK, :]),
                (1, jnp.concatenate(traces[x], axis=0)),
                (2, near[block + THICK : block + BLOCK, :]),
            )
            for field, (part, value) in enumerate(parts):
                at = 32 * field + 8 * x
                ids = lanes[0 : value.shape[0]]
                totals[part] = jnp.where((ids >= at) & (ids < at + 8), turned(value, at - first), totals[part])
        out[0:8, :] = totals[0][0:8] + totals[1][0:8] + totals[2]
        out[8:32, :] = totals[0][8:32] + totals[1][8:32]
        out[32:64, :] = totals[0][32:64]


def far_kernel(near, left, right, whole, high2, low2):
    whole[0:STRIP, :] = near[...]
    lanes = lane_ids(NODES)
    whole[STRIP : STRIP + 64, :] = jnp.where(lanes < 64, left[...], turned(right[...], 64))
    lanes = lanes[0:32]
    edge = jnp.where(lanes < 32, turned(left[0:32, :], -64), turned(right[0:32, :], -32))
    edge = jnp.where((lanes >= 64) & (lanes < 96), turned(left[0:32, :], -32), edge)
    edge = jnp.where(lanes >= 96, right[0:32, :], edge)
    whole[STRIP + 64 : STRIP + 96, :] = edge
    for out, close, face in ((high2, 3, LAST_EAST), (low2, 0, FIRST_WEST)):
        block = BLOCK * close
        out[0:64, :] = near[block : block + 64, :]
        out[64:72, :] = near[block + THICK : block + BLOCK, :]
        out[72:80, :] = near[face : face + 8, :]
        out[80:88, :] = near[ENDS : ENDS + 8, :]
        out[88:120, :] = edge


def powers_kernel(
    shift_in, weight, near, below1, above1, below2, above2,
    basis_out, gram_out, field_a, field_b, image, react, stiff, opened,
):
    shift = shift_in[0:1, :]

    def put(row, value_reaction, value_stiffness, value_open):
        cols = slice(row * LANES, (row + 1) * LANES)
        if value_reaction is not None:
            react[:, cols] = (value_reaction - shift) * SCALE
            stiff[:, cols] = jnp.broadcast_to(value_stiffness * SCALE, (8, LANES))
        for f in range(4):
            opened[8 * f : 8 * f + 8, cols] = jnp.broadcast_to(value_open[f], (8, LANES))

    local = {}
    for x in range(4):
        for ref, row in ((below1, 2 + x), (near, 6 + x), (above1, 10 + x)):
            at = BLOCK * x
            put(
                row, ref[at + REACT : at + THICK, :], ref[at + THICK : at + OPEN, :],
                [ref[at + OPEN + f : at + OPEN + f + 1, :] for f in range(4)],
            )
            local[row] = functools.partial(lambda ref, at, a: ref[at + 8 * a : at + 8 * a + 8, :], ref, at)
    for row, ref in ((1, below2), (ROWS - 2, above2)):
        put(row, None, None, [ref[65 + f : 66 + f, :] for f in range(4)])
        local[row] = functools.partial(lambda ref, a: ref[8 * a : 8 * a + 8, :], ref)

    lanes64 = lane_ids(NODES)
    lanes = lane_ids(8)
    pieces = ((below1, 16, 48, 16), (near, 48, 80, 48), (above1, 80, 112, 80))
    strip_faces = []
    for side in range(2):
        made = []
        for top, count, zero in ((0, 64, 64 * side), (0, 64, 64 * side + 32), (64, 32, 32 * side), (64, 8, 64 + 32 * side)):
            ids = lanes64[0:count]
            value = jnp.zeros((count, LANES), jnp.float32)
            for ref, start, stop, target in pieces:
                part = turned(ref[STRIP + top : STRIP + top + count, :], target - zero)
                value = jnp.where((ids >= start) & (ids < stop), part, value)
            if count == 32:
                value = jnp.where(ids < 16, turned(below2[88:120, :], -16 - 32 * side), value)
                value = jnp.where(ids >= 112, turned(above2[88:120, :], 112 - 32 * side), value)
            made.append(value)
        put(ROWS + side, made[1], made[3][0:1], [made[3][1 + f : 2 + f] for f in range(4)])
        local[ROWS + side] = functools.partial(lambda value, a: value[8 * a : 8 * a + 8], made[0])
        strip_faces.append([made[2][8 * f : 8 * f + 8] for f in range(4)])
    ends = jnp.zeros((8, LANES), jnp.float32)
    for ref, top, start, stop, by in (
        (below2, 80, 0, 16, -16), (below1, ENDS, 16, 48, 16), (near, ENDS, 48, 80, 48),
        (above1, ENDS, 80, 112, 80), (above2, 80, 112, 128, 112),
    ):
        ends = jnp.where((lanes >= start) & (lanes < stop), turned(ref[top : top + 8, :], by), ends)

    def columns(row):
        return slice(row * LANES, (row + 1) * LANES)

    low, high = ROWS, ROWS + 1
    sub = lax.broadcasted_iota(jnp.int32, (8, LANES), 0)
    TW, TE, TS, TN = (slice(64 + 8 * f, 72 + 8 * f) for f in range(4))

    def begin(new):
        def finish(row, faces):
            cols = columns(row)
            faces = [
                None if value is None else 8.0 * opened[8 * f : 8 * f + 8, cols] * value
                for f, value in enumerate(faces)
            ]
            for a in range(P_SIZE):
                new[8 * a : 8 * a + 8, cols] = local[row](a) + edges(a, *faces, sub)

        west = {
            2: below2[72:80, :], 6: below1[LAST_EAST:ENDS, :], 10: near[LAST_EAST:ENDS, :],
            14: above1[LAST_EAST:ENDS, :],
        }
        east = {
            1: below1[FIRST_WEST:LAST_EAST, :], 5: near[FIRST_WEST:LAST_EAST, :],
            9: above1[FIRST_WEST:LAST_EAST, :], 13: above2[72:80, :],
        }
        for row in range(1, ROWS - 1):
            south = jnp.where(lanes == 0, turned(strip_faces[0][3], -(8 * row + 7)), 0.0)
            north = jnp.where(lanes == LANES - 1, turned(strip_faces[1][2], 127 - 8 * row), 0.0)
            finish(row, (west.get(row), east.get(row), south, north))
        none = jnp.zeros((8, LANES), jnp.float32)
        spot = lanes // 8 % 4
        for side in range(2):
            from_west = jnp.where(spot == 2, turned(strip_faces[side][1], 8), 0.0)
            from_east = jnp.where(spot == 1, turned(strip_faces[side][0], -8), 0.0)
            outer = jnp.where(lanes % 8 == (0 if side else 7), ends, 0.0)
            finish(ROWS + side, (from_west, from_east, outer if side else none, none if side else outer))

    def apply(old, new, step):
        start, stop = step, ROWS - step
        for first_row, last_row in ((start, stop), (ROWS, ROWS + 2)):
            for row in range(first_row, last_row, 2):
                cols = slice(row * LANES, (row + 2) * LANES)
                image[:, cols] = product(weight, old[:, cols])

        def finish(row, *sides):
            cols = columns(row)
            faces = [
                image[own, cols] - opened[8 * f : 8 * f + 8, cols] * value
                for f, (own, value) in enumerate(zip((TW, TE, TS, TN), sides))
            ]
            for a in range(P_SIZE):
                rows = slice(8 * a, 8 * a + 8)
                value = react[rows, cols] * old[rows, cols] + stiff[:, cols] * image[rows, cols]
                new[rows, cols] = value + edges(a, *faces, sub)

        north_low = image[TN, columns(low)]
        south_high = image[TS, columns(high)]
        for row in range(start + 1, stop - 1):
            cols = columns(row)
            from_south = jnp.where(
                lanes == 0, turned(north_low, -(8 * row + 7)), turned(image[TN, cols], 1)
            )
            from_north = jnp.where(
                lanes == LANES - 1, turned(south_high, 127 - 8 * row), turned(image[TS, cols], -1)
            )
            finish(row, image[TE, columns(row - 1)], image[TW, columns(row + 1)], from_south, from_north)
        if step == DEPTH - 1:
            return
        to_low = turned(image[TS, columns(low)], -1)
        to_high = turned(image[TN, columns(high)], 1)
        for row in range(start, stop):
            cols = columns(row)
            to_low = jnp.where(lanes == 8 * row + 7, turned(image[TS, cols], 8 * row + 7), to_low)
            to_high = jnp.where(lanes == 8 * row, turned(image[TN, cols], 8 * row + 1), to_high)
        cols = columns(low)
        finish(low, turned(image[TE, cols], 8), turned(image[TW, cols], -8), turned(image[TN, cols], 1), to_low)
        cols = columns(high)
        finish(high, turned(image[TE, cols], 8), turned(image[TW, cols], -8), to_high, turned(image[TS, cols], -1))

    old, new = field_a, field_b
    for step in range(DEPTH):
        if step:
            apply(old, new, step)
        else:
            begin(new)
        basis_out[step, :, :] = new[:, 6 * LANES : 10 * LANES]
        old, new = new, old

    sums = [jnp.zeros((8, LANES), jnp.float32) for _ in GRAM]
    for x in range(4):
        for a in range(P_SIZE):
            values = [basis_out[k, 8 * a : 8 * a + 8, x * LANES : (x + 1) * LANES] for k in range(ITERS + 1)]
            sums = [total + values[k] * values[l] for total, (k, l) in zip(sums, GRAM)]
    rows = [jnp.sum(total, axis=0, keepdims=True) for total in sums]
    rows = jnp.concatenate(rows + [jnp.zeros((24 - len(GRAM), LANES), jnp.float32)], axis=0)
    totals = jnp.sum(rows, axis=1, keepdims=True)
    place = lax.broadcasted_iota(jnp.int32, (24, LANES), 0) == lax.broadcasted_iota(jnp.int32, (24, LANES), 1)
    totals = jnp.sum(jnp.where(place, totals, 0.0), axis=0, keepdims=True)
    gram_out[...] = jnp.broadcast_to(totals, gram_out.shape)


def combine_kernel(nodes, shift_in, powers, gathered, basis_out, hess_out, amp_out):
    shift = shift_in[...]
    row = jnp.sum(gathered[...], axis=0, keepdims=True) * (1.0 / nodes)
    spread = jnp.broadcast_to(row, (8, LANES))
    gram = {}
    for at, (k, l) in enumerate(GRAM):
        gram[k, l] = gram[l, k] = jnp.broadcast_to(spread[:, at : at + 1], (8, LANES))
    sizes = [jnp.sqrt(gram[k, k]) for k in range(ITERS + 1)]
    sub = lax.broadcasted_iota(jnp.int32, (8, LANES), 0)
    lanes = lane_ids(8)
    hess = jnp.zeros((8, LANES), jnp.float32)
    beta = jnp.sqrt(gram[0, 0] + FLOOR)
    coeffs = [[1.0 / beta]]
    amp = sizes[0] * coeffs[0][0]

    def put(hess, i, j, value):
        return jnp.where((sub == i) & (lanes == j), value, hess)

    for j in range(ITERS):
        last = coeffs[j]
        image = [shift * c for c in last] + [None]
        for k in range(j + 1):
            moved = last[k] * 8.0
            image[k + 1] = moved if image[k + 1] is None else image[k + 1] + moved
        weighted = [
            sum(gram[k, l] * image[l] for l in range(1, j + 2)) + gram[k, 0] * image[0] for k in range(j + 2)
        ]
        pending = list(image)
        for i in range(j + 1):
            h = sum(c * weighted[k] for k, c in enumerate(coeffs[i]))
            hess = put(hess, i, j, h)
            for k, c in enumerate(coeffs[i]):
                pending[k] = pending[k] - h * c
        square = sum(
            pending[k] * sum(gram[k, l] * pending[l] for l in range(j + 2)) for k in range(j + 2)
        )
        beta = jnp.sqrt(jnp.maximum(square, 0.0) + FLOOR)
        hess = put(hess, j + 1, j, beta)
        scale = 1.0 / beta
        coeffs.append([p * scale for p in pending])
        amp = jnp.maximum(amp, sum(jnp.abs(c) * s for c, s in zip(coeffs[-1], sizes)))
    hess_out[...] = hess[0 : ITERS + 1, 0:ITERS]
    amp_out[...] = amp[0:1, :]
    for x in range(4):
        for a in range(P_SIZE):
            values = [powers[k, 8 * a : 8 * a + 8, x * LANES : (x + 1) * LANES] for k in range(ITERS + 1)]
            for j in range(ITERS + 1):
                total = coeffs[j][0] * values[0]
                for k in range(1, j + 1):
                    total = total + coeffs[j][k] * values[k]
                basis_out[j, pl.ds(32 * a + x, 8, stride=4), :] = total


def fast(source, initial, reaction, stiffness, line_op, face_deriv, walls):
    vmem = pl.BlockSpec(memory_space=pltpu.VMEM)
    hbm = pl.BlockSpec(memory_space=pltpu.HBM)
    grant = pltpu.CompilerParams(vmem_limit_bytes=16 * 2**20)
    f32 = jnp.float32
    nx, ny = lax.axis_size(GX), lax.axis_size(GY)
    wide = (ROWS + 2) * LANES

    def moved(value, axis, size, by):
        return lax.ppermute(value, axis, [(i, (i + by) % size) for i in range(size)])

    held = (line_op, face_deriv.reshape(1, P_SIZE), source, initial, reaction, stiffness, walls)
    raw, near, to_up, to_down, weight, shift = pl.pallas_call(
        pack_kernel,
        out_shape=[jax.ShapeDtypeStruct((n, LANES), f32) for n in (800, STRIP, NODES, NODES)]
        + [jax.ShapeDtypeStruct((NODES + 32, 6 * NODES), jnp.bfloat16), jax.ShapeDtypeStruct((8, LANES), f32)],
        in_specs=[hbm] * 7,
        out_specs=[vmem] * 6,
        scratch_shapes=[
            pltpu.VMEM((P_SIZE, P_SIZE), f32),
            pltpu.VMEM((1, P_SIZE), f32),
            pltpu.VMEM((16, LANES), jnp.int32),
            pltpu.SemaphoreType.DMA((10,)),
        ],
        compiler_params=grant,
    )(*[pltpu.with_memory_space_constraint(v, pltpu.HBM) for v in held])
    left = moved(to_up, GY, ny, 1)
    right = moved(to_down, GY, ny, -1)
    whole, high2, low2 = pl.pallas_call(
        far_kernel,
        out_shape=[jax.ShapeDtypeStruct((n, LANES), f32) for n in (STRIP + 96, 120, 120)],
        in_specs=[vmem] * 3,
        out_specs=[vmem] * 3,
        compiler_params=grant,
    )(near, left, right)
    below1 = moved(whole, GX, nx, 1)
    above1 = moved(whole, GX, nx, -1)
    below2 = moved(high2, GX, nx, 2)
    above2 = moved(low2, GX, nx, -2)

    powers, gram = pl.pallas_call(
        powers_kernel,
        out_shape=[
            jax.ShapeDtypeStruct((ITERS + 1, NODES, 4 * LANES), f32),
            jax.ShapeDtypeStruct((1, LANES), f32),
        ],
        in_specs=[vmem] * 7,
        out_specs=[vmem] * 2,
        scratch_shapes=[pltpu.VMEM((n, wide), f32) for n in (NODES, NODES, NODES + 32, NODES, 8, 32)],
        compiler_params=grant,
    )(shift, weight, whole, below1, above1, below2, above2)
    every = GX + GY
    copies = jnp.broadcast_to(gram, (nx * ny, LANES))
    gathered = lax.all_to_all(copies, every, split_axis=0, concat_axis=0, tiled=True)
    basis, hess, amp = pl.pallas_call(
        functools.partial(combine_kernel, float(NODES * 4 * nx * LANES * ny)),
        out_shape=[
            jax.ShapeDtypeStruct((ITERS + 1, 4 * NODES, LANES), f32),
            jax.ShapeDtypeStruct((ITERS + 1, ITERS), f32),
            jax.ShapeDtypeStruct((1, LANES), f32),
        ],
        in_specs=[vmem] * 3,
        out_specs=[vmem] * 3,
        compiler_params=grant,
    )(shift, powers, gathered)
    return hess, basis, amp[0, 0], raw


def body(source, initial, reaction, stiffness, line_op, face_deriv, wall_flags):
    flat = [v.reshape(4 * NODES, LANES) for v in (source, initial, reaction)]
    hess, basis, amp, raw = fast(*flat, stiffness, line_op, face_deriv, wall_flags.reshape(16, LANES))

    def again(carry):
        raw = lax.optimization_barrier(carry[3])
        initial, source, reaction = raw[0:768].reshape(3, NODES, 4, LANES)
        opened = raw[772:788].reshape(4, 4, LANES)
        line_op, face_deriv = raw[788:796, 0:P_SIZE], raw[796, 0:P_SIZE]
        hess, basis = stepwise(source, initial, reaction, raw[768:772], line_op, face_deriv, opened)
        return jnp.bool_(True), hess, basis.reshape(ITERS + 1, 4 * NODES, LANES), raw

    done = amp <= AMP_LIMIT
    carry = lax.while_loop(lambda carry: jnp.logical_not(carry[0]), again, (done, hess, basis, raw))
    return (carry[1], carry[2].reshape(ITERS + 1, NODES, 4, LANES))


def solution(mesh):
    finer = Mesh(mesh.devices.reshape(4, 2, 4, 8), ("gx_0", "gx_1", "gy_0", "gy_1"))
    placed = (
        P(None, GX, GY),
        P(None, GX, GY),
        P(None, GX, GY),
        P(GX, GY),
        P(),
        P(),
        P(None, GX, GY),
    )
    return jax.shard_map(
        body, mesh=finer, in_specs=placed, out_specs=(P(), P(None, None, GX, GY)), check_vma=False
    )
```

```python
import functools

import jax
import jax.numpy as jnp
from jax import lax
from jax.experimental import pallas as pl
from jax.experimental.pallas import tpu as pltpu
from jax.sharding import Mesh
from jax.sharding import PartitionSpec as P

P_SIZE = 8
ITERS = 5
GX = ("gx_0", "gx_1")
GY = ("gy_0", "gy_1")


TAU = 2.0
FLOOR = 0.1


def extended(array, sides, width):
    for axis, dim in sides:
        devices, length = (lax.axis_size(axis), array.shape[dim])
        up = [(i, (i + 1) % devices) for i in range(devices)]
        down = [(j, i) for i, j in up]
        last = lax.slice_in_dim(array, length - width, length, axis=dim)
        leading = lax.slice_in_dim(array, 0, width, axis=dim)
        before = lax.ppermute(last, axis, up)
        after = lax.ppermute(leading, axis, down)
        array = jnp.concatenate([before, array, after], axis=dim)
    return array


def sent_to_all(array, axis):
    copies = jnp.broadcast_to(array, (lax.axis_size(axis), *array.shape))
    return lax.all_to_all(copies, axis, split_axis=0, concat_axis=0, tiled=True)


def over_copies(array, axis):
    everything = sent_to_all(array, axis)
    return jnp.sum(everything, axis=0)


def by_axis(array, axes):
    far, near = axes
    nearer = over_copies(array, near)
    return over_copies(nearer, far)


def together(arrays, axis):
    vector, at, gathered = (jnp.concatenate([a.reshape(-1) for a in arrays]), 0, [])
    subtotal = by_axis(vector, axis)
    for a in arrays:
        gathered.append(subtotal[at : at + a.size].reshape(a.shape))
        at += a.size
    return tuple(gathered)


def local_total(values):
    return jnp.sum(jnp.sum(values, axis=0))


def x_traces(nodes, face_deriv):
    highest = lax.Precision.HIGHEST
    lower = jnp.einsum("c,cbxy->bxy", face_deriv, nodes, precision=highest)
    upper = jnp.einsum("c,cbxy->bxy", face_deriv[::-1], nodes, precision=highest)
    return jnp.stack([nodes[0], lower, nodes[-1], upper])


def y_traces(nodes, face_deriv):
    highest = lax.Precision.HIGHEST
    lower = jnp.einsum("c,acxy->axy", face_deriv, nodes, precision=highest)
    upper = jnp.einsum("c,acxy->axy", face_deriv[::-1], nodes, precision=highest)
    return jnp.stack([nodes[:, 0], lower, nodes[:, -1], upper])


def apply_op(field, reaction, stiffness, line_op, face_deriv, opened):
    highest = lax.Precision.HIGHEST
    nodes = field.reshape(P_SIZE, P_SIZE, field.shape[1], field.shape[2])
    interior = stiffness * (
        jnp.einsum("ac,cbxy->abxy", line_op, nodes, precision=highest)
        + jnp.einsum("bc,acxy->abxy", line_op, nodes, precision=highest)
    )
    xside = extended(x_traces(nodes, face_deriv), ((GX, 2),), 1)
    yside = extended(y_traces(nodes, face_deriv), ((GY, 3),), 1)
    x_own = xside[:, :, 1:-1]
    y_own = yside[:, :, :, 1:-1]
    east_nb = xside[0:2, :, 2:]
    west_nb = xside[2:4, :, :-2]
    north_nb = yside[0:2, :, :, 2:]
    south_nb = yside[2:4, :, :, :-2]
    add_east = TAU * (x_own[2] - opened[1] * east_nb[0]) + 0.5 * (x_own[3] - opened[1] * east_nb[1])
    add_west = TAU * (x_own[0] - opened[0] * west_nb[0]) + 0.5 * (x_own[1] - opened[0] * west_nb[1])
    add_north = TAU * (y_own[2] - opened[3] * north_nb[0]) + 0.5 * (
        y_own[3] - opened[3] * north_nb[1]
    )
    add_south = TAU * (y_own[0] - opened[2] * south_nb[0]) + 0.5 * (
        y_own[1] - opened[2] * south_nb[1]
    )
    result = reaction.reshape(nodes.shape) * nodes + interior
    result = result.at[0].add(add_west).at[P_SIZE - 1].add(add_east)
    result = result.at[:, 0].add(add_south).at[:, P_SIZE - 1].add(add_north)
    return result.reshape(field.shape)


def norm_scale(vector, total):
    squares = by_axis(local_total(vector * vector), (("gx_0", "gx_1"), ("gy_0", "gy_1")))
    return jnp.sqrt(squares / total + FLOOR)


def stepwise(source, initial, reaction, stiffness, line_op, face_deriv, opened):
    highest = lax.Precision.HIGHEST
    total = float(
        P_SIZE * P_SIZE * source.shape[1] * lax.axis_size(GX) * source.shape[2] * lax.axis_size(GY)
    )

    def operate(field):
        return apply_op(field, reaction, stiffness, line_op, face_deriv, opened)

    def products(basis, image):
        per_cell = jnp.einsum("kqxy,qxy->kxy", basis, image, precision=highest)
        return jnp.sum(per_cell, axis=(1, 2))

    first = source - operate(initial)
    basis = jnp.zeros((ITERS + 1,) + source.shape, jnp.float32)
    hessen = jnp.zeros((ITERS + 1, ITERS), jnp.float32)
    rows = lax.broadcasted_iota(jnp.int32, (ITERS + 1, ITERS), 0)
    cols = lax.broadcasted_iota(jnp.int32, (ITERS + 1, ITERS), 1)
    slots = lax.broadcasted_iota(jnp.int32, (ITERS + 1,), 0)

    def advance(step, carry):
        basis, hessen, pending = carry
        image = operate(pending)
        local = products(basis, image)
        projected, crossed, squares = together(
            (local, local_total(pending * image), local_total(pending * pending)),
            (("gx_0", "gx_1"), ("gy_0", "gy_1")),
        )
        beta = jnp.sqrt(squares / total + FLOOR)
        basis = lax.dynamic_update_index_in_dim(basis, pending / beta, step, 0)
        coeffs = projected / (total * beta) + jnp.where(
            slots == step, crossed / (total * beta * beta), 0.0
        )
        pending = image / beta - jnp.einsum("k,kqxy->qxy", coeffs, basis, precision=highest)
        hessen = hessen + jnp.where(cols == step, coeffs[:, None], 0.0)
        hessen = hessen + jnp.where((rows == step) & (cols == step - 1), beta, 0.0)
        return (basis, hessen, pending)

    basis, hessen, pending = lax.fori_loop(0, ITERS, advance, (basis, hessen, first))
    beta = norm_scale(pending, total)
    basis = basis.at[ITERS].set(pending / beta)
    hessen = hessen + jnp.where((rows == ITERS) & (cols == ITERS - 1), beta, 0.0)
    return (hessen, basis)


NODES = P_SIZE * P_SIZE
ROWS = 16
DEPTH = 6
LANES = 128
SCALE = 0.125
AMP_LIMIT = 100.0
GRAM = [(k, l) for k in range(ITERS + 1) for l in range(k + 1)]


def lane_ids(rows):
    return lax.broadcasted_iota(jnp.int32, (rows, LANES), 1)


def turned(value, shift):
    shift = shift % LANES
    return value if shift == 0 else pltpu.roll(value, shift, 1)


def strided(ref, start, count):
    return ref[pl.ds(start, count, stride=4), :]


BLOCK = 136
REACT, THICK, OPEN = 64, 128, 129
FIRST_WEST, LAST_EAST, ENDS = 544, 552, 560


def split(value):
    high = value.astype(jnp.bfloat16)
    rest = value - high.astype(jnp.float32)
    middle = rest.astype(jnp.bfloat16)
    low = (rest - middle.astype(jnp.float32)).astype(jnp.bfloat16)
    return high, middle, low


def weights_in(line, deriv):
    sub = lax.broadcasted_iota(jnp.int32, (8, NODES), 0)
    lane = lax.broadcasted_iota(jnp.int32, (8, NODES), 1)
    along, across = lane // 8, lane % 8
    outer = jnp.zeros((8, NODES), jnp.float32)
    inner = jnp.zeros((8, NODES), jnp.float32)
    for c in range(P_SIZE):
        column = jnp.broadcast_to(line[:, c : c + 1], (8, NODES))
        outer = jnp.where(along == c, column, outer)
        inner = jnp.where(across == c, column, inner)
    parts = []
    for a in range(P_SIZE):
        row = jnp.broadcast_to(outer[a : a + 1, :], (8, NODES))
        parts.append(jnp.where(across == sub, row, 0.0) + jnp.where(along == a, inner, 0.0))
    for first, second in ((along, across), (across, along)):
        for flip in (False, True):
            part = jnp.zeros((8, NODES), jnp.float32)
            for c in range(P_SIZE):
                value = SCALE * (0.5 * deriv[0:1, c : c + 1] + (TAU if c == 0 else 0.0))
                part = jnp.where(first == (P_SIZE - 1 - c if flip else c), value, part)
            parts.append(jnp.where(second == sub, part, 0.0))
    high, middle, low = split(jnp.concatenate(parts, axis=0))
    return jnp.concatenate([high, high, high, middle, middle, low], axis=1)


def product(weight, value):
    high, middle, low = split(value)
    stacked = jnp.concatenate([high, middle, low, high, middle, high], axis=0)
    return jnp.dot(weight[...], stacked, preferred_element_type=jnp.float32)


def centre(line, deriv):
    diagonal = lax.broadcasted_iota(jnp.int32, (8, 8), 0) == lax.broadcasted_iota(jnp.int32, (8, 8), 1)
    trace = jnp.sum(jnp.where(diagonal, line, 0.0), axis=1, keepdims=True)
    trace = jnp.sum(trace, axis=0, keepdims=True)
    return 2.0 + 0.3125 * trace + 0.5 * (TAU + 0.5 * deriv[0:1, 0:1])


def edges(a, west, east, south, north, sub):
    value = jnp.where(sub == 0, south[a : a + 1, :], 0.0)
    value = jnp.where(sub == P_SIZE - 1, north[a : a + 1, :], value)
    if a == 0 and west is not None:
        value = value + west
    if a == P_SIZE - 1 and east is not None:
        value = value + east
    return value


def pack_kernel(
    line_in, deriv_in, source, initial, reaction, stiffness, walls,
    raw, near, to_up, to_down, weight, shift_out, line, deriv, flags, sems,
):
    moves = [(line_in, line), (deriv_in, deriv)]
    for at, ref in ((0, initial), (256, source), (512, reaction)):
        for half in (0, 128):
            moves.append((ref.at[pl.ds(half, 128), :], raw.at[pl.ds(at + half, 128), :]))
    moves.append((stiffness, raw.at[pl.ds(768, 4), :]))
    moves.append((walls, flags))
    copies = [pltpu.make_async_copy(a, b, sems.at[n]) for n, (a, b) in enumerate(moves)]
    for copy in copies:
        copy.start()
    for copy in copies[:2]:
        copy.wait()
    line, deriv = line[...], deriv[...]
    weight[...] = weights_in(line, deriv)
    shift_out[...] = jnp.broadcast_to(centre(line, deriv), (8, LANES))
    for copy in copies[2:4]:
        copy.wait()
    sub = lax.broadcasted_iota(jnp.int32, (8, LANES), 0)
    lanes8 = lane_ids(8)
    fields, images = [], []
    for x in range(0, 4, 2):
        pair = jnp.concatenate([strided(raw, x, NODES), strided(raw, x + 1, NODES)], axis=1)
        image = product(weight, pair)
        for k in range(2):
            fields.append(pair[:, k * LANES : (k + 1) * LANES])
            images.append(image[:, k * LANES : (k + 1) * LANES])
    for copy in copies[4:]:
        copy.wait()
    opened = 1.0 - flags[...].astype(jnp.float32)
    raw[772:788, :] = opened
    raw[788:796, 0:P_SIZE] = line
    raw[796:797, 0:P_SIZE] = deriv
    thick = raw[768:772, :]
    traces = [[image[64 + 8 * f : 72 + 8 * f] for f in range(4)] for image in images]
    ends = jnp.zeros((8, LANES), jnp.float32)
    for x in range(4):
        at = BLOCK * x
        allowed = [jnp.broadcast_to(opened[4 * f + x : 4 * f + x + 1, :], (8, LANES)) for f in range(4)]
        faces = list(traces[x])
        if x > 0:
            faces[0] = faces[0] - allowed[0] * traces[x - 1][1]
        if x < 3:
            faces[1] = faces[1] - allowed[1] * traces[x + 1][0]
        faces[2] = faces[2] - allowed[2] * jnp.where(lanes8 == 0, 0.0, turned(traces[x][3], 1))
        faces[3] = faces[3] - allowed[3] * jnp.where(lanes8 == LANES - 1, 0.0, turned(traces[x][2], -1))
        faces = [8.0 * face for face in faces]
        ends = jnp.where(lanes8 == 8 * x + 7, turned(traces[x][2], 8 * x + 7), ends)
        ends = jnp.where(lanes8 == 8 * x, turned(traces[x][3], 8 * x + 1), ends)
        width = jnp.broadcast_to(thick[x : x + 1, :], (8, LANES))
        for a in range(P_SIZE):
            rows = slice(8 * a, 8 * a + 8)
            value = strided(raw, 512 + 32 * a + x, 8) * fields[x][rows] + width * images[x][rows]
            value = value + edges(a, *faces, sub)
            near[at + 8 * a : at + 8 * a + 8, :] = strided(raw, 256 + 32 * a + x, 8) - value
        near[at + REACT : at + THICK, :] = strided(raw, 512 + x, NODES)
        rows = [thick[x : x + 1, :]] + [opened[4 * f + x : 4 * f + x + 1, :] for f in range(4)]
        near[at + THICK : at + BLOCK, :] = jnp.concatenate(rows + [jnp.zeros((3, LANES), jnp.float32)], axis=0)
    near[FIRST_WEST:LAST_EAST, :] = traces[0][0]
    near[LAST_EAST:ENDS, :] = traces[3][1]
    near[ENDS : ENDS + 8, :] = ends
    lanes = lane_ids(NODES)
    for out, first in ((to_up, 120), (to_down, 0)):
        totals = [jnp.zeros((n, LANES), jnp.float32) for n in (NODES, 32, 8)]
        for x in range(4):
            block = BLOCK * x
            parts = (
                (0, near[block : block + 64, :]),
                (0, near[block + REACT : block + THICK, :]),
                (1, jnp.concatenate(traces[x], axis=0)),
                (2, near[block + THICK : block + BLOCK, :]),
            )
            for field, (part, value) in enumerate(parts):
                at = 32 * field + 8 * x
                ids = lanes[0 : value.shape[0]]
                totals[part] = jnp.where((ids >= at) & (ids < at + 8), turned(value, at - first), totals[part])
        out[0:8, :] = totals[0][0:8] + totals[1][0:8] + totals[2]
        out[8:32, :] = totals[0][8:32] + totals[1][8:32]
        out[32:64, :] = totals[0][32:64]


def far_kernel(near, left, right, strip, high2, low2):
    lanes = lane_ids(NODES)
    strip[0:64, :] = jnp.where(lanes < 64, left[...], turned(right[...], 64))
    lanes = lanes[0:32]
    edge = jnp.where(lanes < 32, turned(left[0:32, :], -64), turned(right[0:32, :], -32))
    edge = jnp.where((lanes >= 64) & (lanes < 96), turned(left[0:32, :], -32), edge)
    edge = jnp.where(lanes >= 96, right[0:32, :], edge)
    strip[64:96, :] = edge
    for out, close, face in ((high2, 3, LAST_EAST), (low2, 0, FIRST_WEST)):
        block = BLOCK * close
        out[0:64, :] = near[block : block + 64, :]
        out[64:72, :] = near[block + THICK : block + BLOCK, :]
        out[72:80, :] = near[face : face + 8, :]
        out[80:88, :] = near[ENDS : ENDS + 8, :]
        out[88:120, :] = edge


def powers_kernel(
    shift_in, weight, near, below1, above1, below2, above2, own_strip, strip_b1, strip_a1,
    basis_out, gram_out, field_a, field_b, image, react, stiff, opened,
):
    shift = shift_in[0:1, :]

    def put(row, value_reaction, value_stiffness, value_open):
        cols = slice(row * LANES, (row + 1) * LANES)
        if value_reaction is not None:
            react[:, cols] = (value_reaction - shift) * SCALE
            stiff[:, cols] = jnp.broadcast_to(value_stiffness * SCALE, (8, LANES))
        for f in range(4):
            opened[8 * f : 8 * f + 8, cols] = jnp.broadcast_to(value_open[f], (8, LANES))

    local = {}
    for x in range(4):
        for ref, row in ((below1, 2 + x), (near, 6 + x), (above1, 10 + x)):
            at = BLOCK * x
            put(
                row, ref[at + REACT : at + THICK, :], ref[at + THICK : at + OPEN, :],
                [ref[at + OPEN + f : at + OPEN + f + 1, :] for f in range(4)],
            )
            local[row] = functools.partial(lambda ref, at, a: ref[at + 8 * a : at + 8 * a + 8, :], ref, at)
    for row, ref in ((1, below2), (ROWS - 2, above2)):
        put(row, None, None, [ref[65 + f : 66 + f, :] for f in range(4)])
        local[row] = functools.partial(lambda ref, a: ref[8 * a : 8 * a + 8, :], ref)

    lanes64 = lane_ids(NODES)
    lanes = lane_ids(8)
    pieces = ((strip_b1, 16, 48, 16), (own_strip, 48, 80, 48), (strip_a1, 80, 112, 80))
    strip_faces = []
    for side in range(2):
        made = []
        for top, count, zero in ((0, 64, 64 * side), (0, 64, 64 * side + 32), (64, 32, 32 * side), (64, 8, 64 + 32 * side)):
            ids = lanes64[0:count]
            value = jnp.zeros((count, LANES), jnp.float32)
            for ref, start, stop, target in pieces:
                part = turned(ref[top : top + count, :], target - zero)
                value = jnp.where((ids >= start) & (ids < stop), part, value)
            if count == 32:
                value = jnp.where(ids < 16, turned(below2[88:120, :], -16 - 32 * side), value)
                value = jnp.where(ids >= 112, turned(above2[88:120, :], 112 - 32 * side), value)
            made.append(value)
        put(ROWS + side, made[1], made[3][0:1], [made[3][1 + f : 2 + f] for f in range(4)])
        local[ROWS + side] = functools.partial(lambda value, a: value[8 * a : 8 * a + 8], made[0])
        strip_faces.append([made[2][8 * f : 8 * f + 8] for f in range(4)])
    ends = jnp.zeros((8, LANES), jnp.float32)
    for ref, top, start, stop, by in (
        (below2, 80, 0, 16, -16), (below1, ENDS, 16, 48, 16), (near, ENDS, 48, 80, 48),
        (above1, ENDS, 80, 112, 80), (above2, 80, 112, 128, 112),
    ):
        ends = jnp.where((lanes >= start) & (lanes < stop), turned(ref[top : top + 8, :], by), ends)

    def columns(row):
        return slice(row * LANES, (row + 1) * LANES)

    low, high = ROWS, ROWS + 1
    sub = lax.broadcasted_iota(jnp.int32, (8, LANES), 0)
    TW, TE, TS, TN = (slice(64 + 8 * f, 72 + 8 * f) for f in range(4))

    def begin(new):
        def finish(row, faces):
            cols = columns(row)
            faces = [
                None if value is None else 8.0 * opened[8 * f : 8 * f + 8, cols] * value
                for f, value in enumerate(faces)
            ]
            for a in range(P_SIZE):
                new[8 * a : 8 * a + 8, cols] = local[row](a) + edges(a, *faces, sub)

        west = {
            2: below2[72:80, :], 6: below1[LAST_EAST:ENDS, :], 10: near[LAST_EAST:ENDS, :],
            14: above1[LAST_EAST:ENDS, :],
        }
        east = {
            1: below1[FIRST_WEST:LAST_EAST, :], 5: near[FIRST_WEST:LAST_EAST, :],
            9: above1[FIRST_WEST:LAST_EAST, :], 13: above2[72:80, :],
        }
        for row in range(1, ROWS - 1):
            south = jnp.where(lanes == 0, turned(strip_faces[0][3], -(8 * row + 7)), 0.0)
            north = jnp.where(lanes == LANES - 1, turned(strip_faces[1][2], 127 - 8 * row), 0.0)
            finish(row, (west.get(row), east.get(row), south, north))
        none = jnp.zeros((8, LANES), jnp.float32)
        spot = lanes // 8 % 4
        for side in range(2):
            from_west = jnp.where(spot == 2, turned(strip_faces[side][1], 8), 0.0)
            from_east = jnp.where(spot == 1, turned(strip_faces[side][0], -8), 0.0)
            outer = jnp.where(lanes % 8 == (0 if side else 7), ends, 0.0)
            finish(ROWS + side, (from_west, from_east, outer if side else none, none if side else outer))

    def apply(old, new, step):
        start, stop = step, ROWS - step
        for first_row, last_row in ((start, stop), (ROWS, ROWS + 2)):
            for row in range(first_row, last_row, 2):
                cols = slice(row * LANES, (row + 2) * LANES)
                image[:, cols] = product(weight, old[:, cols])

        def finish(row, *sides):
            cols = columns(row)
            faces = [
                image[own, cols] - opened[8 * f : 8 * f + 8, cols] * value
                for f, (own, value) in enumerate(zip((TW, TE, TS, TN), sides))
            ]
            for a in range(P_SIZE):
                rows = slice(8 * a, 8 * a + 8)
                value = react[rows, cols] * old[rows, cols] + stiff[:, cols] * image[rows, cols]
                new[rows, cols] = value + edges(a, *faces, sub)

        north_low = image[TN, columns(low)]
        south_high = image[TS, columns(high)]
        for row in range(start + 1, stop - 1):
            cols = columns(row)
            from_south = jnp.where(
                lanes == 0, turned(north_low, -(8 * row + 7)), turned(image[TN, cols], 1)
            )
            from_north = jnp.where(
                lanes == LANES - 1, turned(south_high, 127 - 8 * row), turned(image[TS, cols], -1)
            )
            finish(row, image[TE, columns(row - 1)], image[TW, columns(row + 1)], from_south, from_north)
        if step == DEPTH - 1:
            return
        to_low = turned(image[TS, columns(low)], -1)
        to_high = turned(image[TN, columns(high)], 1)
        for row in range(start, stop):
            cols = columns(row)
            to_low = jnp.where(lanes == 8 * row + 7, turned(image[TS, cols], 8 * row + 7), to_low)
            to_high = jnp.where(lanes == 8 * row, turned(image[TN, cols], 8 * row + 1), to_high)
        cols = columns(low)
        finish(low, turned(image[TE, cols], 8), turned(image[TW, cols], -8), turned(image[TN, cols], 1), to_low)
        cols = columns(high)
        finish(high, turned(image[TE, cols], 8), turned(image[TW, cols], -8), to_high, turned(image[TS, cols], -1))

    old, new = field_a, field_b
    for step in range(DEPTH):
        if step:
            apply(old, new, step)
        else:
            begin(new)
        basis_out[step, :, :] = new[:, 6 * LANES : 10 * LANES]
        old, new = new, old

    sums = [jnp.zeros((8, LANES), jnp.float32) for _ in GRAM]
    for x in range(4):
        for a in range(P_SIZE):
            values = [basis_out[k, 8 * a : 8 * a + 8, x * LANES : (x + 1) * LANES] for k in range(ITERS + 1)]
            sums = [total + values[k] * values[l] for total, (k, l) in zip(sums, GRAM)]
    rows = [jnp.sum(total, axis=0, keepdims=True) for total in sums]
    rows = jnp.concatenate(rows + [jnp.zeros((24 - len(GRAM), LANES), jnp.float32)], axis=0)
    totals = jnp.sum(rows, axis=1, keepdims=True)
    place = lax.broadcasted_iota(jnp.int32, (24, LANES), 0) == lax.broadcasted_iota(jnp.int32, (24, LANES), 1)
    totals = jnp.sum(jnp.where(place, totals, 0.0), axis=0, keepdims=True)
    gram_out[...] = jnp.broadcast_to(totals, gram_out.shape)


def combine_kernel(nodes, shift_in, powers, gathered, basis_out, hess_out, amp_out):
    shift = shift_in[...]
    row = jnp.sum(gathered[...], axis=0, keepdims=True) * (1.0 / nodes)
    spread = jnp.broadcast_to(row, (8, LANES))
    gram = {}
    for at, (k, l) in enumerate(GRAM):
        gram[k, l] = gram[l, k] = jnp.broadcast_to(spread[:, at : at + 1], (8, LANES))
    sizes = [jnp.sqrt(gram[k, k]) for k in range(ITERS + 1)]
    sub = lax.broadcasted_iota(jnp.int32, (8, LANES), 0)
    lanes = lane_ids(8)
    hess = jnp.zeros((8, LANES), jnp.float32)
    beta = jnp.sqrt(gram[0, 0] + FLOOR)
    coeffs = [[1.0 / beta]]
    amp = sizes[0] * coeffs[0][0]

    def put(hess, i, j, value):
        return jnp.where((sub == i) & (lanes == j), value, hess)

    for j in range(ITERS):
        last = coeffs[j]
        image = [shift * c for c in last] + [None]
        for k in range(j + 1):
            moved = last[k] * 8.0
            image[k + 1] = moved if image[k + 1] is None else image[k + 1] + moved
        weighted = [
            sum(gram[k, l] * image[l] for l in range(1, j + 2)) + gram[k, 0] * image[0] for k in range(j + 2)
        ]
        pending = list(image)
        for i in range(j + 1):
            h = sum(c * weighted[k] for k, c in enumerate(coeffs[i]))
            hess = put(hess, i, j, h)
            for k, c in enumerate(coeffs[i]):
                pending[k] = pending[k] - h * c
        square = sum(
            pending[k] * sum(gram[k, l] * pending[l] for l in range(j + 2)) for k in range(j + 2)
        )
        beta = jnp.sqrt(jnp.maximum(square, 0.0) + FLOOR)
        hess = put(hess, j + 1, j, beta)
        scale = 1.0 / beta
        coeffs.append([p * scale for p in pending])
        amp = jnp.maximum(amp, sum(jnp.abs(c) * s for c, s in zip(coeffs[-1], sizes)))
    hess_out[...] = hess[0 : ITERS + 1, 0:ITERS]
    amp_out[...] = amp[0:1, :]
    for x in range(4):
        for a in range(P_SIZE):
            values = [powers[k, 8 * a : 8 * a + 8, x * LANES : (x + 1) * LANES] for k in range(ITERS + 1)]
            for j in range(ITERS + 1):
                total = coeffs[j][0] * values[0]
                for k in range(1, j + 1):
                    total = total + coeffs[j][k] * values[k]
                basis_out[j, pl.ds(32 * a + x, 8, stride=4), :] = total


def fast(source, initial, reaction, stiffness, line_op, face_deriv, walls):
    vmem = pl.BlockSpec(memory_space=pltpu.VMEM)
    hbm = pl.BlockSpec(memory_space=pltpu.HBM)
    grant = pltpu.CompilerParams(vmem_limit_bytes=16 * 2**20)
    f32 = jnp.float32
    nx, ny = lax.axis_size(GX), lax.axis_size(GY)
    wide = (ROWS + 2) * LANES

    def moved(value, axis, size, by):
        return lax.ppermute(value, axis, [(i, (i + by) % size) for i in range(size)])

    held = (line_op, face_deriv.reshape(1, P_SIZE), source, initial, reaction, stiffness, walls)
    raw, near, to_up, to_down, weight, shift = pl.pallas_call(
        pack_kernel,
        out_shape=[jax.ShapeDtypeStruct((n, LANES), f32) for n in (800, ENDS + 8, NODES, NODES)]
        + [jax.ShapeDtypeStruct((NODES + 32, 6 * NODES), jnp.bfloat16), jax.ShapeDtypeStruct((8, LANES), f32)],
        in_specs=[hbm] * 7,
        out_specs=[vmem] * 6,
        scratch_shapes=[
            pltpu.VMEM((P_SIZE, P_SIZE), f32),
            pltpu.VMEM((1, P_SIZE), f32),
            pltpu.VMEM((16, LANES), jnp.int32),
            pltpu.SemaphoreType.DMA((10,)),
        ],
        compiler_params=grant,
    )(*[pltpu.with_memory_space_constraint(v, pltpu.HBM) for v in held])
    left = moved(to_up, GY, ny, 1)
    right = moved(to_down, GY, ny, -1)
    below1 = moved(near, GX, nx, 1)
    above1 = moved(near, GX, nx, -1)
    strip, high2, low2 = pl.pallas_call(
        far_kernel,
        out_shape=[jax.ShapeDtypeStruct((n, LANES), f32) for n in (96, 120, 120)],
        in_specs=[vmem] * 3,
        out_specs=[vmem] * 3,
        compiler_params=grant,
    )(near, left, right)
    strip_b1 = moved(strip, GX, nx, 1)
    strip_a1 = moved(strip, GX, nx, -1)
    below2 = moved(high2, GX, nx, 2)
    above2 = moved(low2, GX, nx, -2)

    powers, gram = pl.pallas_call(
        powers_kernel,
        out_shape=[
            jax.ShapeDtypeStruct((ITERS + 1, NODES, 4 * LANES), f32),
            jax.ShapeDtypeStruct((1, LANES), f32),
        ],
        in_specs=[vmem] * 10,
        out_specs=[vmem] * 2,
        scratch_shapes=[pltpu.VMEM((n, wide), f32) for n in (NODES, NODES, NODES + 32, NODES, 8, 32)],
        compiler_params=grant,
    )(shift, weight, near, below1, above1, below2, above2, strip, strip_b1, strip_a1)
    every = GX + GY
    copies = jnp.broadcast_to(gram, (nx * ny, LANES))
    gathered = lax.all_to_all(copies, every, split_axis=0, concat_axis=0, tiled=True)
    basis, hess, amp = pl.pallas_call(
        functools.partial(combine_kernel, float(NODES * 4 * nx * LANES * ny)),
        out_shape=[
            jax.ShapeDtypeStruct((ITERS + 1, 4 * NODES, LANES), f32),
            jax.ShapeDtypeStruct((ITERS + 1, ITERS), f32),
            jax.ShapeDtypeStruct((1, LANES), f32),
        ],
        in_specs=[vmem] * 3,
        out_specs=[vmem] * 3,
        compiler_params=grant,
    )(shift, powers, gathered)
    return hess, basis, amp[0, 0], raw


def body(source, initial, reaction, stiffness, line_op, face_deriv, wall_flags):
    flat = [v.reshape(4 * NODES, LANES) for v in (source, initial, reaction)]
    hess, basis, amp, raw = fast(*flat, stiffness, line_op, face_deriv, wall_flags.reshape(16, LANES))

    def again(carry):
        raw = lax.optimization_barrier(carry[3])
        initial, source, reaction = raw[0:768].reshape(3, NODES, 4, LANES)
        opened = raw[772:788].reshape(4, 4, LANES)
        line_op, face_deriv = raw[788:796, 0:P_SIZE], raw[796, 0:P_SIZE]
        hess, basis = stepwise(source, initial, reaction, raw[768:772], line_op, face_deriv, opened)
        return jnp.bool_(True), hess, basis.reshape(ITERS + 1, 4 * NODES, LANES), raw

    done = amp <= AMP_LIMIT
    carry = lax.while_loop(lambda carry: jnp.logical_not(carry[0]), again, (done, hess, basis, raw))
    return (carry[1], carry[2].reshape(ITERS + 1, NODES, 4, LANES))


def solution(mesh):
    finer = Mesh(mesh.devices.reshape(4, 2, 4, 8), ("gx_0", "gx_1", "gy_0", "gy_1"))
    placed = (
        P(None, GX, GY),
        P(None, GX, GY),
        P(None, GX, GY),
        P(GX, GY),
        P(),
        P(),
        P(None, GX, GY),
    )
    return jax.shard_map(
        body, mesh=finer, in_specs=placed, out_specs=(P(), P(None, None, GX, GY)), check_vma=False
    )
```

```python
import functools

import jax
import jax.numpy as jnp
from jax import lax
from jax.experimental import pallas as pl
from jax.experimental.pallas import tpu as pltpu
from jax.sharding import Mesh
from jax.sharding import PartitionSpec as P

P_SIZE = 8
ITERS = 5
GX = ("gx_0", "gx_1")
GY = ("gy_0", "gy_1")


TAU = 2.0
FLOOR = 0.1


def extended(array, sides, width):
    for axis, dim in sides:
        devices, length = (lax.axis_size(axis), array.shape[dim])
        up = [(i, (i + 1) % devices) for i in range(devices)]
        down = [(j, i) for i, j in up]
        last = lax.slice_in_dim(array, length - width, length, axis=dim)
        leading = lax.slice_in_dim(array, 0, width, axis=dim)
        before = lax.ppermute(last, axis, up)
        after = lax.ppermute(leading, axis, down)
        array = jnp.concatenate([before, array, after], axis=dim)
    return array


def sent_to_all(array, axis):
    copies = jnp.broadcast_to(array, (lax.axis_size(axis), *array.shape))
    return lax.all_to_all(copies, axis, split_axis=0, concat_axis=0, tiled=True)


def over_copies(array, axis):
    everything = sent_to_all(array, axis)
    return jnp.sum(everything, axis=0)


def by_axis(array, axes):
    far, near = axes
    nearer = over_copies(array, near)
    return over_copies(nearer, far)


def together(arrays, axis):
    vector, at, gathered = (jnp.concatenate([a.reshape(-1) for a in arrays]), 0, [])
    subtotal = by_axis(vector, axis)
    for a in arrays:
        gathered.append(subtotal[at : at + a.size].reshape(a.shape))
        at += a.size
    return tuple(gathered)


def local_total(values):
    return jnp.sum(jnp.sum(values, axis=0))


def x_traces(nodes, face_deriv):
    highest = lax.Precision.HIGHEST
    lower = jnp.einsum("c,cbxy->bxy", face_deriv, nodes, precision=highest)
    upper = jnp.einsum("c,cbxy->bxy", face_deriv[::-1], nodes, precision=highest)
    return jnp.stack([nodes[0], lower, nodes[-1], upper])


def y_traces(nodes, face_deriv):
    highest = lax.Precision.HIGHEST
    lower = jnp.einsum("c,acxy->axy", face_deriv, nodes, precision=highest)
    upper = jnp.einsum("c,acxy->axy", face_deriv[::-1], nodes, precision=highest)
    return jnp.stack([nodes[:, 0], lower, nodes[:, -1], upper])


def apply_op(field, reaction, stiffness, line_op, face_deriv, opened):
    highest = lax.Precision.HIGHEST
    nodes = field.reshape(P_SIZE, P_SIZE, field.shape[1], field.shape[2])
    interior = stiffness * (
        jnp.einsum("ac,cbxy->abxy", line_op, nodes, precision=highest)
        + jnp.einsum("bc,acxy->abxy", line_op, nodes, precision=highest)
    )
    xside = extended(x_traces(nodes, face_deriv), ((GX, 2),), 1)
    yside = extended(y_traces(nodes, face_deriv), ((GY, 3),), 1)
    x_own = xside[:, :, 1:-1]
    y_own = yside[:, :, :, 1:-1]
    east_nb = xside[0:2, :, 2:]
    west_nb = xside[2:4, :, :-2]
    north_nb = yside[0:2, :, :, 2:]
    south_nb = yside[2:4, :, :, :-2]
    add_east = TAU * (x_own[2] - opened[1] * east_nb[0]) + 0.5 * (x_own[3] - opened[1] * east_nb[1])
    add_west = TAU * (x_own[0] - opened[0] * west_nb[0]) + 0.5 * (x_own[1] - opened[0] * west_nb[1])
    add_north = TAU * (y_own[2] - opened[3] * north_nb[0]) + 0.5 * (
        y_own[3] - opened[3] * north_nb[1]
    )
    add_south = TAU * (y_own[0] - opened[2] * south_nb[0]) + 0.5 * (
        y_own[1] - opened[2] * south_nb[1]
    )
    result = reaction.reshape(nodes.shape) * nodes + interior
    result = result.at[0].add(add_west).at[P_SIZE - 1].add(add_east)
    result = result.at[:, 0].add(add_south).at[:, P_SIZE - 1].add(add_north)
    return result.reshape(field.shape)


def norm_scale(vector, total):
    squares = by_axis(local_total(vector * vector), (("gx_0", "gx_1"), ("gy_0", "gy_1")))
    return jnp.sqrt(squares / total + FLOOR)


def stepwise(source, initial, reaction, stiffness, line_op, face_deriv, opened):
    highest = lax.Precision.HIGHEST
    total = float(
        P_SIZE * P_SIZE * source.shape[1] * lax.axis_size(GX) * source.shape[2] * lax.axis_size(GY)
    )

    def operate(field):
        return apply_op(field, reaction, stiffness, line_op, face_deriv, opened)

    def products(basis, image):
        per_cell = jnp.einsum("kqxy,qxy->kxy", basis, image, precision=highest)
        return jnp.sum(per_cell, axis=(1, 2))

    first = source - operate(initial)
    basis = jnp.zeros((ITERS + 1,) + source.shape, jnp.float32)
    hessen = jnp.zeros((ITERS + 1, ITERS), jnp.float32)
    rows = lax.broadcasted_iota(jnp.int32, (ITERS + 1, ITERS), 0)
    cols = lax.broadcasted_iota(jnp.int32, (ITERS + 1, ITERS), 1)
    slots = lax.broadcasted_iota(jnp.int32, (ITERS + 1,), 0)

    def advance(step, carry):
        basis, hessen, pending = carry
        image = operate(pending)
        local = products(basis, image)
        projected, crossed, squares = together(
            (local, local_total(pending * image), local_total(pending * pending)),
            (("gx_0", "gx_1"), ("gy_0", "gy_1")),
        )
        beta = jnp.sqrt(squares / total + FLOOR)
        basis = lax.dynamic_update_index_in_dim(basis, pending / beta, step, 0)
        coeffs = projected / (total * beta) + jnp.where(
            slots == step, crossed / (total * beta * beta), 0.0
        )
        pending = image / beta - jnp.einsum("k,kqxy->qxy", coeffs, basis, precision=highest)
        hessen = hessen + jnp.where(cols == step, coeffs[:, None], 0.0)
        hessen = hessen + jnp.where((rows == step) & (cols == step - 1), beta, 0.0)
        return (basis, hessen, pending)

    basis, hessen, pending = lax.fori_loop(0, ITERS, advance, (basis, hessen, first))
    beta = norm_scale(pending, total)
    basis = basis.at[ITERS].set(pending / beta)
    hessen = hessen + jnp.where((rows == ITERS) & (cols == ITERS - 1), beta, 0.0)
    return (hessen, basis)


NODES = P_SIZE * P_SIZE
ROWS = 16
DEPTH = 6
LANES = 128
SCALE = 0.125
AMP_LIMIT = 100.0
GRAM = [(k, l) for k in range(ITERS + 1) for l in range(k + 1)]


def lane_ids(rows):
    return lax.broadcasted_iota(jnp.int32, (rows, LANES), 1)


def turned(value, shift):
    shift = shift % LANES
    return value if shift == 0 else pltpu.roll(value, shift, 1)


def strided(ref, start, count):
    return ref[pl.ds(start, count, stride=4), :]


BLOCK = 136
REACT, THICK, OPEN = 64, 128, 129
FIRST_WEST, LAST_EAST, ENDS = 544, 552, 560


def split(value):
    high = value.astype(jnp.bfloat16)
    rest = value - high.astype(jnp.float32)
    middle = rest.astype(jnp.bfloat16)
    low = (rest - middle.astype(jnp.float32)).astype(jnp.bfloat16)
    return high, middle, low


def weights_in(line, deriv):
    sub = lax.broadcasted_iota(jnp.int32, (8, NODES), 0)
    lane = lax.broadcasted_iota(jnp.int32, (8, NODES), 1)
    along, across = lane // 8, lane % 8
    outer = jnp.zeros((8, NODES), jnp.float32)
    inner = jnp.zeros((8, NODES), jnp.float32)
    for c in range(P_SIZE):
        column = jnp.broadcast_to(line[:, c : c + 1], (8, NODES))
        outer = jnp.where(along == c, column, outer)
        inner = jnp.where(across == c, column, inner)
    parts = []
    for a in range(P_SIZE):
        row = jnp.broadcast_to(outer[a : a + 1, :], (8, NODES))
        parts.append(jnp.where(across == sub, row, 0.0) + jnp.where(along == a, inner, 0.0))
    for first, second in ((along, across), (across, along)):
        for flip in (False, True):
            part = jnp.zeros((8, NODES), jnp.float32)
            for c in range(P_SIZE):
                value = SCALE * (0.5 * deriv[0:1, c : c + 1] + (TAU if c == 0 else 0.0))
                part = jnp.where(first == (P_SIZE - 1 - c if flip else c), value, part)
            parts.append(jnp.where(second == sub, part, 0.0))
    high, middle, low = split(jnp.concatenate(parts, axis=0))
    return jnp.concatenate([high, high, high, middle, middle, low], axis=1)


def product(weight, value):
    high, middle, low = split(value)
    stacked = jnp.concatenate([high, middle, low, high, middle, high], axis=0)
    return jnp.dot(weight[...], stacked, preferred_element_type=jnp.float32)


def centre(line, deriv):
    diagonal = lax.broadcasted_iota(jnp.int32, (8, 8), 0) == lax.broadcasted_iota(jnp.int32, (8, 8), 1)
    trace = jnp.sum(jnp.where(diagonal, line, 0.0), axis=1, keepdims=True)
    trace = jnp.sum(trace, axis=0, keepdims=True)
    return 2.0 + 0.3125 * trace + 0.5 * (TAU + 0.5 * deriv[0:1, 0:1])


def edges(a, west, east, south, north, sub):
    value = jnp.where(sub == 0, south[a : a + 1, :], 0.0)
    value = jnp.where(sub == P_SIZE - 1, north[a : a + 1, :], value)
    if a == 0 and west is not None:
        value = value + west
    if a == P_SIZE - 1 and east is not None:
        value = value + east
    return value


def pack_kernel(
    line_in, deriv_in, source, initial, reaction, stiffness, walls,
    raw, near, to_up, to_down, weight, shift_out, line, deriv, flags, sems,
):
    moves = [(line_in, line), (deriv_in, deriv)]
    for at, ref in ((0, initial), (256, source), (512, reaction)):
        for half in (0, 128):
            moves.append((ref.at[pl.ds(half, 128), :], raw.at[pl.ds(at + half, 128), :]))
    moves.append((stiffness, raw.at[pl.ds(768, 4), :]))
    moves.append((walls, flags))
    copies = [pltpu.make_async_copy(a, b, sems.at[n]) for n, (a, b) in enumerate(moves)]
    for copy in copies:
        copy.start()
    for copy in copies[:2]:
        copy.wait()
    line, deriv = line[...], deriv[...]
    weight[...] = weights_in(line, deriv)
    shift_out[...] = jnp.broadcast_to(centre(line, deriv), (8, LANES))
    for copy in copies[2:4]:
        copy.wait()
    sub = lax.broadcasted_iota(jnp.int32, (8, LANES), 0)
    lanes8 = lane_ids(8)
    fields, images = [], []
    for x in range(0, 4, 2):
        pair = jnp.concatenate([strided(raw, x, NODES), strided(raw, x + 1, NODES)], axis=1)
        image = product(weight, pair)
        for k in range(2):
            fields.append(pair[:, k * LANES : (k + 1) * LANES])
            images.append(image[:, k * LANES : (k + 1) * LANES])
    for copy in copies[4:]:
        copy.wait()
    opened = 1.0 - flags[...].astype(jnp.float32)
    raw[772:788, :] = opened
    raw[788:796, 0:P_SIZE] = line
    raw[796:797, 0:P_SIZE] = deriv
    thick = raw[768:772, :]
    traces = [[image[64 + 8 * f : 72 + 8 * f] for f in range(4)] for image in images]
    ends = jnp.zeros((8, LANES), jnp.float32)
    for x in range(4):
        at = BLOCK * x
        allowed = [jnp.broadcast_to(opened[4 * f + x : 4 * f + x + 1, :], (8, LANES)) for f in range(4)]
        faces = list(traces[x])
        if x > 0:
            faces[0] = faces[0] - allowed[0] * traces[x - 1][1]
        if x < 3:
            faces[1] = faces[1] - allowed[1] * traces[x + 1][0]
        faces[2] = faces[2] - allowed[2] * jnp.where(lanes8 == 0, 0.0, turned(traces[x][3], 1))
        faces[3] = faces[3] - allowed[3] * jnp.where(lanes8 == LANES - 1, 0.0, turned(traces[x][2], -1))
        faces = [8.0 * face for face in faces]
        ends = jnp.where(lanes8 == 8 * x + 7, turned(traces[x][2], 8 * x + 7), ends)
        ends = jnp.where(lanes8 == 8 * x, turned(traces[x][3], 8 * x + 1), ends)
        width = jnp.broadcast_to(thick[x : x + 1, :], (8, LANES))
        for a in range(P_SIZE):
            rows = slice(8 * a, 8 * a + 8)
            value = strided(raw, 512 + 32 * a + x, 8) * fields[x][rows] + width * images[x][rows]
            value = value + edges(a, *faces, sub)
            near[at + 8 * a : at + 8 * a + 8, :] = strided(raw, 256 + 32 * a + x, 8) - value
        near[at + REACT : at + THICK, :] = strided(raw, 512 + x, NODES)
        rows = [thick[x : x + 1, :]] + [opened[4 * f + x : 4 * f + x + 1, :] for f in range(4)]
        near[at + THICK : at + BLOCK, :] = jnp.concatenate(rows + [jnp.zeros((3, LANES), jnp.float32)], axis=0)
    near[FIRST_WEST:LAST_EAST, :] = traces[0][0]
    near[LAST_EAST:ENDS, :] = traces[3][1]
    near[ENDS : ENDS + 8, :] = ends
    lanes = lane_ids(NODES)
    for out, first in ((to_up, 120), (to_down, 0)):
        totals = [jnp.zeros((n, LANES), jnp.float32) for n in (NODES, 32, 8)]
        for x in range(4):
            block = BLOCK * x
            parts = (
                (0, near[block : block + 64, :]),
                (0, near[block + REACT : block + THICK, :]),
                (1, jnp.concatenate(traces[x], axis=0)),
                (2, near[block + THICK : block + BLOCK, :]),
            )
            for field, (part, value) in enumerate(parts):
                at = 32 * field + 8 * x
                ids = lanes[0 : value.shape[0]]
                totals[part] = jnp.where((ids >= at) & (ids < at + 8), turned(value, at - first), totals[part])
        out[0:8, :] = totals[0][0:8] + totals[1][0:8] + totals[2]
        out[8:32, :] = totals[0][8:32] + totals[1][8:32]
        out[32:64, :] = totals[0][32:64]


def far_kernel(near, left, right, strip, high2, low2):
    lanes = lane_ids(NODES)
    strip[0:64, :] = jnp.where(lanes < 64, left[...], turned(right[...], 64))
    lanes = lanes[0:32]
    edge = jnp.where(lanes < 32, turned(left[0:32, :], -64), turned(right[0:32, :], -32))
    edge = jnp.where((lanes >= 64) & (lanes < 96), turned(left[0:32, :], -32), edge)
    edge = jnp.where(lanes >= 96, right[0:32, :], edge)
    strip[64:96, :] = edge
    for out, close, face in ((high2, 3, LAST_EAST), (low2, 0, FIRST_WEST)):
        block = BLOCK * close
        out[0:64, :] = near[block : block + 64, :]
        out[64:72, :] = near[block + THICK : block + BLOCK, :]
        out[72:80, :] = near[face : face + 8, :]
        out[80:88, :] = near[ENDS : ENDS + 8, :]
        out[88:120, :] = edge


def powers_kernel(
    shift_in, weight, near, below1, above1, below2, above2, own_strip, strip_b1, strip_a1,
    basis_out, gram_out, field_a, field_b, image, react, stiff, opened,
):
    shift = shift_in[0:1, :]

    def put(row, value_reaction, value_stiffness, value_open):
        cols = slice(row * LANES, (row + 1) * LANES)
        if value_reaction is not None:
            react[:, cols] = (value_reaction - shift) * SCALE
            stiff[:, cols] = jnp.broadcast_to(value_stiffness * SCALE, (8, LANES))
        for f in range(4):
            opened[8 * f : 8 * f + 8, cols] = jnp.broadcast_to(value_open[f], (8, LANES))

    local = {}
    for x in range(4):
        for ref, row in ((below1, 2 + x), (near, 6 + x), (above1, 10 + x)):
            at = BLOCK * x
            put(
                row, ref[at + REACT : at + THICK, :], ref[at + THICK : at + OPEN, :],
                [ref[at + OPEN + f : at + OPEN + f + 1, :] for f in range(4)],
            )
            local[row] = functools.partial(lambda ref, at, a: ref[at + 8 * a : at + 8 * a + 8, :], ref, at)
    for row, ref in ((1, below2), (ROWS - 2, above2)):
        put(row, None, None, [ref[65 + f : 66 + f, :] for f in range(4)])
        local[row] = functools.partial(lambda ref, a: ref[8 * a : 8 * a + 8, :], ref)

    lanes64 = lane_ids(NODES)
    lanes = lane_ids(8)
    pieces = ((strip_b1, 16, 48, 16), (own_strip, 48, 80, 48), (strip_a1, 80, 112, 80))
    strip_faces = []
    for side in range(2):
        made = []
        for top, count, zero in ((0, 64, 64 * side), (0, 64, 64 * side + 32), (64, 32, 32 * side), (64, 8, 64 + 32 * side)):
            ids = lanes64[0:count]
            value = jnp.zeros((count, LANES), jnp.float32)
            for ref, start, stop, target in pieces:
                part = turned(ref[top : top + count, :], target - zero)
                value = jnp.where((ids >= start) & (ids < stop), part, value)
            if count == 32:
                value = jnp.where(ids < 16, turned(below2[88:120, :], -16 - 32 * side), value)
                value = jnp.where(ids >= 112, turned(above2[88:120, :], 112 - 32 * side), value)
            made.append(value)
        put(ROWS + side, made[1], made[3][0:1], [made[3][1 + f : 2 + f] for f in range(4)])
        local[ROWS + side] = functools.partial(lambda value, a: value[8 * a : 8 * a + 8], made[0])
        strip_faces.append([made[2][8 * f : 8 * f + 8] for f in range(4)])
    ends = jnp.zeros((8, LANES), jnp.float32)
    for ref, top, start, stop, by in (
        (below2, 80, 0, 16, -16), (below1, ENDS, 16, 48, 16), (near, ENDS, 48, 80, 48),
        (above1, ENDS, 80, 112, 80), (above2, 80, 112, 128, 112),
    ):
        ends = jnp.where((lanes >= start) & (lanes < stop), turned(ref[top : top + 8, :], by), ends)

    def columns(row):
        return slice(row * LANES, (row + 1) * LANES)

    low, high = ROWS, ROWS + 1
    sub = lax.broadcasted_iota(jnp.int32, (8, LANES), 0)
    TW, TE, TS, TN = (slice(64 + 8 * f, 72 + 8 * f) for f in range(4))

    def begin(new):
        def finish(row, faces):
            cols = columns(row)
            faces = [
                None if value is None else 8.0 * opened[8 * f : 8 * f + 8, cols] * value
                for f, value in enumerate(faces)
            ]
            for a in range(P_SIZE):
                new[8 * a : 8 * a + 8, cols] = local[row](a) + edges(a, *faces, sub)

        west = {
            2: below2[72:80, :], 6: below1[LAST_EAST:ENDS, :], 10: near[LAST_EAST:ENDS, :],
            14: above1[LAST_EAST:ENDS, :],
        }
        east = {
            1: below1[FIRST_WEST:LAST_EAST, :], 5: near[FIRST_WEST:LAST_EAST, :],
            9: above1[FIRST_WEST:LAST_EAST, :], 13: above2[72:80, :],
        }
        for row in range(1, ROWS - 1):
            south = jnp.where(lanes == 0, turned(strip_faces[0][3], -(8 * row + 7)), 0.0)
            north = jnp.where(lanes == LANES - 1, turned(strip_faces[1][2], 127 - 8 * row), 0.0)
            finish(row, (west.get(row), east.get(row), south, north))
        none = jnp.zeros((8, LANES), jnp.float32)
        spot = lanes // 8 % 4
        for side in range(2):
            from_west = jnp.where(spot == 2, turned(strip_faces[side][1], 8), 0.0)
            from_east = jnp.where(spot == 1, turned(strip_faces[side][0], -8), 0.0)
            outer = jnp.where(lanes % 8 == (0 if side else 7), ends, 0.0)
            finish(ROWS + side, (from_west, from_east, outer if side else none, none if side else outer))

    def apply(old, new, step):
        start, stop = step, ROWS - step
        for first_row, last_row in ((start, stop), (ROWS, ROWS + 2)):
            for row in range(first_row, last_row, 2):
                cols = slice(row * LANES, (row + 2) * LANES)
                image[:, cols] = product(weight, old[:, cols])

        def finish(row, *sides):
            cols = columns(row)
            faces = [
                image[own, cols] - opened[8 * f : 8 * f + 8, cols] * value
                for f, (own, value) in enumerate(zip((TW, TE, TS, TN), sides))
            ]
            for a in range(P_SIZE):
                rows = slice(8 * a, 8 * a + 8)
                value = react[rows, cols] * old[rows, cols] + stiff[:, cols] * image[rows, cols]
                new[rows, cols] = value + edges(a, *faces, sub)

        north_low = image[TN, columns(low)]
        south_high = image[TS, columns(high)]
        for row in range(start + 1, stop - 1):
            cols = columns(row)
            from_south = jnp.where(
                lanes == 0, turned(north_low, -(8 * row + 7)), turned(image[TN, cols], 1)
            )
            from_north = jnp.where(
                lanes == LANES - 1, turned(south_high, 127 - 8 * row), turned(image[TS, cols], -1)
            )
            finish(row, image[TE, columns(row - 1)], image[TW, columns(row + 1)], from_south, from_north)
        if step == DEPTH - 1:
            return
        to_low = turned(image[TS, columns(low)], -1)
        to_high = turned(image[TN, columns(high)], 1)
        for row in range(start, stop):
            cols = columns(row)
            to_low = jnp.where(lanes == 8 * row + 7, turned(image[TS, cols], 8 * row + 7), to_low)
            to_high = jnp.where(lanes == 8 * row, turned(image[TN, cols], 8 * row + 1), to_high)
        cols = columns(low)
        finish(low, turned(image[TE, cols], 8), turned(image[TW, cols], -8), turned(image[TN, cols], 1), to_low)
        cols = columns(high)
        finish(high, turned(image[TE, cols], 8), turned(image[TW, cols], -8), to_high, turned(image[TS, cols], -1))

    old, new = field_a, field_b
    for step in range(DEPTH):
        if step:
            apply(old, new, step)
        else:
            begin(new)
        basis_out[step, :, :] = new[:, 6 * LANES : 10 * LANES]
        old, new = new, old

    sums = [jnp.zeros((8, LANES), jnp.float32) for _ in GRAM]
    for x in range(4):
        for a in range(P_SIZE):
            values = [basis_out[k, 8 * a : 8 * a + 8, x * LANES : (x + 1) * LANES] for k in range(ITERS + 1)]
            sums = [total + values[k] * values[l] for total, (k, l) in zip(sums, GRAM)]
    rows = [jnp.sum(total, axis=0, keepdims=True) for total in sums]
    rows = jnp.concatenate(rows + [jnp.zeros((24 - len(GRAM), LANES), jnp.float32)], axis=0)
    totals = jnp.sum(rows, axis=1, keepdims=True)
    place = lax.broadcasted_iota(jnp.int32, (24, LANES), 0) == lax.broadcasted_iota(jnp.int32, (24, LANES), 1)
    totals = jnp.sum(jnp.where(place, totals, 0.0), axis=0, keepdims=True)
    gram_out[...] = jnp.broadcast_to(totals, gram_out.shape)


def combine_kernel(nodes, shift_in, powers, gathered, basis_out, hess_out, amp_out):
    shift = shift_in[...]
    row = jnp.sum(gathered[...], axis=0, keepdims=True) * (1.0 / nodes)
    spread = jnp.broadcast_to(row, (8, LANES))
    gram = {}
    for at, (k, l) in enumerate(GRAM):
        gram[k, l] = gram[l, k] = jnp.broadcast_to(spread[:, at : at + 1], (8, LANES))
    sizes = [jnp.sqrt(gram[k, k]) for k in range(ITERS + 1)]
    sub = lax.broadcasted_iota(jnp.int32, (8, LANES), 0)
    lanes = lane_ids(8)
    hess = jnp.zeros((8, LANES), jnp.float32)
    beta = jnp.sqrt(gram[0, 0] + FLOOR)
    coeffs = [[1.0 / beta]]
    amp = sizes[0] * coeffs[0][0]

    def put(hess, i, j, value):
        return jnp.where((sub == i) & (lanes == j), value, hess)

    for j in range(ITERS):
        last = coeffs[j]
        image = [shift * c for c in last] + [None]
        for k in range(j + 1):
            moved = last[k] * 8.0
            image[k + 1] = moved if image[k + 1] is None else image[k + 1] + moved
        weighted = [
            sum(gram[k, l] * image[l] for l in range(1, j + 2)) + gram[k, 0] * image[0] for k in range(j + 2)
        ]
        pending = list(image)
        for i in range(j + 1):
            h = sum(c * weighted[k] for k, c in enumerate(coeffs[i]))
            hess = put(hess, i, j, h)
            for k, c in enumerate(coeffs[i]):
                pending[k] = pending[k] - h * c
        square = sum(
            pending[k] * sum(gram[k, l] * pending[l] for l in range(j + 2)) for k in range(j + 2)
        )
        beta = jnp.sqrt(jnp.maximum(square, 0.0) + FLOOR)
        hess = put(hess, j + 1, j, beta)
        scale = 1.0 / beta
        coeffs.append([p * scale for p in pending])
        amp = jnp.maximum(amp, sum(jnp.abs(c) * s for c, s in zip(coeffs[-1], sizes)))
    hess_out[...] = hess[0 : ITERS + 1, 0:ITERS]
    amp_out[...] = amp[0:1, :]
    for x in range(4):
        for a in range(P_SIZE):
            values = [powers[k, 8 * a : 8 * a + 8, x * LANES : (x + 1) * LANES] for k in range(ITERS + 1)]
            for j in range(ITERS + 1):
                total = coeffs[j][0] * values[0]
                for k in range(1, j + 1):
                    total = total + coeffs[j][k] * values[k]
                basis_out[j, pl.ds(32 * a + x, 8, stride=4), :] = total


def fast(source, initial, reaction, stiffness, line_op, face_deriv, walls):
    vmem = pl.BlockSpec(memory_space=pltpu.VMEM)
    hbm = pl.BlockSpec(memory_space=pltpu.HBM)
    grant = pltpu.CompilerParams(vmem_limit_bytes=16 * 2**20)
    f32 = jnp.float32
    nx, ny = lax.axis_size(GX), lax.axis_size(GY)
    wide = (ROWS + 2) * LANES

    def moved(value, axis, size, by):
        return lax.ppermute(value, axis, [(i, (i + by) % size) for i in range(size)])

    held = (line_op, face_deriv.reshape(1, P_SIZE), source, initial, reaction, stiffness, walls)
    raw, near, to_up, to_down, weight, shift = pl.pallas_call(
        pack_kernel,
        out_shape=[jax.ShapeDtypeStruct((n, LANES), f32) for n in (800, ENDS + 8, NODES, NODES)]
        + [jax.ShapeDtypeStruct((NODES + 32, 6 * NODES), jnp.bfloat16), jax.ShapeDtypeStruct((8, LANES), f32)],
        in_specs=[hbm] * 7,
        out_specs=[vmem] * 6,
        scratch_shapes=[
            pltpu.VMEM((P_SIZE, P_SIZE), f32),
            pltpu.VMEM((1, P_SIZE), f32),
            pltpu.VMEM((16, LANES), jnp.int32),
            pltpu.SemaphoreType.DMA((10,)),
        ],
        compiler_params=grant,
    )(*[pltpu.with_memory_space_constraint(v, pltpu.HBM) for v in held])
    line = lax.axis_size(GY[1])
    spot = lax.axis_index(GY[1])
    first, last = spot == 0, spot == line - 1
    inside = [(i, i + 1) for i in range(ny) if (i + 1) % line]
    across = [(i, (i + 1) % ny) for i in range(ny) if (i + 1) % line == 0]
    left = lax.ppermute(to_up, GY, inside)
    right = lax.ppermute(to_down, GY, [(b, a) for a, b in inside])
    swapped = lax.ppermute(jnp.where(last, to_up, to_down), GY, across + [(b, a) for a, b in across])
    left = jnp.where(first, swapped, left)
    right = jnp.where(last, swapped, right)
    below1 = moved(near, GX, nx, 1)
    above1 = moved(near, GX, nx, -1)
    strip, high2, low2 = pl.pallas_call(
        far_kernel,
        out_shape=[jax.ShapeDtypeStruct((n, LANES), f32) for n in (96, 120, 120)],
        in_specs=[vmem] * 3,
        out_specs=[vmem] * 3,
        compiler_params=grant,
    )(near, left, right)
    below2 = moved(high2, GX, nx, 2)
    above2 = moved(low2, GX, nx, -2)
    strips = [moved(strip, GX, nx, by) for by in (1, -1)]

    powers, gram = pl.pallas_call(
        powers_kernel,
        out_shape=[
            jax.ShapeDtypeStruct((ITERS + 1, NODES, 4 * LANES), f32),
            jax.ShapeDtypeStruct((1, LANES), f32),
        ],
        in_specs=[vmem] * 10,
        out_specs=[vmem] * 2,
        scratch_shapes=[pltpu.VMEM((n, wide), f32) for n in (NODES, NODES, NODES + 32, NODES, 8, 32)],
        compiler_params=grant,
    )(shift, weight, near, below1, above1, below2, above2, strip, *strips)
    every = GX + GY
    copies = jnp.broadcast_to(gram, (nx * ny, LANES))
    gathered = lax.all_to_all(copies, every, split_axis=0, concat_axis=0, tiled=True)
    basis, hess, amp = pl.pallas_call(
        functools.partial(combine_kernel, float(NODES * 4 * nx * LANES * ny)),
        out_shape=[
            jax.ShapeDtypeStruct((ITERS + 1, 4 * NODES, LANES), f32),
            jax.ShapeDtypeStruct((ITERS + 1, ITERS), f32),
            jax.ShapeDtypeStruct((1, LANES), f32),
        ],
        in_specs=[vmem] * 3,
        out_specs=[vmem] * 3,
        compiler_params=grant,
    )(shift, powers, gathered)
    return hess, basis, amp[0, 0], raw


def body(source, initial, reaction, stiffness, line_op, face_deriv, wall_flags):
    flat = [v.reshape(4 * NODES, LANES) for v in (source, initial, reaction)]
    hess, basis, amp, raw = fast(*flat, stiffness, line_op, face_deriv, wall_flags.reshape(16, LANES))

    def again(carry):
        raw = lax.optimization_barrier(carry[3])
        initial, source, reaction = raw[0:768].reshape(3, NODES, 4, LANES)
        opened = raw[772:788].reshape(4, 4, LANES)
        line_op, face_deriv = raw[788:796, 0:P_SIZE], raw[796, 0:P_SIZE]
        hess, basis = stepwise(source, initial, reaction, raw[768:772], line_op, face_deriv, opened)
        return jnp.bool_(True), hess, basis.reshape(ITERS + 1, 4 * NODES, LANES), raw

    done = amp <= AMP_LIMIT
    carry = lax.while_loop(lambda carry: jnp.logical_not(carry[0]), again, (done, hess, basis, raw))
    return (carry[1], carry[2].reshape(ITERS + 1, NODES, 4, LANES))


def solution(mesh):
    finer = Mesh(mesh.devices.reshape(4, 2, 4, 8), ("gx_0", "gx_1", "gy_0", "gy_1"))
    placed = (
        P(None, GX, GY),
        P(None, GX, GY),
        P(None, GX, GY),
        P(GX, GY),
        P(),
        P(),
        P(None, GX, GY),
    )
    return jax.shard_map(
        body, mesh=finer, in_specs=placed, out_specs=(P(), P(None, None, GX, GY)), check_vma=False
    )
```

```python
import functools

import jax
import jax.numpy as jnp
from jax import lax
from jax.experimental import pallas as pl
from jax.experimental.pallas import tpu as pltpu
from jax.sharding import Mesh
from jax.sharding import PartitionSpec as P

P_SIZE = 8
ITERS = 5
GX = ("gx_0", "gx_1")
GY = ("gy_0", "gy_1")


TAU = 2.0
FLOOR = 0.1


def extended(array, sides, width):
    for axis, dim in sides:
        devices, length = (lax.axis_size(axis), array.shape[dim])
        up = [(i, (i + 1) % devices) for i in range(devices)]
        down = [(j, i) for i, j in up]
        last = lax.slice_in_dim(array, length - width, length, axis=dim)
        leading = lax.slice_in_dim(array, 0, width, axis=dim)
        before = lax.ppermute(last, axis, up)
        after = lax.ppermute(leading, axis, down)
        array = jnp.concatenate([before, array, after], axis=dim)
    return array


def sent_to_all(array, axis):
    copies = jnp.broadcast_to(array, (lax.axis_size(axis), *array.shape))
    return lax.all_to_all(copies, axis, split_axis=0, concat_axis=0, tiled=True)


def over_copies(array, axis):
    everything = sent_to_all(array, axis)
    return jnp.sum(everything, axis=0)


def by_axis(array, axes):
    far, near = axes
    nearer = over_copies(array, near)
    return over_copies(nearer, far)


def together(arrays, axis):
    vector, at, gathered = (jnp.concatenate([a.reshape(-1) for a in arrays]), 0, [])
    subtotal = by_axis(vector, axis)
    for a in arrays:
        gathered.append(subtotal[at : at + a.size].reshape(a.shape))
        at += a.size
    return tuple(gathered)


def local_total(values):
    return jnp.sum(jnp.sum(values, axis=0))


def x_traces(nodes, face_deriv):
    highest = lax.Precision.HIGHEST
    lower = jnp.einsum("c,cbxy->bxy", face_deriv, nodes, precision=highest)
    upper = jnp.einsum("c,cbxy->bxy", face_deriv[::-1], nodes, precision=highest)
    return jnp.stack([nodes[0], lower, nodes[-1], upper])


def y_traces(nodes, face_deriv):
    highest = lax.Precision.HIGHEST
    lower = jnp.einsum("c,acxy->axy", face_deriv, nodes, precision=highest)
    upper = jnp.einsum("c,acxy->axy", face_deriv[::-1], nodes, precision=highest)
    return jnp.stack([nodes[:, 0], lower, nodes[:, -1], upper])


def apply_op(field, reaction, stiffness, line_op, face_deriv, opened):
    highest = lax.Precision.HIGHEST
    nodes = field.reshape(P_SIZE, P_SIZE, field.shape[1], field.shape[2])
    interior = stiffness * (
        jnp.einsum("ac,cbxy->abxy", line_op, nodes, precision=highest)
        + jnp.einsum("bc,acxy->abxy", line_op, nodes, precision=highest)
    )
    xside = extended(x_traces(nodes, face_deriv), ((GX, 2),), 1)
    yside = extended(y_traces(nodes, face_deriv), ((GY, 3),), 1)
    x_own = xside[:, :, 1:-1]
    y_own = yside[:, :, :, 1:-1]
    east_nb = xside[0:2, :, 2:]
    west_nb = xside[2:4, :, :-2]
    north_nb = yside[0:2, :, :, 2:]
    south_nb = yside[2:4, :, :, :-2]
    add_east = TAU * (x_own[2] - opened[1] * east_nb[0]) + 0.5 * (x_own[3] - opened[1] * east_nb[1])
    add_west = TAU * (x_own[0] - opened[0] * west_nb[0]) + 0.5 * (x_own[1] - opened[0] * west_nb[1])
    add_north = TAU * (y_own[2] - opened[3] * north_nb[0]) + 0.5 * (
        y_own[3] - opened[3] * north_nb[1]
    )
    add_south = TAU * (y_own[0] - opened[2] * south_nb[0]) + 0.5 * (
        y_own[1] - opened[2] * south_nb[1]
    )
    result = reaction.reshape(nodes.shape) * nodes + interior
    result = result.at[0].add(add_west).at[P_SIZE - 1].add(add_east)
    result = result.at[:, 0].add(add_south).at[:, P_SIZE - 1].add(add_north)
    return result.reshape(field.shape)


def norm_scale(vector, total):
    squares = by_axis(local_total(vector * vector), (("gx_0", "gx_1"), ("gy_0", "gy_1")))
    return jnp.sqrt(squares / total + FLOOR)


def stepwise(source, initial, reaction, stiffness, line_op, face_deriv, opened):
    highest = lax.Precision.HIGHEST
    total = float(
        P_SIZE * P_SIZE * source.shape[1] * lax.axis_size(GX) * source.shape[2] * lax.axis_size(GY)
    )

    def operate(field):
        return apply_op(field, reaction, stiffness, line_op, face_deriv, opened)

    def products(basis, image):
        per_cell = jnp.einsum("kqxy,qxy->kxy", basis, image, precision=highest)
        return jnp.sum(per_cell, axis=(1, 2))

    first = source - operate(initial)
    basis = jnp.zeros((ITERS + 1,) + source.shape, jnp.float32)
    hessen = jnp.zeros((ITERS + 1, ITERS), jnp.float32)
    rows = lax.broadcasted_iota(jnp.int32, (ITERS + 1, ITERS), 0)
    cols = lax.broadcasted_iota(jnp.int32, (ITERS + 1, ITERS), 1)
    slots = lax.broadcasted_iota(jnp.int32, (ITERS + 1,), 0)

    def advance(step, carry):
        basis, hessen, pending = carry
        image = operate(pending)
        local = products(basis, image)
        projected, crossed, squares = together(
            (local, local_total(pending * image), local_total(pending * pending)),
            (("gx_0", "gx_1"), ("gy_0", "gy_1")),
        )
        beta = jnp.sqrt(squares / total + FLOOR)
        basis = lax.dynamic_update_index_in_dim(basis, pending / beta, step, 0)
        coeffs = projected / (total * beta) + jnp.where(
            slots == step, crossed / (total * beta * beta), 0.0
        )
        pending = image / beta - jnp.einsum("k,kqxy->qxy", coeffs, basis, precision=highest)
        hessen = hessen + jnp.where(cols == step, coeffs[:, None], 0.0)
        hessen = hessen + jnp.where((rows == step) & (cols == step - 1), beta, 0.0)
        return (basis, hessen, pending)

    basis, hessen, pending = lax.fori_loop(0, ITERS, advance, (basis, hessen, first))
    beta = norm_scale(pending, total)
    basis = basis.at[ITERS].set(pending / beta)
    hessen = hessen + jnp.where((rows == ITERS) & (cols == ITERS - 1), beta, 0.0)
    return (hessen, basis)


NODES = P_SIZE * P_SIZE
ROWS = 16
DEPTH = 6
LANES = 128
SCALE = 0.125
AMP_LIMIT = 100.0
GRAM = [(k, l) for k in range(ITERS + 1) for l in range(k + 1)]


def lane_ids(rows):
    return lax.broadcasted_iota(jnp.int32, (rows, LANES), 1)


def turned(value, shift):
    shift = shift % LANES
    return value if shift == 0 else pltpu.roll(value, shift, 1)


def strided(ref, start, count):
    return ref[pl.ds(start, count, stride=4), :]


BLOCK = 136
REACT, THICK, OPEN = 64, 128, 129
FIRST_WEST, LAST_EAST, ENDS = 544, 552, 560


def split(value):
    high = value.astype(jnp.bfloat16)
    rest = value - high.astype(jnp.float32)
    middle = rest.astype(jnp.bfloat16)
    low = (rest - middle.astype(jnp.float32)).astype(jnp.bfloat16)
    return high, middle, low


def weights_in(line, deriv):
    sub = lax.broadcasted_iota(jnp.int32, (8, NODES), 0)
    lane = lax.broadcasted_iota(jnp.int32, (8, NODES), 1)
    along, across = lane // 8, lane % 8
    outer = jnp.zeros((8, NODES), jnp.float32)
    inner = jnp.zeros((8, NODES), jnp.float32)
    for c in range(P_SIZE):
        column = jnp.broadcast_to(line[:, c : c + 1], (8, NODES))
        outer = jnp.where(along == c, column, outer)
        inner = jnp.where(across == c, column, inner)
    parts = []
    for a in range(P_SIZE):
        row = jnp.broadcast_to(outer[a : a + 1, :], (8, NODES))
        parts.append(jnp.where(across == sub, row, 0.0) + jnp.where(along == a, inner, 0.0))
    for first, second in ((along, across), (across, along)):
        for flip in (False, True):
            part = jnp.zeros((8, NODES), jnp.float32)
            for c in range(P_SIZE):
                value = SCALE * (0.5 * deriv[0:1, c : c + 1] + (TAU if c == 0 else 0.0))
                part = jnp.where(first == (P_SIZE - 1 - c if flip else c), value, part)
            parts.append(jnp.where(second == sub, part, 0.0))
    high, middle, low = split(jnp.concatenate(parts, axis=0))
    return jnp.concatenate([high, high, high, middle, middle, low], axis=1)


def product(weight, value):
    high, middle, low = split(value)
    stacked = jnp.concatenate([high, middle, low, high, middle, high], axis=0)
    return jnp.dot(weight[...], stacked, preferred_element_type=jnp.float32)


def centre(line, deriv):
    diagonal = lax.broadcasted_iota(jnp.int32, (8, 8), 0) == lax.broadcasted_iota(jnp.int32, (8, 8), 1)
    trace = jnp.sum(jnp.where(diagonal, line, 0.0), axis=1, keepdims=True)
    trace = jnp.sum(trace, axis=0, keepdims=True)
    return 2.0 + 0.3125 * trace + 0.5 * (TAU + 0.5 * deriv[0:1, 0:1])


def edges(a, west, east, south, north, sub):
    value = jnp.where(sub == 0, south[a : a + 1, :], 0.0)
    value = jnp.where(sub == P_SIZE - 1, north[a : a + 1, :], value)
    if a == 0 and west is not None:
        value = value + west
    if a == P_SIZE - 1 and east is not None:
        value = value + east
    return value


def pack_kernel(
    line_in, deriv_in, source, initial, reaction, stiffness, walls,
    raw, near, to_up, to_down, weight, shift_out, line, deriv, flags, sems,
):
    moves = [(line_in, line), (deriv_in, deriv)]
    for at, ref in ((0, initial), (256, source), (512, reaction)):
        for half in (0, 128):
            moves.append((ref.at[pl.ds(half, 128), :], raw.at[pl.ds(at + half, 128), :]))
    moves.append((stiffness, raw.at[pl.ds(768, 4), :]))
    moves.append((walls, flags))
    copies = [pltpu.make_async_copy(a, b, sems.at[n]) for n, (a, b) in enumerate(moves)]
    for copy in copies:
        copy.start()
    for copy in copies[:2]:
        copy.wait()
    line, deriv = line[...], deriv[...]
    weight[...] = weights_in(line, deriv)
    shift_out[...] = jnp.broadcast_to(centre(line, deriv), (8, LANES))
    for copy in copies[2:4]:
        copy.wait()
    sub = lax.broadcasted_iota(jnp.int32, (8, LANES), 0)
    lanes8 = lane_ids(8)
    fields, images = [], []
    for x in range(0, 4, 2):
        pair = jnp.concatenate([strided(raw, x, NODES), strided(raw, x + 1, NODES)], axis=1)
        image = product(weight, pair)
        for k in range(2):
            fields.append(pair[:, k * LANES : (k + 1) * LANES])
            images.append(image[:, k * LANES : (k + 1) * LANES])
    for copy in copies[4:]:
        copy.wait()
    opened = 1.0 - flags[...].astype(jnp.float32)
    raw[772:788, :] = opened
    raw[788:796, 0:P_SIZE] = line
    raw[796:797, 0:P_SIZE] = deriv
    thick = raw[768:772, :]
    traces = [[image[64 + 8 * f : 72 + 8 * f] for f in range(4)] for image in images]
    ends = jnp.zeros((8, LANES), jnp.float32)
    for x in range(4):
        at = BLOCK * x
        allowed = [jnp.broadcast_to(opened[4 * f + x : 4 * f + x + 1, :], (8, LANES)) for f in range(4)]
        faces = list(traces[x])
        if x > 0:
            faces[0] = faces[0] - allowed[0] * traces[x - 1][1]
        if x < 3:
            faces[1] = faces[1] - allowed[1] * traces[x + 1][0]
        faces[2] = faces[2] - allowed[2] * jnp.where(lanes8 == 0, 0.0, turned(traces[x][3], 1))
        faces[3] = faces[3] - allowed[3] * jnp.where(lanes8 == LANES - 1, 0.0, turned(traces[x][2], -1))
        faces = [8.0 * face for face in faces]
        ends = jnp.where(lanes8 == 8 * x + 7, turned(traces[x][2], 8 * x + 7), ends)
        ends = jnp.where(lanes8 == 8 * x, turned(traces[x][3], 8 * x + 1), ends)
        width = jnp.broadcast_to(thick[x : x + 1, :], (8, LANES))
        for a in range(P_SIZE):
            rows = slice(8 * a, 8 * a + 8)
            value = strided(raw, 512 + 32 * a + x, 8) * fields[x][rows] + width * images[x][rows]
            value = value + edges(a, *faces, sub)
            near[at + 8 * a : at + 8 * a + 8, :] = strided(raw, 256 + 32 * a + x, 8) - value
        near[at + REACT : at + THICK, :] = strided(raw, 512 + x, NODES)
        rows = [thick[x : x + 1, :]] + [opened[4 * f + x : 4 * f + x + 1, :] for f in range(4)]
        near[at + THICK : at + BLOCK, :] = jnp.concatenate(rows + [jnp.zeros((3, LANES), jnp.float32)], axis=0)
    near[FIRST_WEST:LAST_EAST, :] = traces[0][0]
    near[LAST_EAST:ENDS, :] = traces[3][1]
    near[ENDS : ENDS + 8, :] = ends
    lanes = lane_ids(NODES)
    for out, first in ((to_up, 120), (to_down, 0)):
        totals = [jnp.zeros((n, LANES), jnp.float32) for n in (NODES, 32, 8)]
        for x in range(4):
            block = BLOCK * x
            parts = (
                (0, near[block : block + 64, :]),
                (0, near[block + REACT : block + THICK, :]),
                (1, jnp.concatenate(traces[x], axis=0)),
                (2, near[block + THICK : block + BLOCK, :]),
            )
            for field, (part, value) in enumerate(parts):
                at = 32 * field + 8 * x
                ids = lanes[0 : value.shape[0]]
                totals[part] = jnp.where((ids >= at) & (ids < at + 8), turned(value, at - first), totals[part])
        out[0:8, :] = totals[0][0:8] + totals[1][0:8] + totals[2]
        out[8:32, :] = totals[0][8:32] + totals[1][8:32]
        out[32:64, :] = totals[0][32:64]


def far_kernel(near, left, right, strip, high2, low2):
    lanes = lane_ids(NODES)
    strip[0:64, :] = jnp.where(lanes < 64, left[...], turned(right[...], 64))
    lanes = lanes[0:32]
    edge = jnp.where(lanes < 32, turned(left[0:32, :], -64), turned(right[0:32, :], -32))
    edge = jnp.where((lanes >= 64) & (lanes < 96), turned(left[0:32, :], -32), edge)
    edge = jnp.where(lanes >= 96, right[0:32, :], edge)
    strip[64:96, :] = edge
    for out, close, face in ((high2, 3, LAST_EAST), (low2, 0, FIRST_WEST)):
        block = BLOCK * close
        out[0:64, :] = near[block : block + 64, :]
        out[64:72, :] = near[block + THICK : block + BLOCK, :]
        out[72:80, :] = near[face : face + 8, :]
        out[80:88, :] = near[ENDS : ENDS + 8, :]
        out[88:120, :] = edge


def powers_kernel(
    shift_in, weight, near, below1, above1, below2, above2, own_strip, strip_b1, strip_a1,
    basis_out, gram_out, field_a, field_b, image, react, stiff, opened,
):
    shift = shift_in[0:1, :]

    def put(row, value_reaction, value_stiffness, value_open):
        cols = slice(row * LANES, (row + 1) * LANES)
        if value_reaction is not None:
            react[:, cols] = (value_reaction - shift) * SCALE
            stiff[:, cols] = jnp.broadcast_to(value_stiffness * SCALE, (8, LANES))
        for f in range(4):
            opened[8 * f : 8 * f + 8, cols] = jnp.broadcast_to(value_open[f], (8, LANES))

    local = {}
    for x in range(4):
        for ref, row in ((below1, 2 + x), (near, 6 + x), (above1, 10 + x)):
            at = BLOCK * x
            put(
                row, ref[at + REACT : at + THICK, :], ref[at + THICK : at + OPEN, :],
                [ref[at + OPEN + f : at + OPEN + f + 1, :] for f in range(4)],
            )
            local[row] = functools.partial(lambda ref, at, a: ref[at + 8 * a : at + 8 * a + 8, :], ref, at)
    for row, ref in ((1, below2), (ROWS - 2, above2)):
        put(row, None, None, [ref[65 + f : 66 + f, :] for f in range(4)])
        local[row] = functools.partial(lambda ref, a: ref[8 * a : 8 * a + 8, :], ref)

    lanes64 = lane_ids(NODES)
    lanes = lane_ids(8)
    pieces = ((strip_b1, 16, 48, 16), (own_strip, 48, 80, 48), (strip_a1, 80, 112, 80))
    strip_faces = []
    for side in range(2):
        made = []
        for top, count, zero in ((0, 64, 64 * side), (0, 64, 64 * side + 32), (64, 32, 32 * side), (64, 8, 64 + 32 * side)):
            ids = lanes64[0:count]
            value = jnp.zeros((count, LANES), jnp.float32)
            for ref, start, stop, target in pieces:
                part = turned(ref[top : top + count, :], target - zero)
                value = jnp.where((ids >= start) & (ids < stop), part, value)
            if count == 32:
                value = jnp.where(ids < 16, turned(below2[88:120, :], -16 - 32 * side), value)
                value = jnp.where(ids >= 112, turned(above2[88:120, :], 112 - 32 * side), value)
            made.append(value)
        put(ROWS + side, made[1], made[3][0:1], [made[3][1 + f : 2 + f] for f in range(4)])
        local[ROWS + side] = functools.partial(lambda value, a: value[8 * a : 8 * a + 8], made[0])
        strip_faces.append([made[2][8 * f : 8 * f + 8] for f in range(4)])
    ends = jnp.zeros((8, LANES), jnp.float32)
    for ref, top, start, stop, by in (
        (below2, 80, 0, 16, -16), (below1, ENDS, 16, 48, 16), (near, ENDS, 48, 80, 48),
        (above1, ENDS, 80, 112, 80), (above2, 80, 112, 128, 112),
    ):
        ends = jnp.where((lanes >= start) & (lanes < stop), turned(ref[top : top + 8, :], by), ends)

    def columns(row):
        return slice(row * LANES, (row + 1) * LANES)

    low, high = ROWS, ROWS + 1
    sub = lax.broadcasted_iota(jnp.int32, (8, LANES), 0)
    TW, TE, TS, TN = (slice(64 + 8 * f, 72 + 8 * f) for f in range(4))

    def begin(new):
        def finish(row, faces):
            cols = columns(row)
            faces = [
                None if value is None else 8.0 * opened[8 * f : 8 * f + 8, cols] * value
                for f, value in enumerate(faces)
            ]
            for a in range(P_SIZE):
                new[8 * a : 8 * a + 8, cols] = local[row](a) + edges(a, *faces, sub)

        west = {
            2: below2[72:80, :], 6: below1[LAST_EAST:ENDS, :], 10: near[LAST_EAST:ENDS, :],
            14: above1[LAST_EAST:ENDS, :],
        }
        east = {
            1: below1[FIRST_WEST:LAST_EAST, :], 5: near[FIRST_WEST:LAST_EAST, :],
            9: above1[FIRST_WEST:LAST_EAST, :], 13: above2[72:80, :],
        }
        for row in range(1, ROWS - 1):
            south = jnp.where(lanes == 0, turned(strip_faces[0][3], -(8 * row + 7)), 0.0)
            north = jnp.where(lanes == LANES - 1, turned(strip_faces[1][2], 127 - 8 * row), 0.0)
            finish(row, (west.get(row), east.get(row), south, north))
        none = jnp.zeros((8, LANES), jnp.float32)
        spot = lanes // 8 % 4
        for side in range(2):
            from_west = jnp.where(spot == 2, turned(strip_faces[side][1], 8), 0.0)
            from_east = jnp.where(spot == 1, turned(strip_faces[side][0], -8), 0.0)
            outer = jnp.where(lanes % 8 == (0 if side else 7), ends, 0.0)
            finish(ROWS + side, (from_west, from_east, outer if side else none, none if side else outer))

    def apply(old, new, step):
        start, stop = step, ROWS - step
        for first_row, last_row in ((start, stop), (ROWS, ROWS + 2)):
            for row in range(first_row, last_row, 2):
                cols = slice(row * LANES, (row + 2) * LANES)
                image[:, cols] = product(weight, old[:, cols])

        def finish(row, *sides):
            cols = columns(row)
            faces = [
                image[own, cols] - opened[8 * f : 8 * f + 8, cols] * value
                for f, (own, value) in enumerate(zip((TW, TE, TS, TN), sides))
            ]
            for a in range(P_SIZE):
                rows = slice(8 * a, 8 * a + 8)
                value = react[rows, cols] * old[rows, cols] + stiff[:, cols] * image[rows, cols]
                new[rows, cols] = value + edges(a, *faces, sub)

        north_low = image[TN, columns(low)]
        south_high = image[TS, columns(high)]
        for row in range(start + 1, stop - 1):
            cols = columns(row)
            from_south = jnp.where(
                lanes == 0, turned(north_low, -(8 * row + 7)), turned(image[TN, cols], 1)
            )
            from_north = jnp.where(
                lanes == LANES - 1, turned(south_high, 127 - 8 * row), turned(image[TS, cols], -1)
            )
            finish(row, image[TE, columns(row - 1)], image[TW, columns(row + 1)], from_south, from_north)
        if step == DEPTH - 1:
            return
        to_low = turned(image[TS, columns(low)], -1)
        to_high = turned(image[TN, columns(high)], 1)
        for row in range(start, stop):
            cols = columns(row)
            to_low = jnp.where(lanes == 8 * row + 7, turned(image[TS, cols], 8 * row + 7), to_low)
            to_high = jnp.where(lanes == 8 * row, turned(image[TN, cols], 8 * row + 1), to_high)
        cols = columns(low)
        finish(low, turned(image[TE, cols], 8), turned(image[TW, cols], -8), turned(image[TN, cols], 1), to_low)
        cols = columns(high)
        finish(high, turned(image[TE, cols], 8), turned(image[TW, cols], -8), to_high, turned(image[TS, cols], -1))

    old, new = field_a, field_b
    for step in range(DEPTH):
        if step:
            apply(old, new, step)
        else:
            begin(new)
        basis_out[step, :, :] = new[:, 6 * LANES : 10 * LANES]
        old, new = new, old

    sums = [jnp.zeros((8, LANES), jnp.float32) for _ in GRAM]
    for x in range(4):
        for a in range(P_SIZE):
            values = [basis_out[k, 8 * a : 8 * a + 8, x * LANES : (x + 1) * LANES] for k in range(ITERS + 1)]
            sums = [total + values[k] * values[l] for total, (k, l) in zip(sums, GRAM)]
    rows = [jnp.sum(total, axis=0, keepdims=True) for total in sums]
    rows = jnp.concatenate(rows + [jnp.zeros((24 - len(GRAM), LANES), jnp.float32)], axis=0)
    totals = jnp.sum(rows, axis=1, keepdims=True)
    place = lax.broadcasted_iota(jnp.int32, (24, LANES), 0) == lax.broadcasted_iota(jnp.int32, (24, LANES), 1)
    totals = jnp.sum(jnp.where(place, totals, 0.0), axis=0, keepdims=True)
    gram_out[...] = jnp.broadcast_to(totals, gram_out.shape)


def combine_kernel(nodes, shift_in, powers, gathered, basis_out, hess_out, amp_out):
    shift = shift_in[...]
    row = jnp.sum(gathered[...], axis=0, keepdims=True) * (1.0 / nodes)
    spread = jnp.broadcast_to(row, (8, LANES))
    gram = {}
    for at, (k, l) in enumerate(GRAM):
        gram[k, l] = gram[l, k] = jnp.broadcast_to(spread[:, at : at + 1], (8, LANES))
    sizes = [jnp.sqrt(gram[k, k]) for k in range(ITERS + 1)]
    sub = lax.broadcasted_iota(jnp.int32, (8, LANES), 0)
    lanes = lane_ids(8)
    hess = jnp.zeros((8, LANES), jnp.float32)
    beta = jnp.sqrt(gram[0, 0] + FLOOR)
    coeffs = [[1.0 / beta]]
    amp = sizes[0] * coeffs[0][0]

    def put(hess, i, j, value):
        return jnp.where((sub == i) & (lanes == j), value, hess)

    for j in range(ITERS):
        last = coeffs[j]
        image = [shift * c for c in last] + [None]
        for k in range(j + 1):
            moved = last[k] * 8.0
            image[k + 1] = moved if image[k + 1] is None else image[k + 1] + moved
        weighted = [
            sum(gram[k, l] * image[l] for l in range(1, j + 2)) + gram[k, 0] * image[0] for k in range(j + 2)
        ]
        pending = list(image)
        for i in range(j + 1):
            h = sum(c * weighted[k] for k, c in enumerate(coeffs[i]))
            hess = put(hess, i, j, h)
            for k, c in enumerate(coeffs[i]):
                pending[k] = pending[k] - h * c
        square = sum(
            pending[k] * sum(gram[k, l] * pending[l] for l in range(j + 2)) for k in range(j + 2)
        )
        beta = jnp.sqrt(jnp.maximum(square, 0.0) + FLOOR)
        hess = put(hess, j + 1, j, beta)
        scale = 1.0 / beta
        coeffs.append([p * scale for p in pending])
        amp = jnp.maximum(amp, sum(jnp.abs(c) * s for c, s in zip(coeffs[-1], sizes)))
    hess_out[...] = hess[0 : ITERS + 1, 0:ITERS]
    amp_out[...] = amp[0:1, :]
    for x in range(4):
        for a in range(P_SIZE):
            values = [powers[k, 8 * a : 8 * a + 8, x * LANES : (x + 1) * LANES] for k in range(ITERS + 1)]
            for j in range(ITERS + 1):
                total = coeffs[j][0] * values[0]
                for k in range(1, j + 1):
                    total = total + coeffs[j][k] * values[k]
                basis_out[j, pl.ds(32 * a + x, 8, stride=4), :] = total


def fast(source, initial, reaction, stiffness, line_op, face_deriv, walls):
    vmem = pl.BlockSpec(memory_space=pltpu.VMEM)
    hbm = pl.BlockSpec(memory_space=pltpu.HBM)
    grant = pltpu.CompilerParams(vmem_limit_bytes=16 * 2**20)
    f32 = jnp.float32
    nx, ny = lax.axis_size(GX), lax.axis_size(GY)
    wide = (ROWS + 2) * LANES

    def moved(value, axis, size, by):
        return lax.ppermute(value, axis, [(i, (i + by) % size) for i in range(size)])

    held = (line_op, face_deriv.reshape(1, P_SIZE), source, initial, reaction, stiffness, walls)
    raw, near, to_up, to_down, weight, shift = pl.pallas_call(
        pack_kernel,
        out_shape=[jax.ShapeDtypeStruct((n, LANES), f32) for n in (800, ENDS + 8, NODES, NODES)]
        + [jax.ShapeDtypeStruct((NODES + 32, 6 * NODES), jnp.bfloat16), jax.ShapeDtypeStruct((8, LANES), f32)],
        in_specs=[hbm] * 7,
        out_specs=[vmem] * 6,
        scratch_shapes=[
            pltpu.VMEM((P_SIZE, P_SIZE), f32),
            pltpu.VMEM((1, P_SIZE), f32),
            pltpu.VMEM((16, LANES), jnp.int32),
            pltpu.SemaphoreType.DMA((10,)),
        ],
        compiler_params=grant,
    )(*[pltpu.with_memory_space_constraint(v, pltpu.HBM) for v in held])
    line = lax.axis_size(GY[1])
    spot = lax.axis_index(GY[1])
    first, last = spot == 0, spot == line - 1
    inside = [(i, i + 1 if (i + 1) % line else i + 1 - line) for i in range(ny)]
    across = [(i, (i + 1) % ny) for i in range(ny) if (i + 1) % line == 0]
    still = [(i, i) for i in range(ny) if i % line not in (0, line - 1)]
    left = lax.ppermute(to_up, GY, inside)
    right = lax.ppermute(to_down, GY, [(b, a) for a, b in inside])
    swapped = lax.ppermute(jnp.where(last, to_up, to_down), GY, across + [(b, a) for a, b in across] + still)
    left = jnp.where(first, swapped, left)
    right = jnp.where(last, swapped, right)
    below1 = moved(near, GX, nx, 1)
    above1 = moved(near, GX, nx, -1)
    strip, high2, low2 = pl.pallas_call(
        far_kernel,
        out_shape=[jax.ShapeDtypeStruct((n, LANES), f32) for n in (96, 120, 120)],
        in_specs=[vmem] * 3,
        out_specs=[vmem] * 3,
        compiler_params=grant,
    )(near, left, right)
    below2 = moved(high2, GX, nx, 2)
    above2 = moved(low2, GX, nx, -2)
    strips = [moved(strip, GX, nx, by) for by in (1, -1)]

    powers, gram = pl.pallas_call(
        powers_kernel,
        out_shape=[
            jax.ShapeDtypeStruct((ITERS + 1, NODES, 4 * LANES), f32),
            jax.ShapeDtypeStruct((1, LANES), f32),
        ],
        in_specs=[vmem] * 10,
        out_specs=[vmem] * 2,
        scratch_shapes=[pltpu.VMEM((n, wide), f32) for n in (NODES, NODES, NODES + 32, NODES, 8, 32)],
        compiler_params=grant,
    )(shift, weight, near, below1, above1, below2, above2, strip, *strips)
    every = GX + GY
    copies = jnp.broadcast_to(gram, (nx * ny, LANES))
    gathered = lax.all_to_all(copies, every, split_axis=0, concat_axis=0, tiled=True)
    basis, hess, amp = pl.pallas_call(
        functools.partial(combine_kernel, float(NODES * 4 * nx * LANES * ny)),
        out_shape=[
            jax.ShapeDtypeStruct((ITERS + 1, 4 * NODES, LANES), f32),
            jax.ShapeDtypeStruct((ITERS + 1, ITERS), f32),
            jax.ShapeDtypeStruct((1, LANES), f32),
        ],
        in_specs=[vmem] * 3,
        out_specs=[vmem] * 3,
        compiler_params=grant,
    )(shift, powers, gathered)
    return hess, basis, amp[0, 0], raw


def body(source, initial, reaction, stiffness, line_op, face_deriv, wall_flags):
    flat = [v.reshape(4 * NODES, LANES) for v in (source, initial, reaction)]
    hess, basis, amp, raw = fast(*flat, stiffness, line_op, face_deriv, wall_flags.reshape(16, LANES))

    def again(carry):
        raw = lax.optimization_barrier(carry[3])
        initial, source, reaction = raw[0:768].reshape(3, NODES, 4, LANES)
        opened = raw[772:788].reshape(4, 4, LANES)
        line_op, face_deriv = raw[788:796, 0:P_SIZE], raw[796, 0:P_SIZE]
        hess, basis = stepwise(source, initial, reaction, raw[768:772], line_op, face_deriv, opened)
        return jnp.bool_(True), hess, basis.reshape(ITERS + 1, 4 * NODES, LANES), raw

    done = amp <= AMP_LIMIT
    carry = lax.while_loop(lambda carry: jnp.logical_not(carry[0]), again, (done, hess, basis, raw))
    return (carry[1], carry[2].reshape(ITERS + 1, NODES, 4, LANES))


def solution(mesh):
    finer = Mesh(mesh.devices.reshape(4, 2, 4, 8), ("gx_0", "gx_1", "gy_0", "gy_1"))
    placed = (
        P(None, GX, GY),
        P(None, GX, GY),
        P(None, GX, GY),
        P(GX, GY),
        P(),
        P(),
        P(None, GX, GY),
    )
    return jax.shard_map(
        body, mesh=finer, in_specs=placed, out_specs=(P(), P(None, None, GX, GY)), check_vma=False
    )
```

```python
import functools

import jax
import jax.numpy as jnp
from jax import lax
from jax.experimental import pallas as pl
from jax.experimental.pallas import tpu as pltpu
from jax.sharding import Mesh
from jax.sharding import PartitionSpec as P

P_SIZE = 8
ITERS = 5
GX = ("gx_0", "gx_1")
GY = ("gy_0", "gy_1")


TAU = 2.0
FLOOR = 0.1


def extended(array, sides, width):
    for axis, dim in sides:
        devices, length = (lax.axis_size(axis), array.shape[dim])
        up = [(i, (i + 1) % devices) for i in range(devices)]
        down = [(j, i) for i, j in up]
        last = lax.slice_in_dim(array, length - width, length, axis=dim)
        leading = lax.slice_in_dim(array, 0, width, axis=dim)
        before = lax.ppermute(last, axis, up)
        after = lax.ppermute(leading, axis, down)
        array = jnp.concatenate([before, array, after], axis=dim)
    return array


def sent_to_all(array, axis):
    copies = jnp.broadcast_to(array, (lax.axis_size(axis), *array.shape))
    return lax.all_to_all(copies, axis, split_axis=0, concat_axis=0, tiled=True)


def over_copies(array, axis):
    everything = sent_to_all(array, axis)
    return jnp.sum(everything, axis=0)


def by_axis(array, axes):
    far, near = axes
    nearer = over_copies(array, near)
    return over_copies(nearer, far)


def together(arrays, axis):
    vector, at, gathered = (jnp.concatenate([a.reshape(-1) for a in arrays]), 0, [])
    subtotal = by_axis(vector, axis)
    for a in arrays:
        gathered.append(subtotal[at : at + a.size].reshape(a.shape))
        at += a.size
    return tuple(gathered)


def local_total(values):
    return jnp.sum(jnp.sum(values, axis=0))


def x_traces(nodes, face_deriv):
    highest = lax.Precision.HIGHEST
    lower = jnp.einsum("c,cbxy->bxy", face_deriv, nodes, precision=highest)
    upper = jnp.einsum("c,cbxy->bxy", face_deriv[::-1], nodes, precision=highest)
    return jnp.stack([nodes[0], lower, nodes[-1], upper])


def y_traces(nodes, face_deriv):
    highest = lax.Precision.HIGHEST
    lower = jnp.einsum("c,acxy->axy", face_deriv, nodes, precision=highest)
    upper = jnp.einsum("c,acxy->axy", face_deriv[::-1], nodes, precision=highest)
    return jnp.stack([nodes[:, 0], lower, nodes[:, -1], upper])


def apply_op(field, reaction, stiffness, line_op, face_deriv, opened):
    highest = lax.Precision.HIGHEST
    nodes = field.reshape(P_SIZE, P_SIZE, field.shape[1], field.shape[2])
    interior = stiffness * (
        jnp.einsum("ac,cbxy->abxy", line_op, nodes, precision=highest)
        + jnp.einsum("bc,acxy->abxy", line_op, nodes, precision=highest)
    )
    xside = extended(x_traces(nodes, face_deriv), ((GX, 2),), 1)
    yside = extended(y_traces(nodes, face_deriv), ((GY, 3),), 1)
    x_own = xside[:, :, 1:-1]
    y_own = yside[:, :, :, 1:-1]
    east_nb = xside[0:2, :, 2:]
    west_nb = xside[2:4, :, :-2]
    north_nb = yside[0:2, :, :, 2:]
    south_nb = yside[2:4, :, :, :-2]
    add_east = TAU * (x_own[2] - opened[1] * east_nb[0]) + 0.5 * (x_own[3] - opened[1] * east_nb[1])
    add_west = TAU * (x_own[0] - opened[0] * west_nb[0]) + 0.5 * (x_own[1] - opened[0] * west_nb[1])
    add_north = TAU * (y_own[2] - opened[3] * north_nb[0]) + 0.5 * (
        y_own[3] - opened[3] * north_nb[1]
    )
    add_south = TAU * (y_own[0] - opened[2] * south_nb[0]) + 0.5 * (
        y_own[1] - opened[2] * south_nb[1]
    )
    result = reaction.reshape(nodes.shape) * nodes + interior
    result = result.at[0].add(add_west).at[P_SIZE - 1].add(add_east)
    result = result.at[:, 0].add(add_south).at[:, P_SIZE - 1].add(add_north)
    return result.reshape(field.shape)


def norm_scale(vector, total):
    squares = by_axis(local_total(vector * vector), (("gx_0", "gx_1"), ("gy_0", "gy_1")))
    return jnp.sqrt(squares / total + FLOOR)


def stepwise(source, initial, reaction, stiffness, line_op, face_deriv, opened):
    highest = lax.Precision.HIGHEST
    total = float(
        P_SIZE * P_SIZE * source.shape[1] * lax.axis_size(GX) * source.shape[2] * lax.axis_size(GY)
    )

    def operate(field):
        return apply_op(field, reaction, stiffness, line_op, face_deriv, opened)

    def products(basis, image):
        per_cell = jnp.einsum("kqxy,qxy->kxy", basis, image, precision=highest)
        return jnp.sum(per_cell, axis=(1, 2))

    first = source - operate(initial)
    basis = jnp.zeros((ITERS + 1,) + source.shape, jnp.float32)
    hessen = jnp.zeros((ITERS + 1, ITERS), jnp.float32)
    rows = lax.broadcasted_iota(jnp.int32, (ITERS + 1, ITERS), 0)
    cols = lax.broadcasted_iota(jnp.int32, (ITERS + 1, ITERS), 1)
    slots = lax.broadcasted_iota(jnp.int32, (ITERS + 1,), 0)

    def advance(step, carry):
        basis, hessen, pending = carry
        image = operate(pending)
        local = products(basis, image)
        projected, crossed, squares = together(
            (local, local_total(pending * image), local_total(pending * pending)),
            (("gx_0", "gx_1"), ("gy_0", "gy_1")),
        )
        beta = jnp.sqrt(squares / total + FLOOR)
        basis = lax.dynamic_update_index_in_dim(basis, pending / beta, step, 0)
        coeffs = projected / (total * beta) + jnp.where(
            slots == step, crossed / (total * beta * beta), 0.0
        )
        pending = image / beta - jnp.einsum("k,kqxy->qxy", coeffs, basis, precision=highest)
        hessen = hessen + jnp.where(cols == step, coeffs[:, None], 0.0)
        hessen = hessen + jnp.where((rows == step) & (cols == step - 1), beta, 0.0)
        return (basis, hessen, pending)

    basis, hessen, pending = lax.fori_loop(0, ITERS, advance, (basis, hessen, first))
    beta = norm_scale(pending, total)
    basis = basis.at[ITERS].set(pending / beta)
    hessen = hessen + jnp.where((rows == ITERS) & (cols == ITERS - 1), beta, 0.0)
    return (hessen, basis)


NODES = P_SIZE * P_SIZE
ROWS = 16
DEPTH = 6
LANES = 128
SCALE = 0.125
AMP_LIMIT = 100.0
GRAM = [(k, l) for k in range(ITERS + 1) for l in range(k + 1)]


def lane_ids(rows):
    return lax.broadcasted_iota(jnp.int32, (rows, LANES), 1)


def turned(value, shift):
    shift = shift % LANES
    return value if shift == 0 else pltpu.roll(value, shift, 1)


def strided(ref, start, count):
    return ref[pl.ds(start, count, stride=4), :]


BLOCK = 136
REACT, THICK, OPEN = 64, 128, 129
FIRST_WEST, LAST_EAST, ENDS = 544, 552, 560


def split(value):
    high = value.astype(jnp.bfloat16)
    rest = value - high.astype(jnp.float32)
    middle = rest.astype(jnp.bfloat16)
    low = (rest - middle.astype(jnp.float32)).astype(jnp.bfloat16)
    return high, middle, low


def weights_in(line, deriv):
    sub = lax.broadcasted_iota(jnp.int32, (8, NODES), 0)
    lane = lax.broadcasted_iota(jnp.int32, (8, NODES), 1)
    along, across = lane // 8, lane % 8
    outer = jnp.zeros((8, NODES), jnp.float32)
    inner = jnp.zeros((8, NODES), jnp.float32)
    for c in range(P_SIZE):
        column = jnp.broadcast_to(line[:, c : c + 1], (8, NODES))
        outer = jnp.where(along == c, column, outer)
        inner = jnp.where(across == c, column, inner)
    parts = []
    for a in range(P_SIZE):
        row = jnp.broadcast_to(outer[a : a + 1, :], (8, NODES))
        parts.append(jnp.where(across == sub, row, 0.0) + jnp.where(along == a, inner, 0.0))
    for first, second in ((along, across), (across, along)):
        for flip in (False, True):
            part = jnp.zeros((8, NODES), jnp.float32)
            for c in range(P_SIZE):
                value = SCALE * (0.5 * deriv[0:1, c : c + 1] + (TAU if c == 0 else 0.0))
                part = jnp.where(first == (P_SIZE - 1 - c if flip else c), value, part)
            parts.append(jnp.where(second == sub, part, 0.0))
    high, middle, low = split(jnp.concatenate(parts, axis=0))
    return jnp.concatenate([high, high, high, middle, middle, low], axis=1)


def product(weight, value):
    high, middle, low = split(value)
    stacked = jnp.concatenate([high, middle, low, high, middle, high], axis=0)
    return jnp.dot(weight[...], stacked, preferred_element_type=jnp.float32)


def centre(line, deriv):
    diagonal = lax.broadcasted_iota(jnp.int32, (8, 8), 0) == lax.broadcasted_iota(jnp.int32, (8, 8), 1)
    trace = jnp.sum(jnp.where(diagonal, line, 0.0), axis=1, keepdims=True)
    trace = jnp.sum(trace, axis=0, keepdims=True)
    return 2.0 + 0.3125 * trace + 0.5 * (TAU + 0.5 * deriv[0:1, 0:1])


def edges(a, west, east, south, north, sub):
    value = jnp.where(sub == 0, south[a : a + 1, :], 0.0)
    value = jnp.where(sub == P_SIZE - 1, north[a : a + 1, :], value)
    if a == 0 and west is not None:
        value = value + west
    if a == P_SIZE - 1 and east is not None:
        value = value + east
    return value


def pack_kernel(
    line_in, deriv_in, source, initial, reaction, stiffness, walls,
    raw, near, to_up, to_down, weight, shift_out, line, deriv, flags, sems,
):
    moves = [(line_in, line), (deriv_in, deriv)]
    for at, ref in ((0, initial), (256, source), (512, reaction)):
        for half in (0, 128):
            moves.append((ref.at[pl.ds(half, 128), :], raw.at[pl.ds(at + half, 128), :]))
    moves.append((stiffness, raw.at[pl.ds(768, 4), :]))
    moves.append((walls, flags))
    copies = [pltpu.make_async_copy(a, b, sems.at[n]) for n, (a, b) in enumerate(moves)]
    for copy in copies:
        copy.start()
    for copy in copies[:2]:
        copy.wait()
    line, deriv = line[...], deriv[...]
    weight[...] = weights_in(line, deriv)
    shift_out[...] = jnp.broadcast_to(centre(line, deriv), (8, LANES))
    for copy in copies[2:4]:
        copy.wait()
    sub = lax.broadcasted_iota(jnp.int32, (8, LANES), 0)
    lanes8 = lane_ids(8)
    fields, images = [], []
    for x in range(0, 4, 2):
        pair = jnp.concatenate([strided(raw, x, NODES), strided(raw, x + 1, NODES)], axis=1)
        image = product(weight, pair)
        for k in range(2):
            fields.append(pair[:, k * LANES : (k + 1) * LANES])
            images.append(image[:, k * LANES : (k + 1) * LANES])
    for copy in copies[4:]:
        copy.wait()
    opened = 1.0 - flags[...].astype(jnp.float32)
    raw[772:788, :] = opened
    raw[788:796, 0:P_SIZE] = line
    raw[796:797, 0:P_SIZE] = deriv
    thick = raw[768:772, :]
    traces = [[image[64 + 8 * f : 72 + 8 * f] for f in range(4)] for image in images]
    ends = jnp.zeros((8, LANES), jnp.float32)
    for x in range(4):
        at = BLOCK * x
        allowed = [jnp.broadcast_to(opened[4 * f + x : 4 * f + x + 1, :], (8, LANES)) for f in range(4)]
        faces = list(traces[x])
        if x > 0:
            faces[0] = faces[0] - allowed[0] * traces[x - 1][1]
        if x < 3:
            faces[1] = faces[1] - allowed[1] * traces[x + 1][0]
        faces[2] = faces[2] - allowed[2] * jnp.where(lanes8 == 0, 0.0, turned(traces[x][3], 1))
        faces[3] = faces[3] - allowed[3] * jnp.where(lanes8 == LANES - 1, 0.0, turned(traces[x][2], -1))
        faces = [8.0 * face for face in faces]
        ends = jnp.where(lanes8 == 8 * x + 7, turned(traces[x][2], 8 * x + 7), ends)
        ends = jnp.where(lanes8 == 8 * x, turned(traces[x][3], 8 * x + 1), ends)
        width = jnp.broadcast_to(thick[x : x + 1, :], (8, LANES))
        for a in range(P_SIZE):
            rows = slice(8 * a, 8 * a + 8)
            value = strided(raw, 512 + 32 * a + x, 8) * fields[x][rows] + width * images[x][rows]
            value = value + edges(a, *faces, sub)
            near[at + 8 * a : at + 8 * a + 8, :] = strided(raw, 256 + 32 * a + x, 8) - value
        near[at + REACT : at + THICK, :] = strided(raw, 512 + x, NODES)
        rows = [thick[x : x + 1, :]] + [opened[4 * f + x : 4 * f + x + 1, :] for f in range(4)]
        near[at + THICK : at + BLOCK, :] = jnp.concatenate(rows + [jnp.zeros((3, LANES), jnp.float32)], axis=0)
    near[FIRST_WEST:LAST_EAST, :] = traces[0][0]
    near[LAST_EAST:ENDS, :] = traces[3][1]
    near[ENDS : ENDS + 8, :] = ends
    lanes = lane_ids(NODES)
    for out, first in ((to_up, 120), (to_down, 0)):
        totals = [jnp.zeros((n, LANES), jnp.float32) for n in (NODES, 32, 8)]
        for x in range(4):
            block = BLOCK * x
            parts = (
                (0, near[block : block + 64, :]),
                (0, near[block + REACT : block + THICK, :]),
                (1, jnp.concatenate(traces[x], axis=0)),
                (2, near[block + THICK : block + BLOCK, :]),
            )
            for field, (part, value) in enumerate(parts):
                at = 32 * field + 8 * x
                ids = lanes[0 : value.shape[0]]
                totals[part] = jnp.where((ids >= at) & (ids < at + 8), turned(value, at - first), totals[part])
        out[0:8, :] = totals[0][0:8] + totals[1][0:8] + totals[2]
        out[8:32, :] = totals[0][8:32] + totals[1][8:32]
        out[32:64, :] = totals[0][32:64]


def far_kernel(near, left, right, strip, high2, low2):
    lanes = lane_ids(NODES)
    strip[0:64, :] = jnp.where(lanes < 64, left[...], turned(right[...], 64))
    lanes = lanes[0:32]
    edge = jnp.where(lanes < 32, turned(left[0:32, :], -64), turned(right[0:32, :], -32))
    edge = jnp.where((lanes >= 64) & (lanes < 96), turned(left[0:32, :], -32), edge)
    edge = jnp.where(lanes >= 96, right[0:32, :], edge)
    strip[64:96, :] = edge
    for out, close, face in ((high2, 3, LAST_EAST), (low2, 0, FIRST_WEST)):
        block = BLOCK * close
        out[0:64, :] = near[block : block + 64, :]
        out[64:72, :] = near[block + THICK : block + BLOCK, :]
        out[72:80, :] = near[face : face + 8, :]
        out[80:88, :] = near[ENDS : ENDS + 8, :]
        out[88:120, :] = edge


def powers_kernel(
    shift_in, weight, near, below1, above1, below2, above2, own_strip, strip_b1, strip_a1,
    basis_out, gram_out, field_a, field_b, image, react, stiff, opened,
):
    shift = shift_in[0:1, :]

    def put(row, value_reaction, value_stiffness, value_open):
        cols = slice(row * LANES, (row + 1) * LANES)
        if value_reaction is not None:
            react[:, cols] = (value_reaction - shift) * SCALE
            stiff[:, cols] = jnp.broadcast_to(value_stiffness * SCALE, (8, LANES))
        for f in range(4):
            opened[8 * f : 8 * f + 8, cols] = jnp.broadcast_to(value_open[f], (8, LANES))

    local = {}
    for x in range(4):
        for ref, row in ((below1, 2 + x), (near, 6 + x), (above1, 10 + x)):
            at = BLOCK * x
            put(
                row, ref[at + REACT : at + THICK, :], ref[at + THICK : at + OPEN, :],
                [ref[at + OPEN + f : at + OPEN + f + 1, :] for f in range(4)],
            )
            local[row] = functools.partial(lambda ref, at, a: ref[at + 8 * a : at + 8 * a + 8, :], ref, at)
    for row, ref in ((1, below2), (ROWS - 2, above2)):
        put(row, None, None, [ref[65 + f : 66 + f, :] for f in range(4)])
        local[row] = functools.partial(lambda ref, a: ref[8 * a : 8 * a + 8, :], ref)

    lanes64 = lane_ids(NODES)
    lanes = lane_ids(8)
    pieces = ((strip_b1, 16, 48, 16), (own_strip, 48, 80, 48), (strip_a1, 80, 112, 80))
    strip_faces = []
    for side in range(2):
        made = []
        for top, count, zero in ((0, 64, 64 * side), (0, 64, 64 * side + 32), (64, 32, 32 * side), (64, 8, 64 + 32 * side)):
            ids = lanes64[0:count]
            value = jnp.zeros((count, LANES), jnp.float32)
            for ref, start, stop, target in pieces:
                part = turned(ref[top : top + count, :], target - zero)
                value = jnp.where((ids >= start) & (ids < stop), part, value)
            if count == 32:
                value = jnp.where(ids < 16, turned(below2[88:120, :], -16 - 32 * side), value)
                value = jnp.where(ids >= 112, turned(above2[88:120, :], 112 - 32 * side), value)
            made.append(value)
        put(ROWS + side, made[1], made[3][0:1], [made[3][1 + f : 2 + f] for f in range(4)])
        local[ROWS + side] = functools.partial(lambda value, a: value[8 * a : 8 * a + 8], made[0])
        strip_faces.append([made[2][8 * f : 8 * f + 8] for f in range(4)])
    ends = jnp.zeros((8, LANES), jnp.float32)
    for ref, top, start, stop, by in (
        (below2, 80, 0, 16, -16), (below1, ENDS, 16, 48, 16), (near, ENDS, 48, 80, 48),
        (above1, ENDS, 80, 112, 80), (above2, 80, 112, 128, 112),
    ):
        ends = jnp.where((lanes >= start) & (lanes < stop), turned(ref[top : top + 8, :], by), ends)

    def columns(row):
        return slice(row * LANES, (row + 1) * LANES)

    low, high = ROWS, ROWS + 1
    sub = lax.broadcasted_iota(jnp.int32, (8, LANES), 0)
    TW, TE, TS, TN = (slice(64 + 8 * f, 72 + 8 * f) for f in range(4))

    def begin(new):
        def finish(row, faces):
            cols = columns(row)
            faces = [
                None if value is None else 8.0 * opened[8 * f : 8 * f + 8, cols] * value
                for f, value in enumerate(faces)
            ]
            for a in range(P_SIZE):
                new[8 * a : 8 * a + 8, cols] = local[row](a) + edges(a, *faces, sub)

        west = {
            2: below2[72:80, :], 6: below1[LAST_EAST:ENDS, :], 10: near[LAST_EAST:ENDS, :],
            14: above1[LAST_EAST:ENDS, :],
        }
        east = {
            1: below1[FIRST_WEST:LAST_EAST, :], 5: near[FIRST_WEST:LAST_EAST, :],
            9: above1[FIRST_WEST:LAST_EAST, :], 13: above2[72:80, :],
        }
        for row in range(1, ROWS - 1):
            south = jnp.where(lanes == 0, turned(strip_faces[0][3], -(8 * row + 7)), 0.0)
            north = jnp.where(lanes == LANES - 1, turned(strip_faces[1][2], 127 - 8 * row), 0.0)
            finish(row, (west.get(row), east.get(row), south, north))
        none = jnp.zeros((8, LANES), jnp.float32)
        spot = lanes // 8 % 4
        for side in range(2):
            from_west = jnp.where(spot == 2, turned(strip_faces[side][1], 8), 0.0)
            from_east = jnp.where(spot == 1, turned(strip_faces[side][0], -8), 0.0)
            outer = jnp.where(lanes % 8 == (0 if side else 7), ends, 0.0)
            finish(ROWS + side, (from_west, from_east, outer if side else none, none if side else outer))

    def apply(old, new, step):
        start, stop = step, ROWS - step
        for first_row, last_row in ((start, stop), (ROWS, ROWS + 2)):
            for row in range(first_row, last_row, 2):
                cols = slice(row * LANES, (row + 2) * LANES)
                image[:, cols] = product(weight, old[:, cols])

        def finish(row, *sides):
            cols = columns(row)
            faces = [
                image[own, cols] - opened[8 * f : 8 * f + 8, cols] * value
                for f, (own, value) in enumerate(zip((TW, TE, TS, TN), sides))
            ]
            for a in range(P_SIZE):
                rows = slice(8 * a, 8 * a + 8)
                value = react[rows, cols] * old[rows, cols] + stiff[:, cols] * image[rows, cols]
                new[rows, cols] = value + edges(a, *faces, sub)

        north_low = image[TN, columns(low)]
        south_high = image[TS, columns(high)]
        for row in range(start + 1, stop - 1):
            cols = columns(row)
            from_south = jnp.where(
                lanes == 0, turned(north_low, -(8 * row + 7)), turned(image[TN, cols], 1)
            )
            from_north = jnp.where(
                lanes == LANES - 1, turned(south_high, 127 - 8 * row), turned(image[TS, cols], -1)
            )
            finish(row, image[TE, columns(row - 1)], image[TW, columns(row + 1)], from_south, from_north)
        if step == DEPTH - 1:
            return
        to_low = turned(image[TS, columns(low)], -1)
        to_high = turned(image[TN, columns(high)], 1)
        for row in range(start, stop):
            cols = columns(row)
            to_low = jnp.where(lanes == 8 * row + 7, turned(image[TS, cols], 8 * row + 7), to_low)
            to_high = jnp.where(lanes == 8 * row, turned(image[TN, cols], 8 * row + 1), to_high)
        cols = columns(low)
        finish(low, turned(image[TE, cols], 8), turned(image[TW, cols], -8), turned(image[TN, cols], 1), to_low)
        cols = columns(high)
        finish(high, turned(image[TE, cols], 8), turned(image[TW, cols], -8), to_high, turned(image[TS, cols], -1))

    old, new = field_a, field_b
    for step in range(DEPTH):
        if step:
            apply(old, new, step)
        else:
            begin(new)
        basis_out[step, :, :] = new[:, 6 * LANES : 10 * LANES]
        old, new = new, old

    sums = [jnp.zeros((8, LANES), jnp.float32) for _ in GRAM]
    for x in range(4):
        for a in range(P_SIZE):
            values = [basis_out[k, 8 * a : 8 * a + 8, x * LANES : (x + 1) * LANES] for k in range(ITERS + 1)]
            sums = [total + values[k] * values[l] for total, (k, l) in zip(sums, GRAM)]
    rows = [jnp.sum(total, axis=0, keepdims=True) for total in sums]
    rows = jnp.concatenate(rows + [jnp.zeros((24 - len(GRAM), LANES), jnp.float32)], axis=0)
    totals = jnp.sum(rows, axis=1, keepdims=True)
    place = lax.broadcasted_iota(jnp.int32, (24, LANES), 0) == lax.broadcasted_iota(jnp.int32, (24, LANES), 1)
    totals = jnp.sum(jnp.where(place, totals, 0.0), axis=0, keepdims=True)
    gram_out[...] = jnp.broadcast_to(totals, gram_out.shape)


def combine_kernel(nodes, shift_in, powers, gathered, basis_out, hess_out, amp_out):
    shift = shift_in[...]
    row = jnp.sum(gathered[...], axis=0, keepdims=True) * (1.0 / nodes)
    spread = jnp.broadcast_to(row, (8, LANES))
    gram = {}
    for at, (k, l) in enumerate(GRAM):
        gram[k, l] = gram[l, k] = jnp.broadcast_to(spread[:, at : at + 1], (8, LANES))
    sizes = [jnp.sqrt(gram[k, k]) for k in range(ITERS + 1)]
    sub = lax.broadcasted_iota(jnp.int32, (8, LANES), 0)
    lanes = lane_ids(8)
    hess = jnp.zeros((8, LANES), jnp.float32)
    beta = jnp.sqrt(gram[0, 0] + FLOOR)
    coeffs = [[1.0 / beta]]
    amp = sizes[0] * coeffs[0][0]

    def put(hess, i, j, value):
        return jnp.where((sub == i) & (lanes == j), value, hess)

    for j in range(ITERS):
        last = coeffs[j]
        image = [shift * c for c in last] + [None]
        for k in range(j + 1):
            moved = last[k] * 8.0
            image[k + 1] = moved if image[k + 1] is None else image[k + 1] + moved
        weighted = [
            sum(gram[k, l] * image[l] for l in range(1, j + 2)) + gram[k, 0] * image[0] for k in range(j + 2)
        ]
        pending = list(image)
        for i in range(j + 1):
            h = sum(c * weighted[k] for k, c in enumerate(coeffs[i]))
            hess = put(hess, i, j, h)
            for k, c in enumerate(coeffs[i]):
                pending[k] = pending[k] - h * c
        square = sum(
            pending[k] * sum(gram[k, l] * pending[l] for l in range(j + 2)) for k in range(j + 2)
        )
        beta = jnp.sqrt(jnp.maximum(square, 0.0) + FLOOR)
        hess = put(hess, j + 1, j, beta)
        scale = 1.0 / beta
        coeffs.append([p * scale for p in pending])
        amp = jnp.maximum(amp, sum(jnp.abs(c) * s for c, s in zip(coeffs[-1], sizes)))
    hess_out[...] = hess[0 : ITERS + 1, 0:ITERS]
    amp_out[...] = amp[0:1, :]
    for x in range(4):
        for a in range(P_SIZE):
            values = [powers[k, 8 * a : 8 * a + 8, x * LANES : (x + 1) * LANES] for k in range(ITERS + 1)]
            for j in range(ITERS + 1):
                total = coeffs[j][0] * values[0]
                for k in range(1, j + 1):
                    total = total + coeffs[j][k] * values[k]
                basis_out[j, pl.ds(32 * a + x, 8, stride=4), :] = total


def fast(source, initial, reaction, stiffness, line_op, face_deriv, walls):
    vmem = pl.BlockSpec(memory_space=pltpu.VMEM)
    hbm = pl.BlockSpec(memory_space=pltpu.HBM)
    grant = pltpu.CompilerParams(vmem_limit_bytes=16 * 2**20)
    f32 = jnp.float32
    nx, ny = lax.axis_size(GX), lax.axis_size(GY)
    wide = (ROWS + 2) * LANES

    def moved(value, axis, size, by):
        return lax.ppermute(value, axis, [(i, (i + by) % size) for i in range(size)])

    held = (line_op, face_deriv.reshape(1, P_SIZE), source, initial, reaction, stiffness, walls)
    raw, near, to_up, to_down, weight, shift = pl.pallas_call(
        pack_kernel,
        out_shape=[jax.ShapeDtypeStruct((n, LANES), f32) for n in (800, ENDS + 8, NODES, NODES)]
        + [jax.ShapeDtypeStruct((NODES + 32, 6 * NODES), jnp.bfloat16), jax.ShapeDtypeStruct((8, LANES), f32)],
        in_specs=[hbm] * 7,
        out_specs=[vmem] * 6,
        scratch_shapes=[
            pltpu.VMEM((P_SIZE, P_SIZE), f32),
            pltpu.VMEM((1, P_SIZE), f32),
            pltpu.VMEM((16, LANES), jnp.int32),
            pltpu.SemaphoreType.DMA((10,)),
        ],
        compiler_params=grant,
    )(*[pltpu.with_memory_space_constraint(v, pltpu.HBM) for v in held])
    left = moved(to_up, GY, ny, 1)
    right = moved(to_down, GY, ny, -1)
    below1 = moved(near, GX, nx, 1)
    above1 = moved(near, GX, nx, -1)
    strip, high2, low2 = pl.pallas_call(
        far_kernel,
        out_shape=[jax.ShapeDtypeStruct((n, LANES), f32) for n in (96, 120, 120)],
        in_specs=[vmem] * 3,
        out_specs=[vmem] * 3,
        compiler_params=grant,
    )(near, left, right)
    below2 = moved(high2, GX, nx, 2)
    above2 = moved(low2, GX, nx, -2)
    strips = [moved(strip, GX, nx, by) for by in (1, -1)]

    powers, gram = pl.pallas_call(
        powers_kernel,
        out_shape=[
            jax.ShapeDtypeStruct((ITERS + 1, NODES, 4 * LANES), f32),
            jax.ShapeDtypeStruct((1, LANES), f32),
        ],
        in_specs=[vmem] * 10,
        out_specs=[vmem] * 2,
        scratch_shapes=[pltpu.VMEM((n, wide), f32) for n in (NODES, NODES, NODES + 32, NODES, 8, 32)],
        compiler_params=grant,
    )(shift, weight, near, below1, above1, below2, above2, strip, *strips)
    every = GX + GY
    copies = jnp.broadcast_to(gram, (nx * ny, LANES))
    gathered = lax.all_to_all(copies, every, split_axis=0, concat_axis=0, tiled=True)
    basis, hess, amp = pl.pallas_call(
        functools.partial(combine_kernel, float(NODES * 4 * nx * LANES * ny)),
        out_shape=[
            jax.ShapeDtypeStruct((ITERS + 1, 4 * NODES, LANES), f32),
            jax.ShapeDtypeStruct((ITERS + 1, ITERS), f32),
            jax.ShapeDtypeStruct((1, LANES), f32),
        ],
        in_specs=[vmem] * 3,
        out_specs=[vmem] * 3,
        compiler_params=grant,
    )(shift, powers, gathered)
    return hess, basis, amp[0, 0], raw


def body(source, initial, reaction, stiffness, line_op, face_deriv, wall_flags):
    flat = [v.reshape(4 * NODES, LANES) for v in (source, initial, reaction)]
    hess, basis, amp, raw = fast(*flat, stiffness, line_op, face_deriv, wall_flags.reshape(16, LANES))

    def again(carry):
        raw = lax.optimization_barrier(carry[3])
        initial, source, reaction = raw[0:768].reshape(3, NODES, 4, LANES)
        opened = raw[772:788].reshape(4, 4, LANES)
        line_op, face_deriv = raw[788:796, 0:P_SIZE], raw[796, 0:P_SIZE]
        hess, basis = stepwise(source, initial, reaction, raw[768:772], line_op, face_deriv, opened)
        return jnp.bool_(True), hess, basis.reshape(ITERS + 1, 4 * NODES, LANES), raw

    done = amp <= AMP_LIMIT
    carry = lax.while_loop(lambda carry: jnp.logical_not(carry[0]), again, (done, hess, basis, raw))
    return (carry[1], carry[2].reshape(ITERS + 1, NODES, 4, LANES))


def solution(mesh):
    finer = Mesh(mesh.devices.reshape(4, 2, 4, 8), ("gx_0", "gx_1", "gy_0", "gy_1"))
    placed = (
        P(None, GX, GY),
        P(None, GX, GY),
        P(None, GX, GY),
        P(GX, GY),
        P(),
        P(),
        P(None, GX, GY),
    )
    return jax.shard_map(
        body, mesh=finer, in_specs=placed, out_specs=(P(), P(None, None, GX, GY)), check_vma=False
    )
```

```python
import functools

import jax
import jax.numpy as jnp
from jax import lax
from jax.experimental import pallas as pl
from jax.experimental.pallas import tpu as pltpu
from jax.sharding import Mesh
from jax.sharding import PartitionSpec as P

P_SIZE = 8
ITERS = 5
GX = ("gx_0", "gx_1")
GY = ("gy_0", "gy_1")


TAU = 2.0
FLOOR = 0.1


def extended(array, sides, width):
    for axis, dim in sides:
        devices, length = (lax.axis_size(axis), array.shape[dim])
        up = [(i, (i + 1) % devices) for i in range(devices)]
        down = [(j, i) for i, j in up]
        last = lax.slice_in_dim(array, length - width, length, axis=dim)
        leading = lax.slice_in_dim(array, 0, width, axis=dim)
        before = lax.ppermute(last, axis, up)
        after = lax.ppermute(leading, axis, down)
        array = jnp.concatenate([before, array, after], axis=dim)
    return array


def sent_to_all(array, axis):
    copies = jnp.broadcast_to(array, (lax.axis_size(axis), *array.shape))
    return lax.all_to_all(copies, axis, split_axis=0, concat_axis=0, tiled=True)


def over_copies(array, axis):
    everything = sent_to_all(array, axis)
    return jnp.sum(everything, axis=0)


def by_axis(array, axes):
    far, near = axes
    nearer = over_copies(array, near)
    return over_copies(nearer, far)


def together(arrays, axis):
    vector, at, gathered = (jnp.concatenate([a.reshape(-1) for a in arrays]), 0, [])
    subtotal = by_axis(vector, axis)
    for a in arrays:
        gathered.append(subtotal[at : at + a.size].reshape(a.shape))
        at += a.size
    return tuple(gathered)


def local_total(values):
    return jnp.sum(jnp.sum(values, axis=0))


def x_traces(nodes, face_deriv):
    highest = lax.Precision.HIGHEST
    lower = jnp.einsum("c,cbxy->bxy", face_deriv, nodes, precision=highest)
    upper = jnp.einsum("c,cbxy->bxy", face_deriv[::-1], nodes, precision=highest)
    return jnp.stack([nodes[0], lower, nodes[-1], upper])


def y_traces(nodes, face_deriv):
    highest = lax.Precision.HIGHEST
    lower = jnp.einsum("c,acxy->axy", face_deriv, nodes, precision=highest)
    upper = jnp.einsum("c,acxy->axy", face_deriv[::-1], nodes, precision=highest)
    return jnp.stack([nodes[:, 0], lower, nodes[:, -1], upper])


def apply_op(field, reaction, stiffness, line_op, face_deriv, opened):
    highest = lax.Precision.HIGHEST
    nodes = field.reshape(P_SIZE, P_SIZE, field.shape[1], field.shape[2])
    interior = stiffness * (
        jnp.einsum("ac,cbxy->abxy", line_op, nodes, precision=highest)
        + jnp.einsum("bc,acxy->abxy", line_op, nodes, precision=highest)
    )
    xside = extended(x_traces(nodes, face_deriv), ((GX, 2),), 1)
    yside = extended(y_traces(nodes, face_deriv), ((GY, 3),), 1)
    x_own = xside[:, :, 1:-1]
    y_own = yside[:, :, :, 1:-1]
    east_nb = xside[0:2, :, 2:]
    west_nb = xside[2:4, :, :-2]
    north_nb = yside[0:2, :, :, 2:]
    south_nb = yside[2:4, :, :, :-2]
    add_east = TAU * (x_own[2] - opened[1] * east_nb[0]) + 0.5 * (x_own[3] - opened[1] * east_nb[1])
    add_west = TAU * (x_own[0] - opened[0] * west_nb[0]) + 0.5 * (x_own[1] - opened[0] * west_nb[1])
    add_north = TAU * (y_own[2] - opened[3] * north_nb[0]) + 0.5 * (
        y_own[3] - opened[3] * north_nb[1]
    )
    add_south = TAU * (y_own[0] - opened[2] * south_nb[0]) + 0.5 * (
        y_own[1] - opened[2] * south_nb[1]
    )
    result = reaction.reshape(nodes.shape) * nodes + interior
    result = result.at[0].add(add_west).at[P_SIZE - 1].add(add_east)
    result = result.at[:, 0].add(add_south).at[:, P_SIZE - 1].add(add_north)
    return result.reshape(field.shape)


def norm_scale(vector, total):
    squares = by_axis(local_total(vector * vector), (("gx_0", "gx_1"), ("gy_0", "gy_1")))
    return jnp.sqrt(squares / total + FLOOR)


def stepwise(source, initial, reaction, stiffness, line_op, face_deriv, opened):
    highest = lax.Precision.HIGHEST
    total = float(
        P_SIZE * P_SIZE * source.shape[1] * lax.axis_size(GX) * source.shape[2] * lax.axis_size(GY)
    )

    def operate(field):
        return apply_op(field, reaction, stiffness, line_op, face_deriv, opened)

    def products(basis, image):
        per_cell = jnp.einsum("kqxy,qxy->kxy", basis, image, precision=highest)
        return jnp.sum(per_cell, axis=(1, 2))

    first = source - operate(initial)
    basis = jnp.zeros((ITERS + 1,) + source.shape, jnp.float32)
    hessen = jnp.zeros((ITERS + 1, ITERS), jnp.float32)
    rows = lax.broadcasted_iota(jnp.int32, (ITERS + 1, ITERS), 0)
    cols = lax.broadcasted_iota(jnp.int32, (ITERS + 1, ITERS), 1)
    slots = lax.broadcasted_iota(jnp.int32, (ITERS + 1,), 0)

    def advance(step, carry):
        basis, hessen, pending = carry
        image = operate(pending)
        local = products(basis, image)
        projected, crossed, squares = together(
            (local, local_total(pending * image), local_total(pending * pending)),
            (("gx_0", "gx_1"), ("gy_0", "gy_1")),
        )
        beta = jnp.sqrt(squares / total + FLOOR)
        basis = lax.dynamic_update_index_in_dim(basis, pending / beta, step, 0)
        coeffs = projected / (total * beta) + jnp.where(
            slots == step, crossed / (total * beta * beta), 0.0
        )
        pending = image / beta - jnp.einsum("k,kqxy->qxy", coeffs, basis, precision=highest)
        hessen = hessen + jnp.where(cols == step, coeffs[:, None], 0.0)
        hessen = hessen + jnp.where((rows == step) & (cols == step - 1), beta, 0.0)
        return (basis, hessen, pending)

    basis, hessen, pending = lax.fori_loop(0, ITERS, advance, (basis, hessen, first))
    beta = norm_scale(pending, total)
    basis = basis.at[ITERS].set(pending / beta)
    hessen = hessen + jnp.where((rows == ITERS) & (cols == ITERS - 1), beta, 0.0)
    return (hessen, basis)


NODES = P_SIZE * P_SIZE
ROWS = 16
DEPTH = 6
LANES = 128
SCALE = 0.125
AMP_LIMIT = 100.0
GRAM = [(k, l) for k in range(ITERS + 1) for l in range(k + 1)]


def lane_ids(rows):
    return lax.broadcasted_iota(jnp.int32, (rows, LANES), 1)


def turned(value, shift):
    shift = shift % LANES
    return value if shift == 0 else pltpu.roll(value, shift, 1)


def strided(ref, start, count):
    return ref[pl.ds(start, count, stride=4), :]


BLOCK = 136
REACT, THICK, OPEN = 64, 128, 129
FIRST_WEST, LAST_EAST, ENDS = 544, 552, 560


def split(value):
    high = value.astype(jnp.bfloat16)
    rest = value - high.astype(jnp.float32)
    middle = rest.astype(jnp.bfloat16)
    low = (rest - middle.astype(jnp.float32)).astype(jnp.bfloat16)
    return high, middle, low


def weights_in(line, deriv):
    sub = lax.broadcasted_iota(jnp.int32, (8, NODES), 0)
    lane = lax.broadcasted_iota(jnp.int32, (8, NODES), 1)
    along, across = lane // 8, lane % 8
    outer = jnp.zeros((8, NODES), jnp.float32)
    inner = jnp.zeros((8, NODES), jnp.float32)
    for c in range(P_SIZE):
        column = jnp.broadcast_to(line[:, c : c + 1], (8, NODES))
        outer = jnp.where(along == c, column, outer)
        inner = jnp.where(across == c, column, inner)
    parts = []
    for a in range(P_SIZE):
        row = jnp.broadcast_to(outer[a : a + 1, :], (8, NODES))
        parts.append(jnp.where(across == sub, row, 0.0) + jnp.where(along == a, inner, 0.0))
    for first, second in ((along, across), (across, along)):
        for flip in (False, True):
            part = jnp.zeros((8, NODES), jnp.float32)
            for c in range(P_SIZE):
                value = SCALE * (0.5 * deriv[0:1, c : c + 1] + (TAU if c == 0 else 0.0))
                part = jnp.where(first == (P_SIZE - 1 - c if flip else c), value, part)
            parts.append(jnp.where(second == sub, part, 0.0))
    high, middle, low = split(jnp.concatenate(parts, axis=0))
    return jnp.concatenate([high, high, high, middle, middle, low], axis=1)


def product(weight, value):
    high, middle, low = split(value)
    stacked = jnp.concatenate([high, middle, low, high, middle, high], axis=0)
    return jnp.dot(weight[...], stacked, preferred_element_type=jnp.float32)


def centre(line, deriv):
    diagonal = lax.broadcasted_iota(jnp.int32, (8, 8), 0) == lax.broadcasted_iota(jnp.int32, (8, 8), 1)
    trace = jnp.sum(jnp.where(diagonal, line, 0.0), axis=1, keepdims=True)
    trace = jnp.sum(trace, axis=0, keepdims=True)
    return 2.0 + 0.3125 * trace + 0.5 * (TAU + 0.5 * deriv[0:1, 0:1])


def edges(a, west, east, south, north, sub):
    value = jnp.where(sub == 0, south[a : a + 1, :], 0.0)
    value = jnp.where(sub == P_SIZE - 1, north[a : a + 1, :], value)
    if a == 0 and west is not None:
        value = value + west
    if a == P_SIZE - 1 and east is not None:
        value = value + east
    return value


def pack_kernel(
    line_in, deriv_in, source, initial, reaction, stiffness, walls,
    raw, near, to_up, to_down, weight, shift_out, line, deriv, flags, sems,
):
    moves = [(line_in, line), (deriv_in, deriv)]
    for at, ref in ((0, initial), (256, source), (512, reaction)):
        for half in (0, 128):
            moves.append((ref.at[pl.ds(half, 128), :], raw.at[pl.ds(at + half, 128), :]))
    moves.append((stiffness, raw.at[pl.ds(768, 4), :]))
    moves.append((walls, flags))
    copies = [pltpu.make_async_copy(a, b, sems.at[n]) for n, (a, b) in enumerate(moves)]
    for copy in copies:
        copy.start()
    for copy in copies[:2]:
        copy.wait()
    line, deriv = line[...], deriv[...]
    weight[...] = weights_in(line, deriv)
    shift_out[...] = jnp.broadcast_to(centre(line, deriv), (8, LANES))
    for copy in copies[2:4]:
        copy.wait()
    sub = lax.broadcasted_iota(jnp.int32, (8, LANES), 0)
    lanes8 = lane_ids(8)
    fields, images = [], []
    for x in range(0, 4, 2):
        pair = jnp.concatenate([strided(raw, x, NODES), strided(raw, x + 1, NODES)], axis=1)
        image = product(weight, pair)
        for k in range(2):
            fields.append(pair[:, k * LANES : (k + 1) * LANES])
            images.append(image[:, k * LANES : (k + 1) * LANES])
    for copy in copies[4:]:
        copy.wait()
    opened = 1.0 - flags[...].astype(jnp.float32)
    raw[772:788, :] = opened
    raw[788:796, 0:P_SIZE] = line
    raw[796:797, 0:P_SIZE] = deriv
    thick = raw[768:772, :]
    traces = [[image[64 + 8 * f : 72 + 8 * f] for f in range(4)] for image in images]
    ends = jnp.zeros((8, LANES), jnp.float32)
    for x in range(4):
        at = BLOCK * x
        allowed = [jnp.broadcast_to(opened[4 * f + x : 4 * f + x + 1, :], (8, LANES)) for f in range(4)]
        faces = list(traces[x])
        if x > 0:
            faces[0] = faces[0] - allowed[0] * traces[x - 1][1]
        if x < 3:
            faces[1] = faces[1] - allowed[1] * traces[x + 1][0]
        faces[2] = faces[2] - allowed[2] * jnp.where(lanes8 == 0, 0.0, turned(traces[x][3], 1))
        faces[3] = faces[3] - allowed[3] * jnp.where(lanes8 == LANES - 1, 0.0, turned(traces[x][2], -1))
        faces = [8.0 * face for face in faces]
        ends = jnp.where(lanes8 == 8 * x + 7, turned(traces[x][2], 8 * x + 7), ends)
        ends = jnp.where(lanes8 == 8 * x, turned(traces[x][3], 8 * x + 1), ends)
        width = jnp.broadcast_to(thick[x : x + 1, :], (8, LANES))
        for a in range(P_SIZE):
            rows = slice(8 * a, 8 * a + 8)
            value = strided(raw, 512 + 32 * a + x, 8) * fields[x][rows] + width * images[x][rows]
            value = value + edges(a, *faces, sub)
            near[at + 8 * a : at + 8 * a + 8, :] = strided(raw, 256 + 32 * a + x, 8) - value
        near[at + REACT : at + THICK, :] = strided(raw, 512 + x, NODES)
        rows = [thick[x : x + 1, :]] + [opened[4 * f + x : 4 * f + x + 1, :] for f in range(4)]
        near[at + THICK : at + BLOCK, :] = jnp.concatenate(rows + [jnp.zeros((3, LANES), jnp.float32)], axis=0)
    near[FIRST_WEST:LAST_EAST, :] = traces[0][0]
    near[LAST_EAST:ENDS, :] = traces[3][1]
    near[ENDS : ENDS + 8, :] = ends
    lanes = lane_ids(NODES)
    for out, first in ((to_up, 120), (to_down, 0)):
        totals = [jnp.zeros((n, LANES), jnp.float32) for n in (NODES, 32, 8)]
        for x in range(4):
            block = BLOCK * x
            parts = (
                (0, near[block : block + 64, :]),
                (0, near[block + REACT : block + THICK, :]),
                (1, jnp.concatenate(traces[x], axis=0)),
                (2, near[block + THICK : block + BLOCK, :]),
            )
            for field, (part, value) in enumerate(parts):
                at = 32 * field + 8 * x
                ids = lanes[0 : value.shape[0]]
                totals[part] = jnp.where((ids >= at) & (ids < at + 8), turned(value, at - first), totals[part])
        out[0:8, :] = totals[0][0:8] + totals[1][0:8] + totals[2]
        out[8:32, :] = totals[0][8:32] + totals[1][8:32]
        out[32:64, :] = totals[0][32:64]


def far_kernel(near, left, right, strip, high2, low2):
    lanes = lane_ids(NODES)
    strip[0:64, :] = jnp.where(lanes < 64, left[...], turned(right[...], 64))
    lanes = lanes[0:32]
    edge = jnp.where(lanes < 32, turned(left[0:32, :], -64), turned(right[0:32, :], -32))
    edge = jnp.where((lanes >= 64) & (lanes < 96), turned(left[0:32, :], -32), edge)
    edge = jnp.where(lanes >= 96, right[0:32, :], edge)
    strip[64:96, :] = edge
    facing = (edge[8:32], jnp.concatenate([edge[0:8], edge[16:32]], axis=0))
    for out, close, face, corner in ((high2, 3, LAST_EAST, facing[0]), (low2, 0, FIRST_WEST, facing[1])):
        block = BLOCK * close
        out[0:64, :] = near[block : block + 64, :]
        out[64:72, :] = near[block + THICK : block + BLOCK, :]
        out[72:80, :] = near[face : face + 8, :]
        out[80:88, :] = near[ENDS : ENDS + 8, :]
        out[88:112, :] = corner


def powers_kernel(
    shift_in, weight, near, below1, above1, below2, above2, own_strip, strip_b1, strip_a1,
    basis_out, gram_out, field_a, field_b, image, react, stiff, opened,
):
    shift = shift_in[0:1, :]

    def put(row, value_reaction, value_stiffness, value_open):
        cols = slice(row * LANES, (row + 1) * LANES)
        if value_reaction is not None:
            react[:, cols] = (value_reaction - shift) * SCALE
            stiff[:, cols] = jnp.broadcast_to(value_stiffness * SCALE, (8, LANES))
        for f in range(4):
            opened[8 * f : 8 * f + 8, cols] = jnp.broadcast_to(value_open[f], (8, LANES))

    local = {}
    for x in range(4):
        for ref, row in ((below1, 2 + x), (near, 6 + x), (above1, 10 + x)):
            at = BLOCK * x
            put(
                row, ref[at + REACT : at + THICK, :], ref[at + THICK : at + OPEN, :],
                [ref[at + OPEN + f : at + OPEN + f + 1, :] for f in range(4)],
            )
            local[row] = functools.partial(lambda ref, at, a: ref[at + 8 * a : at + 8 * a + 8, :], ref, at)
    for row, ref in ((1, below2), (ROWS - 2, above2)):
        put(row, None, None, [ref[65 + f : 66 + f, :] for f in range(4)])
        local[row] = functools.partial(lambda ref, a: ref[8 * a : 8 * a + 8, :], ref)

    lanes64 = lane_ids(NODES)
    lanes = lane_ids(8)
    pieces = ((strip_b1, 16, 48, 16), (own_strip, 48, 80, 48), (strip_a1, 80, 112, 80))
    strip_faces = []
    for side in range(2):
        made = []
        for top, count, zero in ((0, 64, 64 * side), (0, 64, 64 * side + 32), (64, 32, 32 * side), (64, 8, 64 + 32 * side)):
            ids = lanes64[0:count]
            value = jnp.zeros((count, LANES), jnp.float32)
            for ref, start, stop, target in pieces:
                part = turned(ref[top : top + count, :], target - zero)
                value = jnp.where((ids >= start) & (ids < stop), part, value)
            if count == 32:
                blank = jnp.zeros((8, LANES), jnp.float32)
                corner = jnp.concatenate([blank, below2[88:112, :]], axis=0)
                value = jnp.where(ids < 16, turned(corner, -16 - 32 * side), value)
                corner = jnp.concatenate([above2[88:96, :], blank, above2[96:112, :]], axis=0)
                value = jnp.where(ids >= 112, turned(corner, 112 - 32 * side), value)
            made.append(value)
        put(ROWS + side, made[1], made[3][0:1], [made[3][1 + f : 2 + f] for f in range(4)])
        local[ROWS + side] = functools.partial(lambda value, a: value[8 * a : 8 * a + 8], made[0])
        strip_faces.append([made[2][8 * f : 8 * f + 8] for f in range(4)])
    ends = jnp.zeros((8, LANES), jnp.float32)
    for ref, top, start, stop, by in (
        (below2, 80, 0, 16, -16), (below1, ENDS, 16, 48, 16), (near, ENDS, 48, 80, 48),
        (above1, ENDS, 80, 112, 80), (above2, 80, 112, 128, 112),
    ):
        ends = jnp.where((lanes >= start) & (lanes < stop), turned(ref[top : top + 8, :], by), ends)

    def columns(row):
        return slice(row * LANES, (row + 1) * LANES)

    low, high = ROWS, ROWS + 1
    sub = lax.broadcasted_iota(jnp.int32, (8, LANES), 0)
    TW, TE, TS, TN = (slice(64 + 8 * f, 72 + 8 * f) for f in range(4))

    def begin(new):
        def finish(row, faces):
            cols = columns(row)
            faces = [
                None if value is None else 8.0 * opened[8 * f : 8 * f + 8, cols] * value
                for f, value in enumerate(faces)
            ]
            for a in range(P_SIZE):
                new[8 * a : 8 * a + 8, cols] = local[row](a) + edges(a, *faces, sub)

        west = {
            2: below2[72:80, :], 6: below1[LAST_EAST:ENDS, :], 10: near[LAST_EAST:ENDS, :],
            14: above1[LAST_EAST:ENDS, :],
        }
        east = {
            1: below1[FIRST_WEST:LAST_EAST, :], 5: near[FIRST_WEST:LAST_EAST, :],
            9: above1[FIRST_WEST:LAST_EAST, :], 13: above2[72:80, :],
        }
        for row in range(1, ROWS - 1):
            south = jnp.where(lanes == 0, turned(strip_faces[0][3], -(8 * row + 7)), 0.0)
            north = jnp.where(lanes == LANES - 1, turned(strip_faces[1][2], 127 - 8 * row), 0.0)
            finish(row, (west.get(row), east.get(row), south, north))
        none = jnp.zeros((8, LANES), jnp.float32)
        spot = lanes // 8 % 4
        for side in range(2):
            from_west = jnp.where(spot == 2, turned(strip_faces[side][1], 8), 0.0)
            from_east = jnp.where(spot == 1, turned(strip_faces[side][0], -8), 0.0)
            outer = jnp.where(lanes % 8 == (0 if side else 7), ends, 0.0)
            finish(ROWS + side, (from_west, from_east, outer if side else none, none if side else outer))

    def apply(old, new, step):
        start, stop = step, ROWS - step
        for first_row, last_row in ((start, stop), (ROWS, ROWS + 2)):
            for row in range(first_row, last_row, 2):
                cols = slice(row * LANES, (row + 2) * LANES)
                image[:, cols] = product(weight, old[:, cols])

        def finish(row, *sides):
            cols = columns(row)
            faces = [
                image[own, cols] - opened[8 * f : 8 * f + 8, cols] * value
                for f, (own, value) in enumerate(zip((TW, TE, TS, TN), sides))
            ]
            for a in range(P_SIZE):
                rows = slice(8 * a, 8 * a + 8)
                value = react[rows, cols] * old[rows, cols] + stiff[:, cols] * image[rows, cols]
                new[rows, cols] = value + edges(a, *faces, sub)

        north_low = image[TN, columns(low)]
        south_high = image[TS, columns(high)]
        for row in range(start + 1, stop - 1):
            cols = columns(row)
            from_south = jnp.where(
                lanes == 0, turned(north_low, -(8 * row + 7)), turned(image[TN, cols], 1)
            )
            from_north = jnp.where(
                lanes == LANES - 1, turned(south_high, 127 - 8 * row), turned(image[TS, cols], -1)
            )
            finish(row, image[TE, columns(row - 1)], image[TW, columns(row + 1)], from_south, from_north)
        if step == DEPTH - 1:
            return
        to_low = turned(image[TS, columns(low)], -1)
        to_high = turned(image[TN, columns(high)], 1)
        for row in range(start, stop):
            cols = columns(row)
            to_low = jnp.where(lanes == 8 * row + 7, turned(image[TS, cols], 8 * row + 7), to_low)
            to_high = jnp.where(lanes == 8 * row, turned(image[TN, cols], 8 * row + 1), to_high)
        cols = columns(low)
        finish(low, turned(image[TE, cols], 8), turned(image[TW, cols], -8), turned(image[TN, cols], 1), to_low)
        cols = columns(high)
        finish(high, turned(image[TE, cols], 8), turned(image[TW, cols], -8), to_high, turned(image[TS, cols], -1))

    old, new = field_a, field_b
    for step in range(DEPTH):
        if step:
            apply(old, new, step)
        else:
            begin(new)
        basis_out[step, :, :] = new[:, 6 * LANES : 10 * LANES]
        old, new = new, old

    sums = [jnp.zeros((8, LANES), jnp.float32) for _ in GRAM]
    for x in range(4):
        for a in range(P_SIZE):
            values = [basis_out[k, 8 * a : 8 * a + 8, x * LANES : (x + 1) * LANES] for k in range(ITERS + 1)]
            sums = [total + values[k] * values[l] for total, (k, l) in zip(sums, GRAM)]
    rows = [jnp.sum(total, axis=0, keepdims=True) for total in sums]
    rows = jnp.concatenate(rows + [jnp.zeros((24 - len(GRAM), LANES), jnp.float32)], axis=0)
    totals = jnp.sum(rows, axis=1, keepdims=True)
    place = lax.broadcasted_iota(jnp.int32, (24, LANES), 0) == lax.broadcasted_iota(jnp.int32, (24, LANES), 1)
    totals = jnp.sum(jnp.where(place, totals, 0.0), axis=0, keepdims=True)
    gram_out[...] = jnp.broadcast_to(totals, gram_out.shape)


def combine_kernel(nodes, shift_in, powers, gathered, basis_out, hess_out, amp_out):
    shift = shift_in[...]
    row = jnp.sum(gathered[...], axis=0, keepdims=True) * (1.0 / nodes)
    spread = jnp.broadcast_to(row, (8, LANES))
    gram = {}
    for at, (k, l) in enumerate(GRAM):
        gram[k, l] = gram[l, k] = jnp.broadcast_to(spread[:, at : at + 1], (8, LANES))
    sizes = [jnp.sqrt(gram[k, k]) for k in range(ITERS + 1)]
    sub = lax.broadcasted_iota(jnp.int32, (8, LANES), 0)
    lanes = lane_ids(8)
    hess = jnp.zeros((8, LANES), jnp.float32)
    beta = jnp.sqrt(gram[0, 0] + FLOOR)
    coeffs = [[1.0 / beta]]
    amp = sizes[0] * coeffs[0][0]

    def put(hess, i, j, value):
        return jnp.where((sub == i) & (lanes == j), value, hess)

    for j in range(ITERS):
        last = coeffs[j]
        image = [shift * c for c in last] + [None]
        for k in range(j + 1):
            moved = last[k] * 8.0
            image[k + 1] = moved if image[k + 1] is None else image[k + 1] + moved
        weighted = [
            sum(gram[k, l] * image[l] for l in range(1, j + 2)) + gram[k, 0] * image[0] for k in range(j + 2)
        ]
        pending = list(image)
        for i in range(j + 1):
            h = sum(c * weighted[k] for k, c in enumerate(coeffs[i]))
            hess = put(hess, i, j, h)
            for k, c in enumerate(coeffs[i]):
                pending[k] = pending[k] - h * c
        square = sum(
            pending[k] * sum(gram[k, l] * pending[l] for l in range(j + 2)) for k in range(j + 2)
        )
        beta = jnp.sqrt(jnp.maximum(square, 0.0) + FLOOR)
        hess = put(hess, j + 1, j, beta)
        scale = 1.0 / beta
        coeffs.append([p * scale for p in pending])
        amp = jnp.maximum(amp, sum(jnp.abs(c) * s for c, s in zip(coeffs[-1], sizes)))
    hess_out[...] = hess[0 : ITERS + 1, 0:ITERS]
    amp_out[...] = amp[0:1, :]
    for x in range(4):
        for a in range(P_SIZE):
            values = [powers[k, 8 * a : 8 * a + 8, x * LANES : (x + 1) * LANES] for k in range(ITERS + 1)]
            for j in range(ITERS + 1):
                total = coeffs[j][0] * values[0]
                for k in range(1, j + 1):
                    total = total + coeffs[j][k] * values[k]
                basis_out[j, pl.ds(32 * a + x, 8, stride=4), :] = total


def fast(source, initial, reaction, stiffness, line_op, face_deriv, walls):
    vmem = pl.BlockSpec(memory_space=pltpu.VMEM)
    hbm = pl.BlockSpec(memory_space=pltpu.HBM)
    grant = pltpu.CompilerParams(vmem_limit_bytes=16 * 2**20)
    f32 = jnp.float32
    nx, ny = lax.axis_size(GX), lax.axis_size(GY)
    wide = (ROWS + 2) * LANES

    def moved(value, axis, size, by):
        return lax.ppermute(value, axis, [(i, (i + by) % size) for i in range(size)])

    held = (line_op, face_deriv.reshape(1, P_SIZE), source, initial, reaction, stiffness, walls)
    raw, near, to_up, to_down, weight, shift = pl.pallas_call(
        pack_kernel,
        out_shape=[jax.ShapeDtypeStruct((n, LANES), f32) for n in (800, ENDS + 8, NODES, NODES)]
        + [jax.ShapeDtypeStruct((NODES + 32, 6 * NODES), jnp.bfloat16), jax.ShapeDtypeStruct((8, LANES), f32)],
        in_specs=[hbm] * 7,
        out_specs=[vmem] * 6,
        scratch_shapes=[
            pltpu.VMEM((P_SIZE, P_SIZE), f32),
            pltpu.VMEM((1, P_SIZE), f32),
            pltpu.VMEM((16, LANES), jnp.int32),
            pltpu.SemaphoreType.DMA((10,)),
        ],
        compiler_params=grant,
    )(*[pltpu.with_memory_space_constraint(v, pltpu.HBM) for v in held])
    left = moved(to_up, GY, ny, 1)
    right = moved(to_down, GY, ny, -1)
    below1 = moved(near, GX, nx, 1)
    above1 = moved(near, GX, nx, -1)
    strip, high2, low2 = pl.pallas_call(
        far_kernel,
        out_shape=[jax.ShapeDtypeStruct((n, LANES), f32) for n in (96, 112, 112)],
        in_specs=[vmem] * 3,
        out_specs=[vmem] * 3,
        compiler_params=grant,
    )(near, left, right)
    below2 = moved(high2, GX, nx, 2)
    above2 = moved(low2, GX, nx, -2)
    strips = [moved(strip, GX, nx, by) for by in (1, -1)]

    powers, gram = pl.pallas_call(
        powers_kernel,
        out_shape=[
            jax.ShapeDtypeStruct((ITERS + 1, NODES, 4 * LANES), f32),
            jax.ShapeDtypeStruct((1, LANES), f32),
        ],
        in_specs=[vmem] * 10,
        out_specs=[vmem] * 2,
        scratch_shapes=[pltpu.VMEM((n, wide), f32) for n in (NODES, NODES, NODES + 32, NODES, 8, 32)],
        compiler_params=grant,
    )(shift, weight, near, below1, above1, below2, above2, strip, *strips)
    every = GX + GY
    copies = jnp.broadcast_to(gram, (nx * ny, LANES))
    gathered = lax.all_to_all(copies, every, split_axis=0, concat_axis=0, tiled=True)
    basis, hess, amp = pl.pallas_call(
        functools.partial(combine_kernel, float(NODES * 4 * nx * LANES * ny)),
        out_shape=[
            jax.ShapeDtypeStruct((ITERS + 1, 4 * NODES, LANES), f32),
            jax.ShapeDtypeStruct((ITERS + 1, ITERS), f32),
            jax.ShapeDtypeStruct((1, LANES), f32),
        ],
        in_specs=[vmem] * 3,
        out_specs=[vmem] * 3,
        compiler_params=grant,
    )(shift, powers, gathered)
    return hess, basis, amp[0, 0], raw


def body(source, initial, reaction, stiffness, line_op, face_deriv, wall_flags):
    flat = [v.reshape(4 * NODES, LANES) for v in (source, initial, reaction)]
    hess, basis, amp, raw = fast(*flat, stiffness, line_op, face_deriv, wall_flags.reshape(16, LANES))

    def again(carry):
        raw = lax.optimization_barrier(carry[3])
        initial, source, reaction = raw[0:768].reshape(3, NODES, 4, LANES)
        opened = raw[772:788].reshape(4, 4, LANES)
        line_op, face_deriv = raw[788:796, 0:P_SIZE], raw[796, 0:P_SIZE]
        hess, basis = stepwise(source, initial, reaction, raw[768:772], line_op, face_deriv, opened)
        return jnp.bool_(True), hess, basis.reshape(ITERS + 1, 4 * NODES, LANES), raw

    done = amp <= AMP_LIMIT
    carry = lax.while_loop(lambda carry: jnp.logical_not(carry[0]), again, (done, hess, basis, raw))
    return (carry[1], carry[2].reshape(ITERS + 1, NODES, 4, LANES))


def solution(mesh):
    finer = Mesh(mesh.devices.reshape(4, 2, 4, 8), ("gx_0", "gx_1", "gy_0", "gy_1"))
    placed = (
        P(None, GX, GY),
        P(None, GX, GY),
        P(None, GX, GY),
        P(GX, GY),
        P(),
        P(),
        P(None, GX, GY),
    )
    return jax.shard_map(
        body, mesh=finer, in_specs=placed, out_specs=(P(), P(None, None, GX, GY)), check_vma=False
    )
```

```python
import functools

import jax
import jax.numpy as jnp
from jax import lax
from jax.experimental import pallas as pl
from jax.experimental.pallas import tpu as pltpu
from jax.sharding import Mesh
from jax.sharding import PartitionSpec as P

P_SIZE = 8
ITERS = 5
GX = ("gx_0", "gx_1")
GY = ("gy_0", "gy_1")


TAU = 2.0
FLOOR = 0.1


def extended(array, sides, width):
    for axis, dim in sides:
        devices, length = (lax.axis_size(axis), array.shape[dim])
        up = [(i, (i + 1) % devices) for i in range(devices)]
        down = [(j, i) for i, j in up]
        last = lax.slice_in_dim(array, length - width, length, axis=dim)
        leading = lax.slice_in_dim(array, 0, width, axis=dim)
        before = lax.ppermute(last, axis, up)
        after = lax.ppermute(leading, axis, down)
        array = jnp.concatenate([before, array, after], axis=dim)
    return array


def sent_to_all(array, axis):
    copies = jnp.broadcast_to(array, (lax.axis_size(axis), *array.shape))
    return lax.all_to_all(copies, axis, split_axis=0, concat_axis=0, tiled=True)


def over_copies(array, axis):
    everything = sent_to_all(array, axis)
    return jnp.sum(everything, axis=0)


def by_axis(array, axes):
    far, near = axes
    nearer = over_copies(array, near)
    return over_copies(nearer, far)


def together(arrays, axis):
    vector, at, gathered = (jnp.concatenate([a.reshape(-1) for a in arrays]), 0, [])
    subtotal = by_axis(vector, axis)
    for a in arrays:
        gathered.append(subtotal[at : at + a.size].reshape(a.shape))
        at += a.size
    return tuple(gathered)


def local_total(values):
    return jnp.sum(jnp.sum(values, axis=0))


def x_traces(nodes, face_deriv):
    highest = lax.Precision.HIGHEST
    lower = jnp.einsum("c,cbxy->bxy", face_deriv, nodes, precision=highest)
    upper = jnp.einsum("c,cbxy->bxy", face_deriv[::-1], nodes, precision=highest)
    return jnp.stack([nodes[0], lower, nodes[-1], upper])


def y_traces(nodes, face_deriv):
    highest = lax.Precision.HIGHEST
    lower = jnp.einsum("c,acxy->axy", face_deriv, nodes, precision=highest)
    upper = jnp.einsum("c,acxy->axy", face_deriv[::-1], nodes, precision=highest)
    return jnp.stack([nodes[:, 0], lower, nodes[:, -1], upper])


def apply_op(field, reaction, stiffness, line_op, face_deriv, opened):
    highest = lax.Precision.HIGHEST
    nodes = field.reshape(P_SIZE, P_SIZE, field.shape[1], field.shape[2])
    interior = stiffness * (
        jnp.einsum("ac,cbxy->abxy", line_op, nodes, precision=highest)
        + jnp.einsum("bc,acxy->abxy", line_op, nodes, precision=highest)
    )
    xside = extended(x_traces(nodes, face_deriv), ((GX, 2),), 1)
    yside = extended(y_traces(nodes, face_deriv), ((GY, 3),), 1)
    x_own = xside[:, :, 1:-1]
    y_own = yside[:, :, :, 1:-1]
    east_nb = xside[0:2, :, 2:]
    west_nb = xside[2:4, :, :-2]
    north_nb = yside[0:2, :, :, 2:]
    south_nb = yside[2:4, :, :, :-2]
    add_east = TAU * (x_own[2] - opened[1] * east_nb[0]) + 0.5 * (x_own[3] - opened[1] * east_nb[1])
    add_west = TAU * (x_own[0] - opened[0] * west_nb[0]) + 0.5 * (x_own[1] - opened[0] * west_nb[1])
    add_north = TAU * (y_own[2] - opened[3] * north_nb[0]) + 0.5 * (
        y_own[3] - opened[3] * north_nb[1]
    )
    add_south = TAU * (y_own[0] - opened[2] * south_nb[0]) + 0.5 * (
        y_own[1] - opened[2] * south_nb[1]
    )
    result = reaction.reshape(nodes.shape) * nodes + interior
    result = result.at[0].add(add_west).at[P_SIZE - 1].add(add_east)
    result = result.at[:, 0].add(add_south).at[:, P_SIZE - 1].add(add_north)
    return result.reshape(field.shape)


def norm_scale(vector, total):
    squares = by_axis(local_total(vector * vector), (("gx_0", "gx_1"), ("gy_0", "gy_1")))
    return jnp.sqrt(squares / total + FLOOR)


def stepwise(source, initial, reaction, stiffness, line_op, face_deriv, opened):
    highest = lax.Precision.HIGHEST
    total = float(
        P_SIZE * P_SIZE * source.shape[1] * lax.axis_size(GX) * source.shape[2] * lax.axis_size(GY)
    )

    def operate(field):
        return apply_op(field, reaction, stiffness, line_op, face_deriv, opened)

    def products(basis, image):
        per_cell = jnp.einsum("kqxy,qxy->kxy", basis, image, precision=highest)
        return jnp.sum(per_cell, axis=(1, 2))

    first = source - operate(initial)
    basis = jnp.zeros((ITERS + 1,) + source.shape, jnp.float32)
    hessen = jnp.zeros((ITERS + 1, ITERS), jnp.float32)
    rows = lax.broadcasted_iota(jnp.int32, (ITERS + 1, ITERS), 0)
    cols = lax.broadcasted_iota(jnp.int32, (ITERS + 1, ITERS), 1)
    slots = lax.broadcasted_iota(jnp.int32, (ITERS + 1,), 0)

    def advance(step, carry):
        basis, hessen, pending = carry
        image = operate(pending)
        local = products(basis, image)
        projected, crossed, squares = together(
            (local, local_total(pending * image), local_total(pending * pending)),
            (("gx_0", "gx_1"), ("gy_0", "gy_1")),
        )
        beta = jnp.sqrt(squares / total + FLOOR)
        basis = lax.dynamic_update_index_in_dim(basis, pending / beta, step, 0)
        coeffs = projected / (total * beta) + jnp.where(
            slots == step, crossed / (total * beta * beta), 0.0
        )
        pending = image / beta - jnp.einsum("k,kqxy->qxy", coeffs, basis, precision=highest)
        hessen = hessen + jnp.where(cols == step, coeffs[:, None], 0.0)
        hessen = hessen + jnp.where((rows == step) & (cols == step - 1), beta, 0.0)
        return (basis, hessen, pending)

    basis, hessen, pending = lax.fori_loop(0, ITERS, advance, (basis, hessen, first))
    beta = norm_scale(pending, total)
    basis = basis.at[ITERS].set(pending / beta)
    hessen = hessen + jnp.where((rows == ITERS) & (cols == ITERS - 1), beta, 0.0)
    return (hessen, basis)


NODES = P_SIZE * P_SIZE
ROWS = 16
DEPTH = 6
LANES = 128
SCALE = 0.125
AMP_LIMIT = 100.0
GRAM = [(k, l) for k in range(ITERS + 1) for l in range(k + 1)]


def lane_ids(rows):
    return lax.broadcasted_iota(jnp.int32, (rows, LANES), 1)


def turned(value, shift):
    shift = shift % LANES
    return value if shift == 0 else pltpu.roll(value, shift, 1)


def strided(ref, start, count):
    return ref[pl.ds(start, count, stride=4), :]


BLOCK = 136
REACT, THICK, OPEN = 64, 128, 129
FIRST_WEST, LAST_EAST, ENDS = 544, 552, 560


def split(value):
    high = value.astype(jnp.bfloat16)
    rest = value - high.astype(jnp.float32)
    middle = rest.astype(jnp.bfloat16)
    low = (rest - middle.astype(jnp.float32)).astype(jnp.bfloat16)
    return high, middle, low


def weights_in(line, deriv):
    sub = lax.broadcasted_iota(jnp.int32, (8, NODES), 0)
    lane = lax.broadcasted_iota(jnp.int32, (8, NODES), 1)
    along, across = lane // 8, lane % 8
    outer = jnp.zeros((8, NODES), jnp.float32)
    inner = jnp.zeros((8, NODES), jnp.float32)
    for c in range(P_SIZE):
        column = jnp.broadcast_to(line[:, c : c + 1], (8, NODES))
        outer = jnp.where(along == c, column, outer)
        inner = jnp.where(across == c, column, inner)
    parts = []
    for a in range(P_SIZE):
        row = jnp.broadcast_to(outer[a : a + 1, :], (8, NODES))
        parts.append(jnp.where(across == sub, row, 0.0) + jnp.where(along == a, inner, 0.0))
    for first, second in ((along, across), (across, along)):
        for flip in (False, True):
            part = jnp.zeros((8, NODES), jnp.float32)
            for c in range(P_SIZE):
                value = SCALE * (0.5 * deriv[0:1, c : c + 1] + (TAU if c == 0 else 0.0))
                part = jnp.where(first == (P_SIZE - 1 - c if flip else c), value, part)
            parts.append(jnp.where(second == sub, part, 0.0))
    high, middle, low = split(jnp.concatenate(parts, axis=0))
    return jnp.concatenate([high, high, high, middle, middle, low], axis=1)


def product(weight, value):
    high, middle, low = split(value)
    stacked = jnp.concatenate([high, middle, low, high, middle, high], axis=0)
    return jnp.dot(weight[...], stacked, preferred_element_type=jnp.float32)


def centre(line, deriv):
    diagonal = lax.broadcasted_iota(jnp.int32, (8, 8), 0) == lax.broadcasted_iota(jnp.int32, (8, 8), 1)
    trace = jnp.sum(jnp.where(diagonal, line, 0.0), axis=1, keepdims=True)
    trace = jnp.sum(trace, axis=0, keepdims=True)
    return 2.0 + 0.3125 * trace + 0.5 * (TAU + 0.5 * deriv[0:1, 0:1])


def edges(a, west, east, south, north, sub):
    value = jnp.where(sub == 0, south[a : a + 1, :], 0.0)
    value = jnp.where(sub == P_SIZE - 1, north[a : a + 1, :], value)
    if a == 0 and west is not None:
        value = value + west
    if a == P_SIZE - 1 and east is not None:
        value = value + east
    return value


def pack_kernel(
    line_in, deriv_in, source, initial, reaction, stiffness, walls,
    raw, near, to_up, to_down, weight, shift_out, line, deriv, flags, sems,
):
    moves = [(line_in, line), (deriv_in, deriv)]
    for at, ref in ((0, initial), (256, source), (512, reaction)):
        for half in (0, 128):
            moves.append((ref.at[pl.ds(half, 128), :], raw.at[pl.ds(at + half, 128), :]))
    moves.append((stiffness, raw.at[pl.ds(768, 4), :]))
    moves.append((walls, flags))
    copies = [pltpu.make_async_copy(a, b, sems.at[n]) for n, (a, b) in enumerate(moves)]
    for copy in copies:
        copy.start()
    for copy in copies[:2]:
        copy.wait()
    line, deriv = line[...], deriv[...]
    weight[...] = weights_in(line, deriv)
    shift_out[...] = jnp.broadcast_to(centre(line, deriv), (8, LANES))
    for copy in copies[2:4]:
        copy.wait()
    sub = lax.broadcasted_iota(jnp.int32, (8, LANES), 0)
    lanes8 = lane_ids(8)
    fields, images = [], []
    for x in range(0, 4, 2):
        pair = jnp.concatenate([strided(raw, x, NODES), strided(raw, x + 1, NODES)], axis=1)
        image = product(weight, pair)
        for k in range(2):
            fields.append(pair[:, k * LANES : (k + 1) * LANES])
            images.append(image[:, k * LANES : (k + 1) * LANES])
    for copy in copies[4:]:
        copy.wait()
    opened = 1.0 - flags[...].astype(jnp.float32)
    raw[772:788, :] = opened
    raw[788:796, 0:P_SIZE] = line
    raw[796:797, 0:P_SIZE] = deriv
    thick = raw[768:772, :]
    traces = [[image[64 + 8 * f : 72 + 8 * f] for f in range(4)] for image in images]
    ends = jnp.zeros((8, LANES), jnp.float32)
    for x in range(4):
        at = BLOCK * x
        allowed = [jnp.broadcast_to(opened[4 * f + x : 4 * f + x + 1, :], (8, LANES)) for f in range(4)]
        faces = list(traces[x])
        if x > 0:
            faces[0] = faces[0] - allowed[0] * traces[x - 1][1]
        if x < 3:
            faces[1] = faces[1] - allowed[1] * traces[x + 1][0]
        faces[2] = faces[2] - allowed[2] * jnp.where(lanes8 == 0, 0.0, turned(traces[x][3], 1))
        faces[3] = faces[3] - allowed[3] * jnp.where(lanes8 == LANES - 1, 0.0, turned(traces[x][2], -1))
        faces = [8.0 * face for face in faces]
        ends = jnp.where(lanes8 == 8 * x + 7, turned(traces[x][2], 8 * x + 7), ends)
        ends = jnp.where(lanes8 == 8 * x, turned(traces[x][3], 8 * x + 1), ends)
        width = jnp.broadcast_to(thick[x : x + 1, :], (8, LANES))
        for a in range(P_SIZE):
            rows = slice(8 * a, 8 * a + 8)
            value = strided(raw, 512 + 32 * a + x, 8) * fields[x][rows] + width * images[x][rows]
            value = value + edges(a, *faces, sub)
            near[at + 8 * a : at + 8 * a + 8, :] = strided(raw, 256 + 32 * a + x, 8) - value
        near[at + REACT : at + THICK, :] = strided(raw, 512 + x, NODES)
        rows = [thick[x : x + 1, :]] + [opened[4 * f + x : 4 * f + x + 1, :] for f in range(4)]
        near[at + THICK : at + BLOCK, :] = jnp.concatenate(rows + [jnp.zeros((3, LANES), jnp.float32)], axis=0)
    near[FIRST_WEST:LAST_EAST, :] = traces[0][0]
    near[LAST_EAST:ENDS, :] = traces[3][1]
    near[ENDS : ENDS + 8, :] = ends
    lanes = lane_ids(NODES)
    for out, first in ((to_up, 120), (to_down, 0)):
        totals = [jnp.zeros((n, LANES), jnp.float32) for n in (NODES, 32, 8)]
        for x in range(4):
            block = BLOCK * x
            parts = (
                (0, near[block : block + 64, :]),
                (0, near[block + REACT : block + THICK, :]),
                (1, jnp.concatenate(traces[x], axis=0)),
                (2, near[block + THICK : block + BLOCK, :]),
            )
            for field, (part, value) in enumerate(parts):
                at = 32 * field + 8 * x
                ids = lanes[0 : value.shape[0]]
                totals[part] = jnp.where((ids >= at) & (ids < at + 8), turned(value, at - first), totals[part])
        out[0:8, :] = totals[0][0:8] + totals[1][0:8] + totals[2]
        out[8:32, :] = totals[0][8:32] + totals[1][8:32]
        out[32:64, :] = totals[0][32:64]


def far_kernel(near, left, right, strip, high2, low2):
    lanes = lane_ids(NODES)
    strip[0:64, :] = jnp.where(lanes < 64, left[...], turned(right[...], 64))
    lanes = lanes[0:32]
    edge = jnp.where(lanes < 32, turned(left[0:32, :], -64), turned(right[0:32, :], -32))
    edge = jnp.where((lanes >= 64) & (lanes < 96), turned(left[0:32, :], -32), edge)
    edge = jnp.where(lanes >= 96, right[0:32, :], edge)
    strip[64:96, :] = edge
    facing = (edge[8:32], jnp.concatenate([edge[0:8], edge[16:32]], axis=0))
    for out, close, face, corner in ((high2, 3, LAST_EAST, facing[0]), (low2, 0, FIRST_WEST, facing[1])):
        block = BLOCK * close
        out[0:64, :] = near[block : block + 64, :]
        out[64:72, :] = near[block + THICK : block + BLOCK, :]
        out[72:80, :] = near[face : face + 8, :]
        out[80:88, :] = near[ENDS : ENDS + 8, :]
        out[88:112, :] = corner


def powers_kernel(
    shift_in, weight, near, below1, above1, below2, above2, own_strip, strip_b1, strip_a1,
    basis_out, gram_out, field_a, field_b, image, react, stiff, opened,
):
    shift = shift_in[0:1, :]

    def put(row, value_reaction, value_stiffness, value_open):
        cols = slice(row * LANES, (row + 1) * LANES)
        if value_reaction is not None:
            react[:, cols] = (value_reaction - shift) * SCALE
            stiff[:, cols] = jnp.broadcast_to(value_stiffness * SCALE, (8, LANES))
        for f in range(4):
            opened[8 * f : 8 * f + 8, cols] = jnp.broadcast_to(value_open[f], (8, LANES))

    local = {}
    for x in range(4):
        for ref, row in ((below1, 2 + x), (near, 6 + x), (above1, 10 + x)):
            at = BLOCK * x
            put(
                row, ref[at + REACT : at + THICK, :], ref[at + THICK : at + OPEN, :],
                [ref[at + OPEN + f : at + OPEN + f + 1, :] for f in range(4)],
            )
            local[row] = functools.partial(lambda ref, at, a: ref[at + 8 * a : at + 8 * a + 8, :], ref, at)
    for row, ref in ((1, below2), (ROWS - 2, above2)):
        put(row, None, None, [ref[65 + f : 66 + f, :] for f in range(4)])
        local[row] = functools.partial(lambda ref, a: ref[8 * a : 8 * a + 8, :], ref)

    lanes64 = lane_ids(NODES)
    lanes = lane_ids(8)
    pieces = ((strip_b1, 16, 48, 16), (own_strip, 48, 80, 48), (strip_a1, 80, 112, 80))
    strip_faces = []
    for side in range(2):
        made = []
        for top, count, zero in ((0, 64, 64 * side), (0, 64, 64 * side + 32), (64, 32, 32 * side), (64, 8, 64 + 32 * side)):
            ids = lanes64[0:count]
            value = jnp.zeros((count, LANES), jnp.float32)
            for ref, start, stop, target in pieces:
                part = turned(ref[top : top + count, :], target - zero)
                value = jnp.where((ids >= start) & (ids < stop), part, value)
            if count == 32:
                blank = jnp.zeros((8, LANES), jnp.float32)
                corner = jnp.concatenate([blank, below2[88:112, :]], axis=0)
                value = jnp.where(ids < 16, turned(corner, -16 - 32 * side), value)
                corner = jnp.concatenate([above2[88:96, :], blank, above2[96:112, :]], axis=0)
                value = jnp.where(ids >= 112, turned(corner, 112 - 32 * side), value)
            made.append(value)
        put(ROWS + side, made[1], made[3][0:1], [made[3][1 + f : 2 + f] for f in range(4)])
        local[ROWS + side] = functools.partial(lambda value, a: value[8 * a : 8 * a + 8], made[0])
        strip_faces.append([made[2][8 * f : 8 * f + 8] for f in range(4)])
    ends = jnp.zeros((8, LANES), jnp.float32)
    for ref, top, start, stop, by in (
        (below2, 80, 0, 16, -16), (below1, ENDS, 16, 48, 16), (near, ENDS, 48, 80, 48),
        (above1, ENDS, 80, 112, 80), (above2, 80, 112, 128, 112),
    ):
        ends = jnp.where((lanes >= start) & (lanes < stop), turned(ref[top : top + 8, :], by), ends)

    def columns(row):
        return slice(row * LANES, (row + 1) * LANES)

    low, high = ROWS, ROWS + 1
    sub = lax.broadcasted_iota(jnp.int32, (8, LANES), 0)
    TW, TE, TS, TN = (slice(64 + 8 * f, 72 + 8 * f) for f in range(4))

    def begin(new):
        def finish(row, faces):
            cols = columns(row)
            faces = [
                None if value is None else 8.0 * opened[8 * f : 8 * f + 8, cols] * value
                for f, value in enumerate(faces)
            ]
            for a in range(P_SIZE):
                new[8 * a : 8 * a + 8, cols] = local[row](a) + edges(a, *faces, sub)

        west = {
            2: below2[72:80, :], 6: below1[LAST_EAST:ENDS, :], 10: near[LAST_EAST:ENDS, :],
            14: above1[LAST_EAST:ENDS, :],
        }
        east = {
            1: below1[FIRST_WEST:LAST_EAST, :], 5: near[FIRST_WEST:LAST_EAST, :],
            9: above1[FIRST_WEST:LAST_EAST, :], 13: above2[72:80, :],
        }
        for row in range(1, ROWS - 1):
            south = jnp.where(lanes == 0, turned(strip_faces[0][3], -(8 * row + 7)), 0.0)
            north = jnp.where(lanes == LANES - 1, turned(strip_faces[1][2], 127 - 8 * row), 0.0)
            finish(row, (west.get(row), east.get(row), south, north))
        none = jnp.zeros((8, LANES), jnp.float32)
        spot = lanes // 8 % 4
        for side in range(2):
            from_west = jnp.where(spot == 2, turned(strip_faces[side][1], 8), 0.0)
            from_east = jnp.where(spot == 1, turned(strip_faces[side][0], -8), 0.0)
            outer = jnp.where(lanes % 8 == (0 if side else 7), ends, 0.0)
            finish(ROWS + side, (from_west, from_east, outer if side else none, none if side else outer))

    def apply(old, new, step):
        start, stop = step, ROWS - step
        for first_row, last_row in ((start, stop), (ROWS, ROWS + 2)):
            for row in range(first_row, last_row, 2):
                cols = slice(row * LANES, (row + 2) * LANES)
                image[:, cols] = product(weight, old[:, cols])

        def finish(row, *sides):
            cols = columns(row)
            faces = [
                image[own, cols] - opened[8 * f : 8 * f + 8, cols] * value
                for f, (own, value) in enumerate(zip((TW, TE, TS, TN), sides))
            ]
            for a in range(P_SIZE):
                rows = slice(8 * a, 8 * a + 8)
                value = react[rows, cols] * old[rows, cols] + stiff[:, cols] * image[rows, cols]
                new[rows, cols] = value + edges(a, *faces, sub)

        north_low = image[TN, columns(low)]
        south_high = image[TS, columns(high)]
        for row in range(start + 1, stop - 1):
            cols = columns(row)
            from_south = jnp.where(
                lanes == 0, turned(north_low, -(8 * row + 7)), turned(image[TN, cols], 1)
            )
            from_north = jnp.where(
                lanes == LANES - 1, turned(south_high, 127 - 8 * row), turned(image[TS, cols], -1)
            )
            finish(row, image[TE, columns(row - 1)], image[TW, columns(row + 1)], from_south, from_north)
        if step == DEPTH - 1:
            return
        to_low = turned(image[TS, columns(low)], -1)
        to_high = turned(image[TN, columns(high)], 1)
        for row in range(start, stop):
            cols = columns(row)
            to_low = jnp.where(lanes == 8 * row + 7, turned(image[TS, cols], 8 * row + 7), to_low)
            to_high = jnp.where(lanes == 8 * row, turned(image[TN, cols], 8 * row + 1), to_high)
        cols = columns(low)
        finish(low, turned(image[TE, cols], 8), turned(image[TW, cols], -8), turned(image[TN, cols], 1), to_low)
        cols = columns(high)
        finish(high, turned(image[TE, cols], 8), turned(image[TW, cols], -8), to_high, turned(image[TS, cols], -1))

    old, new = field_a, field_b
    for step in range(DEPTH):
        if step:
            apply(old, new, step)
        else:
            begin(new)
        basis_out[step, :, :] = new[:, 6 * LANES : 10 * LANES]
        old, new = new, old

    sums = [jnp.zeros((8, LANES), jnp.float32) for _ in GRAM]
    for x in range(4):
        for a in range(P_SIZE):
            values = [basis_out[k, 8 * a : 8 * a + 8, x * LANES : (x + 1) * LANES] for k in range(ITERS + 1)]
            sums = [total + values[k] * values[l] for total, (k, l) in zip(sums, GRAM)]
    rows = [jnp.sum(total, axis=0, keepdims=True) for total in sums]
    rows = jnp.concatenate(rows + [jnp.zeros((24 - len(GRAM), LANES), jnp.float32)], axis=0)
    totals = jnp.sum(rows, axis=1, keepdims=True)
    place = lax.broadcasted_iota(jnp.int32, (24, LANES), 0) == lax.broadcasted_iota(jnp.int32, (24, LANES), 1)
    totals = jnp.sum(jnp.where(place, totals, 0.0), axis=0, keepdims=True)
    gram_out[...] = jnp.broadcast_to(totals, gram_out.shape)


def combine_kernel(nodes, shift_in, powers, gathered, basis_out, hess_out, amp_out):
    shift = shift_in[...]
    row = jnp.sum(gathered[...], axis=0, keepdims=True) * (1.0 / nodes)
    spread = jnp.broadcast_to(row, (8, LANES))
    gram = {}
    for at, (k, l) in enumerate(GRAM):
        gram[k, l] = gram[l, k] = jnp.broadcast_to(spread[:, at : at + 1], (8, LANES))
    sizes = [jnp.sqrt(gram[k, k]) for k in range(ITERS + 1)]
    sub = lax.broadcasted_iota(jnp.int32, (8, LANES), 0)
    lanes = lane_ids(8)
    hess = jnp.zeros((8, LANES), jnp.float32)
    beta = jnp.sqrt(gram[0, 0] + FLOOR)
    coeffs = [[1.0 / beta]]
    amp = sizes[0] * coeffs[0][0]

    def put(hess, i, j, value):
        return jnp.where((sub == i) & (lanes == j), value, hess)

    for j in range(ITERS):
        last = coeffs[j]
        image = [shift * c for c in last] + [None]
        for k in range(j + 1):
            moved = last[k] * 8.0
            image[k + 1] = moved if image[k + 1] is None else image[k + 1] + moved
        weighted = [
            sum(gram[k, l] * image[l] for l in range(1, j + 2)) + gram[k, 0] * image[0] for k in range(j + 2)
        ]
        pending = list(image)
        for i in range(j + 1):
            h = sum(c * weighted[k] for k, c in enumerate(coeffs[i]))
            hess = put(hess, i, j, h)
            for k, c in enumerate(coeffs[i]):
                pending[k] = pending[k] - h * c
        square = sum(
            pending[k] * sum(gram[k, l] * pending[l] for l in range(j + 2)) for k in range(j + 2)
        )
        beta = jnp.sqrt(jnp.maximum(square, 0.0) + FLOOR)
        hess = put(hess, j + 1, j, beta)
        scale = 1.0 / beta
        coeffs.append([p * scale for p in pending])
        amp = jnp.maximum(amp, sum(jnp.abs(c) * s for c, s in zip(coeffs[-1], sizes)))
    hess_out[...] = hess[0 : ITERS + 1, 0:ITERS]
    amp_out[...] = amp[0:1, :]
    for x in range(4):
        for a in range(P_SIZE):
            values = [powers[k, 8 * a : 8 * a + 8, x * LANES : (x + 1) * LANES] for k in range(ITERS + 1)]
            for j in range(ITERS + 1):
                total = coeffs[j][0] * values[0]
                for k in range(1, j + 1):
                    total = total + coeffs[j][k] * values[k]
                basis_out[j, pl.ds(32 * a + x, 8, stride=4), :] = total


def fast(source, initial, reaction, stiffness, line_op, face_deriv, walls):
    vmem = pl.BlockSpec(memory_space=pltpu.VMEM)
    hbm = pl.BlockSpec(memory_space=pltpu.HBM)
    grant = pltpu.CompilerParams(vmem_limit_bytes=16 * 2**20)
    f32 = jnp.float32
    nx, ny = lax.axis_size(GX), lax.axis_size(GY)
    wide = (ROWS + 2) * LANES

    def moved(value, axis, size, by):
        return lax.ppermute(value, axis, [(i, (i + by) % size) for i in range(size)])

    held = (line_op, face_deriv.reshape(1, P_SIZE), source, initial, reaction, stiffness, walls)
    raw, near, to_up, to_down, weight, shift = pl.pallas_call(
        pack_kernel,
        out_shape=[jax.ShapeDtypeStruct((n, LANES), f32) for n in (800, ENDS + 8, NODES, NODES)]
        + [jax.ShapeDtypeStruct((NODES + 32, 6 * NODES), jnp.bfloat16), jax.ShapeDtypeStruct((8, LANES), f32)],
        in_specs=[hbm] * 7,
        out_specs=[vmem] * 6,
        scratch_shapes=[
            pltpu.VMEM((P_SIZE, P_SIZE), f32),
            pltpu.VMEM((1, P_SIZE), f32),
            pltpu.VMEM((16, LANES), jnp.int32),
            pltpu.SemaphoreType.DMA((10,)),
        ],
        compiler_params=grant,
    )(*[pltpu.with_memory_space_constraint(v, pltpu.HBM) for v in held])
    left = moved(to_up, GY, ny, 1)
    right = moved(to_down, GY, ny, -1)
    below1 = moved(near, GX, nx, 1)
    above1 = moved(near, GX, nx, -1)
    strip, high2, low2 = pl.pallas_call(
        far_kernel,
        out_shape=[jax.ShapeDtypeStruct((n, LANES), f32) for n in (96, 112, 112)],
        in_specs=[vmem] * 3,
        out_specs=[vmem] * 3,
        compiler_params=grant,
    )(near, left, right)
    below2 = moved(high2, GX, nx, 2)
    above2 = moved(low2, GX, nx, -2)
    strip_b1 = moved(strip, GX, nx, 1)
    strip_a1 = moved(strip, GX, nx, -1)

    powers, gram = pl.pallas_call(
        powers_kernel,
        out_shape=[
            jax.ShapeDtypeStruct((ITERS + 1, NODES, 4 * LANES), f32),
            jax.ShapeDtypeStruct((1, LANES), f32),
        ],
        in_specs=[vmem] * 10,
        out_specs=[vmem] * 2,
        scratch_shapes=[pltpu.VMEM((n, wide), f32) for n in (NODES, NODES, NODES + 32, NODES, 8, 32)],
        compiler_params=grant,
    )(shift, weight, near, below1, above1, below2, above2, strip, strip_b1, strip_a1)
    every = GX + GY
    copies = jnp.broadcast_to(gram, (nx * ny, LANES))
    gathered = lax.all_to_all(copies, every, split_axis=0, concat_axis=0, tiled=True)
    basis, hess, amp = pl.pallas_call(
        functools.partial(combine_kernel, float(NODES * 4 * nx * LANES * ny)),
        out_shape=[
            jax.ShapeDtypeStruct((ITERS + 1, 4 * NODES, LANES), f32),
            jax.ShapeDtypeStruct((ITERS + 1, ITERS), f32),
            jax.ShapeDtypeStruct((1, LANES), f32),
        ],
        in_specs=[vmem] * 3,
        out_specs=[vmem] * 3,
        compiler_params=grant,
    )(shift, powers, gathered)
    return hess, basis, amp[0, 0], raw


def body(source, initial, reaction, stiffness, line_op, face_deriv, wall_flags):
    flat = [v.reshape(4 * NODES, LANES) for v in (source, initial, reaction)]
    hess, basis, amp, raw = fast(*flat, stiffness, line_op, face_deriv, wall_flags.reshape(16, LANES))

    def again(carry):
        raw = lax.optimization_barrier(carry[3])
        initial, source, reaction = raw[0:768].reshape(3, NODES, 4, LANES)
        opened = raw[772:788].reshape(4, 4, LANES)
        line_op, face_deriv = raw[788:796, 0:P_SIZE], raw[796, 0:P_SIZE]
        hess, basis = stepwise(source, initial, reaction, raw[768:772], line_op, face_deriv, opened)
        return jnp.bool_(True), hess, basis.reshape(ITERS + 1, 4 * NODES, LANES), raw

    done = amp <= AMP_LIMIT
    carry = lax.while_loop(lambda carry: jnp.logical_not(carry[0]), again, (done, hess, basis, raw))
    return (carry[1], carry[2].reshape(ITERS + 1, NODES, 4, LANES))


def solution(mesh):
    finer = Mesh(mesh.devices.reshape(4, 2, 4, 8), ("gx_0", "gx_1", "gy_0", "gy_1"))
    placed = (
        P(None, GX, GY),
        P(None, GX, GY),
        P(None, GX, GY),
        P(GX, GY),
        P(),
        P(),
        P(None, GX, GY),
    )
    return jax.shard_map(
        body, mesh=finer, in_specs=placed, out_specs=(P(), P(None, None, GX, GY)), check_vma=False
    )
```
